32 devices in a mesh: scene: 2 (over y), pulse: 8 (over z, x), scat: 2 (over core).
Axes of the slice: x: 2, y: 2, z: 4, core: 2. Of those that a mesh axis runs over, the one named last changes fastest.
Arguments:
- positions: float32 [32768], P(('scene', 'scat')), parts along dimension 0, may hold values from -1000 to 1000
- amplitude: float32 [2, 32768], P(None, ('scene', 'scat')), parts along dimension 1, may hold values from -3 to 3
- range_cells: int32 [32768], P(('scene', 'scat')), parts along dimension 0, may hold values from 0 to 1007
- bounce: int32 [32768], P(('scene', 'scat')), parts along dimension 0, may hold values 0 or 1
- stolt_block: int32 [512, 32], P(('pulse', 'scat')), may hold values from 0 to 30
- kernel_choice: int32 [512, 32], P(('pulse', 'scat')), may hold values from 0 to 15
- kernel_bank: float32 [16, 256, 128], replicated, may hold values from -0.375 to 0.375
Outputs:
- image: float32 [2, 1024, 4096], P(None, 'scene', ('pulse', 'scat')), parts along dimension 1
The draws below stay inside these ranges and needn't reach their ends.
There are 2 independent parts, one for each index of `scene`. The reference program is written for one: setup_inputs(seed, part) draws one part's arguments, and reference() takes and returns one part's arrays. A program takes and returns all parts, laid end to end along the dimension named above; an argument that names none is the same for every part. Nothing has to cross between parts.
All inputs are finite; a program needn't handle non-finite values. No bound on the sum of `bounce` on one device may be relied on, other than what follows from the above.
Results may differ from the reference program's by a relative error of at most 0.0003.
Values sent between devices are 32-bit elements; how exact they have to be, the bound alone decides.
A program may use at most 64 MiB of HBM per device.

```python
import jax
import jax.numpy as jnp
from jax import lax

P_SIZE = 512
SPECTRAL_BIN_LEN = 4096
B = 1024
SHIFT = 16
STOLT = 128
KERNELS = 16
S = 16384
BLOCKS = 32


def draw_positions(key, part):
    spread = jax.random.uniform(jax.random.fold_in(key, 11), (S,), jnp.float32, -1000.0, 1000.0)
    return spread.astype(jnp.float32)


def touch_ends(values, own_key, low, top_value):
    longest = values.shape.index(max(values.shape))
    spots = []
    for shift in (0, 1):
        where = [jax.random.randint(jax.random.fold_in(own_key, axis), (), 0, length) for axis, length in enumerate(values.shape)]
        where[longest] = (where[longest] + shift) % values.shape[longest]
        spots.append(tuple(where))
    return values.at[spots[0]].set(low).at[spots[1]].set(top_value)


def level_of(key, extent, shards, low, high):
    def one(dim, shards_of):
        draws = jax.random.uniform(jax.random.fold_in(jax.random.fold_in(key, 6), dim), (shards_of,), jnp.float32, low / len(shards), high / len(shards))
        return jnp.repeat(jnp.exp(draws), extent[dim] // shards_of).reshape((-1,) + (1,) * (len(extent) - dim - 1))

    level = one(*shards[0])
    for cut in shards[1:]:
        level = level * one(*cut)
    return level


def bell_draw(key, dims, deviation, bound, split=(), kind=jnp.bfloat16):
    values = deviation * jax.random.normal(key, dims, jnp.float32)
    if split:
        values = values * level_of(key, dims, split, -0.22, 0.18)
    return jnp.clip(values, -bound, bound).astype(kind)


def setup_inputs(seed: int = 0, part: int = 0) -> dict:
    keys = jax.random.split(jax.random.key(seed), 8)
    own_keys = jax.random.split(jax.random.fold_in(keys[7], part), 8)
    return {
        "positions": draw_positions(jax.random.fold_in(jax.random.fold_in(keys[7], part), 71), part),
        "amplitude": bell_draw(own_keys[1], (2, S), 0.5, 3.0, ((1, 2),), jnp.float32),
        "range_cells": touch_ends(jax.random.randint(own_keys[2], (S,), 0, B - SHIFT), jax.random.fold_in(own_keys[2], 1), 0, (B - SHIFT) - 1).astype(jnp.int32),
        "bounce": touch_ends((jax.random.randint(own_keys[3], (S,), 0, 4) < 1).astype(jnp.int32), jax.random.fold_in(own_keys[3], 1), 0, 1),
        "stolt_block": touch_ends(jax.random.randint(keys[4], (P_SIZE, BLOCKS), 0, BLOCKS - 1), jax.random.fold_in(keys[4], 1), 0, (BLOCKS - 1) - 1).astype(jnp.int32),
        "kernel_choice": touch_ends(jax.random.randint(keys[5], (P_SIZE, BLOCKS), 0, KERNELS), jax.random.fold_in(keys[5], 1), 0, KERNELS - 1).astype(jnp.int32),
        "kernel_bank": bell_draw(keys[6], (KERNELS, 2 * STOLT, STOLT), (2 * STOLT) ** -0.5, 0.375, (), jnp.float32),
    }


wavelength = 0.03125
spacing = 2.0
near_range = 700000.0
cell_size = 1.0
center_radio_tone = 9600000000.0
pulse_slope_rate = 150000000.0
wave_propagation_velocity = 300000000.0
highest_frequency = lax.Precision.HIGHEST

def steering(positions, amplitude, target, bounce, pulse_ids):
    along_track = (pulse_ids.astype(jnp.float32) - P_SIZE // 2) * spacing
    slant_range = near_range + cell_size * target.astype(jnp.float32)
    offset = along_track[:, None] - positions[None, :]
    excess = offset * offset / (jnp.sqrt(slant_range * slant_range + offset * offset) + slant_range)
    phase_angle = -4.0 * jnp.pi / wavelength * excess
    bounce_sign = 1.0 - 2.0 * bounce.astype(jnp.float32)
    real_part = bounce_sign * amplitude[0]
    imag_part = bounce_sign * amplitude[1]
    cos_part = jnp.cos(phase_angle)
    sin_part = jnp.sin(phase_angle)
    return (real_part * cos_part - imag_part * sin_part, real_part * sin_part + imag_part * cos_part)

def binning(steer_re, guiding_phasor_quadrature, target):
    stacked = jnp.concatenate([steer_re, guiding_phasor_quadrature], axis=0).T
    return jax.ops.segment_sum(stacked, target, num_segments=B)

def reference_phase(row_ids, matrix_slot_numbers):
    centered = (row_ids + P_SIZE // 2) % P_SIZE - P_SIZE // 2
    along_k = 2.0 * jnp.pi / (P_SIZE * spacing) * centered.astype(jnp.float32)
    slant_spatial_radian_rate = 4.0 * jnp.pi / wave_propagation_velocity * (center_radio_tone + (matrix_slot_numbers.astype(jnp.float32) - SPECTRAL_BIN_LEN // 2) * (pulse_slope_rate / SPECTRAL_BIN_LEN))
    squared = along_k * along_k
    depth = near_range + cell_size * (B // 2)
    return -depth * squared[:, None] / (jnp.sqrt(slant_spatial_radian_rate[None, :] * slant_spatial_radian_rate[None, :] - squared[:, None]) + slant_spatial_radian_rate[None, :])

def reference(positions, amplitude, range_cells, bounce, stolt_block, kernel_choice, kernel_bank):
    target = range_cells + SHIFT * bounce
    group_size = 64
    groups = jnp.arange(P_SIZE, dtype=jnp.int32).reshape(P_SIZE // group_size, group_size)

    def one_group(pulse_ids):
        steer_re, guiding_phasor_quadrature = steering(positions, amplitude, target, bounce, pulse_ids)
        return binning(steer_re, guiding_phasor_quadrature, target)
    binned = lax.map(one_group, groups)
    binned_re = binned[:, :, :group_size].transpose(0, 2, 1).reshape(P_SIZE, B)
    binned_im = binned[:, :, group_size:].transpose(0, 2, 1).reshape(P_SIZE, B)
    signal = jnp.pad(binned_re + 1j * binned_im, ((0, 0), (0, SPECTRAL_BIN_LEN - B)))
    echo = jnp.fft.fft(signal, axis=1)
    spectrum = jnp.fft.fft(echo, axis=0)
    phase_angle = reference_phase(jnp.arange(P_SIZE, dtype=jnp.int32), jnp.arange(SPECTRAL_BIN_LEN, dtype=jnp.int32))
    focused = spectrum * (jnp.cos(phase_angle) + 1j * jnp.sin(phase_angle))

    def window_pairs(row_data):
        tiled = row_data.reshape(BLOCKS, STOLT)
        return jnp.concatenate([tiled[:-1], tiled[1:]], axis=1)

    def stolt_row(row_item):
        row_re, row_im, first_blocks, kinds = row_item
        windows = jnp.stack([window_pairs(row_re), window_pairs(row_im)])
        chosen = windows[:, first_blocks, :]
        kernels = kernel_bank[kinds]
        result = jnp.einsum('cbu,but->cbt', chosen, kernels, precision=highest_frequency)
        return result.reshape(2, SPECTRAL_BIN_LEN)
    stolted = lax.map(stolt_row, (jnp.real(focused), jnp.imag(focused), stolt_block, kernel_choice))
    complex_rows = stolted[:, 0] + 1j * stolted[:, 1]
    ranged = jnp.fft.ifft(complex_rows, axis=1)
    image = jnp.fft.ifft(ranged, axis=0)
    return jnp.stack([jnp.real(image), jnp.imag(image)]).astype(jnp.float32)
```

```python
import functools

import jax
import jax.numpy as jnp
import numpy as np
from jax import lax
from jax.experimental import pallas as pl
from jax.experimental.pallas import tpu as pltpu
from jax.sharding import PartitionSpec as P

P_SIZE = 512
F_LEN = 4096
B = 1024
SHIFT = 16
STOLT = 128
BLOCKS = 32
SPACING = 2.0
NEAR = 700000.0
BIN_SIDE = 32
GROUP = 4
CHUNK = 1024
SLOTS = 192
WIDE = 256
HIGH = lax.Precision.HIGH
f32 = jnp.float32
bf16 = jnp.bfloat16


def trig_coefs():
    x = np.cos(np.pi * (np.arange(400) + 0.5) / 400) * 0.5
    u = x * x
    s = np.polynomial.chebyshev.Chebyshev.fit(u, np.sin(np.pi * x) / x, 5).convert(
        kind=np.polynomial.Polynomial
    )
    c = np.polynomial.chebyshev.Chebyshev.fit(u, np.cos(np.pi * x), 5).convert(
        kind=np.polynomial.Polynomial
    )
    return [float(v) for v in s.coef], [float(v) for v in c.coef]


def horner(u, coefs):
    acc = jnp.full_like(u, coefs[-1])
    for c in coefs[-2::-1]:
        acc = acc * u + c
    return acc


def split(x):
    hi = x.astype(bf16)
    lo = (x - hi.astype(f32)).astype(bf16)
    return hi, lo


def np_split(x):
    x = np.asarray(x, np.float64)
    hi = np.asarray(x, jnp.bfloat16)
    lo = np.asarray(x - hi.astype(np.float64), jnp.bfloat16)
    return np.stack([hi, lo])


def dots(a, b, dims):
    d = functools.partial(
        lax.dot_general, dimension_numbers=(dims, ((), ())), preferred_element_type=f32
    )
    return d(a[0], b[0]) + (d(a[0], b[1]) + d(a[1], b[0]))


def bin_kernel(pulse_base, pos, amp, tgt, bnc, out, acc, *, pulses, sin_c, cos_c):
    step = pl.program_id(0)
    width = pos.shape[1]

    @pl.when(step == 0)
    def _():
        acc[...] = jnp.zeros_like(acc)

    base = pulse_base[0]
    ids = base + lax.broadcasted_iota(jnp.int32, (pulses, width), 0)
    along = (ids.astype(f32) - P_SIZE // 2) * SPACING
    target = tgt[...] + SHIFT * bnc[...]
    slant = NEAR + target.astype(f32)
    offset = along - pos[...]
    square = offset * offset
    excess = square / (jnp.sqrt(slant * slant + square) + slant)
    halves = excess * -128.0
    whole = jnp.round(halves)
    r = halves - whole
    u = r * r
    odd = whole - 2.0 * jnp.floor(whole * 0.5)
    sign = 1.0 - 2.0 * odd
    sin_p = sign * r * horner(u, sin_c)
    cos_p = sign * horner(u, cos_c)
    flip = 1.0 - 2.0 * bnc[...].astype(f32)
    are = flip * amp[0:1]
    aim = flip * amp[1:2]
    re = are * cos_p - aim * sin_p
    im = are * sin_p + aim * cos_p
    steer = jnp.concatenate([re, im], 0)
    hi, lo = split(steer)
    rhs = jnp.concatenate([hi, lo], 0)
    bins = lax.broadcasted_iota(jnp.int32, (B, width), 0)
    hot = jnp.where(bins == target, 1.0, 0.0).astype(bf16)
    acc[...] += lax.dot_general(
        hot, rhs, (((1,), (1,)), ((), ())), preferred_element_type=f32
    )

    @pl.when(step == pl.num_programs(0) - 1)
    def _():
        out[...] = acc[:, : 2 * pulses] + acc[:, 2 * pulses :]


def binning(positions, amplitude, cells, bounce, pulse_base, pulses):
    count = positions.shape[0]
    width = min(2048, count)
    sin_c, cos_c = trig_coefs()
    row = lambda n: pl.BlockSpec((n, width), lambda i: (0, i))
    return pl.pallas_call(
        functools.partial(bin_kernel, pulses=pulses, sin_c=sin_c, cos_c=cos_c),
        grid=(count // width,),
        in_specs=[pl.BlockSpec(memory_space=pltpu.SMEM), row(1), row(2), row(1), row(1)],
        out_specs=pl.BlockSpec((B, 2 * pulses), lambda i: (0, 0)),
        out_shape=jax.ShapeDtypeStruct((B, 2 * pulses), f32),
        scratch_shapes=[pltpu.VMEM((B, 4 * pulses), f32)],
        name="binning",
    )(
        pulse_base.reshape(1),
        positions.reshape(1, count),
        amplitude,
        cells.reshape(1, count),
        bounce.reshape(1, count),
    )


def range_trig_coefs(degree):
    x = np.cos(np.pi * (np.arange(400) + 0.5) / 400) * 0.5
    u = x * x
    fit = lambda y: np.polynomial.chebyshev.Chebyshev.fit(u, y, degree).convert(
        kind=np.polynomial.Polynomial
    )
    return [float(v) for v in fit(np.sin(np.pi * x) / x).coef], [
        float(v) for v in fit(np.cos(np.pi * x)).coef
    ]


def split3(x):
    hi = x.astype(bf16).astype(f32)
    rest = x - hi
    mid = rest.astype(bf16).astype(f32)
    return hi, mid, rest - mid


def range_bin_kernel(
    base_ref, cells8, bounce8, pos, amp, cells, bnc, out, buf, acc, *, span, sin_c, cos_c
):
    base = base_ref[0]
    rows = cells8.shape[0]
    chunks = rows // 8
    target = cells8[...] + SHIFT * bounce8[...] - base
    match = jnp.where((target >= 0) & (target < span), 1.0, 0.0)
    mb = match.astype(bf16)
    a = lax.broadcasted_iota(jnp.int32, (128, 128), 0)
    b = lax.broadcasted_iota(jnp.int32, (128, 128), 1)
    upto = jnp.where(a <= b, 1.0, 0.0).astype(bf16)
    count = jnp.dot(mb, upto, preferred_element_type=f32)
    total = jnp.dot(mb, jnp.ones((128, 128), bf16), preferred_element_type=f32)
    a = lax.broadcasted_iota(jnp.int32, (rows, rows), 0)
    b = lax.broadcasted_iota(jnp.int32, (rows, rows), 1)
    below = jnp.where((a // 8 == b // 8) & (b < a), 1.0, 0.0).astype(bf16)
    ahead = jnp.dot(below, total.astype(bf16), preferred_element_type=f32)
    rank = jnp.where(match > 0.0, count + ahead - 1.0, -1.0)
    counts = [
        jnp.sum(match[8 * c : 8 * c + 8]).astype(jnp.int32) for c in range(chunks)
    ]

    def values(c):
        lanes = slice(CHUNK * c, CHUNK * (c + 1))
        flip = 1.0 - 2.0 * bnc[:, lanes].astype(f32)
        rel = (cells[:, lanes] + SHIFT * bnc[:, lanes] - base).astype(f32)
        zero = jnp.zeros_like(rel)
        data = jnp.concatenate(
            [pos[:, lanes], amp[0:1, lanes] * flip, amp[1:2, lanes] * flip, rel] + [zero] * 4, 0
        )
        return jnp.concatenate(list(split3(data)) + [jnp.zeros_like(data)], 0).astype(bf16)

    def pick(c, first):
        slots = lax.broadcasted_iota(jnp.int32, (SLOTS, 128), 0).astype(f32) + first
        hot = jnp.concatenate(
            [jnp.where(rank[8 * c + j : 8 * c + j + 1] == slots, 1.0, 0.0) for j in range(8)], 1
        ).astype(bf16)
        return lax.dot_general(
            hot, values(c), (((1,), (1,)), ((), ())), preferred_element_type=f32
        )

    start = 0
    for c in range(chunks):
        buf[pl.ds(start, SLOTS), 0:32] = pick(c, 0.0)
        start = start + counts[c]
    most = functools.reduce(jnp.maximum, counts)

    @pl.when(most > SLOTS)
    def _():
        begin = 0
        for c in range(chunks):

            @pl.loop(0, (counts[c] + SLOTS - 1) // SLOTS)
            def _(i):
                first = (i * SLOTS).astype(f32)
                buf[pl.ds(begin + i * SLOTS, SLOTS), 0:32] = pick(c, first)

            begin = begin + counts[c]

    buf[pl.ds(start, WIDE), :] = jnp.zeros((WIDE, 128), f32)
    acc[...] = jnp.zeros_like(acc)
    bins = lax.broadcasted_iota(jnp.int32, (span, WIDE), 0).astype(f32)
    nearest = base.astype(f32) + NEAR

    @pl.loop(0, (start + WIDE - 1) // WIDE)
    def _(i):
        cols = []
        for h in range(WIDE // 128):
            t = buf[pl.ds(i * WIDE + h * 128, 128), :].T
            cols.append(t[0:8] + t[8:16] + t[16:24])
        data = jnp.concatenate(cols, 1)
        where, re_amp, im_amp, rel = (data[j : j + 1] for j in range(4))
        re2, im2 = 2.0 * re_amp, 2.0 * im_amp
        inverse = 0.5 / (rel + nearest)
        gain = inverse * -64.0
        bend = inverse * (1.0 / 64.0)
        hot = jnp.where(bins == rel, 1.0, 0.0).astype(bf16)
        for q in range(P_SIZE // 128):
            parts = []
            for p in range(0, 128, 16):
                ids = lax.broadcasted_iota(jnp.int32, (16, WIDE), 0)
                along = (ids + (q * 128 + p - P_SIZE // 2)).astype(f32) * SPACING
                offset = along - where
                t = offset * offset * gain
                y = t * bend
                t = t * (1.0 + y * (1.0 + 2.0 * y))
                r = t - jnp.round(t)
                u = r * r
                sn = r * horner(u, sin_c)
                cs = horner(u, cos_c)
                re = re_amp - sn * (re2 * sn + im2 * cs)
                im = im_amp + sn * (re2 * cs - im2 * sn)
                parts.append(split(re) + split(im))
            for c in range(2):
                lanes = slice(c * P_SIZE + q * 128, c * P_SIZE + (q + 1) * 128)
                hi = jnp.concatenate([v[2 * c] for v in parts], 0)
                lo = jnp.concatenate([v[2 * c + 1] for v in parts], 0)
                d = functools.partial(
                    lax.dot_general,
                    dimension_numbers=(((1,), (1,)), ((), ())),
                    preferred_element_type=f32,
                )
                acc[:, lanes] += d(hot, hi) + d(hot, lo)

    out[...] = acc[...]


def range_binning(positions, amplitude, cells, bounce, base, span):
    count = positions.shape[0]
    sin_c, cos_c = range_trig_coefs(4)
    whole = pl.BlockSpec(memory_space=pltpu.VMEM)
    return pl.pallas_call(
        functools.partial(range_bin_kernel, span=span, sin_c=sin_c, cos_c=cos_c),
        in_specs=[pl.BlockSpec(memory_space=pltpu.SMEM)] + [whole] * 6,
        out_specs=whole,
        out_shape=jax.ShapeDtypeStruct((span, 2 * P_SIZE), f32),
        scratch_shapes=[
            pltpu.VMEM((count + SLOTS + WIDE, 128), f32),
            pltpu.VMEM((span, 2 * P_SIZE), f32),
        ],
        name="range_binning",
    )(
        base.reshape(1),
        cells.reshape(count // 128, 128),
        bounce.reshape(count // 128, 128),
        positions.reshape(1, count),
        amplitude,
        cells.reshape(1, count),
        bounce.reshape(1, count),
    )


def complex_rows(c, s):
    return np.block([[c, s], [-s, c]])


def mid_tables(n_dev, order):
    side = np.arange(BIN_SIDE)
    t = np.arange(STOLT)
    eye = np.eye(GROUP)
    a = -2 * np.pi / STOLT * ((side[:, None] * t[None, :]) % STOLT)
    ta = complex_rows(np.cos(a), np.sin(a))[order]
    a = -2 * np.pi / F_LEN * (side[:, None] * t[None, :])
    wa = np.stack([np.tile(np.cos(a), (GROUP, 1)), np.tile(np.sin(a), (GROUP, 1))])
    a = -2 * np.pi / BIN_SIDE * ((side[:, None] * side[None, :]) % BIN_SIDE)
    c, s = np.kron(eye, np.cos(a)), np.kron(eye, np.sin(a))
    tb = complex_rows(c, s).T
    blk = np.arange(BLOCKS)
    a = 2 * np.pi / BLOCKS * ((blk[:, None] * blk[None, :]) % BLOCKS)
    c, s = np.kron(eye, np.cos(a)), np.kron(eye, np.sin(a))
    tc = complex_rows(c, s)
    a = 2 * np.pi / F_LEN * (t[:, None] * blk[None, :])
    wc = np.stack([np.tile(np.cos(a), (1, GROUP)), np.tile(np.sin(a), (1, GROUP))])
    a = 2 * np.pi / STOLT * ((t[:, None] * t[None, :]) % STOLT)
    td = complex_rows(np.cos(a), np.sin(a)).T / F_LEN
    td = td.reshape(2, n_dev, STOLT // n_dev, 2 * STOLT).transpose(1, 0, 2, 3)
    td = td.reshape(2 * STOLT, 2 * STOLT)
    return (
        np_split(ta),
        wa.astype(np.float32),
        np_split(tb),
        np_split(tc),
        wc.astype(np.float32),
        np_split(td),
    )


def mid_kernel(
    x, cos_p, sin_p, hot, kind, bank_hi, bank_lo, ta, wa, tb, tc, wc, td, out, xs, os, *, subs
):
    n = GROUP * BLOCKS
    step = pl.program_id(0)
    groups = x.shape[1]

    @pl.when(step == 0)
    def _():
        for g in range(groups):
            xs[g] = x[:, g, :]

    parts_hi, parts_lo = [], []
    for g in range(subs):
        lanes = slice(g * n, (g + 1) * n)
        y = dots(split(xs[step * subs + g]), (ta[0], ta[1]), ((0,), (0,)))
        yr, yi = y[:, :STOLT], y[:, STOLT:]
        y = jnp.concatenate([yr * wa[0] - yi * wa[1], yr * wa[1] + yi * wa[0]], 0)
        z = dots((tb[0], tb[1]), split(y), ((1,), (0,)))
        zr, zi = z[:n], z[n:]
        cp, sp = cos_p[lanes], sin_p[lanes]
        z = jnp.concatenate([zr * cp - zi * sp, zr * sp + zi * cp], 1)
        hi, lo = split(z)
        picked = jnp.dot(
            hot[g], jnp.concatenate([hi, lo], 1), preferred_element_type=f32
        ).astype(bf16)
        first, second = picked[:n], picked[n:]
        for c in range(2):
            for base, keep in ((0, parts_hi), (2 * STOLT, parts_lo)):
                cut = slice(base + c * STOLT, base + (c + 1) * STOLT)
                keep.append(jnp.concatenate([first[:, cut], second[:, cut]], 1))
    ghi = jnp.concatenate(parts_hi, 0)
    glo = jnp.concatenate(parts_lo, 0)
    kinds = kind[...].reshape(subs * 2 * n, 1)
    kinds = jnp.broadcast_to(kinds, (subs * 2 * n, STOLT))
    acc = jnp.zeros((subs * 2 * n, STOLT), f32)
    for k in range(0, bank_hi.shape[0], 2):
        khi = jnp.concatenate([bank_hi[k], bank_hi[k + 1]], 1)
        klo = jnp.concatenate([bank_lo[k], bank_lo[k + 1]], 1)
        r = dots((ghi, glo), (khi, klo), ((1,), (0,)))
        for half in range(2):
            acc = jnp.where(kinds == k + half, r[:, half * STOLT : (half + 1) * STOLT], acc)
    for g in range(subs):
        s = acc[g * 2 * n : (g + 1) * 2 * n]
        y = dots(split(s), (tc[0], tc[1]), ((0,), (0,)))
        yr, yi = y[:, :n], y[:, n:]
        y = jnp.concatenate([yr * wc[0] - yi * wc[1], yr * wc[1] + yi * wc[0]], 0)
        os[step * subs + g] = dots((td[0], td[1]), split(y), ((1,), (0,)))

    @pl.when(step == pl.num_programs(0) - 1)
    def _():
        for g in range(groups):
            out[:, g, :] = os[g]


def middle(x, cos_p, sin_p, hot, kind, bank_hi, bank_lo, tables):
    groups = x.shape[1]
    subs = min(4, groups)
    n = GROUP * BLOCKS
    whole = lambda a: pl.BlockSpec(a.shape, lambda i: (0,) * a.ndim)
    return pl.pallas_call(
        functools.partial(mid_kernel, subs=subs),
        grid=(groups // subs,),
        in_specs=[
            whole(x),
            pl.BlockSpec((subs * n, STOLT), lambda i: (i, 0)),
            pl.BlockSpec((subs * n, STOLT), lambda i: (i, 0)),
            pl.BlockSpec((subs, 2 * n, n), lambda i: (i, 0, 0)),
            pl.BlockSpec((subs, 2 * n, 1), lambda i: (i, 0, 0)),
            whole(bank_hi),
            whole(bank_lo),
        ]
        + [whole(t) for t in tables],
        out_specs=pl.BlockSpec((2 * STOLT, groups, n), lambda i: (0, 0, 0)),
        out_shape=jax.ShapeDtypeStruct((2 * STOLT, groups, n), f32),
        scratch_shapes=[
            pltpu.VMEM((groups, x.shape[0], n), f32),
            pltpu.VMEM((groups, 2 * STOLT, n), f32),
        ],
        name="middle",
    )(x, cos_p, sin_p, hot, kind, bank_hi, bank_lo, *tables)


def quarter_tables():
    q = P_SIZE // 4
    m = np.arange(q)
    fwd, inv = [], []
    for low in range(4):
        a = 2 * np.pi / P_SIZE * (((4 * m[:, None] + low) * m[None, :]) % P_SIZE)
        fwd.append(np.concatenate([np.cos(a), np.sin(a)], 0))
        inv.append(np.concatenate([np.cos(a.T), np.sin(a.T)], 0) / P_SIZE)
    return np_split(np.stack(fwd)), np_split(np.stack(inv))


def swap_blocks(arrays):
    count = len(arrays)
    lanes = arrays[0].shape[-1]
    size = lanes // count
    block = lax.broadcasted_iota(jnp.int32, arrays[0].shape, 1) // size
    outs = []
    for b in range(count):
        acc = None
        for a in range(count):
            shift = (a - b) % count * size
            moved = pltpu.roll(arrays[a], shift, 1) if shift else arrays[a]
            acc = moved if acc is None else jnp.where(block == a, moved, acc)
        outs.append(acc)
    return outs


def azimuth_kernel(x, table, out):
    half = x.shape[0]
    lanes = 2 * half
    size = P_SIZE // 4
    quarters = []
    for q in range(4):
        re = x[:, q * size : (q + 1) * size]
        im = x[:, P_SIZE + q * size : P_SIZE + (q + 1) * size]
        quarters.append((re, im))
    (r0, i0), (r1, i1), (r2, i2), (r3, i3) = quarters
    sr, si, dr, di = r0 + r2, i0 + i2, r0 - r2, i0 - i2
    tr, ti, er, ei = r1 + r3, i1 + i3, r1 - r3, i1 - i3
    mixed = (
        (sr + tr, si + ti),
        (dr + ei, di - er),
        (sr - tr, si - ti),
        (dr - ei, di + er),
    )
    low = lax.broadcasted_iota(jnp.int32, (size, lanes), 1) < half
    rows = []
    for k in range(4):
        u = jnp.concatenate(mixed[k], 0)
        g = dots((table[0, k], table[1, k]), split(u), ((1,), (1,)))
        turned = pltpu.roll(g[size:], half, 1)
        rows.append(g[:size] + jnp.where(low, turned, -turned))
    for q, z in enumerate(swap_blocks(rows)):
        out[:, q] = z.reshape(out.shape[0], out.shape[2], lanes)


def image_kernel(x, table, out):
    devs, _, per, kh, lanes = x.shape
    size = P_SIZE // 4
    columns = [[] for _ in range(4)]
    for c in range(2):
        for h in range(per // 4):
            tiles = [x[:, c, 4 * h + j].reshape(devs * kh, lanes) for j in range(4)]
            for k, z in enumerate(swap_blocks(tiles)):
                columns[k].append(z)
    width = lanes * (per // 4)
    v = []
    for k in range(4):
        g = dots((table[0, k], table[1, k]), split(jnp.concatenate(columns[k], 1)), ((1,), (0,)))
        cos_g, sin_g = g[:size], g[size:]
        v.append((cos_g[:, :width] - sin_g[:, width:], cos_g[:, width:] + sin_g[:, :width]))
    (r0, i0), (r1, i1), (r2, i2), (r3, i3) = v
    sr, si, dr, di = r0 + r2, i0 + i2, r0 - r2, i0 - i2
    tr, ti, er, ei = r1 + r3, i1 + i3, r1 - r3, i1 - i3
    mixed = (
        (sr + tr, si + ti),
        (dr - ei, di + er),
        (sr - tr, si - ti),
        (dr + ei, di - er),
    )
    for q in range(4):
        for c in range(2):
            out[c, q * size : (q + 1) * size, :] = mixed[q][c]


def reference_phase(row_ids, cols):
    centered = (row_ids + P_SIZE // 2) % P_SIZE - P_SIZE // 2
    along_k = 2.0 * jnp.pi / (P_SIZE * SPACING) * centered.astype(f32)
    kr = 4.0 * jnp.pi / 3e8 * (9.6e9 + (cols.astype(f32) - F_LEN // 2) * (1.5e8 / F_LEN))
    squared = along_k * along_k
    depth = NEAR + B // 2
    return (
        -depth
        * squared[:, None]
        / (jnp.sqrt(kr[None, :] * kr[None, :] - squared[:, None]) + kr[None, :])
    )


def on_device(positions, amplitude, range_cells, bounce, stolt_block, kernel_choice, kernel_bank):
    n_pulse = lax.axis_size("pulse")
    n_scat = lax.axis_size("scat")
    n_dev = n_pulse * n_scat
    pulse_here = lax.axis_index("pulse")
    scat_here = lax.axis_index("scat")
    pulses = P_SIZE // n_pulse
    rows = P_SIZE // n_dev
    width = F_LEN // n_dev
    groups = rows // GROUP
    n = GROUP * BLOCKS
    bins_scat = B // n_scat
    bins_here = bins_scat // n_pulse

    ids = jnp.arange(GROUP, dtype=jnp.int32)[None, :, None] * BLOCKS
    first = stolt_block.reshape(groups, GROUP, BLOCKS) + ids
    pick = jnp.stack([first, first + 1], 1).reshape(groups, 2 * n, 1)
    hot = (pick == jnp.arange(n, dtype=jnp.int32)[None, None, :]).astype(bf16)
    kind = jnp.stack([kernel_choice.reshape(groups, n)] * 2, 1).reshape(groups, 2 * n, 1)
    bank_hi = lax.reduce_precision(kernel_bank, 8, 7)
    bank_lo = (kernel_bank - bank_hi).astype(bf16)
    bank_hi = bank_hi.astype(bf16)
    row_ids = (pulse_here * n_scat + scat_here) * rows + jnp.arange(rows, dtype=jnp.int32)
    theta = reference_phase(row_ids, jnp.arange(F_LEN, dtype=jnp.int32))
    theta = theta.reshape(rows * BLOCKS, STOLT)
    cos_p, sin_p = jnp.cos(theta), jnp.sin(theta)

    per = STOLT // n_dev
    span = B // n_pulse
    packed = (
        span == 128
        and n_scat == 2
        and per % 4 == 0
        and groups % 8 == 0
        and positions.shape[0] % CHUNK == 0
    )
    if packed:
        forward, backward = (jnp.asarray(t) for t in quarter_tables())
        partial = range_binning(
            positions, amplitude, range_cells, bounce, pulse_here * span, span
        )
        own = lax.dynamic_slice_in_dim(partial, scat_here * bins_here, bins_here, 0)
        other = lax.dynamic_slice_in_dim(partial, (1 - scat_here) * bins_here, bins_here, 0)
        binned = own + lax.ppermute(other, "scat", [(0, 1), (1, 0)])
        spectrum = pl.pallas_call(
            azimuth_kernel,
            out_shape=jax.ShapeDtypeStruct((n_dev, 4, groups, n), f32),
            name="azimuth",
        )(binned, forward)
        x = lax.all_to_all(spectrum, ("pulse", "scat"), 0, 0, tiled=True)
        x = x.reshape(4 * n_dev, groups, n)
        local = bins_here // BIN_SIDE
        i, s, c, l = np.meshgrid(
            np.arange(n_pulse), np.arange(n_scat), np.arange(2), np.arange(local), indexing="ij"
        )
        order = (c * BIN_SIDE + (i * n_scat + s) * local + l).reshape(-1)
    else:
        partial = binning(positions, amplitude, range_cells, bounce, pulse_here * pulses, pulses)
        partial = partial.reshape(n_scat, bins_scat, 2 * pulses)
        binned = lax.dynamic_index_in_dim(partial, scat_here, 0, keepdims=False)
        for shift in range(1, n_scat):
            other = lax.dynamic_index_in_dim(
                partial, (scat_here + shift) % n_scat, 0, keepdims=False
            )
            ring = [(i, (i + shift) % n_scat) for i in range(n_scat)]
            binned = binned + lax.ppermute(other, "scat", ring)
        turned = lax.all_to_all(
            binned.reshape(n_pulse, bins_here, 2 * pulses), "pulse", 0, 0, tiled=True
        )
        turned = turned.reshape(n_pulse, bins_here, 2, pulses).transpose(0, 3, 2, 1)
        turned = turned.reshape(P_SIZE, 2 * bins_here)
        k = np.arange(P_SIZE)
        angle = 2 * np.pi / P_SIZE * ((k[:, None] * k[None, :]) % P_SIZE)
        az = jnp.asarray(np.concatenate([np.cos(angle), np.sin(angle)], 0), f32)
        product = jnp.dot(az, turned, precision=HIGH, preferred_element_type=f32)
        pc, ps = product[:P_SIZE], product[P_SIZE:]
        spectrum = pc + jnp.concatenate([ps[:, bins_here:], -ps[:, :bins_here]], 1)
        az_rows = lax.all_to_all(
            spectrum.reshape(n_dev, rows, 2 * bins_here), ("pulse", "scat"), 0, 0, tiled=True
        )
        x = az_rows.reshape(n_pulse, n_scat, rows, 2, bins_here).transpose(3, 1, 0, 4, 2)
        x = x.reshape(2, BIN_SIDE, BIN_SIDE, rows).transpose(0, 1, 3, 2)
        x = x.reshape(2 * BIN_SIDE, groups, n)
        order = np.arange(2 * BIN_SIDE)

    tables = tuple(jnp.asarray(t) for t in mid_tables(n_dev, order))
    ranged = middle(x, cos_p, sin_p, hot, kind, bank_hi, bank_lo, tables)
    if packed:
        columns = lax.all_to_all(
            ranged.reshape(n_dev, 2, per, groups, n), ("pulse", "scat"), 0, 0, tiled=True
        )
        return pl.pallas_call(
            image_kernel,
            out_shape=jax.ShapeDtypeStruct((2, P_SIZE, width), f32),
            name="image",
        )(columns, backward)
    columns = lax.all_to_all(
        ranged.reshape(n_dev, 2 * per, rows * BLOCKS), ("pulse", "scat"), 0, 0, tiled=True
    )
    columns = columns.reshape(n_dev, 2, per, rows, BLOCKS).transpose(0, 3, 1, 2, 4)
    columns = columns.reshape(P_SIZE, 2 * width)
    final = jnp.dot(az, columns, precision=HIGH, preferred_element_type=f32)
    fc, fs = final[:P_SIZE], final[P_SIZE:]
    re = (fc[:, :width] - fs[:, width:]) / P_SIZE
    im = (fc[:, width:] + fs[:, :width]) / P_SIZE
    return jnp.stack([re, im])


def solution(mesh):
    placed = (
        P(("scene", "scat")),
        P(None, ("scene", "scat")),
        P(("scene", "scat")),
        P(("scene", "scat")),
        P(("pulse", "scat"), None),
        P(("pulse", "scat"), None),
        P(),
    )
    return jax.shard_map(
        on_device,
        mesh=mesh,
        in_specs=placed,
        out_specs=P(None, "scene", ("pulse", "scat")),
        check_vma=False,
    )
```

```python
import functools

import jax
import jax.numpy as jnp
import numpy as np
from jax import lax
from jax.experimental import pallas as pl
from jax.experimental.pallas import tpu as pltpu
from jax.sharding import PartitionSpec as P

P_SIZE = 512
F_LEN = 4096
B = 1024
SHIFT = 16
STOLT = 128
BLOCKS = 32
SPACING = 2.0
NEAR = 700000.0
BIN_SIDE = 32
GROUP = 4
CHUNK = 1024
SLOTS = 192
WIDE = 256
HIGH = lax.Precision.HIGH
MESH = pl.DeviceIdType.MESH
f32 = jnp.float32
bf16 = jnp.bfloat16


def trig_coefs():
    x = np.cos(np.pi * (np.arange(400) + 0.5) / 400) * 0.5
    u = x * x
    s = np.polynomial.chebyshev.Chebyshev.fit(u, np.sin(np.pi * x) / x, 5).convert(
        kind=np.polynomial.Polynomial
    )
    c = np.polynomial.chebyshev.Chebyshev.fit(u, np.cos(np.pi * x), 5).convert(
        kind=np.polynomial.Polynomial
    )
    return [float(v) for v in s.coef], [float(v) for v in c.coef]


def horner(u, coefs):
    acc = jnp.full_like(u, coefs[-1])
    for c in coefs[-2::-1]:
        acc = acc * u + c
    return acc


def split(x):
    hi = x.astype(bf16)
    lo = (x - hi.astype(f32)).astype(bf16)
    return hi, lo


def np_split(x):
    x = np.asarray(x, np.float64)
    hi = np.asarray(x, jnp.bfloat16)
    lo = np.asarray(x - hi.astype(np.float64), jnp.bfloat16)
    return np.stack([hi, lo])


def dots(a, b, dims):
    d = functools.partial(
        lax.dot_general, dimension_numbers=(dims, ((), ())), preferred_element_type=f32
    )
    return d(a[0], b[0]) + (d(a[0], b[1]) + d(a[1], b[0]))


def bin_kernel(pulse_base, pos, amp, tgt, bnc, out, acc, *, pulses, sin_c, cos_c):
    step = pl.program_id(0)
    width = pos.shape[1]

    @pl.when(step == 0)
    def _():
        acc[...] = jnp.zeros_like(acc)

    base = pulse_base[0]
    ids = base + lax.broadcasted_iota(jnp.int32, (pulses, width), 0)
    along = (ids.astype(f32) - P_SIZE // 2) * SPACING
    target = tgt[...] + SHIFT * bnc[...]
    slant = NEAR + target.astype(f32)
    offset = along - pos[...]
    square = offset * offset
    excess = square / (jnp.sqrt(slant * slant + square) + slant)
    halves = excess * -128.0
    whole = jnp.round(halves)
    r = halves - whole
    u = r * r
    odd = whole - 2.0 * jnp.floor(whole * 0.5)
    sign = 1.0 - 2.0 * odd
    sin_p = sign * r * horner(u, sin_c)
    cos_p = sign * horner(u, cos_c)
    flip = 1.0 - 2.0 * bnc[...].astype(f32)
    are = flip * amp[0:1]
    aim = flip * amp[1:2]
    re = are * cos_p - aim * sin_p
    im = are * sin_p + aim * cos_p
    steer = jnp.concatenate([re, im], 0)
    hi, lo = split(steer)
    rhs = jnp.concatenate([hi, lo], 0)
    bins = lax.broadcasted_iota(jnp.int32, (B, width), 0)
    hot = jnp.where(bins == target, 1.0, 0.0).astype(bf16)
    acc[...] += lax.dot_general(
        hot, rhs, (((1,), (1,)), ((), ())), preferred_element_type=f32
    )

    @pl.when(step == pl.num_programs(0) - 1)
    def _():
        out[...] = acc[:, : 2 * pulses] + acc[:, 2 * pulses :]


def binning(positions, amplitude, cells, bounce, pulse_base, pulses):
    count = positions.shape[0]
    width = min(2048, count)
    sin_c, cos_c = trig_coefs()
    row = lambda n: pl.BlockSpec((n, width), lambda i: (0, i))
    return pl.pallas_call(
        functools.partial(bin_kernel, pulses=pulses, sin_c=sin_c, cos_c=cos_c),
        grid=(count // width,),
        in_specs=[pl.BlockSpec(memory_space=pltpu.SMEM), row(1), row(2), row(1), row(1)],
        out_specs=pl.BlockSpec((B, 2 * pulses), lambda i: (0, 0)),
        out_shape=jax.ShapeDtypeStruct((B, 2 * pulses), f32),
        scratch_shapes=[pltpu.VMEM((B, 4 * pulses), f32)],
        name="binning",
    )(
        pulse_base.reshape(1),
        positions.reshape(1, count),
        amplitude,
        cells.reshape(1, count),
        bounce.reshape(1, count),
    )


def range_trig_coefs(degree):
    x = np.cos(np.pi * (np.arange(400) + 0.5) / 400) * 0.5
    u = x * x
    fit = lambda y: np.polynomial.chebyshev.Chebyshev.fit(u, y, degree).convert(
        kind=np.polynomial.Polynomial
    )
    return [float(v) for v in fit(np.sin(np.pi * x) / x).coef], [
        float(v) for v in fit(np.cos(np.pi * x)).coef
    ]


def split3(x):
    hi = x.astype(bf16).astype(f32)
    rest = x - hi
    mid = rest.astype(bf16).astype(f32)
    return hi, mid, rest - mid


def range_bin_kernel(
    base_ref, cells8, bounce8, pos, amp, cells, bnc, out, buf, acc, *, span, sin_c, cos_c
):
    base = base_ref[0]
    rows = cells8.shape[0]
    chunks = rows // 8
    target = cells8[...] + SHIFT * bounce8[...] - base
    match = jnp.where((target >= 0) & (target < span), 1.0, 0.0)
    mb = match.astype(bf16)
    a = lax.broadcasted_iota(jnp.int32, (128, 128), 0)
    b = lax.broadcasted_iota(jnp.int32, (128, 128), 1)
    upto = jnp.where(a <= b, 1.0, 0.0).astype(bf16)
    count = jnp.dot(mb, upto, preferred_element_type=f32)
    total = jnp.dot(mb, jnp.ones((128, 128), bf16), preferred_element_type=f32)
    a = lax.broadcasted_iota(jnp.int32, (rows, rows), 0)
    b = lax.broadcasted_iota(jnp.int32, (rows, rows), 1)
    below = jnp.where((a // 8 == b // 8) & (b < a), 1.0, 0.0).astype(bf16)
    ahead = jnp.dot(below, total.astype(bf16), preferred_element_type=f32)
    rank = jnp.where(match > 0.0, count + ahead - 1.0, -1.0)
    counts = [
        jnp.sum(match[8 * c : 8 * c + 8]).astype(jnp.int32) for c in range(chunks)
    ]

    def values(c):
        lanes = slice(CHUNK * c, CHUNK * (c + 1))
        flip = 1.0 - 2.0 * bnc[:, lanes].astype(f32)
        rel = (cells[:, lanes] + SHIFT * bnc[:, lanes] - base).astype(f32)
        zero = jnp.zeros_like(rel)
        data = jnp.concatenate(
            [pos[:, lanes], amp[0:1, lanes] * flip, amp[1:2, lanes] * flip, rel] + [zero] * 4, 0
        )
        return jnp.concatenate(list(split3(data)) + [jnp.zeros_like(data)], 0).astype(bf16)

    def pick(c, first):
        slots = lax.broadcasted_iota(jnp.int32, (SLOTS, 128), 0).astype(f32) + first
        hot = jnp.concatenate(
            [jnp.where(rank[8 * c + j : 8 * c + j + 1] == slots, 1.0, 0.0) for j in range(8)], 1
        ).astype(bf16)
        return lax.dot_general(
            hot, values(c), (((1,), (1,)), ((), ())), preferred_element_type=f32
        )

    start = 0
    for c in range(chunks):
        buf[pl.ds(start, SLOTS), 0:32] = pick(c, 0.0)
        start = start + counts[c]
    most = functools.reduce(jnp.maximum, counts)

    @pl.when(most > SLOTS)
    def _():
        begin = 0
        for c in range(chunks):

            @pl.loop(0, (counts[c] + SLOTS - 1) // SLOTS)
            def _(i):
                first = (i * SLOTS).astype(f32)
                buf[pl.ds(begin + i * SLOTS, SLOTS), 0:32] = pick(c, first)

            begin = begin + counts[c]

    buf[pl.ds(start, WIDE), :] = jnp.zeros((WIDE, 128), f32)
    acc[...] = jnp.zeros_like(acc)
    bins = lax.broadcasted_iota(jnp.int32, (span, WIDE), 0).astype(f32)
    nearest = base.astype(f32) + NEAR

    @pl.loop(0, (start + WIDE - 1) // WIDE)
    def _(i):
        cols = []
        for h in range(WIDE // 128):
            t = buf[pl.ds(i * WIDE + h * 128, 128), :].T
            cols.append(t[0:8] + t[8:16] + t[16:24])
        data = jnp.concatenate(cols, 1)
        where, re_amp, im_amp, rel = (data[j : j + 1] for j in range(4))
        re2, im2 = 2.0 * re_amp, 2.0 * im_amp
        inverse = 0.5 / (rel + nearest)
        gain = inverse * -64.0
        bend = inverse * (1.0 / 64.0)
        hot = jnp.where(bins == rel, 1.0, 0.0).astype(bf16)
        for q in range(P_SIZE // 128):
            parts = []
            for p in range(0, 128, 16):
                ids = lax.broadcasted_iota(jnp.int32, (16, WIDE), 0)
                along = (ids + (q * 128 + p - P_SIZE // 2)).astype(f32) * SPACING
                offset = along - where
                t = offset * offset * gain
                y = t * bend
                t = t * (1.0 + y * (1.0 + 2.0 * y))
                r = t - jnp.round(t)
                u = r * r
                sn = r * horner(u, sin_c)
                cs = horner(u, cos_c)
                re = re_amp - sn * (re2 * sn + im2 * cs)
                im = im_amp + sn * (re2 * cs - im2 * sn)
                parts.append(split(re) + split(im))
            for c in range(2):
                lanes = slice(c * P_SIZE + q * 128, c * P_SIZE + (q + 1) * 128)
                hi = jnp.concatenate([v[2 * c] for v in parts], 0)
                lo = jnp.concatenate([v[2 * c + 1] for v in parts], 0)
                d = functools.partial(
                    lax.dot_general,
                    dimension_numbers=(((1,), (1,)), ((), ())),
                    preferred_element_type=f32,
                )
                acc[:, lanes] += d(hot, hi) + d(hot, lo)

    out[...] = acc[...]


def range_binning(positions, amplitude, cells, bounce, base, span):
    count = positions.shape[0]
    sin_c, cos_c = range_trig_coefs(4)
    whole = pl.BlockSpec(memory_space=pltpu.VMEM)
    return pl.pallas_call(
        functools.partial(range_bin_kernel, span=span, sin_c=sin_c, cos_c=cos_c),
        in_specs=[pl.BlockSpec(memory_space=pltpu.SMEM)] + [whole] * 6,
        out_specs=whole,
        out_shape=jax.ShapeDtypeStruct((span, 2 * P_SIZE), f32),
        scratch_shapes=[
            pltpu.VMEM((count + SLOTS + WIDE, 128), f32),
            pltpu.VMEM((span, 2 * P_SIZE), f32),
        ],
        name="range_binning",
    )(
        base.reshape(1),
        cells.reshape(count // 128, 128),
        bounce.reshape(count // 128, 128),
        positions.reshape(1, count),
        amplitude,
        cells.reshape(1, count),
        bounce.reshape(1, count),
    )


def complex_rows(c, s):
    return np.block([[c, s], [-s, c]])


def mid_tables(n_dev, order):
    side = np.arange(BIN_SIDE)
    t = np.arange(STOLT)
    eye = np.eye(GROUP)
    a = -2 * np.pi / STOLT * ((side[:, None] * t[None, :]) % STOLT)
    ta = complex_rows(np.cos(a), np.sin(a))[order]
    a = -2 * np.pi / F_LEN * (side[:, None] * t[None, :])
    wa = np.stack([np.tile(np.cos(a), (GROUP, 1)), np.tile(np.sin(a), (GROUP, 1))])
    a = -2 * np.pi / BIN_SIDE * ((side[:, None] * side[None, :]) % BIN_SIDE)
    c, s = np.kron(eye, np.cos(a)), np.kron(eye, np.sin(a))
    tb = complex_rows(c, s).T
    blk = np.arange(BLOCKS)
    a = 2 * np.pi / BLOCKS * ((blk[:, None] * blk[None, :]) % BLOCKS)
    c, s = np.kron(eye, np.cos(a)), np.kron(eye, np.sin(a))
    tc = complex_rows(c, s)
    a = 2 * np.pi / F_LEN * (t[:, None] * blk[None, :])
    wc = np.stack([np.tile(np.cos(a), (1, GROUP)), np.tile(np.sin(a), (1, GROUP))])
    a = 2 * np.pi / STOLT * ((t[:, None] * t[None, :]) % STOLT)
    td = complex_rows(np.cos(a), np.sin(a)).T / F_LEN
    td = td.reshape(2, n_dev, STOLT // n_dev, 2 * STOLT).transpose(1, 0, 2, 3)
    td = td.reshape(2 * STOLT, 2 * STOLT)
    return (
        np_split(ta),
        wa.astype(np.float32),
        np_split(tb),
        np_split(tc),
        wc.astype(np.float32),
        np_split(td),
    )


def mid_kernel(
    x, cos_p, sin_p, hot, kind, bank_hi, bank_lo, ta, wa, tb, tc, wc, td, out, xs, os, *, subs
):
    n = GROUP * BLOCKS
    step = pl.program_id(0)
    groups = x.shape[1]

    @pl.when(step == 0)
    def _():
        for g in range(groups):
            xs[g] = x[:, g, :]

    parts_hi, parts_lo = [], []
    for g in range(subs):
        lanes = slice(g * n, (g + 1) * n)
        y = dots(split(xs[step * subs + g]), (ta[0], ta[1]), ((0,), (0,)))
        yr, yi = y[:, :STOLT], y[:, STOLT:]
        y = jnp.concatenate([yr * wa[0] - yi * wa[1], yr * wa[1] + yi * wa[0]], 0)
        z = dots((tb[0], tb[1]), split(y), ((1,), (0,)))
        zr, zi = z[:n], z[n:]
        cp, sp = cos_p[lanes], sin_p[lanes]
        z = jnp.concatenate([zr * cp - zi * sp, zr * sp + zi * cp], 1)
        hi, lo = split(z)
        picked = jnp.dot(
            hot[g], jnp.concatenate([hi, lo], 1), preferred_element_type=f32
        ).astype(bf16)
        first, second = picked[:n], picked[n:]
        for c in range(2):
            for base, keep in ((0, parts_hi), (2 * STOLT, parts_lo)):
                cut = slice(base + c * STOLT, base + (c + 1) * STOLT)
                keep.append(jnp.concatenate([first[:, cut], second[:, cut]], 1))
    ghi = jnp.concatenate(parts_hi, 0)
    glo = jnp.concatenate(parts_lo, 0)
    kinds = kind[...].reshape(subs * 2 * n, 1)
    kinds = jnp.broadcast_to(kinds, (subs * 2 * n, STOLT))
    acc = jnp.zeros((subs * 2 * n, STOLT), f32)
    for k in range(0, bank_hi.shape[0], 2):
        khi = jnp.concatenate([bank_hi[k], bank_hi[k + 1]], 1)
        klo = jnp.concatenate([bank_lo[k], bank_lo[k + 1]], 1)
        r = dots((ghi, glo), (khi, klo), ((1,), (0,)))
        for half in range(2):
            acc = jnp.where(kinds == k + half, r[:, half * STOLT : (half + 1) * STOLT], acc)
    for g in range(subs):
        s = acc[g * 2 * n : (g + 1) * 2 * n]
        y = dots(split(s), (tc[0], tc[1]), ((0,), (0,)))
        yr, yi = y[:, :n], y[:, n:]
        y = jnp.concatenate([yr * wc[0] - yi * wc[1], yr * wc[1] + yi * wc[0]], 0)
        os[step * subs + g] = dots((td[0], td[1]), split(y), ((1,), (0,)))

    @pl.when(step == pl.num_programs(0) - 1)
    def _():
        for g in range(groups):
            out[:, g, :] = os[g]


def middle(x, cos_p, sin_p, hot, kind, bank_hi, bank_lo, tables):
    groups = x.shape[1]
    subs = min(4, groups)
    n = GROUP * BLOCKS
    whole = lambda a: pl.BlockSpec(a.shape, lambda i: (0,) * a.ndim)
    return pl.pallas_call(
        functools.partial(mid_kernel, subs=subs),
        grid=(groups // subs,),
        in_specs=[
            whole(x),
            pl.BlockSpec((subs * n, STOLT), lambda i: (i, 0)),
            pl.BlockSpec((subs * n, STOLT), lambda i: (i, 0)),
            pl.BlockSpec((subs, 2 * n, n), lambda i: (i, 0, 0)),
            pl.BlockSpec((subs, 2 * n, 1), lambda i: (i, 0, 0)),
            whole(bank_hi),
            whole(bank_lo),
        ]
        + [whole(t) for t in tables],
        out_specs=pl.BlockSpec((2 * STOLT, groups, n), lambda i: (0, 0, 0)),
        out_shape=jax.ShapeDtypeStruct((2 * STOLT, groups, n), f32),
        scratch_shapes=[
            pltpu.VMEM((groups, x.shape[0], n), f32),
            pltpu.VMEM((groups, 2 * STOLT, n), f32),
        ],
        name="middle",
    )(x, cos_p, sin_p, hot, kind, bank_hi, bank_lo, *tables)


def quarter_tables():
    q = P_SIZE // 4
    m = np.arange(q)
    fwd, inv = [], []
    for low in range(4):
        a = 2 * np.pi / P_SIZE * (((4 * m[:, None] + low) * m[None, :]) % P_SIZE)
        fwd.append(np.concatenate([np.cos(a), np.sin(a)], 0))
        inv.append(np.concatenate([np.cos(a.T), np.sin(a.T)], 0) / P_SIZE)
    return np_split(np.stack(fwd)), np_split(np.stack(inv))


def swap_blocks(arrays):
    count = len(arrays)
    lanes = arrays[0].shape[-1]
    size = lanes // count
    block = lax.broadcasted_iota(jnp.int32, arrays[0].shape, 1) // size
    outs = []
    for b in range(count):
        acc = None
        for a in range(count):
            shift = (a - b) % count * size
            moved = pltpu.roll(arrays[a], shift, 1) if shift else arrays[a]
            acc = moved if acc is None else jnp.where(block == a, moved, acc)
        outs.append(acc)
    return outs


def core_kernel(
    partial, steps_in, kinds_in, bank, table, ta, wa, tb, tc, wc, td,
    out,
    peer, binned, spec, x, xs, cos_p, sin_p, hot, kind, bank_hi, bank_lo, bank_f, os,
    bank_sem, pair_send, pair_recv, near_send, near_recv, far_send, far_recv,
    *, n_pulse, n_scat, subs, trig,
):
    n_dev = n_pulse * n_scat
    pulse = lax.axis_index("pulse")
    scat = lax.axis_index("scat")
    me = pulse * n_scat + scat
    half = binned.shape[0]
    lanes = 2 * half
    size = P_SIZE // 4
    n = GROUP * BLOCKS
    groups = xs.shape[0]
    moves = [(a, b) for a in range(n_pulse) for b in range(n_scat) if (a, b) != (0, 0)]
    moves.sort(key=lambda m: (-min(m[0], n_pulse - m[0]), m))

    def other(a, b):
        return lax.rem(pulse + a, n_pulse), lax.rem(scat + b, n_scat)

    fetch = pltpu.make_async_copy(bank, bank_f, bank_sem)
    fetch.start()
    barrier = pltpu.get_barrier_semaphore()
    for a, b in moves:
        p, c = other(a, b)
        pl.semaphore_signal(
            barrier, inc=1, device_id={"pulse": p, "scat": c}, device_id_type=MESH
        )
    pl.semaphore_wait(barrier, n_dev - 1)

    away = 1 - scat
    pair = pltpu.make_async_remote_copy(
        src_ref=partial.at[pl.ds(pl.multiple_of(away * half, half), half), :],
        dst_ref=peer,
        send_sem=pair_send,
        recv_sem=pair_recv,
        device_id={"pulse": pulse, "scat": away},
        device_id_type=MESH,
    )
    pair.start()
    pair.wait()
    binned[...] = partial[pl.ds(pl.multiple_of(scat * half, half), half), :] + peer[...]

    quarters = []
    for q in range(4):
        re = binned[:, q * size : (q + 1) * size]
        im = binned[:, P_SIZE + q * size : P_SIZE + (q + 1) * size]
        quarters.append((re, im))
    (r0, i0), (r1, i1), (r2, i2), (r3, i3) = quarters
    sr, si, dr, di = r0 + r2, i0 + i2, r0 - r2, i0 - i2
    tr, ti, er, ei = r1 + r3, i1 + i3, r1 - r3, i1 - i3
    mixed = (
        (sr + tr, si + ti),
        (dr + ei, di - er),
        (sr - tr, si - ti),
        (dr - ei, di + er),
    )
    low = lax.broadcasted_iota(jnp.int32, (size, lanes), 1) < half
    rows = []
    for k in range(4):
        u = jnp.concatenate(mixed[k], 0)
        g = dots((table[0, k], table[1, k]), split(u), ((1,), (1,)))
        turned = pltpu.roll(g[size:], half, 1)
        rows.append(g[:size] + jnp.where(low, turned, -turned))
    for q, z in enumerate(swap_blocks(rows)):
        spec[:, q] = z.reshape(spec.shape[0], groups, n)

    sends = []
    for i, (a, b) in enumerate(moves):
        p, c = other(a, b)
        copy = pltpu.make_async_remote_copy(
            src_ref=spec.at[p * n_scat + c],
            dst_ref=x.at[me],
            send_sem=near_send.at[i],
            recv_sem=near_recv.at[me],
            device_id={"pulse": p, "scat": c},
            device_id_type=MESH,
        )
        copy.start()
        sends.append(copy)
    x[me] = spec[me]

    block = lax.broadcasted_iota(jnp.int32, (n, STOLT), 0)
    lane = lax.broadcasted_iota(jnp.int32, (n, STOLT), 1)
    cols = (lane + (block % BLOCKS) * STOLT).astype(f32)
    kr = 4.0 * np.pi / 3e8 * (9.6e9 + (cols - F_LEN // 2) * (1.5e8 / F_LEN))
    flat = []
    for ref in (steps_in, kinds_in):
        flat.append(
            jnp.concatenate([ref[pl.ds(j, groups, stride=GROUP), :] for j in range(GROUP)], 1)
        )
    for g in range(groups):
        row = me * (groups * GROUP) + g * GROUP + block // BLOCKS
        centered = lax.rem(row + P_SIZE // 2, P_SIZE) - P_SIZE // 2
        along = 2.0 * np.pi / (P_SIZE * SPACING) * centered.astype(f32)
        squared = along * along
        depth = NEAR + B // 2
        theta = -depth * squared / (jnp.sqrt(kr * kr - squared) + kr)
        whole = jnp.round(theta * (0.5 / np.pi))
        for part in turn_parts():
            theta = theta - whole * part
        r = theta * (0.5 / np.pi)
        u = r * r
        sn = r * horner(u, trig[0])
        cs = horner(u, trig[1])
        cos_p[g] = 1.0 - 2.0 * sn * sn
        sin_p[g] = 2.0 * sn * cs
        first = jnp.broadcast_to(flat[0][g : g + 1].astype(f32), (n, n)).T
        first = first + (block // BLOCKS * BLOCKS).astype(f32)
        spot = lane.astype(f32)
        hot[g, :n] = jnp.where(first == spot, 1.0, 0.0).astype(bf16)
        hot[g, n:] = jnp.where(first + 1.0 == spot, 1.0, 0.0).astype(bf16)
        kind[g] = jnp.broadcast_to(flat[1][g : g + 1].astype(f32), (n, n)).T
    fetch.wait()
    for k in range(bank_f.shape[0]):
        hi, lo = split(bank_f[k])
        cut = slice(k % 2 * STOLT, (k % 2 + 1) * STOLT)
        bank_hi[k // 2, :, cut] = hi
        bank_lo[k // 2, :, cut] = lo

    for i, (a, b) in enumerate(moves):
        sends[i].wait_send()
    for a, b in moves:
        p, c = other(a, b)
        src = p * n_scat + c
        pltpu.make_async_copy(x.at[src], x.at[src], near_recv.at[src]).wait()
    for g in range(groups):
        xs[g] = x[:, :, g, :].reshape(xs.shape[1], n)

    per = 2 * STOLT // n_dev

    def step(i, carry):
        parts_hi, parts_lo = [], []
        for s in range(subs):
            g = i * subs + s
            y = dots(split(xs[g]), (ta[0], ta[1]), ((0,), (0,)))
            yr, yi = y[:, :STOLT], y[:, STOLT:]
            y = jnp.concatenate([yr * wa[0] - yi * wa[1], yr * wa[1] + yi * wa[0]], 0)
            z = dots((tb[0], tb[1]), split(y), ((1,), (0,)))
            zr, zi = z[:n], z[n:]
            cp, sp = cos_p[g], sin_p[g]
            z = jnp.concatenate([zr * cp - zi * sp, zr * sp + zi * cp], 1)
            hi, lo = split(z)
            picked = jnp.dot(
                hot[g], jnp.concatenate([hi, lo], 1), preferred_element_type=f32
            ).astype(bf16)
            first, second = picked[:n], picked[n:]
            for c in range(2):
                for base, keep in ((0, parts_hi), (2 * STOLT, parts_lo)):
                    cut = slice(base + c * STOLT, base + (c + 1) * STOLT)
                    keep.append(jnp.concatenate([first[:, cut], second[:, cut]], 1))
        ghi = jnp.concatenate(parts_hi, 0)
        glo = jnp.concatenate(parts_lo, 0)
        kinds = jnp.concatenate([kind[i * subs + s // 2] for s in range(2 * subs)], 0)
        acc = jnp.zeros((subs * 2 * n, STOLT), f32)
        for k in range(bank_hi.shape[0]):
            r = dots((ghi, glo), (bank_hi[k], bank_lo[k]), ((1,), (0,)))
            for h in range(2):
                acc = jnp.where(kinds == 2 * k + h, r[:, h * STOLT : (h + 1) * STOLT], acc)
        for s in range(subs):
            y = dots(split(acc[s * 2 * n : (s + 1) * 2 * n]), (tc[0], tc[1]), ((0,), (0,)))
            yr, yi = y[:, :n], y[:, n:]
            y = jnp.concatenate([yr * wc[0] - yi * wc[1], yr * wc[1] + yi * wc[0]], 0)
            z = dots((td[0], td[1]), split(y), ((1,), (0,)))
            os[:, i * subs + s] = z.reshape(n_dev, per, n)
        span = pl.ds(i * subs, subs)
        for j, (a, b) in enumerate(moves):
            p, c = other(a, b)
            pltpu.make_async_remote_copy(
                src_ref=os.at[p * n_scat + c, span],
                dst_ref=out.at[me, span],
                send_sem=far_send.at[j],
                recv_sem=far_recv.at[me],
                device_id={"pulse": p, "scat": c},
                device_id_type=MESH,
            ).start()
        return carry

    lax.fori_loop(0, groups // subs, step, 0)
    mine = pltpu.make_async_copy(os.at[me], out.at[me], bank_sem)
    mine.start()
    mine.wait()
    for j, (a, b) in enumerate(moves):
        p, c = other(a, b)
        src = p * n_scat + c
        pltpu.make_async_copy(os.at[src], os.at[src], far_send.at[j]).wait()
        pltpu.make_async_copy(out.at[src], out.at[src], far_recv.at[src]).wait()


def turn_parts():
    parts, rest = [], 2.0 * np.pi
    for bits in (10, 22, 60):
        scale = 2.0**bits
        part = float(np.float32(np.round(rest * scale) / scale))
        parts.append(part)
        rest -= part
    return parts


def core(partial, steps_in, kinds_in, bank, table, tables, n_pulse, n_scat):
    n_dev = n_pulse * n_scat
    rows = steps_in.shape[0]
    groups = rows // GROUP
    subs = 2
    n = GROUP * BLOCKS
    span, width = partial.shape
    half = span // n_scat
    quads = 2 * half // BIN_SIDE
    kernels = bank.shape[0]
    per = 2 * STOLT // n_dev
    vmem = pl.BlockSpec(memory_space=pltpu.VMEM)
    dma = pltpu.SemaphoreType.DMA
    return pl.pallas_call(
        functools.partial(
            core_kernel, n_pulse=n_pulse, n_scat=n_scat, subs=subs, trig=range_trig_coefs(5)
        ),
        in_specs=[vmem] * 3 + [pl.BlockSpec(memory_space=pl.ANY)] + [vmem] * (1 + len(tables)),
        out_specs=vmem,
        out_shape=jax.ShapeDtypeStruct((n_dev, groups, per, n), f32),
        scratch_shapes=[
            pltpu.VMEM((half, width), f32),
            pltpu.VMEM((half, width), f32),
            pltpu.VMEM((n_dev, quads, groups, n), f32),
            pltpu.VMEM((n_dev, quads, groups, n), f32),
            pltpu.VMEM((groups, n_dev * quads, n), f32),
            pltpu.VMEM((groups, n, STOLT), f32),
            pltpu.VMEM((groups, n, STOLT), f32),
            pltpu.VMEM((groups, 2 * n, n), bf16),
            pltpu.VMEM((groups, n, STOLT), f32),
            pltpu.VMEM((kernels // 2, 2 * STOLT, 2 * STOLT), bf16),
            pltpu.VMEM((kernels // 2, 2 * STOLT, 2 * STOLT), bf16),
            pltpu.VMEM(bank.shape, f32),
            pltpu.VMEM((n_dev, groups, per, n), f32),
            dma,
            dma,
            dma,
            dma((n_dev,)),
            dma((n_dev,)),
            dma((n_dev,)),
            dma((n_dev,)),
        ],
        compiler_params=pltpu.CompilerParams(collective_id=0, has_side_effects=True),
        name="core",
    )(partial, steps_in, kinds_in, bank, table, *tables)


def image_kernel(x, table, out):
    devs, kh, per, lanes = x.shape
    per = per // 2
    size = P_SIZE // 4
    columns = [[] for _ in range(4)]
    for c in range(2):
        for h in range(per // 4):
            tiles = [x[:, :, c * per + 4 * h + j, :].reshape(devs * kh, lanes) for j in range(4)]
            for k, z in enumerate(swap_blocks(tiles)):
                columns[k].append(z)
    width = lanes * (per // 4)
    v = []
    for k in range(4):
        g = dots((table[0, k], table[1, k]), split(jnp.concatenate(columns[k], 1)), ((1,), (0,)))
        cos_g, sin_g = g[:size], g[size:]
        v.append((cos_g[:, :width] - sin_g[:, width:], cos_g[:, width:] + sin_g[:, :width]))
    (r0, i0), (r1, i1), (r2, i2), (r3, i3) = v
    sr, si, dr, di = r0 + r2, i0 + i2, r0 - r2, i0 - i2
    tr, ti, er, ei = r1 + r3, i1 + i3, r1 - r3, i1 - i3
    mixed = (
        (sr + tr, si + ti),
        (dr - ei, di + er),
        (sr - tr, si - ti),
        (dr + ei, di - er),
    )
    for q in range(4):
        for c in range(2):
            out[c, q * size : (q + 1) * size, :] = mixed[q][c]


def reference_phase(row_ids, cols):
    centered = (row_ids + P_SIZE // 2) % P_SIZE - P_SIZE // 2
    along_k = 2.0 * jnp.pi / (P_SIZE * SPACING) * centered.astype(f32)
    kr = 4.0 * jnp.pi / 3e8 * (9.6e9 + (cols.astype(f32) - F_LEN // 2) * (1.5e8 / F_LEN))
    squared = along_k * along_k
    depth = NEAR + B // 2
    return (
        -depth
        * squared[:, None]
        / (jnp.sqrt(kr[None, :] * kr[None, :] - squared[:, None]) + kr[None, :])
    )


def on_device(positions, amplitude, range_cells, bounce, stolt_block, kernel_choice, kernel_bank):
    n_pulse = lax.axis_size("pulse")
    n_scat = lax.axis_size("scat")
    n_dev = n_pulse * n_scat
    pulse_here = lax.axis_index("pulse")
    scat_here = lax.axis_index("scat")
    pulses = P_SIZE // n_pulse
    rows = P_SIZE // n_dev
    width = F_LEN // n_dev
    groups = rows // GROUP
    n = GROUP * BLOCKS
    bins_scat = B // n_scat
    bins_here = bins_scat // n_pulse

    per = STOLT // n_dev
    span = B // n_pulse
    packed = (
        span == 128
        and n_scat == 2
        and per % 4 == 0
        and groups % 8 == 0
        and positions.shape[0] % CHUNK == 0
    )
    if packed:
        forward, backward = (jnp.asarray(t) for t in quarter_tables())
        partial = range_binning(
            positions, amplitude, range_cells, bounce, pulse_here * span, span
        )
        local = bins_here // BIN_SIDE
        i, s, c, l = np.meshgrid(
            np.arange(n_pulse), np.arange(n_scat), np.arange(2), np.arange(local), indexing="ij"
        )
        order = (c * BIN_SIDE + (i * n_scat + s) * local + l).reshape(-1)
        tables = tuple(jnp.asarray(t) for t in mid_tables(n_dev, order))
        columns = core(
            partial, stolt_block, kernel_choice, kernel_bank, forward, tables, n_pulse, n_scat
        )
        return pl.pallas_call(
            image_kernel,
            out_shape=jax.ShapeDtypeStruct((2, P_SIZE, width), f32),
            name="image",
        )(columns, backward)

    ids = jnp.arange(GROUP, dtype=jnp.int32)[None, :, None] * BLOCKS
    first = stolt_block.reshape(groups, GROUP, BLOCKS) + ids
    pick = jnp.stack([first, first + 1], 1).reshape(groups, 2 * n, 1)
    hot = (pick == jnp.arange(n, dtype=jnp.int32)[None, None, :]).astype(bf16)
    kind = jnp.stack([kernel_choice.reshape(groups, n)] * 2, 1).reshape(groups, 2 * n, 1)
    bank_hi = lax.reduce_precision(kernel_bank, 8, 7)
    bank_lo = (kernel_bank - bank_hi).astype(bf16)
    bank_hi = bank_hi.astype(bf16)
    row_ids = (pulse_here * n_scat + scat_here) * rows + jnp.arange(rows, dtype=jnp.int32)
    theta = reference_phase(row_ids, jnp.arange(F_LEN, dtype=jnp.int32))
    theta = theta.reshape(rows * BLOCKS, STOLT)
    cos_p, sin_p = jnp.cos(theta), jnp.sin(theta)

    partial = binning(positions, amplitude, range_cells, bounce, pulse_here * pulses, pulses)
    partial = partial.reshape(n_scat, bins_scat, 2 * pulses)
    binned = lax.dynamic_index_in_dim(partial, scat_here, 0, keepdims=False)
    for shift in range(1, n_scat):
        other = lax.dynamic_index_in_dim(
            partial, (scat_here + shift) % n_scat, 0, keepdims=False
        )
        ring = [(i, (i + shift) % n_scat) for i in range(n_scat)]
        binned = binned + lax.ppermute(other, "scat", ring)
    turned = lax.all_to_all(
        binned.reshape(n_pulse, bins_here, 2 * pulses), "pulse", 0, 0, tiled=True
    )
    turned = turned.reshape(n_pulse, bins_here, 2, pulses).transpose(0, 3, 2, 1)
    turned = turned.reshape(P_SIZE, 2 * bins_here)
    k = np.arange(P_SIZE)
    angle = 2 * np.pi / P_SIZE * ((k[:, None] * k[None, :]) % P_SIZE)
    az = jnp.asarray(np.concatenate([np.cos(angle), np.sin(angle)], 0), f32)
    product = jnp.dot(az, turned, precision=HIGH, preferred_element_type=f32)
    pc, ps = product[:P_SIZE], product[P_SIZE:]
    spectrum = pc + jnp.concatenate([ps[:, bins_here:], -ps[:, :bins_here]], 1)
    az_rows = lax.all_to_all(
        spectrum.reshape(n_dev, rows, 2 * bins_here), ("pulse", "scat"), 0, 0, tiled=True
    )
    x = az_rows.reshape(n_pulse, n_scat, rows, 2, bins_here).transpose(3, 1, 0, 4, 2)
    x = x.reshape(2, BIN_SIDE, BIN_SIDE, rows).transpose(0, 1, 3, 2)
    x = x.reshape(2 * BIN_SIDE, groups, n)
    order = np.arange(2 * BIN_SIDE)

    tables = tuple(jnp.asarray(t) for t in mid_tables(n_dev, order))
    ranged = middle(x, cos_p, sin_p, hot, kind, bank_hi, bank_lo, tables)
    columns = lax.all_to_all(
        ranged.reshape(n_dev, 2 * per, rows * BLOCKS), ("pulse", "scat"), 0, 0, tiled=True
    )
    columns = columns.reshape(n_dev, 2, per, rows, BLOCKS).transpose(0, 3, 1, 2, 4)
    columns = columns.reshape(P_SIZE, 2 * width)
    final = jnp.dot(az, columns, precision=HIGH, preferred_element_type=f32)
    fc, fs = final[:P_SIZE], final[P_SIZE:]
    re = (fc[:, :width] - fs[:, width:]) / P_SIZE
    im = (fc[:, width:] + fs[:, :width]) / P_SIZE
    return jnp.stack([re, im])


def solution(mesh):
    placed = (
        P(("scene", "scat")),
        P(None, ("scene", "scat")),
        P(("scene", "scat")),
        P(("scene", "scat")),
        P(("pulse", "scat"), None),
        P(("pulse", "scat"), None),
        P(),
    )
    return jax.shard_map(
        on_device,
        mesh=mesh,
        in_specs=placed,
        out_specs=P(None, "scene", ("pulse", "scat")),
        check_vma=False,
    )
```

```python
import functools

import jax
import jax.numpy as jnp
import numpy as np
from jax import lax
from jax.experimental import pallas as pl
from jax.experimental.pallas import tpu as pltpu
from jax.sharding import PartitionSpec as P

P_SIZE = 512
F_LEN = 4096
B = 1024
SHIFT = 16
STOLT = 128
BLOCKS = 32
SPACING = 2.0
NEAR = 700000.0
BIN_SIDE = 32
GROUP = 4
CHUNK = 1024
SLOTS = 192
WIDE = 256
HIGH = lax.Precision.HIGH
MESH = pl.DeviceIdType.MESH
f32 = jnp.float32
bf16 = jnp.bfloat16


def trig_coefs():
    x = np.cos(np.pi * (np.arange(400) + 0.5) / 400) * 0.5
    u = x * x
    s = np.polynomial.chebyshev.Chebyshev.fit(u, np.sin(np.pi * x) / x, 5).convert(
        kind=np.polynomial.Polynomial
    )
    c = np.polynomial.chebyshev.Chebyshev.fit(u, np.cos(np.pi * x), 5).convert(
        kind=np.polynomial.Polynomial
    )
    return [float(v) for v in s.coef], [float(v) for v in c.coef]


def horner(u, coefs):
    acc = jnp.full_like(u, coefs[-1])
    for c in coefs[-2::-1]:
        acc = acc * u + c
    return acc


def split(x):
    hi = x.astype(bf16)
    lo = (x - hi.astype(f32)).astype(bf16)
    return hi, lo


def np_split(x):
    x = np.asarray(x, np.float64)
    hi = np.asarray(x, jnp.bfloat16)
    lo = np.asarray(x - hi.astype(np.float64), jnp.bfloat16)
    return np.stack([hi, lo])


def dots(a, b, dims):
    d = functools.partial(
        lax.dot_general, dimension_numbers=(dims, ((), ())), preferred_element_type=f32
    )
    return d(a[0], b[0]) + (d(a[0], b[1]) + d(a[1], b[0]))


def bin_kernel(pulse_base, pos, amp, tgt, bnc, out, acc, *, pulses, sin_c, cos_c):
    step = pl.program_id(0)
    width = pos.shape[1]

    @pl.when(step == 0)
    def _():
        acc[...] = jnp.zeros_like(acc)

    base = pulse_base[0]
    ids = base + lax.broadcasted_iota(jnp.int32, (pulses, width), 0)
    along = (ids.astype(f32) - P_SIZE // 2) * SPACING
    target = tgt[...] + SHIFT * bnc[...]
    slant = NEAR + target.astype(f32)
    offset = along - pos[...]
    square = offset * offset
    excess = square / (jnp.sqrt(slant * slant + square) + slant)
    halves = excess * -128.0
    whole = jnp.round(halves)
    r = halves - whole
    u = r * r
    odd = whole - 2.0 * jnp.floor(whole * 0.5)
    sign = 1.0 - 2.0 * odd
    sin_p = sign * r * horner(u, sin_c)
    cos_p = sign * horner(u, cos_c)
    flip = 1.0 - 2.0 * bnc[...].astype(f32)
    are = flip * amp[0:1]
    aim = flip * amp[1:2]
    re = are * cos_p - aim * sin_p
    im = are * sin_p + aim * cos_p
    steer = jnp.concatenate([re, im], 0)
    hi, lo = split(steer)
    rhs = jnp.concatenate([hi, lo], 0)
    bins = lax.broadcasted_iota(jnp.int32, (B, width), 0)
    hot = jnp.where(bins == target, 1.0, 0.0).astype(bf16)
    acc[...] += lax.dot_general(
        hot, rhs, (((1,), (1,)), ((), ())), preferred_element_type=f32
    )

    @pl.when(step == pl.num_programs(0) - 1)
    def _():
        out[...] = acc[:, : 2 * pulses] + acc[:, 2 * pulses :]


def binning(positions, amplitude, cells, bounce, pulse_base, pulses):
    count = positions.shape[0]
    width = min(2048, count)
    sin_c, cos_c = trig_coefs()
    row = lambda n: pl.BlockSpec((n, width), lambda i: (0, i))
    return pl.pallas_call(
        functools.partial(bin_kernel, pulses=pulses, sin_c=sin_c, cos_c=cos_c),
        grid=(count // width,),
        in_specs=[pl.BlockSpec(memory_space=pltpu.SMEM), row(1), row(2), row(1), row(1)],
        out_specs=pl.BlockSpec((B, 2 * pulses), lambda i: (0, 0)),
        out_shape=jax.ShapeDtypeStruct((B, 2 * pulses), f32),
        scratch_shapes=[pltpu.VMEM((B, 4 * pulses), f32)],
        name="binning",
    )(
        pulse_base.reshape(1),
        positions.reshape(1, count),
        amplitude,
        cells.reshape(1, count),
        bounce.reshape(1, count),
    )


def range_trig_coefs(degree):
    x = np.cos(np.pi * (np.arange(400) + 0.5) / 400) * 0.5
    u = x * x
    fit = lambda y: np.polynomial.chebyshev.Chebyshev.fit(u, y, degree).convert(
        kind=np.polynomial.Polynomial
    )
    return [float(v) for v in fit(np.sin(np.pi * x) / x).coef], [
        float(v) for v in fit(np.cos(np.pi * x)).coef
    ]


def split3(x):
    hi = x.astype(bf16).astype(f32)
    rest = x - hi
    mid = rest.astype(bf16).astype(f32)
    return hi, mid, rest - mid


def range_bin_kernel(
    base_ref, cells8, bounce8, pos, amp, cells, bnc, out, buf, acc, *, span, sin_c, cos_c
):
    base = base_ref[0]
    rows = cells8.shape[0]
    chunks = rows // 8
    target = cells8[...] + SHIFT * bounce8[...] - base
    match = jnp.where((target >= 0) & (target < span), 1.0, 0.0)
    mb = match.astype(bf16)
    a = lax.broadcasted_iota(jnp.int32, (128, 128), 0)
    b = lax.broadcasted_iota(jnp.int32, (128, 128), 1)
    upto = jnp.where(a <= b, 1.0, 0.0).astype(bf16)
    count = jnp.dot(mb, upto, preferred_element_type=f32)
    total = jnp.dot(mb, jnp.ones((128, 128), bf16), preferred_element_type=f32)
    a = lax.broadcasted_iota(jnp.int32, (rows, rows), 0)
    b = lax.broadcasted_iota(jnp.int32, (rows, rows), 1)
    below = jnp.where((a // 8 == b // 8) & (b < a), 1.0, 0.0).astype(bf16)
    ahead = jnp.dot(below, total.astype(bf16), preferred_element_type=f32)
    rank = jnp.where(match > 0.0, count + ahead - 1.0, -1.0)
    counts = [
        jnp.sum(match[8 * c : 8 * c + 8]).astype(jnp.int32) for c in range(chunks)
    ]

    def values(c):
        lanes = slice(CHUNK * c, CHUNK * (c + 1))
        flip = 1.0 - 2.0 * bnc[:, lanes].astype(f32)
        rel = (cells[:, lanes] + SHIFT * bnc[:, lanes] - base).astype(f32)
        zero = jnp.zeros_like(rel)
        data = jnp.concatenate(
            [pos[:, lanes], amp[0:1, lanes] * flip, amp[1:2, lanes] * flip, rel] + [zero] * 4, 0
        )
        return jnp.concatenate(list(split3(data)) + [jnp.zeros_like(data)], 0).astype(bf16)

    def pick(c, first):
        slots = lax.broadcasted_iota(jnp.int32, (SLOTS, 128), 0).astype(f32) + first
        hot = jnp.concatenate(
            [jnp.where(rank[8 * c + j : 8 * c + j + 1] == slots, 1.0, 0.0) for j in range(8)], 1
        ).astype(bf16)
        return lax.dot_general(
            hot, values(c), (((1,), (1,)), ((), ())), preferred_element_type=f32
        )

    start = 0
    for c in range(chunks):
        buf[pl.ds(start, SLOTS), 0:32] = pick(c, 0.0)
        start = start + counts[c]
    most = functools.reduce(jnp.maximum, counts)

    @pl.when(most > SLOTS)
    def _():
        begin = 0
        for c in range(chunks):

            @pl.loop(0, (counts[c] + SLOTS - 1) // SLOTS)
            def _(i):
                first = (i * SLOTS).astype(f32)
                buf[pl.ds(begin + i * SLOTS, SLOTS), 0:32] = pick(c, first)

            begin = begin + counts[c]

    buf[pl.ds(start, WIDE), :] = jnp.zeros((WIDE, 128), f32)
    acc[...] = jnp.zeros_like(acc)
    bins = lax.broadcasted_iota(jnp.int32, (span, WIDE), 0).astype(f32)
    nearest = base.astype(f32) + NEAR

    @pl.loop(0, (start + WIDE - 1) // WIDE)
    def _(i):
        cols = []
        for h in range(WIDE // 128):
            t = buf[pl.ds(i * WIDE + h * 128, 128), :].T
            cols.append(t[0:8] + t[8:16] + t[16:24])
        data = jnp.concatenate(cols, 1)
        where, re_amp, im_amp, rel = (data[j : j + 1] for j in range(4))
        re2, im2 = 2.0 * re_amp, 2.0 * im_amp
        inverse = 0.5 / (rel + nearest)
        gain = inverse * -64.0
        bend = inverse * (1.0 / 64.0)
        hot = jnp.where(bins == rel, 1.0, 0.0).astype(bf16)
        for q in range(P_SIZE // 128):
            parts = []
            for p in range(0, 128, 16):
                ids = lax.broadcasted_iota(jnp.int32, (16, WIDE), 0)
                along = (ids + (q * 128 + p - P_SIZE // 2)).astype(f32) * SPACING
                offset = along - where
                t = offset * offset * gain
                y = t * bend
                t = t * (1.0 + y * (1.0 + 2.0 * y))
                r = t - jnp.round(t)
                u = r * r
                sn = r * horner(u, sin_c)
                cs = horner(u, cos_c)
                re = re_amp - sn * (re2 * sn + im2 * cs)
                im = im_amp + sn * (re2 * cs - im2 * sn)
                parts.append(split(re) + split(im))
            for c in range(2):
                lanes = slice(c * P_SIZE + q * 128, c * P_SIZE + (q + 1) * 128)
                hi = jnp.concatenate([v[2 * c] for v in parts], 0)
                lo = jnp.concatenate([v[2 * c + 1] for v in parts], 0)
                d = functools.partial(
                    lax.dot_general,
                    dimension_numbers=(((1,), (1,)), ((), ())),
                    preferred_element_type=f32,
                )
                acc[:, lanes] += d(hot, hi) + d(hot, lo)

    out[...] = acc[...]


def range_binning(positions, amplitude, cells, bounce, base, span):
    count = positions.shape[0]
    sin_c, cos_c = range_trig_coefs(4)
    whole = pl.BlockSpec(memory_space=pltpu.VMEM)
    return pl.pallas_call(
        functools.partial(range_bin_kernel, span=span, sin_c=sin_c, cos_c=cos_c),
        in_specs=[pl.BlockSpec(memory_space=pltpu.SMEM)] + [whole] * 6,
        out_specs=whole,
        out_shape=jax.ShapeDtypeStruct((span, 2 * P_SIZE), f32),
        scratch_shapes=[
            pltpu.VMEM((count + SLOTS + WIDE, 128), f32),
            pltpu.VMEM((span, 2 * P_SIZE), f32),
        ],
        name="range_binning",
    )(
        base.reshape(1),
        cells.reshape(count // 128, 128),
        bounce.reshape(count // 128, 128),
        positions.reshape(1, count),
        amplitude,
        cells.reshape(1, count),
        bounce.reshape(1, count),
    )


def complex_rows(c, s):
    return np.block([[c, s], [-s, c]])


def mid_tables(n_dev, order):
    side = np.arange(BIN_SIDE)
    t = np.arange(STOLT)
    eye = np.eye(GROUP)
    a = -2 * np.pi / STOLT * ((side[:, None] * t[None, :]) % STOLT)
    ta = complex_rows(np.cos(a), np.sin(a))[order]
    a = -2 * np.pi / F_LEN * (side[:, None] * t[None, :])
    wa = np.stack([np.tile(np.cos(a), (GROUP, 1)), np.tile(np.sin(a), (GROUP, 1))])
    a = -2 * np.pi / BIN_SIDE * ((side[:, None] * side[None, :]) % BIN_SIDE)
    c, s = np.kron(eye, np.cos(a)), np.kron(eye, np.sin(a))
    tb = complex_rows(c, s).T
    blk = np.arange(BLOCKS)
    a = 2 * np.pi / BLOCKS * ((blk[:, None] * blk[None, :]) % BLOCKS)
    c, s = np.kron(eye, np.cos(a)), np.kron(eye, np.sin(a))
    tc = complex_rows(c, s)
    a = 2 * np.pi / F_LEN * (t[:, None] * blk[None, :])
    wc = np.stack([np.tile(np.cos(a), (1, GROUP)), np.tile(np.sin(a), (1, GROUP))])
    a = 2 * np.pi / STOLT * ((t[:, None] * t[None, :]) % STOLT)
    td = complex_rows(np.cos(a), np.sin(a)).T / F_LEN
    td = td.reshape(2, n_dev, STOLT // n_dev, 2 * STOLT).transpose(1, 0, 2, 3)
    td = td.reshape(2 * STOLT, 2 * STOLT)
    return (
        np_split(ta),
        wa.astype(np.float32),
        np_split(tb),
        np_split(tc),
        wc.astype(np.float32),
        np_split(td),
    )


def mid_kernel(
    x, cos_p, sin_p, hot, kind, bank_hi, bank_lo, ta, wa, tb, tc, wc, td, out, xs, os, *, subs
):
    n = GROUP * BLOCKS
    step = pl.program_id(0)
    groups = x.shape[1]

    @pl.when(step == 0)
    def _():
        for g in range(groups):
            xs[g] = x[:, g, :]

    parts_hi, parts_lo = [], []
    for g in range(subs):
        lanes = slice(g * n, (g + 1) * n)
        y = dots(split(xs[step * subs + g]), (ta[0], ta[1]), ((0,), (0,)))
        yr, yi = y[:, :STOLT], y[:, STOLT:]
        y = jnp.concatenate([yr * wa[0] - yi * wa[1], yr * wa[1] + yi * wa[0]], 0)
        z = dots((tb[0], tb[1]), split(y), ((1,), (0,)))
        zr, zi = z[:n], z[n:]
        cp, sp = cos_p[lanes], sin_p[lanes]
        z = jnp.concatenate([zr * cp - zi * sp, zr * sp + zi * cp], 1)
        hi, lo = split(z)
        picked = jnp.dot(
            hot[g], jnp.concatenate([hi, lo], 1), preferred_element_type=f32
        ).astype(bf16)
        first, second = picked[:n], picked[n:]
        for c in range(2):
            for base, keep in ((0, parts_hi), (2 * STOLT, parts_lo)):
                cut = slice(base + c * STOLT, base + (c + 1) * STOLT)
                keep.append(jnp.concatenate([first[:, cut], second[:, cut]], 1))
    ghi = jnp.concatenate(parts_hi, 0)
    glo = jnp.concatenate(parts_lo, 0)
    kinds = kind[...].reshape(subs * 2 * n, 1)
    kinds = jnp.broadcast_to(kinds, (subs * 2 * n, STOLT))
    acc = jnp.zeros((subs * 2 * n, STOLT), f32)
    for k in range(0, bank_hi.shape[0], 2):
        khi = jnp.concatenate([bank_hi[k], bank_hi[k + 1]], 1)
        klo = jnp.concatenate([bank_lo[k], bank_lo[k + 1]], 1)
        r = dots((ghi, glo), (khi, klo), ((1,), (0,)))
        for half in range(2):
            acc = jnp.where(kinds == k + half, r[:, half * STOLT : (half + 1) * STOLT], acc)
    for g in range(subs):
        s = acc[g * 2 * n : (g + 1) * 2 * n]
        y = dots(split(s), (tc[0], tc[1]), ((0,), (0,)))
        yr, yi = y[:, :n], y[:, n:]
        y = jnp.concatenate([yr * wc[0] - yi * wc[1], yr * wc[1] + yi * wc[0]], 0)
        os[step * subs + g] = dots((td[0], td[1]), split(y), ((1,), (0,)))

    @pl.when(step == pl.num_programs(0) - 1)
    def _():
        for g in range(groups):
            out[:, g, :] = os[g]


def middle(x, cos_p, sin_p, hot, kind, bank_hi, bank_lo, tables):
    groups = x.shape[1]
    subs = min(4, groups)
    n = GROUP * BLOCKS
    whole = lambda a: pl.BlockSpec(a.shape, lambda i: (0,) * a.ndim)
    return pl.pallas_call(
        functools.partial(mid_kernel, subs=subs),
        grid=(groups // subs,),
        in_specs=[
            whole(x),
            pl.BlockSpec((subs * n, STOLT), lambda i: (i, 0)),
            pl.BlockSpec((subs * n, STOLT), lambda i: (i, 0)),
            pl.BlockSpec((subs, 2 * n, n), lambda i: (i, 0, 0)),
            pl.BlockSpec((subs, 2 * n, 1), lambda i: (i, 0, 0)),
            whole(bank_hi),
            whole(bank_lo),
        ]
        + [whole(t) for t in tables],
        out_specs=pl.BlockSpec((2 * STOLT, groups, n), lambda i: (0, 0, 0)),
        out_shape=jax.ShapeDtypeStruct((2 * STOLT, groups, n), f32),
        scratch_shapes=[
            pltpu.VMEM((groups, x.shape[0], n), f32),
            pltpu.VMEM((groups, 2 * STOLT, n), f32),
        ],
        name="middle",
    )(x, cos_p, sin_p, hot, kind, bank_hi, bank_lo, *tables)


def quarter_tables():
    q = P_SIZE // 4
    m = np.arange(q)
    fwd, inv = [], []
    for low in range(4):
        a = 2 * np.pi / P_SIZE * (((4 * m[:, None] + low) * m[None, :]) % P_SIZE)
        turn = a.reshape(-1, 2, q).transpose(1, 0, 2).reshape(q, q)
        fwd.append(np.concatenate([np.cos(turn), np.sin(turn)], 0))
        inv.append(np.concatenate([np.cos(a.T), np.sin(a.T)], 0) / P_SIZE)
    return np_split(np.stack(fwd)), np_split(np.stack(inv))


def swap_blocks(arrays):
    count = len(arrays)
    lanes = arrays[0].shape[-1]
    size = lanes // count
    block = lax.broadcasted_iota(jnp.int32, arrays[0].shape, 1) // size
    outs = []
    for b in range(count):
        acc = None
        for a in range(count):
            shift = (a - b) % count * size
            moved = pltpu.roll(arrays[a], shift, 1) if shift else arrays[a]
            acc = moved if acc is None else jnp.where(block == a, moved, acc)
        outs.append(acc)
    return outs


def core_kernel(
    partial, steps_in, kinds_in, bank, table, ta, wa, tb, tc, wc, td,
    out,
    peer, binned, spec, x, hot, kind, bank_hi, bank_lo, bank_f, os,
    bank_sem, pair_send, pair_recv, near_send, near_recv, far_send, far_recv,
    *, n_pulse, n_scat, subs, trig,
):
    n_dev = n_pulse * n_scat
    pulse = lax.axis_index("pulse")
    scat = lax.axis_index("scat")
    me = pulse * n_scat + scat
    half = binned.shape[0]
    lanes = 2 * half
    size = P_SIZE // 4
    n = GROUP * BLOCKS
    groups = os.shape[1]
    pieces = groups // subs
    moves = [(a, b) for a in range(n_pulse) for b in range(n_scat) if (a, b) != (0, 0)]
    moves.sort(key=lambda m: (-min(m[0], n_pulse - m[0]), m))

    def other(a, b):
        return lax.rem(pulse + a, n_pulse), lax.rem(scat + b, n_scat)

    fetch = pltpu.make_async_copy(bank, bank_f, bank_sem)
    fetch.start()
    barrier = pltpu.get_barrier_semaphore()
    for a, b in moves:
        p, c = other(a, b)
        pl.semaphore_signal(
            barrier, inc=1, device_id={"pulse": p, "scat": c}, device_id_type=MESH
        )

    block = lax.broadcasted_iota(jnp.int32, (n, STOLT), 0)
    lane = lax.broadcasted_iota(jnp.int32, (n, STOLT), 1)
    spot = lane.astype(f32)
    above = (block // BLOCKS * BLOCKS).astype(f32)
    flat = []
    for ref in (steps_in, kinds_in):
        flat.append(
            jnp.concatenate([ref[pl.ds(j, groups, stride=GROUP), :] for j in range(GROUP)], 1)
        )
    for g in range(groups):
        first = jnp.broadcast_to(flat[0][g : g + 1].astype(f32), (n, n)).T + above
        hot[g, :n] = jnp.where(first == spot, 1.0, 0.0).astype(bf16)
        hot[g, n:] = jnp.where(first + 1.0 == spot, 1.0, 0.0).astype(bf16)
        kind[g] = jnp.broadcast_to(flat[1][g : g + 1].astype(f32), (n, n)).T
    pl.semaphore_wait(barrier, n_dev - 1)

    away = 1 - scat
    pair = pltpu.make_async_remote_copy(
        src_ref=partial.at[pl.ds(pl.multiple_of(away * half, half), half), :],
        dst_ref=peer,
        send_sem=pair_send,
        recv_sem=pair_recv,
        device_id={"pulse": pulse, "scat": away},
        device_id_type=MESH,
    )
    pair.start()
    fetch.wait()
    for k in range(bank_f.shape[0]):
        hi, lo = split(bank_f[k])
        cut = slice(k % 2 * STOLT, (k % 2 + 1) * STOLT)
        bank_hi[k // 2, :, cut] = hi
        bank_lo[k // 2, :, cut] = lo
    pair.wait()
    binned[...] = partial[pl.ds(pl.multiple_of(scat * half, half), half), :] + peer[...]

    quarters = []
    for q in range(4):
        re = binned[:, q * size : (q + 1) * size]
        im = binned[:, P_SIZE + q * size : P_SIZE + (q + 1) * size]
        quarters.append((re, im))
    (r0, i0), (r1, i1), (r2, i2), (r3, i3) = quarters
    sr, si, dr, di = r0 + r2, i0 + i2, r0 - r2, i0 - i2
    tr, ti, er, ei = r1 + r3, i1 + i3, r1 - r3, i1 - i3
    mixed = (
        (sr + tr, si + ti),
        (dr + ei, di - er),
        (sr - tr, si - ti),
        (dr - ei, di + er),
    )
    low = lax.broadcasted_iota(jnp.int32, (size, lanes), 1) < half
    rows = []
    for k in range(4):
        u = jnp.concatenate(mixed[k], 0)
        g = dots((table[0, k], table[1, k]), split(u), ((1,), (1,)))
        turned = pltpu.roll(g[size:], half, 1)
        rows.append(g[:size] + jnp.where(low, turned, -turned))
    quads = 2 * half // BIN_SIDE
    unit = subs * quads
    for q, z in enumerate(swap_blocks(rows)):
        for h in range(subs):
            spec[pl.ds(q * subs + h, size // subs, stride=unit), :] = z[
                h * (size // subs) : (h + 1) * (size // subs)
            ]

    def piece(dev, i):
        return pl.ds(pl.multiple_of((dev * pieces + i) * unit, unit), unit)

    own = pl.ds(pl.multiple_of(me * unit, unit), unit)
    for i in range(pieces):
        for j, (a, b) in enumerate(moves):
            p, c = other(a, b)
            pltpu.make_async_remote_copy(
                src_ref=spec.at[piece(p * n_scat + c, i), :],
                dst_ref=x.at[i, own, :],
                send_sem=near_send.at[j],
                recv_sem=near_recv.at[i, me],
                device_id={"pulse": p, "scat": c},
                device_id_type=MESH,
            ).start()
    for i in range(pieces):
        x[i, own, :] = spec[piece(me, i), :]

    cols = (lane + (block % BLOCKS) * STOLT).astype(f32)
    kr = 4.0 * np.pi / 3e8 * (9.6e9 + (cols - F_LEN // 2) * (1.5e8 / F_LEN))

    def phase(g):
        row = me * (groups * GROUP) + g * GROUP + block // BLOCKS
        centered = lax.rem(row + P_SIZE // 2, P_SIZE) - P_SIZE // 2
        along = 2.0 * np.pi / (P_SIZE * SPACING) * centered.astype(f32)
        squared = along * along
        depth = NEAR + B // 2
        theta = -depth * squared / (jnp.sqrt(kr * kr - squared) + kr)
        whole = jnp.round(theta * (0.5 / np.pi))
        for part in turn_parts():
            theta = theta - whole * part
        r = theta * (0.5 / np.pi)
        u = r * r
        sn = r * horner(u, trig[0])
        cs = horner(u, trig[1])
        return 1.0 - 2.0 * sn * sn, 2.0 * sn * cs

    per = 2 * STOLT // n_dev

    def ranged(i, h):
        g = i * subs + h
        cp, sp = phase(g)
        y = dots(split(x[i, pl.ds(h, n_dev * quads, stride=subs), :]), (ta[0], ta[1]), ((0,), (0,)))
        yr, yi = y[:, :STOLT], y[:, STOLT:]
        y = jnp.concatenate([yr * wa[0] - yi * wa[1], yr * wa[1] + yi * wa[0]], 0)
        z = dots((tb[0], tb[1]), split(y), ((1,), (0,)))
        zr, zi = z[:n], z[n:]
        z = jnp.concatenate([zr * cp - zi * sp, zr * sp + zi * cp], 1)
        hi, lo = split(z)
        picked = jnp.dot(
            hot[g], jnp.concatenate([hi, lo], 1), preferred_element_type=f32
        ).astype(bf16)
        first, second = picked[:n], picked[n:]
        parts = [[], []]
        for c in range(2):
            for base, keep in zip((0, 2 * STOLT), parts):
                cut = slice(base + c * STOLT, base + (c + 1) * STOLT)
                keep.append(jnp.concatenate([first[:, cut], second[:, cut]], 1))
        ghi, glo = (jnp.concatenate(v, 0) for v in parts)
        kinds = jnp.concatenate([kind[g]] * 2, 0)
        acc = jnp.zeros((2 * n, STOLT), f32)
        for k in range(bank_hi.shape[0]):
            r = dots((ghi, glo), (bank_hi[k], bank_lo[k]), ((1,), (0,)))
            for v in range(2):
                acc = jnp.where(kinds == 2 * k + v, r[:, v * STOLT : (v + 1) * STOLT], acc)
        y = dots(split(acc), (tc[0], tc[1]), ((0,), (0,)))
        yr, yi = y[:, :n], y[:, n:]
        y = jnp.concatenate([yr * wc[0] - yi * wc[1], yr * wc[1] + yi * wc[0]], 0)
        z = dots((td[0], td[1]), split(y), ((1,), (0,)))
        os[:, g] = z.reshape(n_dev, per, n)
        for j, (a, b) in enumerate(moves):
            p, c = other(a, b)
            pltpu.make_async_remote_copy(
                src_ref=os.at[p * n_scat + c, g],
                dst_ref=out.at[me, g],
                send_sem=far_send.at[j],
                recv_sem=far_recv.at[me],
                device_id={"pulse": p, "scat": c},
                device_id_type=MESH,
            ).start()

    def step(i, carry):
        for a, b in moves:
            p, c = other(a, b)
            src = p * n_scat + c
            spot = pl.ds(pl.multiple_of(src * unit, unit), unit)
            pltpu.make_async_copy(
                x.at[i, spot, :], x.at[i, spot, :], near_recv.at[i, src]
            ).wait()
        for h in range(subs):
            ranged(i, h)
        return carry

    lax.fori_loop(0, pieces, step, 0)
    mine = pltpu.make_async_copy(os.at[me], out.at[me], bank_sem)
    mine.start()
    mine.wait()
    for j, (a, b) in enumerate(moves):
        p, c = other(a, b)
        src = p * n_scat + c
        all_of = spec.at[pl.ds(0, pieces * unit), :]
        pltpu.make_async_copy(all_of, all_of, near_send.at[j]).wait()
        pltpu.make_async_copy(os.at[src], os.at[src], far_send.at[j]).wait()
        pltpu.make_async_copy(out.at[src], out.at[src], far_recv.at[src]).wait()


def turn_parts():
    parts, rest = [], 2.0 * np.pi
    for bits in (10, 22, 60):
        scale = 2.0**bits
        part = float(np.float32(np.round(rest * scale) / scale))
        parts.append(part)
        rest -= part
    return parts


def core(partial, steps_in, kinds_in, bank, table, tables, n_pulse, n_scat):
    n_dev = n_pulse * n_scat
    rows = steps_in.shape[0]
    groups = rows // GROUP
    subs = 2
    n = GROUP * BLOCKS
    span, width = partial.shape
    half = span // n_scat
    quads = 2 * half // BIN_SIDE
    kernels = bank.shape[0]
    per = 2 * STOLT // n_dev
    vmem = pl.BlockSpec(memory_space=pltpu.VMEM)
    dma = pltpu.SemaphoreType.DMA
    return pl.pallas_call(
        functools.partial(
            core_kernel, n_pulse=n_pulse, n_scat=n_scat, subs=subs, trig=range_trig_coefs(5)
        ),
        in_specs=[vmem] * 3 + [pl.BlockSpec(memory_space=pl.ANY)] + [vmem] * (1 + len(tables)),
        out_specs=vmem,
        out_shape=jax.ShapeDtypeStruct((n_dev, groups, per, n), f32),
        scratch_shapes=[
            pltpu.VMEM((half, width), f32),
            pltpu.VMEM((half, width), f32),
            pltpu.VMEM((n_dev * groups * quads, n), f32),
            pltpu.VMEM((groups // subs, n_dev * subs * quads, n), f32),
            pltpu.VMEM((groups, 2 * n, n), bf16),
            pltpu.VMEM((groups, n, STOLT), f32),
            pltpu.VMEM((kernels // 2, 2 * STOLT, 2 * STOLT), bf16),
            pltpu.VMEM((kernels // 2, 2 * STOLT, 2 * STOLT), bf16),
            pltpu.VMEM(bank.shape, f32),
            pltpu.VMEM((n_dev, groups, per, n), f32),
            dma,
            dma,
            dma,
            dma((n_dev,)),
            dma((groups // subs, n_dev)),
            dma((n_dev,)),
            dma((n_dev,)),
        ],
        compiler_params=pltpu.CompilerParams(collective_id=0, has_side_effects=True),
        name="core",
    )(partial, steps_in, kinds_in, bank, table, *tables)


def image_kernel(x, table, out):
    devs, kh, per, lanes = x.shape
    per = per // 2
    size = P_SIZE // 4
    columns = [[] for _ in range(4)]
    for c in range(2):
        for h in range(per // 4):
            tiles = [x[:, :, c * per + 4 * h + j, :].reshape(devs * kh, lanes) for j in range(4)]
            for k, z in enumerate(swap_blocks(tiles)):
                columns[k].append(z)
    width = lanes * (per // 4)
    v = []
    for k in range(4):
        g = dots((table[0, k], table[1, k]), split(jnp.concatenate(columns[k], 1)), ((1,), (0,)))
        cos_g, sin_g = g[:size], g[size:]
        v.append((cos_g[:, :width] - sin_g[:, width:], cos_g[:, width:] + sin_g[:, :width]))
    (r0, i0), (r1, i1), (r2, i2), (r3, i3) = v
    sr, si, dr, di = r0 + r2, i0 + i2, r0 - r2, i0 - i2
    tr, ti, er, ei = r1 + r3, i1 + i3, r1 - r3, i1 - i3
    mixed = (
        (sr + tr, si + ti),
        (dr - ei, di + er),
        (sr - tr, si - ti),
        (dr + ei, di - er),
    )
    for q in range(4):
        for c in range(2):
            out[c, q * size : (q + 1) * size, :] = mixed[q][c]


def reference_phase(row_ids, cols):
    centered = (row_ids + P_SIZE // 2) % P_SIZE - P_SIZE // 2
    along_k = 2.0 * jnp.pi / (P_SIZE * SPACING) * centered.astype(f32)
    kr = 4.0 * jnp.pi / 3e8 * (9.6e9 + (cols.astype(f32) - F_LEN // 2) * (1.5e8 / F_LEN))
    squared = along_k * along_k
    depth = NEAR + B // 2
    return (
        -depth
        * squared[:, None]
        / (jnp.sqrt(kr[None, :] * kr[None, :] - squared[:, None]) + kr[None, :])
    )


def on_device(positions, amplitude, range_cells, bounce, stolt_block, kernel_choice, kernel_bank):
    n_pulse = lax.axis_size("pulse")
    n_scat = lax.axis_size("scat")
    n_dev = n_pulse * n_scat
    pulse_here = lax.axis_index("pulse")
    scat_here = lax.axis_index("scat")
    pulses = P_SIZE // n_pulse
    rows = P_SIZE // n_dev
    width = F_LEN // n_dev
    groups = rows // GROUP
    n = GROUP * BLOCKS
    bins_scat = B // n_scat
    bins_here = bins_scat // n_pulse

    per = STOLT // n_dev
    span = B // n_pulse
    packed = (
        span == 128
        and n_scat == 2
        and per % 4 == 0
        and groups % 8 == 0
        and positions.shape[0] % CHUNK == 0
    )
    if packed:
        forward, backward = (jnp.asarray(t) for t in quarter_tables())
        partial = range_binning(
            positions, amplitude, range_cells, bounce, pulse_here * span, span
        )
        local = bins_here // BIN_SIDE
        i, s, c, l = np.meshgrid(
            np.arange(n_pulse), np.arange(n_scat), np.arange(2), np.arange(local), indexing="ij"
        )
        order = (c * BIN_SIDE + (i * n_scat + s) * local + l).reshape(-1)
        tables = tuple(jnp.asarray(t) for t in mid_tables(n_dev, order))
        columns = core(
            partial, stolt_block, kernel_choice, kernel_bank, forward, tables, n_pulse, n_scat
        )
        return pl.pallas_call(
            image_kernel,
            out_shape=jax.ShapeDtypeStruct((2, P_SIZE, width), f32),
            name="image",
        )(columns, backward)

    ids = jnp.arange(GROUP, dtype=jnp.int32)[None, :, None] * BLOCKS
    first = stolt_block.reshape(groups, GROUP, BLOCKS) + ids
    pick = jnp.stack([first, first + 1], 1).reshape(groups, 2 * n, 1)
    hot = (pick == jnp.arange(n, dtype=jnp.int32)[None, None, :]).astype(bf16)
    kind = jnp.stack([kernel_choice.reshape(groups, n)] * 2, 1).reshape(groups, 2 * n, 1)
    bank_hi = lax.reduce_precision(kernel_bank, 8, 7)
    bank_lo = (kernel_bank - bank_hi).astype(bf16)
    bank_hi = bank_hi.astype(bf16)
    row_ids = (pulse_here * n_scat + scat_here) * rows + jnp.arange(rows, dtype=jnp.int32)
    theta = reference_phase(row_ids, jnp.arange(F_LEN, dtype=jnp.int32))
    theta = theta.reshape(rows * BLOCKS, STOLT)
    cos_p, sin_p = jnp.cos(theta), jnp.sin(theta)

    partial = binning(positions, amplitude, range_cells, bounce, pulse_here * pulses, pulses)
    partial = partial.reshape(n_scat, bins_scat, 2 * pulses)
    binned = lax.dynamic_index_in_dim(partial, scat_here, 0, keepdims=False)
    for shift in range(1, n_scat):
        other = lax.dynamic_index_in_dim(
            partial, (scat_here + shift) % n_scat, 0, keepdims=False
        )
        ring = [(i, (i + shift) % n_scat) for i in range(n_scat)]
        binned = binned + lax.ppermute(other, "scat", ring)
    turned = lax.all_to_all(
        binned.reshape(n_pulse, bins_here, 2 * pulses), "pulse", 0, 0, tiled=True
    )
    turned = turned.reshape(n_pulse, bins_here, 2, pulses).transpose(0, 3, 2, 1)
    turned = turned.reshape(P_SIZE, 2 * bins_here)
    k = np.arange(P_SIZE)
    angle = 2 * np.pi / P_SIZE * ((k[:, None] * k[None, :]) % P_SIZE)
    az = jnp.asarray(np.concatenate([np.cos(angle), np.sin(angle)], 0), f32)
    product = jnp.dot(az, turned, precision=HIGH, preferred_element_type=f32)
    pc, ps = product[:P_SIZE], product[P_SIZE:]
    spectrum = pc + jnp.concatenate([ps[:, bins_here:], -ps[:, :bins_here]], 1)
    az_rows = lax.all_to_all(
        spectrum.reshape(n_dev, rows, 2 * bins_here), ("pulse", "scat"), 0, 0, tiled=True
    )
    x = az_rows.reshape(n_pulse, n_scat, rows, 2, bins_here).transpose(3, 1, 0, 4, 2)
    x = x.reshape(2, BIN_SIDE, BIN_SIDE, rows).transpose(0, 1, 3, 2)
    x = x.reshape(2 * BIN_SIDE, groups, n)
    order = np.arange(2 * BIN_SIDE)

    tables = tuple(jnp.asarray(t) for t in mid_tables(n_dev, order))
    ranged = middle(x, cos_p, sin_p, hot, kind, bank_hi, bank_lo, tables)
    columns = lax.all_to_all(
        ranged.reshape(n_dev, 2 * per, rows * BLOCKS), ("pulse", "scat"), 0, 0, tiled=True
    )
    columns = columns.reshape(n_dev, 2, per, rows, BLOCKS).transpose(0, 3, 1, 2, 4)
    columns = columns.reshape(P_SIZE, 2 * width)
    final = jnp.dot(az, columns, precision=HIGH, preferred_element_type=f32)
    fc, fs = final[:P_SIZE], final[P_SIZE:]
    re = (fc[:, :width] - fs[:, width:]) / P_SIZE
    im = (fc[:, width:] + fs[:, :width]) / P_SIZE
    return jnp.stack([re, im])


def solution(mesh):
    placed = (
        P(("scene", "scat")),
        P(None, ("scene", "scat")),
        P(("scene", "scat")),
        P(("scene", "scat")),
        P(("pulse", "scat"), None),
        P(("pulse", "scat"), None),
        P(),
    )
    return jax.shard_map(
        on_device,
        mesh=mesh,
        in_specs=placed,
        out_specs=P(None, "scene", ("pulse", "scat")),
        check_vma=False,
    )
```

```python
import functools

import jax
import jax.numpy as jnp
import numpy as np
from jax import lax
from jax.experimental import pallas as pl
from jax.experimental.pallas import tpu as pltpu
from jax.sharding import PartitionSpec as P

P_SIZE = 512
F_LEN = 4096
B = 1024
SHIFT = 16
STOLT = 128
BLOCKS = 32
SPACING = 2.0
NEAR = 700000.0
BIN_SIDE = 32
GROUP = 4
CHUNK = 1024
SLOTS = 192
WIDE = 128
AHEAD = 1024
HIGH = lax.Precision.HIGH
MESH = pl.DeviceIdType.MESH
f32 = jnp.float32
bf16 = jnp.bfloat16


def trig_coefs():
    x = np.cos(np.pi * (np.arange(400) + 0.5) / 400) * 0.5
    u = x * x
    s = np.polynomial.chebyshev.Chebyshev.fit(u, np.sin(np.pi * x) / x, 5).convert(
        kind=np.polynomial.Polynomial
    )
    c = np.polynomial.chebyshev.Chebyshev.fit(u, np.cos(np.pi * x), 5).convert(
        kind=np.polynomial.Polynomial
    )
    return [float(v) for v in s.coef], [float(v) for v in c.coef]


def horner(u, coefs):
    acc = jnp.full_like(u, coefs[-1])
    for c in coefs[-2::-1]:
        acc = acc * u + c
    return acc


def split(x):
    hi = x.astype(bf16)
    lo = (x - hi.astype(f32)).astype(bf16)
    return hi, lo


def np_split(x):
    x = np.asarray(x, np.float64)
    hi = np.asarray(x, jnp.bfloat16)
    lo = np.asarray(x - hi.astype(np.float64), jnp.bfloat16)
    return np.stack([hi, lo])


def dots(a, b, dims):
    d = functools.partial(
        lax.dot_general, dimension_numbers=(dims, ((), ())), preferred_element_type=f32
    )
    return d(a[0], b[0]) + (d(a[0], b[1]) + d(a[1], b[0]))


def joined(hi, lo, axis):
    return jnp.concatenate([hi, hi, lo], axis)


def triple(x, axis):
    hi, lo = split(x)
    return jnp.concatenate([hi, lo, hi], axis)


def product(a, b, dims=((1,), (0,))):
    return lax.dot_general(a, b, (dims, ((), ())), preferred_element_type=f32)


def bin_kernel(pulse_base, pos, amp, tgt, bnc, out, acc, *, pulses, sin_c, cos_c):
    step = pl.program_id(0)
    width = pos.shape[1]

    @pl.when(step == 0)
    def _():
        acc[...] = jnp.zeros_like(acc)

    base = pulse_base[0]
    ids = base + lax.broadcasted_iota(jnp.int32, (pulses, width), 0)
    along = (ids.astype(f32) - P_SIZE // 2) * SPACING
    target = tgt[...] + SHIFT * bnc[...]
    slant = NEAR + target.astype(f32)
    offset = along - pos[...]
    square = offset * offset
    excess = square / (jnp.sqrt(slant * slant + square) + slant)
    halves = excess * -128.0
    whole = jnp.round(halves)
    r = halves - whole
    u = r * r
    odd = whole - 2.0 * jnp.floor(whole * 0.5)
    sign = 1.0 - 2.0 * odd
    sin_p = sign * r * horner(u, sin_c)
    cos_p = sign * horner(u, cos_c)
    flip = 1.0 - 2.0 * bnc[...].astype(f32)
    are = flip * amp[0:1]
    aim = flip * amp[1:2]
    re = are * cos_p - aim * sin_p
    im = are * sin_p + aim * cos_p
    steer = jnp.concatenate([re, im], 0)
    hi, lo = split(steer)
    rhs = jnp.concatenate([hi, lo], 0)
    bins = lax.broadcasted_iota(jnp.int32, (B, width), 0)
    hot = jnp.where(bins == target, 1.0, 0.0).astype(bf16)
    acc[...] += lax.dot_general(
        hot, rhs, (((1,), (1,)), ((), ())), preferred_element_type=f32
    )

    @pl.when(step == pl.num_programs(0) - 1)
    def _():
        out[...] = acc[:, : 2 * pulses] + acc[:, 2 * pulses :]


def binning(positions, amplitude, cells, bounce, pulse_base, pulses):
    count = positions.shape[0]
    width = min(2048, count)
    sin_c, cos_c = trig_coefs()
    row = lambda n: pl.BlockSpec((n, width), lambda i: (0, i))
    return pl.pallas_call(
        functools.partial(bin_kernel, pulses=pulses, sin_c=sin_c, cos_c=cos_c),
        grid=(count // width,),
        in_specs=[pl.BlockSpec(memory_space=pltpu.SMEM), row(1), row(2), row(1), row(1)],
        out_specs=pl.BlockSpec((B, 2 * pulses), lambda i: (0, 0)),
        out_shape=jax.ShapeDtypeStruct((B, 2 * pulses), f32),
        scratch_shapes=[pltpu.VMEM((B, 4 * pulses), f32)],
        name="binning",
    )(
        pulse_base.reshape(1),
        positions.reshape(1, count),
        amplitude,
        cells.reshape(1, count),
        bounce.reshape(1, count),
    )


def range_trig_coefs(degree):
    x = np.cos(np.pi * (np.arange(400) + 0.5) / 400) * 0.5
    u = x * x
    fit = lambda y: np.polynomial.chebyshev.Chebyshev.fit(u, y, degree).convert(
        kind=np.polynomial.Polynomial
    )
    return [float(v) for v in fit(np.sin(np.pi * x) / x).coef], [
        float(v) for v in fit(np.cos(np.pi * x)).coef
    ]


def split3(x):
    hi = x.astype(bf16).astype(f32)
    rest = x - hi
    mid = rest.astype(bf16).astype(f32)
    return hi, mid, rest - mid


def echoes(data, base, bins, trig):
    where, re_amp, im_amp, rel = (data[j : j + 1] for j in range(4))
    re2, im2 = 2.0 * re_amp, 2.0 * im_amp
    inverse = 0.5 / (rel + (base.astype(f32) + NEAR))
    gain = inverse * -64.0
    bend = inverse * (1.0 / 64.0)
    width = data.shape[1]
    rows = lax.broadcasted_iota(jnp.int32, (bins, width), 0).astype(f32)
    hot = jnp.where(rows == rel, 1.0, 0.0).astype(bf16)
    hot = jnp.concatenate([hot, hot], 1)
    for q in range(P_SIZE // 128):
        parts = [[], []]
        for p in range(0, 128, 16):
            ids = lax.broadcasted_iota(jnp.int32, (16, width), 0)
            along = (ids + (q * 128 + p - P_SIZE // 2)).astype(f32) * SPACING
            offset = along - where
            t = offset * offset * gain
            y = t * bend
            t = t * (1.0 + y * (1.0 + 2.0 * y))
            r = t - jnp.round(t)
            u = r * r
            sn = r * horner(u, trig[0])
            cs = horner(u, trig[1])
            re = re_amp - sn * (re2 * sn + im2 * cs)
            im = im_amp + sn * (re2 * cs - im2 * sn)
            for c, v in enumerate((re, im)):
                parts[c].append(jnp.concatenate(split(v), 1))
        for c in range(2):
            lanes = slice(c * P_SIZE + q * 128, c * P_SIZE + (q + 1) * 128)
            yield lanes, product(hot, jnp.concatenate(parts[c], 0), ((1,), (1,)))


def range_bin_kernel(
    base_ref, cells8, bounce8, pos, amp, cells, bnc, out, lead, buf, *, span, trig
):
    base = base_ref[0]
    rows = cells8.shape[0]
    chunks = rows // 8
    target = cells8[...] + SHIFT * bounce8[...] - base
    match = jnp.where((target >= 0) & (target < span), 1.0, 0.0)
    mb = match.astype(bf16)
    a = lax.broadcasted_iota(jnp.int32, (128, 128), 0)
    b = lax.broadcasted_iota(jnp.int32, (128, 128), 1)
    upto = jnp.where(a <= b, 1.0, 0.0).astype(bf16)
    count = jnp.dot(mb, upto, preferred_element_type=f32)
    total = jnp.dot(mb, jnp.ones((128, 128), bf16), preferred_element_type=f32)
    a = lax.broadcasted_iota(jnp.int32, (rows, rows), 0)
    b = lax.broadcasted_iota(jnp.int32, (rows, rows), 1)
    below = jnp.where((a // 8 == b // 8) & (b < a), 1.0, 0.0).astype(bf16)
    ahead = jnp.dot(below, total.astype(bf16), preferred_element_type=f32)
    rank = jnp.where(match > 0.0, count + ahead - 1.0, -1.0)
    counts = [
        jnp.sum(match[8 * c : 8 * c + 8]).astype(jnp.int32) for c in range(chunks)
    ]

    def values(c):
        lanes = slice(CHUNK * c, CHUNK * (c + 1))
        flip = 1.0 - 2.0 * bnc[:, lanes].astype(f32)
        rel = (cells[:, lanes] + SHIFT * bnc[:, lanes] - base).astype(f32)
        zero = jnp.zeros_like(rel)
        data = jnp.concatenate(
            [pos[:, lanes], amp[0:1, lanes] * flip, amp[1:2, lanes] * flip, rel] + [zero] * 4, 0
        )
        return jnp.concatenate(list(split3(data)) + [jnp.zeros_like(data)], 0).astype(bf16)

    def pick(c, first):
        slots = lax.broadcasted_iota(jnp.int32, (SLOTS, 128), 0).astype(f32) + first
        hot = jnp.concatenate(
            [jnp.where(rank[8 * c + j : 8 * c + j + 1] == slots, 1.0, 0.0) for j in range(8)], 1
        ).astype(bf16)
        return lax.dot_general(
            hot, values(c), (((1,), (1,)), ((), ())), preferred_element_type=f32
        )

    start = 0
    for c in range(chunks):
        buf[pl.ds(start, SLOTS), 0:32] = pick(c, 0.0)
        start = start + counts[c]
    most = functools.reduce(jnp.maximum, counts)

    @pl.when(most > SLOTS)
    def _():
        begin = 0
        for c in range(chunks):

            @pl.loop(0, (counts[c] + SLOTS - 1) // SLOTS)
            def _(i):
                first = (i * SLOTS).astype(f32)
                buf[pl.ds(begin + i * SLOTS, SLOTS), 0:32] = pick(c, first)

            begin = begin + counts[c]

    buf[pl.ds(start, AHEAD), :] = jnp.zeros((AHEAD, 128), f32)

    def data(first, width):
        cols = []
        for h in range(width // 128):
            t = buf[pl.ds(first + h * 128, 128), :].T
            cols.append(t[0:8] + t[8:16] + t[16:24])
        return jnp.concatenate(cols, 1)

    lead[...] = data(0, AHEAD)
    out[...] = jnp.zeros_like(out)

    @pl.loop(AHEAD // WIDE, (start + WIDE - 1) // WIDE)
    def _(i):
        for lanes, sums in echoes(data(i * WIDE, WIDE), base, span, trig):
            out[:, lanes] += sums


def range_binning(positions, amplitude, cells, bounce, base, span):
    count = positions.shape[0]
    whole = pl.BlockSpec(memory_space=pltpu.VMEM)
    return pl.pallas_call(
        functools.partial(range_bin_kernel, span=span, trig=range_trig_coefs(4)),
        in_specs=[pl.BlockSpec(memory_space=pltpu.SMEM)] + [whole] * 6,
        out_specs=(whole, whole),
        out_shape=(
            jax.ShapeDtypeStruct((span, 2 * P_SIZE), f32),
            jax.ShapeDtypeStruct((8, AHEAD), f32),
        ),
        scratch_shapes=[pltpu.VMEM((count + SLOTS + AHEAD, 128), f32)],
        name="range_binning",
    )(
        base.reshape(1),
        cells.reshape(count // 128, 128),
        bounce.reshape(count // 128, 128),
        positions.reshape(1, count),
        amplitude,
        cells.reshape(1, count),
        bounce.reshape(1, count),
    )


def complex_rows(c, s):
    return np.block([[c, s], [-s, c]])


def mid_factors(n_dev, order):
    side = np.arange(BIN_SIDE)
    t = np.arange(STOLT)
    eye = np.eye(GROUP)
    a = -2 * np.pi / STOLT * ((side[:, None] * t[None, :]) % STOLT)
    ta = complex_rows(np.cos(a), np.sin(a))[order]
    a = -2 * np.pi / F_LEN * (side[:, None] * t[None, :])
    wa = np.stack([np.tile(np.cos(a), (GROUP, 1)), np.tile(np.sin(a), (GROUP, 1))])
    a = -2 * np.pi / BIN_SIDE * ((side[:, None] * side[None, :]) % BIN_SIDE)
    c, s = np.kron(eye, np.cos(a)), np.kron(eye, np.sin(a))
    tb = complex_rows(c, s).T
    blk = np.arange(BLOCKS)
    a = 2 * np.pi / BLOCKS * ((blk[:, None] * blk[None, :]) % BLOCKS)
    c, s = np.kron(eye, np.cos(a)), np.kron(eye, np.sin(a))
    tc = complex_rows(c, s)
    a = 2 * np.pi / F_LEN * (t[:, None] * blk[None, :])
    wc = np.stack([np.tile(np.cos(a), (1, GROUP)), np.tile(np.sin(a), (1, GROUP))])
    a = 2 * np.pi / STOLT * ((t[:, None] * t[None, :]) % STOLT)
    td = complex_rows(np.cos(a), np.sin(a)).T / F_LEN
    td = td.reshape(2, n_dev, STOLT // n_dev, 2 * STOLT).transpose(1, 0, 2, 3)
    return ta, wa.astype(np.float32), tb, tc, wc.astype(np.float32), td


def mid_tables(n_dev, order):
    ta, wa, tb, tc, wc, td = mid_factors(n_dev, order)
    td = td.reshape(2 * STOLT, 2 * STOLT)
    return np_split(ta), wa, np_split(tb), np_split(tc), wc, np_split(td)


def core_tables(n_dev, order):
    ta, wa, tb, tc, wc, td = mid_factors(n_dev, order)
    td = td.reshape(n_dev, 2, -1, GROUP, 2 * STOLT).transpose(0, 2, 1, 3, 4)
    td = td.reshape(2 * STOLT, 2 * STOLT)
    forward, inverse = quarter_tables()
    return (
        np_split(forward),
        np_split(ta),
        wa,
        np_split(tb),
        np_split(tc),
        wc,
        np_split(td),
    ), np_split(inverse)


def mid_kernel(
    x, cos_p, sin_p, hot, kind, bank_hi, bank_lo, ta, wa, tb, tc, wc, td, out, xs, os, *, subs
):
    n = GROUP * BLOCKS
    step = pl.program_id(0)
    groups = x.shape[1]

    @pl.when(step == 0)
    def _():
        for g in range(groups):
            xs[g] = x[:, g, :]

    parts_hi, parts_lo = [], []
    for g in range(subs):
        lanes = slice(g * n, (g + 1) * n)
        y = dots(split(xs[step * subs + g]), (ta[0], ta[1]), ((0,), (0,)))
        yr, yi = y[:, :STOLT], y[:, STOLT:]
        y = jnp.concatenate([yr * wa[0] - yi * wa[1], yr * wa[1] + yi * wa[0]], 0)
        z = dots((tb[0], tb[1]), split(y), ((1,), (0,)))
        zr, zi = z[:n], z[n:]
        cp, sp = cos_p[lanes], sin_p[lanes]
        z = jnp.concatenate([zr * cp - zi * sp, zr * sp + zi * cp], 1)
        hi, lo = split(z)
        picked = jnp.dot(
            hot[g], jnp.concatenate([hi, lo], 1), preferred_element_type=f32
        ).astype(bf16)
        first, second = picked[:n], picked[n:]
        for c in range(2):
            for base, keep in ((0, parts_hi), (2 * STOLT, parts_lo)):
                cut = slice(base + c * STOLT, base + (c + 1) * STOLT)
                keep.append(jnp.concatenate([first[:, cut], second[:, cut]], 1))
    ghi = jnp.concatenate(parts_hi, 0)
    glo = jnp.concatenate(parts_lo, 0)
    kinds = kind[...].reshape(subs * 2 * n, 1)
    kinds = jnp.broadcast_to(kinds, (subs * 2 * n, STOLT))
    acc = jnp.zeros((subs * 2 * n, STOLT), f32)
    for k in range(0, bank_hi.shape[0], 2):
        khi = jnp.concatenate([bank_hi[k], bank_hi[k + 1]], 1)
        klo = jnp.concatenate([bank_lo[k], bank_lo[k + 1]], 1)
        r = dots((ghi, glo), (khi, klo), ((1,), (0,)))
        for half in range(2):
            acc = jnp.where(kinds == k + half, r[:, half * STOLT : (half + 1) * STOLT], acc)
    for g in range(subs):
        s = acc[g * 2 * n : (g + 1) * 2 * n]
        y = dots(split(s), (tc[0], tc[1]), ((0,), (0,)))
        yr, yi = y[:, :n], y[:, n:]
        y = jnp.concatenate([yr * wc[0] - yi * wc[1], yr * wc[1] + yi * wc[0]], 0)
        os[step * subs + g] = dots((td[0], td[1]), split(y), ((1,), (0,)))

    @pl.when(step == pl.num_programs(0) - 1)
    def _():
        for g in range(groups):
            out[:, g, :] = os[g]


def middle(x, cos_p, sin_p, hot, kind, bank_hi, bank_lo, tables):
    groups = x.shape[1]
    subs = min(4, groups)
    n = GROUP * BLOCKS
    whole = lambda a: pl.BlockSpec(a.shape, lambda i: (0,) * a.ndim)
    return pl.pallas_call(
        functools.partial(mid_kernel, subs=subs),
        grid=(groups // subs,),
        in_specs=[
            whole(x),
            pl.BlockSpec((subs * n, STOLT), lambda i: (i, 0)),
            pl.BlockSpec((subs * n, STOLT), lambda i: (i, 0)),
            pl.BlockSpec((subs, 2 * n, n), lambda i: (i, 0, 0)),
            pl.BlockSpec((subs, 2 * n, 1), lambda i: (i, 0, 0)),
            whole(bank_hi),
            whole(bank_lo),
        ]
        + [whole(t) for t in tables],
        out_specs=pl.BlockSpec((2 * STOLT, groups, n), lambda i: (0, 0, 0)),
        out_shape=jax.ShapeDtypeStruct((2 * STOLT, groups, n), f32),
        scratch_shapes=[
            pltpu.VMEM((groups, x.shape[0], n), f32),
            pltpu.VMEM((groups, 2 * STOLT, n), f32),
        ],
        name="middle",
    )(x, cos_p, sin_p, hot, kind, bank_hi, bank_lo, *tables)


def quarter_tables():
    q = P_SIZE // 4
    m = np.arange(q)
    fwd, inv = [], []
    for low in range(4):
        a = 2 * np.pi / P_SIZE * (((4 * m[:, None] + low) * m[None, :]) % P_SIZE)
        turn = a.reshape(-1, 2, q).transpose(1, 0, 2).reshape(q, q)
        fwd.append(np.concatenate([np.cos(turn), np.sin(turn)], 0))
        inv.append(np.concatenate([np.cos(a.T), np.sin(a.T)], 0) / P_SIZE)
    return np.stack(fwd), np.stack(inv)


def swap_blocks(arrays):
    count = len(arrays)
    lanes = arrays[0].shape[-1]
    size = lanes // count
    block = lax.broadcasted_iota(jnp.int32, arrays[0].shape, 1) // size
    outs = []
    for b in range(count):
        acc = None
        for a in range(count):
            shift = (a - b) % count * size
            moved = pltpu.roll(arrays[a], shift, 1) if shift else arrays[a]
            acc = moved if acc is None else jnp.where(block == a, moved, acc)
        outs.append(acc)
    return outs


def core_kernel(*refs, n_pulse, n_scat, subs, trig, trig_low):
    sources = refs[:12]
    out = refs[12]
    local = refs[13:25]
    lead, binned, steps_in, kinds_in, bank, table, ta, wa, tb, tc, wc, td = local
    peer, spec, x, hot, kind, banks, os = refs[25:32]
    (
        load, own_store, pair_send, pair_recv, near_send, near_recv, far_send, far_recv,
    ) = refs[32:]
    n_dev = n_pulse * n_scat
    pulse = lax.axis_index("pulse")
    scat = lax.axis_index("scat")
    me = pulse * n_scat + scat
    half = peer.shape[0]
    lanes = 2 * half
    size = P_SIZE // 4
    n = GROUP * BLOCKS
    groups = os.shape[1]
    pieces = groups // subs
    quads = lanes // BIN_SIDE
    unit = subs * quads
    per = os.shape[2]
    moves = [(a, b) for a in range(n_pulse) for b in range(n_scat) if (a, b) != (0, 0)]
    moves.sort(key=lambda m: (-min(m[0], n_pulse - m[0]), m))

    def other(a, b):
        return lax.rem(pulse + a, n_pulse), lax.rem(scat + b, n_scat)

    barrier = pltpu.get_barrier_semaphore()
    for a, b in moves:
        p, c = other(a, b)
        pl.semaphore_signal(
            barrier, inc=1, device_id={"pulse": p, "scat": c}, device_id_type=MESH
        )
    keep = pl.ds(pl.multiple_of(scat * half, half), half)
    give = pl.ds(pl.multiple_of((1 - scat) * half, half), half)
    loads = [
        pltpu.make_async_copy(src, dst, load.at[i])
        for i, (src, dst) in enumerate(zip(sources, local))
    ]
    for copy in loads:
        copy.start()
    loads[0].wait()
    loads[1].wait()
    for cut, sums in echoes(lead[...], pulse * 2 * half, 2 * half, trig_low):
        binned[:, cut] += sums
    pl.semaphore_wait(barrier, n_dev - 1)

    pair = pltpu.make_async_remote_copy(
        src_ref=binned.at[give, :],
        dst_ref=peer,
        send_sem=pair_send,
        recv_sem=pair_recv,
        device_id={"pulse": pulse, "scat": 1 - scat},
        device_id_type=MESH,
    )
    pair.start()
    loads[5].wait()
    pair.wait()

    quarters = []
    for q in range(4):
        pair_of = []
        for c in range(2):
            cut = slice(c * P_SIZE + q * size, c * P_SIZE + (q + 1) * size)
            pair_of.append(binned[keep, cut] + peer[:, cut])
        quarters.append(pair_of)
    (r0, i0), (r1, i1), (r2, i2), (r3, i3) = quarters
    sr, si, dr, di = r0 + r2, i0 + i2, r0 - r2, i0 - i2
    tr, ti, er, ei = r1 + r3, i1 + i3, r1 - r3, i1 - i3
    mixed = (
        (sr + tr, si + ti),
        (dr + ei, di - er),
        (sr - tr, si - ti),
        (dr - ei, di + er),
    )
    low = lax.broadcasted_iota(jnp.int32, (size, lanes), 1) < half
    rows = []
    for k in range(4):
        g = product(
            joined(table[0, k], table[1, k], 1),
            triple(jnp.concatenate(mixed[k], 0), 1),
            ((1,), (1,)),
        )
        turned = pltpu.roll(g[size:], half, 1)
        rows.append(g[:size] + jnp.where(low, turned, -turned))
    for q, z in enumerate(swap_blocks(rows)):
        for h in range(subs):
            spec[pl.ds(q * subs + h, size // subs, stride=unit), :] = z[
                h * (size // subs) : (h + 1) * (size // subs)
            ]

    def piece(dev, i):
        return pl.ds(pl.multiple_of((dev * pieces + i) * unit, unit), unit)

    own = pl.ds(pl.multiple_of(me * unit, unit), unit)
    for i in range(pieces):
        for j, (a, b) in enumerate(moves):
            p, c = other(a, b)
            pltpu.make_async_remote_copy(
                src_ref=spec.at[piece(p * n_scat + c, i), :],
                dst_ref=x.at[i, own, :],
                send_sem=near_send.at[j],
                recv_sem=near_recv.at[i, me],
                device_id={"pulse": p, "scat": c},
                device_id_type=MESH,
            ).start()
    for i in range(pieces):
        x[i, own, :] = spec[piece(me, i), :]

    for i in (2, 3, 4, 6, 7, 8, 9, 10, 11):
        loads[i].wait()
    block = lax.broadcasted_iota(jnp.int32, (n, STOLT), 0)
    lane = lax.broadcasted_iota(jnp.int32, (n, STOLT), 1)
    spot = lane.astype(f32)
    above = (block // BLOCKS * BLOCKS).astype(f32)
    flat = []
    for ref in (steps_in, kinds_in):
        flat.append(
            jnp.concatenate([ref[pl.ds(j, groups, stride=GROUP), :] for j in range(GROUP)], 1)
        )
    for g in range(groups):
        first = jnp.broadcast_to(flat[0][g : g + 1].astype(f32), (n, n)).T + above
        hot[g, :n] = jnp.where(first == spot, 1.0, 0.0).astype(bf16)
        hot[g, n:] = jnp.where(first + 1.0 == spot, 1.0, 0.0).astype(bf16)
        kind[g] = jnp.broadcast_to(flat[1][g : g + 1].astype(f32), (n, n)).T
    for k in range(bank.shape[0]):
        hi, lo = split(bank[k])
        cut = slice(k % 2 * STOLT, (k % 2 + 1) * STOLT)
        banks[k // 2, :, cut] = jnp.concatenate([hi, hi, lo], 0)

    cols = (lane + (block % BLOCKS) * STOLT).astype(f32)
    kr = 4.0 * np.pi / 3e8 * (9.6e9 + (cols - F_LEN // 2) * (1.5e8 / F_LEN))

    def phase(g):
        row = me * (groups * GROUP) + g * GROUP + block // BLOCKS
        centered = lax.rem(row + P_SIZE // 2, P_SIZE) - P_SIZE // 2
        along = 2.0 * np.pi / (P_SIZE * SPACING) * centered.astype(f32)
        squared = along * along
        depth = NEAR + B // 2
        theta = -depth * squared / (jnp.sqrt(kr * kr - squared) + kr)
        whole = jnp.round(theta * (0.5 / np.pi))
        for part in turn_parts():
            theta = theta - whole * part
        r = theta * (0.5 / np.pi)
        u = r * r
        sn = r * horner(u, trig[0])
        cs = horner(u, trig[1])
        return 1.0 - 2.0 * sn * sn, 2.0 * sn * cs

    def ranged(i, h):
        g = i * subs + h
        cp, sp = phase(g)
        rows_in = x[i, pl.ds(h, n_dev * quads, stride=subs), :]
        y = product(triple(rows_in, 0), joined(ta[0], ta[1], 0), ((0,), (0,)))
        yr, yi = y[:, :STOLT], y[:, STOLT:]
        y = jnp.concatenate([yr * wa[0] - yi * wa[1], yr * wa[1] + yi * wa[0]], 0)
        z = product(joined(tb[0], tb[1], 1), triple(y, 0))
        zr, zi = z[:n], z[n:]
        z = jnp.concatenate([zr * cp - zi * sp, zr * sp + zi * cp], 1)
        picked = product(hot[g], jnp.concatenate(split(z), 1)).astype(bf16)
        first, second = picked[:n], picked[n:]
        parts = []
        for base in (0, 2 * STOLT):
            cuts = [slice(base + c * STOLT, base + (c + 1) * STOLT) for c in range(2)]
            parts.append(
                jnp.concatenate(
                    [jnp.concatenate([first[:, v], second[:, v]], 1) for v in cuts], 0
                )
            )
        ghi, glo = parts
        windows = jnp.concatenate([ghi, glo, ghi], 1)
        kinds = jnp.concatenate([kind[g]] * 2, 0)
        acc = jnp.zeros((2 * n, STOLT), f32)
        for k in range(banks.shape[0]):
            r = product(windows, banks[k])
            for v in range(2):
                acc = jnp.where(kinds == 2 * k + v, r[:, v * STOLT : (v + 1) * STOLT], acc)
        y = product(triple(acc, 0), joined(tc[0], tc[1], 0), ((0,), (0,)))
        yr, yi = y[:, :n], y[:, n:]
        y = jnp.concatenate([yr * wc[0] - yi * wc[1], yr * wc[1] + yi * wc[0]], 0)
        z = product(joined(td[0], td[1], 1), triple(y, 0))
        os[:, g] = z.reshape(n_dev, per, n)
        for j, (a, b) in enumerate(moves):
            p, c = other(a, b)
            pltpu.make_async_remote_copy(
                src_ref=os.at[p * n_scat + c, g],
                dst_ref=out.at[me, g],
                send_sem=far_send.at[j],
                recv_sem=far_recv.at[me],
                device_id={"pulse": p, "scat": c},
                device_id_type=MESH,
            ).start()

    def step(i, carry):
        for a, b in moves:
            p, c = other(a, b)
            src = p * n_scat + c
            here = pl.ds(pl.multiple_of(src * unit, unit), unit)
            pltpu.make_async_copy(
                x.at[i, here, :], x.at[i, here, :], near_recv.at[i, src]
            ).wait()
        for h in range(subs):
            ranged(i, h)
        return carry

    lax.fori_loop(0, pieces, step, 0)
    mine = pltpu.make_async_copy(os.at[me], out.at[me], own_store)
    mine.start()
    mine.wait()
    for j, (a, b) in enumerate(moves):
        p, c = other(a, b)
        src = p * n_scat + c
        all_of = spec.at[pl.ds(0, pieces * unit), :]
        pltpu.make_async_copy(all_of, all_of, near_send.at[j]).wait()
        pltpu.make_async_copy(os.at[src], os.at[src], far_send.at[j]).wait()
        pltpu.make_async_copy(out.at[src], out.at[src], far_recv.at[src]).wait()


def turn_parts():
    parts, rest = [], 2.0 * np.pi
    for bits in (10, 22, 60):
        scale = 2.0**bits
        part = float(np.float32(np.round(rest * scale) / scale))
        parts.append(part)
        rest -= part
    return parts


def core(partial, lead, steps_in, kinds_in, bank, tables, n_pulse, n_scat):
    n_dev = n_pulse * n_scat
    groups = steps_in.shape[0] // GROUP
    subs = 2
    n = GROUP * BLOCKS
    span, width = partial.shape
    half = span // n_scat
    quads = 2 * half // BIN_SIDE
    kernels = bank.shape[0]
    per = 2 * STOLT // n_dev
    sources = (lead, partial, steps_in, kinds_in, bank, *tables)
    hbm = pl.BlockSpec(memory_space=pl.ANY)
    dma = pltpu.SemaphoreType.DMA
    return pl.pallas_call(
        functools.partial(
            core_kernel,
            n_pulse=n_pulse,
            n_scat=n_scat,
            subs=subs,
            trig=range_trig_coefs(5),
            trig_low=range_trig_coefs(4),
        ),
        in_specs=[hbm] * len(sources),
        out_specs=hbm,
        out_shape=jax.ShapeDtypeStruct((n_dev, groups, per, n), f32),
        scratch_shapes=[pltpu.VMEM(a.shape, a.dtype) for a in sources]
        + [
            pltpu.VMEM((half, width), f32),
            pltpu.VMEM((n_dev * groups * quads, n), f32),
            pltpu.VMEM((groups // subs, n_dev * subs * quads, n), f32),
            pltpu.VMEM((groups, 2 * n, n), bf16),
            pltpu.VMEM((groups, n, STOLT), f32),
            pltpu.VMEM((kernels // 2, 6 * STOLT, 2 * STOLT), bf16),
            pltpu.VMEM((n_dev, groups, per, n), f32),
            dma((len(sources),)),
            dma,
            dma,
            dma,
            dma((n_dev,)),
            dma((groups // subs, n_dev)),
            dma((n_dev,)),
            dma((n_dev,)),
        ],
        compiler_params=pltpu.CompilerParams(collective_id=0, has_side_effects=True),
        name="core",
    )(*sources)


def image_kernel(x, table, out):
    devs, kh, _, lanes = x.shape
    size = P_SIZE // 4
    columns = [[] for _ in range(4)]
    for c in range(2):
        tiles = [x[:, :, c * GROUP + j, :].reshape(devs * kh, lanes) for j in range(4)]
        for k, z in enumerate(swap_blocks(tiles)):
            columns[k].append(z)
    v = []
    for k in range(4):
        g = product(
            joined(table[0, k], table[1, k], 1), triple(jnp.concatenate(columns[k], 1), 0)
        )
        cos_g, sin_g = g[:size], g[size:]
        v.append((cos_g[:, :lanes] - sin_g[:, lanes:], cos_g[:, lanes:] + sin_g[:, :lanes]))
    (r0, i0), (r1, i1), (r2, i2), (r3, i3) = v
    sr, si, dr, di = r0 + r2, i0 + i2, r0 - r2, i0 - i2
    tr, ti, er, ei = r1 + r3, i1 + i3, r1 - r3, i1 - i3
    mixed = (
        (sr + tr, si + ti),
        (dr - ei, di + er),
        (sr - tr, si - ti),
        (dr + ei, di - er),
    )
    for q in range(4):
        for c in range(2):
            out[c, q * size : (q + 1) * size, :] = mixed[q][c]


def reference_phase(row_ids, cols):
    centered = (row_ids + P_SIZE // 2) % P_SIZE - P_SIZE // 2
    along_k = 2.0 * jnp.pi / (P_SIZE * SPACING) * centered.astype(f32)
    kr = 4.0 * jnp.pi / 3e8 * (9.6e9 + (cols.astype(f32) - F_LEN // 2) * (1.5e8 / F_LEN))
    squared = along_k * along_k
    depth = NEAR + B // 2
    return (
        -depth
        * squared[:, None]
        / (jnp.sqrt(kr[None, :] * kr[None, :] - squared[:, None]) + kr[None, :])
    )


def on_device(positions, amplitude, range_cells, bounce, stolt_block, kernel_choice, kernel_bank):
    n_pulse = lax.axis_size("pulse")
    n_scat = lax.axis_size("scat")
    n_dev = n_pulse * n_scat
    pulse_here = lax.axis_index("pulse")
    scat_here = lax.axis_index("scat")
    pulses = P_SIZE // n_pulse
    rows = P_SIZE // n_dev
    width = F_LEN // n_dev
    groups = rows // GROUP
    n = GROUP * BLOCKS
    bins_scat = B // n_scat
    bins_here = bins_scat // n_pulse

    per = STOLT // n_dev
    span = B // n_pulse
    packed = (
        span == 128
        and n_scat == 2
        and per % 4 == 0
        and groups % 8 == 0
        and positions.shape[0] % CHUNK == 0
    )
    if packed:
        partial, lead = range_binning(
            positions, amplitude, range_cells, bounce, pulse_here * span, span
        )
        local = bins_here // BIN_SIDE
        i, s, c, l = np.meshgrid(
            np.arange(n_pulse), np.arange(n_scat), np.arange(2), np.arange(local), indexing="ij"
        )
        order = (c * BIN_SIDE + (i * n_scat + s) * local + l).reshape(-1)
        tables, backward = core_tables(n_dev, order)
        tables = tuple(jnp.asarray(t) for t in tables)
        columns = core(
            partial, lead, stolt_block, kernel_choice, kernel_bank, tables, n_pulse, n_scat
        )
        block = (n_dev, groups, 2 * GROUP, n)
        return pl.pallas_call(
            image_kernel,
            grid=(per // GROUP,),
            in_specs=[
                pl.BlockSpec(block, lambda h: (0, 0, h, 0)),
                pl.BlockSpec(backward.shape, lambda h: (0, 0, 0, 0)),
            ],
            out_specs=pl.BlockSpec((2, P_SIZE, n), lambda h: (0, 0, h)),
            out_shape=jax.ShapeDtypeStruct((2, P_SIZE, width), f32),
            name="image",
        )(columns, jnp.asarray(backward))

    ids = jnp.arange(GROUP, dtype=jnp.int32)[None, :, None] * BLOCKS
    first = stolt_block.reshape(groups, GROUP, BLOCKS) + ids
    pick = jnp.stack([first, first + 1], 1).reshape(groups, 2 * n, 1)
    hot = (pick == jnp.arange(n, dtype=jnp.int32)[None, None, :]).astype(bf16)
    kind = jnp.stack([kernel_choice.reshape(groups, n)] * 2, 1).reshape(groups, 2 * n, 1)
    bank_hi = lax.reduce_precision(kernel_bank, 8, 7)
    bank_lo = (kernel_bank - bank_hi).astype(bf16)
    bank_hi = bank_hi.astype(bf16)
    row_ids = (pulse_here * n_scat + scat_here) * rows + jnp.arange(rows, dtype=jnp.int32)
    theta = reference_phase(row_ids, jnp.arange(F_LEN, dtype=jnp.int32))
    theta = theta.reshape(rows * BLOCKS, STOLT)
    cos_p, sin_p = jnp.cos(theta), jnp.sin(theta)

    partial = binning(positions, amplitude, range_cells, bounce, pulse_here * pulses, pulses)
    partial = partial.reshape(n_scat, bins_scat, 2 * pulses)
    binned = lax.dynamic_index_in_dim(partial, scat_here, 0, keepdims=False)
    for shift in range(1, n_scat):
        other = lax.dynamic_index_in_dim(
            partial, (scat_here + shift) % n_scat, 0, keepdims=False
        )
        ring = [(i, (i + shift) % n_scat) for i in range(n_scat)]
        binned = binned + lax.ppermute(other, "scat", ring)
    turned = lax.all_to_all(
        binned.reshape(n_pulse, bins_here, 2 * pulses), "pulse", 0, 0, tiled=True
    )
    turned = turned.reshape(n_pulse, bins_here, 2, pulses).transpose(0, 3, 2, 1)
    turned = turned.reshape(P_SIZE, 2 * bins_here)
    k = np.arange(P_SIZE)
    angle = 2 * np.pi / P_SIZE * ((k[:, None] * k[None, :]) % P_SIZE)
    az = jnp.asarray(np.concatenate([np.cos(angle), np.sin(angle)], 0), f32)
    product = jnp.dot(az, turned, precision=HIGH, preferred_element_type=f32)
    pc, ps = product[:P_SIZE], product[P_SIZE:]
    spectrum = pc + jnp.concatenate([ps[:, bins_here:], -ps[:, :bins_here]], 1)
    az_rows = lax.all_to_all(
        spectrum.reshape(n_dev, rows, 2 * bins_here), ("pulse", "scat"), 0, 0, tiled=True
    )
    x = az_rows.reshape(n_pulse, n_scat, rows, 2, bins_here).transpose(3, 1, 0, 4, 2)
    x = x.reshape(2, BIN_SIDE, BIN_SIDE, rows).transpose(0, 1, 3, 2)
    x = x.reshape(2 * BIN_SIDE, groups, n)
    order = np.arange(2 * BIN_SIDE)

    tables = tuple(jnp.asarray(t) for t in mid_tables(n_dev, order))
    ranged = middle(x, cos_p, sin_p, hot, kind, bank_hi, bank_lo, tables)
    columns = lax.all_to_all(
        ranged.reshape(n_dev, 2 * per, rows * BLOCKS), ("pulse", "scat"), 0, 0, tiled=True
    )
    columns = columns.reshape(n_dev, 2, per, rows, BLOCKS).transpose(0, 3, 1, 2, 4)
    columns = columns.reshape(P_SIZE, 2 * width)
    final = jnp.dot(az, columns, precision=HIGH, preferred_element_type=f32)
    fc, fs = final[:P_SIZE], final[P_SIZE:]
    re = (fc[:, :width] - fs[:, width:]) / P_SIZE
    im = (fc[:, width:] + fs[:, :width]) / P_SIZE
    return jnp.stack([re, im])


def solution(mesh):
    placed = (
        P(("scene", "scat")),
        P(None, ("scene", "scat")),
        P(("scene", "scat")),
        P(("scene", "scat")),
        P(("pulse", "scat"), None),
        P(("pulse", "scat"), None),
        P(),
    )
    return jax.shard_map(
        on_device,
        mesh=mesh,
        in_specs=placed,
        out_specs=P(None, "scene", ("pulse", "scat")),
        check_vma=False,
    )
```

```python
import functools

import jax
import jax.numpy as jnp
import numpy as np
from jax import lax
from jax.experimental import pallas as pl
from jax.experimental.pallas import tpu as pltpu
from jax.sharding import PartitionSpec as P

P_SIZE = 512
F_LEN = 4096
B = 1024
SHIFT = 16
STOLT = 128
BLOCKS = 32
SPACING = 2.0
NEAR = 700000.0
BIN_SIDE = 32
GROUP = 4
CHUNK = 1024
SLOTS = 192
WIDE = 128
AHEAD = 1024
HIGH = lax.Precision.HIGH
MESH = pl.DeviceIdType.MESH
IN_HBM = pl.BlockSpec(memory_space=pltpu.HBM)
IN_VMEM = pl.BlockSpec(memory_space=pltpu.VMEM)
f32 = jnp.float32
bf16 = jnp.bfloat16


def trig_coefs():
    x = np.cos(np.pi * (np.arange(400) + 0.5) / 400) * 0.5
    u = x * x
    s = np.polynomial.chebyshev.Chebyshev.fit(u, np.sin(np.pi * x) / x, 5).convert(
        kind=np.polynomial.Polynomial
    )
    c = np.polynomial.chebyshev.Chebyshev.fit(u, np.cos(np.pi * x), 5).convert(
        kind=np.polynomial.Polynomial
    )
    return [float(v) for v in s.coef], [float(v) for v in c.coef]


def horner(u, coefs):
    acc = jnp.full_like(u, coefs[-1])
    for c in coefs[-2::-1]:
        acc = acc * u + c
    return acc


def split(x):
    hi = x.astype(bf16)
    lo = (x - hi.astype(f32)).astype(bf16)
    return hi, lo


def np_split(x):
    x = np.asarray(x, np.float64)
    hi = np.asarray(x, jnp.bfloat16)
    lo = np.asarray(x - hi.astype(np.float64), jnp.bfloat16)
    return np.stack([hi, lo])


def dots(a, b, dims):
    d = functools.partial(
        lax.dot_general, dimension_numbers=(dims, ((), ())), preferred_element_type=f32
    )
    return d(a[0], b[0]) + (d(a[0], b[1]) + d(a[1], b[0]))


def in_hbm(arrays):
    return [pltpu.with_memory_space_constraint(a, pltpu.HBM) for a in arrays]


def joined(hi, lo, axis):
    return jnp.concatenate([hi, hi, lo], axis)


def triple(x, axis):
    hi, lo = split(x)
    return jnp.concatenate([hi, lo, hi], axis)


def product(a, b, dims=((1,), (0,))):
    return lax.dot_general(a, b, (dims, ((), ())), preferred_element_type=f32)


def bin_kernel(pulse_base, pos, amp, tgt, bnc, out, acc, *, pulses, sin_c, cos_c):
    step = pl.program_id(0)
    width = pos.shape[1]

    @pl.when(step == 0)
    def _():
        acc[...] = jnp.zeros_like(acc)

    base = pulse_base[0]
    ids = base + lax.broadcasted_iota(jnp.int32, (pulses, width), 0)
    along = (ids.astype(f32) - P_SIZE // 2) * SPACING
    target = tgt[...] + SHIFT * bnc[...]
    slant = NEAR + target.astype(f32)
    offset = along - pos[...]
    square = offset * offset
    excess = square / (jnp.sqrt(slant * slant + square) + slant)
    halves = excess * -128.0
    whole = jnp.round(halves)
    r = halves - whole
    u = r * r
    odd = whole - 2.0 * jnp.floor(whole * 0.5)
    sign = 1.0 - 2.0 * odd
    sin_p = sign * r * horner(u, sin_c)
    cos_p = sign * horner(u, cos_c)
    flip = 1.0 - 2.0 * bnc[...].astype(f32)
    are = flip * amp[0:1]
    aim = flip * amp[1:2]
    re = are * cos_p - aim * sin_p
    im = are * sin_p + aim * cos_p
    steer = jnp.concatenate([re, im], 0)
    hi, lo = split(steer)
    rhs = jnp.concatenate([hi, lo], 0)
    bins = lax.broadcasted_iota(jnp.int32, (B, width), 0)
    hot = jnp.where(bins == target, 1.0, 0.0).astype(bf16)
    acc[...] += lax.dot_general(
        hot, rhs, (((1,), (1,)), ((), ())), preferred_element_type=f32
    )

    @pl.when(step == pl.num_programs(0) - 1)
    def _():
        out[...] = acc[:, : 2 * pulses] + acc[:, 2 * pulses :]


def binning(positions, amplitude, cells, bounce, pulse_base, pulses):
    count = positions.shape[0]
    width = min(2048, count)
    sin_c, cos_c = trig_coefs()
    row = lambda n: pl.BlockSpec((n, width), lambda i: (0, i))
    return pl.pallas_call(
        functools.partial(bin_kernel, pulses=pulses, sin_c=sin_c, cos_c=cos_c),
        grid=(count // width,),
        in_specs=[pl.BlockSpec(memory_space=pltpu.SMEM), row(1), row(2), row(1), row(1)],
        out_specs=pl.BlockSpec((B, 2 * pulses), lambda i: (0, 0)),
        out_shape=jax.ShapeDtypeStruct((B, 2 * pulses), f32),
        scratch_shapes=[pltpu.VMEM((B, 4 * pulses), f32)],
        name="binning",
    )(
        pulse_base.reshape(1),
        positions.reshape(1, count),
        amplitude,
        cells.reshape(1, count),
        bounce.reshape(1, count),
    )


def range_trig_coefs(degree):
    x = np.cos(np.pi * (np.arange(400) + 0.5) / 400) * 0.5
    u = x * x
    fit = lambda y: np.polynomial.chebyshev.Chebyshev.fit(u, y, degree).convert(
        kind=np.polynomial.Polynomial
    )
    return [float(v) for v in fit(np.sin(np.pi * x) / x).coef], [
        float(v) for v in fit(np.cos(np.pi * x)).coef
    ]


def split3(x):
    hi = x.astype(bf16).astype(f32)
    rest = x - hi
    mid = rest.astype(bf16).astype(f32)
    return hi, mid, rest - mid


def echoes(data, base, bins, trig):
    where, re_amp, im_amp, rel = (data[j : j + 1] for j in range(4))
    re2, im2 = 2.0 * re_amp, 2.0 * im_amp
    inverse = 0.5 / (rel + (base.astype(f32) + NEAR))
    gain = inverse * -64.0
    bend = inverse * (1.0 / 64.0)
    width = data.shape[1]
    rows = lax.broadcasted_iota(jnp.int32, (bins, width), 0).astype(f32)
    hot = jnp.where(rows == rel, 1.0, 0.0).astype(bf16)
    hot = jnp.concatenate([hot, hot], 1)
    for q in range(P_SIZE // 128):
        parts = [[], []]
        for p in range(0, 128, 16):
            ids = lax.broadcasted_iota(jnp.int32, (16, width), 0)
            along = (ids + (q * 128 + p - P_SIZE // 2)).astype(f32) * SPACING
            offset = along - where
            t = offset * offset * gain
            y = t * bend
            t = t * (1.0 + y * (1.0 + 2.0 * y))
            r = t - jnp.round(t)
            u = r * r
            sn = r * horner(u, trig[0])
            cs = horner(u, trig[1])
            re = re_amp - sn * (re2 * sn + im2 * cs)
            im = im_amp + sn * (re2 * cs - im2 * sn)
            for c, v in enumerate((re, im)):
                parts[c].append(jnp.concatenate(split(v), 1))
        for c in range(2):
            lanes = slice(c * P_SIZE + q * 128, c * P_SIZE + (q + 1) * 128)
            yield lanes, product(hot, jnp.concatenate(parts[c], 0), ((1,), (1,)))


def range_bin_kernel(base_ref, *refs, span, trig):
    out, lead = refs[6:8]
    buf, load = refs[14:]
    cells8, bounce8, pos, amp, cells, bnc = refs[8:14]
    loads = [
        pltpu.make_async_copy(src, dst, load.at[i])
        for i, (src, dst) in enumerate(zip(refs[:6], refs[8:14]))
    ]
    for copy in loads:
        copy.start()
    for copy in loads:
        copy.wait()
    base = base_ref[0]
    rows = cells8.shape[0]
    chunks = rows // 8
    target = cells8[...] + SHIFT * bounce8[...] - base
    match = jnp.where((target >= 0) & (target < span), 1.0, 0.0)
    mb = match.astype(bf16)
    a = lax.broadcasted_iota(jnp.int32, (128, 128), 0)
    b = lax.broadcasted_iota(jnp.int32, (128, 128), 1)
    upto = jnp.where(a <= b, 1.0, 0.0).astype(bf16)
    count = jnp.dot(mb, upto, preferred_element_type=f32)
    total = jnp.dot(mb, jnp.ones((128, 128), bf16), preferred_element_type=f32)
    a = lax.broadcasted_iota(jnp.int32, (rows, rows), 0)
    b = lax.broadcasted_iota(jnp.int32, (rows, rows), 1)
    below = jnp.where((a // 8 == b // 8) & (b < a), 1.0, 0.0).astype(bf16)
    ahead = jnp.dot(below, total.astype(bf16), preferred_element_type=f32)
    rank = jnp.where(match > 0.0, count + ahead - 1.0, -1.0)
    counts = [
        jnp.sum(match[8 * c : 8 * c + 8]).astype(jnp.int32) for c in range(chunks)
    ]

    def values(c):
        lanes = slice(CHUNK * c, CHUNK * (c + 1))
        flip = 1.0 - 2.0 * bnc[:, lanes].astype(f32)
        rel = (cells[:, lanes] + SHIFT * bnc[:, lanes] - base).astype(f32)
        zero = jnp.zeros_like(rel)
        data = jnp.concatenate(
            [pos[:, lanes], amp[0:1, lanes] * flip, amp[1:2, lanes] * flip, rel] + [zero] * 4, 0
        )
        return jnp.concatenate(list(split3(data)) + [jnp.zeros_like(data)], 0).astype(bf16)

    def pick(c, first):
        slots = lax.broadcasted_iota(jnp.int32, (SLOTS, 128), 0).astype(f32) + first
        hot = jnp.concatenate(
            [jnp.where(rank[8 * c + j : 8 * c + j + 1] == slots, 1.0, 0.0) for j in range(8)], 1
        ).astype(bf16)
        return lax.dot_general(
            hot, values(c), (((1,), (1,)), ((), ())), preferred_element_type=f32
        )

    start = 0
    for c in range(chunks):
        buf[pl.ds(start, SLOTS), 0:32] = pick(c, 0.0)
        start = start + counts[c]
    most = functools.reduce(jnp.maximum, counts)

    @pl.when(most > SLOTS)
    def _():
        begin = 0
        for c in range(chunks):

            @pl.loop(0, (counts[c] + SLOTS - 1) // SLOTS)
            def _(i):
                first = (i * SLOTS).astype(f32)
                buf[pl.ds(begin + i * SLOTS, SLOTS), 0:32] = pick(c, first)

            begin = begin + counts[c]

    buf[pl.ds(start, AHEAD), :] = jnp.zeros((AHEAD, 128), f32)

    def data(first, width):
        cols = []
        for h in range(width // 128):
            t = buf[pl.ds(first + h * 128, 128), :].T
            cols.append(t[0:8] + t[8:16] + t[16:24])
        return jnp.concatenate(cols, 1)

    lead[...] = data(0, AHEAD)
    out[...] = jnp.zeros_like(out)

    @pl.loop(AHEAD // WIDE, (start + WIDE - 1) // WIDE)
    def _(i):
        for lanes, sums in echoes(data(i * WIDE, WIDE), base, span, trig):
            out[:, lanes] += sums


def range_binning(positions, amplitude, cells, bounce, base, span):
    count = positions.shape[0]
    rows = count // 128
    sources = (
        cells.reshape(rows, 128),
        bounce.reshape(rows, 128),
        positions.reshape(1, count),
        amplitude,
        cells.reshape(1, count),
        bounce.reshape(1, count),
    )
    return pl.pallas_call(
        functools.partial(range_bin_kernel, span=span, trig=range_trig_coefs(4)),
        in_specs=[pl.BlockSpec(memory_space=pltpu.SMEM)] + [IN_HBM] * len(sources),
        out_specs=(IN_VMEM, IN_VMEM),
        out_shape=(
            jax.ShapeDtypeStruct((span, 2 * P_SIZE), f32),
            jax.ShapeDtypeStruct((8, AHEAD), f32),
        ),
        scratch_shapes=[pltpu.VMEM(a.shape, a.dtype) for a in sources]
        + [
            pltpu.VMEM((count + SLOTS + AHEAD, 128), f32),
            pltpu.SemaphoreType.DMA((len(sources),)),
        ],
        compiler_params=pltpu.CompilerParams(vmem_limit_bytes=16 << 20),
        name="range_binning",
    )(base.reshape(1), *in_hbm(sources))


def complex_rows(c, s):
    return np.block([[c, s], [-s, c]])


def mid_factors(n_dev, order):
    side = np.arange(BIN_SIDE)
    t = np.arange(STOLT)
    eye = np.eye(GROUP)
    a = -2 * np.pi / STOLT * ((side[:, None] * t[None, :]) % STOLT)
    ta = complex_rows(np.cos(a), np.sin(a))[order]
    a = -2 * np.pi / F_LEN * (side[:, None] * t[None, :])
    wa = np.stack([np.tile(np.cos(a), (GROUP, 1)), np.tile(np.sin(a), (GROUP, 1))])
    a = -2 * np.pi / BIN_SIDE * ((side[:, None] * side[None, :]) % BIN_SIDE)
    c, s = np.kron(eye, np.cos(a)), np.kron(eye, np.sin(a))
    tb = complex_rows(c, s).T
    blk = np.arange(BLOCKS)
    a = 2 * np.pi / BLOCKS * ((blk[:, None] * blk[None, :]) % BLOCKS)
    c, s = np.kron(eye, np.cos(a)), np.kron(eye, np.sin(a))
    tc = complex_rows(c, s)
    a = 2 * np.pi / F_LEN * (t[:, None] * blk[None, :])
    wc = np.stack([np.tile(np.cos(a), (1, GROUP)), np.tile(np.sin(a), (1, GROUP))])
    a = 2 * np.pi / STOLT * ((t[:, None] * t[None, :]) % STOLT)
    td = complex_rows(np.cos(a), np.sin(a)).T / F_LEN
    td = td.reshape(2, n_dev, STOLT // n_dev, 2 * STOLT).transpose(1, 0, 2, 3)
    return ta, wa.astype(np.float32), tb, tc, wc.astype(np.float32), td


def mid_tables(n_dev, order):
    ta, wa, tb, tc, wc, td = mid_factors(n_dev, order)
    td = td.reshape(2 * STOLT, 2 * STOLT)
    return np_split(ta), wa, np_split(tb), np_split(tc), wc, np_split(td)


def core_tables(n_dev, order):
    ta, wa, tb, tc, wc, td = mid_factors(n_dev, order)
    td = td.reshape(n_dev, 2, -1, GROUP, 2 * STOLT).transpose(0, 2, 1, 3, 4)
    td = td.reshape(2 * STOLT, 2 * STOLT)
    forward, inverse = quarter_tables()
    return (
        np_split(forward),
        np_split(ta),
        wa,
        np_split(tb),
        np_split(tc),
        wc,
        np_split(td),
    ), np_split(inverse)


def mid_kernel(
    x, cos_p, sin_p, hot, kind, bank_hi, bank_lo, ta, wa, tb, tc, wc, td, out, xs, os, *, subs
):
    n = GROUP * BLOCKS
    step = pl.program_id(0)
    groups = x.shape[1]

    @pl.when(step == 0)
    def _():
        for g in range(groups):
            xs[g] = x[:, g, :]

    parts_hi, parts_lo = [], []
    for g in range(subs):
        lanes = slice(g * n, (g + 1) * n)
        y = dots(split(xs[step * subs + g]), (ta[0], ta[1]), ((0,), (0,)))
        yr, yi = y[:, :STOLT], y[:, STOLT:]
        y = jnp.concatenate([yr * wa[0] - yi * wa[1], yr * wa[1] + yi * wa[0]], 0)
        z = dots((tb[0], tb[1]), split(y), ((1,), (0,)))
        zr, zi = z[:n], z[n:]
        cp, sp = cos_p[lanes], sin_p[lanes]
        z = jnp.concatenate([zr * cp - zi * sp, zr * sp + zi * cp], 1)
        hi, lo = split(z)
        picked = jnp.dot(
            hot[g], jnp.concatenate([hi, lo], 1), preferred_element_type=f32
        ).astype(bf16)
        first, second = picked[:n], picked[n:]
        for c in range(2):
            for base, keep in ((0, parts_hi), (2 * STOLT, parts_lo)):
                cut = slice(base + c * STOLT, base + (c + 1) * STOLT)
                keep.append(jnp.concatenate([first[:, cut], second[:, cut]], 1))
    ghi = jnp.concatenate(parts_hi, 0)
    glo = jnp.concatenate(parts_lo, 0)
    kinds = kind[...].reshape(subs * 2 * n, 1)
    kinds = jnp.broadcast_to(kinds, (subs * 2 * n, STOLT))
    acc = jnp.zeros((subs * 2 * n, STOLT), f32)
    for k in range(0, bank_hi.shape[0], 2):
        khi = jnp.concatenate([bank_hi[k], bank_hi[k + 1]], 1)
        klo = jnp.concatenate([bank_lo[k], bank_lo[k + 1]], 1)
        r = dots((ghi, glo), (khi, klo), ((1,), (0,)))
        for half in range(2):
            acc = jnp.where(kinds == k + half, r[:, half * STOLT : (half + 1) * STOLT], acc)
    for g in range(subs):
        s = acc[g * 2 * n : (g + 1) * 2 * n]
        y = dots(split(s), (tc[0], tc[1]), ((0,), (0,)))
        yr, yi = y[:, :n], y[:, n:]
        y = jnp.concatenate([yr * wc[0] - yi * wc[1], yr * wc[1] + yi * wc[0]], 0)
        os[step * subs + g] = dots((td[0], td[1]), split(y), ((1,), (0,)))

    @pl.when(step == pl.num_programs(0) - 1)
    def _():
        for g in range(groups):
            out[:, g, :] = os[g]


def middle(x, cos_p, sin_p, hot, kind, bank_hi, bank_lo, tables):
    groups = x.shape[1]
    subs = min(4, groups)
    n = GROUP * BLOCKS
    whole = lambda a: pl.BlockSpec(a.shape, lambda i: (0,) * a.ndim)
    return pl.pallas_call(
        functools.partial(mid_kernel, subs=subs),
        grid=(groups // subs,),
        in_specs=[
            whole(x),
            pl.BlockSpec((subs * n, STOLT), lambda i: (i, 0)),
            pl.BlockSpec((subs * n, STOLT), lambda i: (i, 0)),
            pl.BlockSpec((subs, 2 * n, n), lambda i: (i, 0, 0)),
            pl.BlockSpec((subs, 2 * n, 1), lambda i: (i, 0, 0)),
            whole(bank_hi),
            whole(bank_lo),
        ]
        + [whole(t) for t in tables],
        out_specs=pl.BlockSpec((2 * STOLT, groups, n), lambda i: (0, 0, 0)),
        out_shape=jax.ShapeDtypeStruct((2 * STOLT, groups, n), f32),
        scratch_shapes=[
            pltpu.VMEM((groups, x.shape[0], n), f32),
            pltpu.VMEM((groups, 2 * STOLT, n), f32),
        ],
        name="middle",
    )(x, cos_p, sin_p, hot, kind, bank_hi, bank_lo, *tables)


def quarter_tables():
    q = P_SIZE // 4
    m = np.arange(q)
    fwd, inv = [], []
    for low in range(4):
        a = 2 * np.pi / P_SIZE * (((4 * m[:, None] + low) * m[None, :]) % P_SIZE)
        turn = a.reshape(-1, 2, q).transpose(1, 0, 2).reshape(q, q)
        fwd.append(np.concatenate([np.cos(turn), np.sin(turn)], 0))
        inv.append(np.concatenate([np.cos(a.T), np.sin(a.T)], 0) / P_SIZE)
    return np.stack(fwd), np.stack(inv)


def swap_blocks(arrays):
    count = len(arrays)
    lanes = arrays[0].shape[-1]
    size = lanes // count
    block = lax.broadcasted_iota(jnp.int32, arrays[0].shape, 1) // size
    outs = []
    for b in range(count):
        acc = None
        for a in range(count):
            shift = (a - b) % count * size
            moved = pltpu.roll(arrays[a], shift, 1) if shift else arrays[a]
            acc = moved if acc is None else jnp.where(block == a, moved, acc)
        outs.append(acc)
    return outs


def core_kernel(*refs, n_pulse, n_scat, subs, trig, trig_low):
    lead, partial = refs[:2]
    sources = refs[2:12]
    out = refs[12]
    local = refs[13:23]
    steps_in, kinds_in, bank, table, ta, wa, tb, tc, wc, td = local
    binned, peer, spec, x, hot, kind, banks, os = refs[23:31]
    (
        load, own_store, pair_send, pair_recv, near_send, near_recv, far_send, far_recv,
    ) = refs[31:]
    n_dev = n_pulse * n_scat
    pulse = lax.axis_index("pulse")
    scat = lax.axis_index("scat")
    me = pulse * n_scat + scat
    half = peer.shape[0]
    lanes = 2 * half
    size = P_SIZE // 4
    n = GROUP * BLOCKS
    groups = os.shape[1]
    pieces = groups // subs
    quads = lanes // BIN_SIDE
    unit = subs * quads
    per = os.shape[2]
    moves = [(a, b) for a in range(n_pulse) for b in range(n_scat) if (a, b) != (0, 0)]
    moves.sort(key=lambda m: (-min(m[0], n_pulse - m[0]), m))

    def other(a, b):
        return lax.rem(pulse + a, n_pulse), lax.rem(scat + b, n_scat)

    barrier = pltpu.get_barrier_semaphore()
    for a, b in moves:
        p, c = other(a, b)
        pl.semaphore_signal(
            barrier, inc=1, device_id={"pulse": p, "scat": c}, device_id_type=MESH
        )
    keep = pl.ds(pl.multiple_of(scat * half, half), half)
    give = pl.ds(pl.multiple_of((1 - scat) * half, half), half)
    loads = [
        pltpu.make_async_copy(src, dst, load.at[i])
        for i, (src, dst) in enumerate(zip(sources, local))
    ]
    for copy in loads:
        copy.start()
    for cut, sums in echoes(lead[...], pulse * 2 * half, 2 * half, trig_low):
        binned[:, cut] = partial[:, cut] + sums
    pl.semaphore_wait(barrier, n_dev - 1)

    pair = pltpu.make_async_remote_copy(
        src_ref=binned.at[give, :],
        dst_ref=peer,
        send_sem=pair_send,
        recv_sem=pair_recv,
        device_id={"pulse": pulse, "scat": 1 - scat},
        device_id_type=MESH,
    )
    pair.start()
    loads[3].wait()
    pair.wait()

    quarters = []
    for q in range(4):
        pair_of = []
        for c in range(2):
            cut = slice(c * P_SIZE + q * size, c * P_SIZE + (q + 1) * size)
            pair_of.append(binned[keep, cut] + peer[:, cut])
        quarters.append(pair_of)
    (r0, i0), (r1, i1), (r2, i2), (r3, i3) = quarters
    sr, si, dr, di = r0 + r2, i0 + i2, r0 - r2, i0 - i2
    tr, ti, er, ei = r1 + r3, i1 + i3, r1 - r3, i1 - i3
    mixed = (
        (sr + tr, si + ti),
        (dr + ei, di - er),
        (sr - tr, si - ti),
        (dr - ei, di + er),
    )
    low = lax.broadcasted_iota(jnp.int32, (size, lanes), 1) < half
    rows = []
    for k in range(4):
        g = product(
            joined(table[0, k], table[1, k], 1),
            triple(jnp.concatenate(mixed[k], 0), 1),
            ((1,), (1,)),
        )
        turned = pltpu.roll(g[size:], half, 1)
        rows.append(g[:size] + jnp.where(low, turned, -turned))
    for q, z in enumerate(swap_blocks(rows)):
        for h in range(subs):
            spec[pl.ds(q * subs + h, size // subs, stride=unit), :] = z[
                h * (size // subs) : (h + 1) * (size // subs)
            ]

    def piece(dev, i):
        return pl.ds(pl.multiple_of((dev * pieces + i) * unit, unit), unit)

    own = pl.ds(pl.multiple_of(me * unit, unit), unit)
    for i in range(pieces):
        for j, (a, b) in enumerate(moves):
            p, c = other(a, b)
            pltpu.make_async_remote_copy(
                src_ref=spec.at[piece(p * n_scat + c, i), :],
                dst_ref=x.at[i, own, :],
                send_sem=near_send.at[j],
                recv_sem=near_recv.at[i, me],
                device_id={"pulse": p, "scat": c},
                device_id_type=MESH,
            ).start()
    for i in range(pieces):
        x[i, own, :] = spec[piece(me, i), :]

    for i in (0, 1, 2, 4, 5, 6, 7, 8, 9):
        loads[i].wait()
    block = lax.broadcasted_iota(jnp.int32, (n, STOLT), 0)
    lane = lax.broadcasted_iota(jnp.int32, (n, STOLT), 1)
    spot = lane.astype(f32)
    above = (block // BLOCKS * BLOCKS).astype(f32)
    flat = []
    for ref in (steps_in, kinds_in):
        flat.append(
            jnp.concatenate([ref[pl.ds(j, groups, stride=GROUP), :] for j in range(GROUP)], 1)
        )
    for g in range(groups):
        first = jnp.broadcast_to(flat[0][g : g + 1].astype(f32), (n, n)).T + above
        hot[g, :n] = jnp.where(first == spot, 1.0, 0.0).astype(bf16)
        hot[g, n:] = jnp.where(first + 1.0 == spot, 1.0, 0.0).astype(bf16)
        kind[g] = jnp.broadcast_to(flat[1][g : g + 1].astype(f32), (n, n)).T
    for k in range(bank.shape[0]):
        hi, lo = split(bank[k])
        cut = slice(k % 2 * STOLT, (k % 2 + 1) * STOLT)
        banks[k // 2, :, cut] = jnp.concatenate([hi, hi, lo], 0)

    cols = (lane + (block % BLOCKS) * STOLT).astype(f32)
    kr = 4.0 * np.pi / 3e8 * (9.6e9 + (cols - F_LEN // 2) * (1.5e8 / F_LEN))

    def phase(g):
        row = me * (groups * GROUP) + g * GROUP + block // BLOCKS
        centered = lax.rem(row + P_SIZE // 2, P_SIZE) - P_SIZE // 2
        along = 2.0 * np.pi / (P_SIZE * SPACING) * centered.astype(f32)
        squared = along * along
        depth = NEAR + B // 2
        theta = -depth * squared / (jnp.sqrt(kr * kr - squared) + kr)
        whole = jnp.round(theta * (0.5 / np.pi))
        for part in turn_parts():
            theta = theta - whole * part
        r = theta * (0.5 / np.pi)
        u = r * r
        sn = r * horner(u, trig[0])
        cs = horner(u, trig[1])
        return 1.0 - 2.0 * sn * sn, 2.0 * sn * cs

    def ranged(i, h):
        g = i * subs + h
        cp, sp = phase(g)
        rows_in = x[i, pl.ds(h, n_dev * quads, stride=subs), :]
        y = product(triple(rows_in, 0), joined(ta[0], ta[1], 0), ((0,), (0,)))
        yr, yi = y[:, :STOLT], y[:, STOLT:]
        y = jnp.concatenate([yr * wa[0] - yi * wa[1], yr * wa[1] + yi * wa[0]], 0)
        z = product(joined(tb[0], tb[1], 1), triple(y, 0))
        zr, zi = z[:n], z[n:]
        z = jnp.concatenate([zr * cp - zi * sp, zr * sp + zi * cp], 1)
        picked = product(hot[g], jnp.concatenate(split(z), 1)).astype(bf16)
        first, second = picked[:n], picked[n:]
        parts = []
        for base in (0, 2 * STOLT):
            cuts = [slice(base + c * STOLT, base + (c + 1) * STOLT) for c in range(2)]
            parts.append(
                jnp.concatenate(
                    [jnp.concatenate([first[:, v], second[:, v]], 1) for v in cuts], 0
                )
            )
        ghi, glo = parts
        windows = jnp.concatenate([ghi, glo, ghi], 1)
        kinds = jnp.concatenate([kind[g]] * 2, 0)
        acc = jnp.zeros((2 * n, STOLT), f32)
        for k in range(banks.shape[0]):
            r = product(windows, banks[k])
            for v in range(2):
                acc = jnp.where(kinds == 2 * k + v, r[:, v * STOLT : (v + 1) * STOLT], acc)
        y = product(triple(acc, 0), joined(tc[0], tc[1], 0), ((0,), (0,)))
        yr, yi = y[:, :n], y[:, n:]
        y = jnp.concatenate([yr * wc[0] - yi * wc[1], yr * wc[1] + yi * wc[0]], 0)
        z = product(joined(td[0], td[1], 1), triple(y, 0))
        os[:, g] = z.reshape(n_dev, per, n)
        for j, (a, b) in enumerate(moves):
            p, c = other(a, b)
            pltpu.make_async_remote_copy(
                src_ref=os.at[p * n_scat + c, g],
                dst_ref=out.at[me, g],
                send_sem=far_send.at[j],
                recv_sem=far_recv.at[me],
                device_id={"pulse": p, "scat": c},
                device_id_type=MESH,
            ).start()

    def step(i, carry):
        for a, b in moves:
            p, c = other(a, b)
            src = p * n_scat + c
            here = pl.ds(pl.multiple_of(src * unit, unit), unit)
            pltpu.make_async_copy(
                x.at[i, here, :], x.at[i, here, :], near_recv.at[i, src]
            ).wait()
        for h in range(subs):
            ranged(i, h)
        return carry

    lax.fori_loop(0, pieces, step, 0)
    mine = pltpu.make_async_copy(os.at[me], out.at[me], own_store)
    mine.start()
    mine.wait()
    for j, (a, b) in enumerate(moves):
        p, c = other(a, b)
        src = p * n_scat + c
        all_of = spec.at[pl.ds(0, pieces * unit), :]
        pltpu.make_async_copy(all_of, all_of, near_send.at[j]).wait()
        pltpu.make_async_copy(os.at[src], os.at[src], far_send.at[j]).wait()
        pltpu.make_async_copy(out.at[src], out.at[src], far_recv.at[src]).wait()


def turn_parts():
    parts, rest = [], 2.0 * np.pi
    for bits in (10, 22, 60):
        scale = 2.0**bits
        part = float(np.float32(np.round(rest * scale) / scale))
        parts.append(part)
        rest -= part
    return parts


def core(partial, lead, steps_in, kinds_in, bank, tables, n_pulse, n_scat):
    n_dev = n_pulse * n_scat
    groups = steps_in.shape[0] // GROUP
    subs = 2
    n = GROUP * BLOCKS
    span, width = partial.shape
    half = span // n_scat
    quads = 2 * half // BIN_SIDE
    kernels = bank.shape[0]
    per = 2 * STOLT // n_dev
    sources = (steps_in, kinds_in, bank, *tables)
    dma = pltpu.SemaphoreType.DMA
    return pl.pallas_call(
        functools.partial(
            core_kernel,
            n_pulse=n_pulse,
            n_scat=n_scat,
            subs=subs,
            trig=range_trig_coefs(5),
            trig_low=range_trig_coefs(4),
        ),
        in_specs=[IN_VMEM] * 2 + [IN_HBM] * len(sources),
        out_specs=pl.BlockSpec(memory_space=pl.ANY),
        out_shape=jax.ShapeDtypeStruct((n_dev, groups, per, n), f32),
        scratch_shapes=[pltpu.VMEM(a.shape, a.dtype) for a in sources]
        + [
            pltpu.VMEM((span, width), f32),
            pltpu.VMEM((half, width), f32),
            pltpu.VMEM((n_dev * groups * quads, n), f32),
            pltpu.VMEM((groups // subs, n_dev * subs * quads, n), f32),
            pltpu.VMEM((groups, 2 * n, n), bf16),
            pltpu.VMEM((groups, n, STOLT), f32),
            pltpu.VMEM((kernels // 2, 6 * STOLT, 2 * STOLT), bf16),
            pltpu.VMEM((n_dev, groups, per, n), f32),
            dma((len(sources),)),
            dma,
            dma,
            dma,
            dma((n_dev,)),
            dma((groups // subs, n_dev)),
            dma((n_dev,)),
            dma((n_dev,)),
        ],
        compiler_params=pltpu.CompilerParams(
            collective_id=0, has_side_effects=True, vmem_limit_bytes=24 << 20
        ),
        name="core",
    )(lead, partial, *in_hbm(sources))


def image_kernel(x, table, out, done, sems):
    devs, kh, per, lanes = x.shape
    size = P_SIZE // 4
    copies = []
    for h in range(per // (2 * GROUP)):
        columns = [[] for _ in range(4)]
        for c in range(2):
            first = (2 * h + c) * GROUP
            tiles = [x[:, :, first + j, :].reshape(devs * kh, lanes) for j in range(4)]
            for k, z in enumerate(swap_blocks(tiles)):
                columns[k].append(z)
        v = []
        for k in range(4):
            g = product(
                joined(table[0, k], table[1, k], 1), triple(jnp.concatenate(columns[k], 1), 0)
            )
            cos_g, sin_g = g[:size], g[size:]
            v.append((cos_g[:, :lanes] - sin_g[:, lanes:], cos_g[:, lanes:] + sin_g[:, :lanes]))
        (r0, i0), (r1, i1), (r2, i2), (r3, i3) = v
        sr, si, dr, di = r0 + r2, i0 + i2, r0 - r2, i0 - i2
        tr, ti, er, ei = r1 + r3, i1 + i3, r1 - r3, i1 - i3
        mixed = (
            (sr + tr, si + ti),
            (dr - ei, di + er),
            (sr - tr, si - ti),
            (dr + ei, di - er),
        )
        for q in range(4):
            for c in range(2):
                done[h, c, q * size : (q + 1) * size, :] = mixed[q][c]
        copy = pltpu.make_async_copy(
            done.at[h], out.at[:, :, pl.ds(h * lanes, lanes)], sems.at[h]
        )
        copy.start()
        copies.append(copy)
    for copy in copies:
        copy.wait()


def reference_phase(row_ids, cols):
    centered = (row_ids + P_SIZE // 2) % P_SIZE - P_SIZE // 2
    along_k = 2.0 * jnp.pi / (P_SIZE * SPACING) * centered.astype(f32)
    kr = 4.0 * jnp.pi / 3e8 * (9.6e9 + (cols.astype(f32) - F_LEN // 2) * (1.5e8 / F_LEN))
    squared = along_k * along_k
    depth = NEAR + B // 2
    return (
        -depth
        * squared[:, None]
        / (jnp.sqrt(kr[None, :] * kr[None, :] - squared[:, None]) + kr[None, :])
    )


def on_device(positions, amplitude, range_cells, bounce, stolt_block, kernel_choice, kernel_bank):
    n_pulse = lax.axis_size("pulse")
    n_scat = lax.axis_size("scat")
    n_dev = n_pulse * n_scat
    pulse_here = lax.axis_index("pulse")
    scat_here = lax.axis_index("scat")
    pulses = P_SIZE // n_pulse
    rows = P_SIZE // n_dev
    width = F_LEN // n_dev
    groups = rows // GROUP
    n = GROUP * BLOCKS
    bins_scat = B // n_scat
    bins_here = bins_scat // n_pulse

    per = STOLT // n_dev
    span = B // n_pulse
    packed = (
        span == 128
        and n_scat == 2
        and per % 4 == 0
        and groups % 8 == 0
        and positions.shape[0] % CHUNK == 0
    )
    if packed:
        partial, lead = range_binning(
            positions, amplitude, range_cells, bounce, pulse_here * span, span
        )
        local = bins_here // BIN_SIDE
        i, s, c, l = np.meshgrid(
            np.arange(n_pulse), np.arange(n_scat), np.arange(2), np.arange(local), indexing="ij"
        )
        order = (c * BIN_SIDE + (i * n_scat + s) * local + l).reshape(-1)
        tables, backward = core_tables(n_dev, order)
        tables = tuple(jnp.asarray(t) for t in tables)
        columns = core(
            partial, lead, stolt_block, kernel_choice, kernel_bank, tables, n_pulse, n_scat
        )
        return pl.pallas_call(
            image_kernel,
            in_specs=[IN_VMEM, IN_VMEM],
            out_specs=pl.BlockSpec(memory_space=pl.ANY),
            out_shape=jax.ShapeDtypeStruct((2, P_SIZE, width), f32),
            scratch_shapes=[
                pltpu.VMEM((width // n, 2, P_SIZE, n), f32),
                pltpu.SemaphoreType.DMA((width // n,)),
            ],
            compiler_params=pltpu.CompilerParams(vmem_limit_bytes=16 << 20),
            name="image",
        )(columns, jnp.asarray(backward))

    ids = jnp.arange(GROUP, dtype=jnp.int32)[None, :, None] * BLOCKS
    first = stolt_block.reshape(groups, GROUP, BLOCKS) + ids
    pick = jnp.stack([first, first + 1], 1).reshape(groups, 2 * n, 1)
    hot = (pick == jnp.arange(n, dtype=jnp.int32)[None, None, :]).astype(bf16)
    kind = jnp.stack([kernel_choice.reshape(groups, n)] * 2, 1).reshape(groups, 2 * n, 1)
    bank_hi = lax.reduce_precision(kernel_bank, 8, 7)
    bank_lo = (kernel_bank - bank_hi).astype(bf16)
    bank_hi = bank_hi.astype(bf16)
    row_ids = (pulse_here * n_scat + scat_here) * rows + jnp.arange(rows, dtype=jnp.int32)
    theta = reference_phase(row_ids, jnp.arange(F_LEN, dtype=jnp.int32))
    theta = theta.reshape(rows * BLOCKS, STOLT)
    cos_p, sin_p = jnp.cos(theta), jnp.sin(theta)

    partial = binning(positions, amplitude, range_cells, bounce, pulse_here * pulses, pulses)
    partial = partial.reshape(n_scat, bins_scat, 2 * pulses)
    binned = lax.dynamic_index_in_dim(partial, scat_here, 0, keepdims=False)
    for shift in range(1, n_scat):
        other = lax.dynamic_index_in_dim(
            partial, (scat_here + shift) % n_scat, 0, keepdims=False
        )
        ring = [(i, (i + shift) % n_scat) for i in range(n_scat)]
        binned = binned + lax.ppermute(other, "scat", ring)
    turned = lax.all_to_all(
        binned.reshape(n_pulse, bins_here, 2 * pulses), "pulse", 0, 0, tiled=True
    )
    turned = turned.reshape(n_pulse, bins_here, 2, pulses).transpose(0, 3, 2, 1)
    turned = turned.reshape(P_SIZE, 2 * bins_here)
    k = np.arange(P_SIZE)
    angle = 2 * np.pi / P_SIZE * ((k[:, None] * k[None, :]) % P_SIZE)
    az = jnp.asarray(np.concatenate([np.cos(angle), np.sin(angle)], 0), f32)
    product = jnp.dot(az, turned, precision=HIGH, preferred_element_type=f32)
    pc, ps = product[:P_SIZE], product[P_SIZE:]
    spectrum = pc + jnp.concatenate([ps[:, bins_here:], -ps[:, :bins_here]], 1)
    az_rows = lax.all_to_all(
        spectrum.reshape(n_dev, rows, 2 * bins_here), ("pulse", "scat"), 0, 0, tiled=True
    )
    x = az_rows.reshape(n_pulse, n_scat, rows, 2, bins_here).transpose(3, 1, 0, 4, 2)
    x = x.reshape(2, BIN_SIDE, BIN_SIDE, rows).transpose(0, 1, 3, 2)
    x = x.reshape(2 * BIN_SIDE, groups, n)
    order = np.arange(2 * BIN_SIDE)

    tables = tuple(jnp.asarray(t) for t in mid_tables(n_dev, order))
    ranged = middle(x, cos_p, sin_p, hot, kind, bank_hi, bank_lo, tables)
    columns = lax.all_to_all(
        ranged.reshape(n_dev, 2 * per, rows * BLOCKS), ("pulse", "scat"), 0, 0, tiled=True
    )
    columns = columns.reshape(n_dev, 2, per, rows, BLOCKS).transpose(0, 3, 1, 2, 4)
    columns = columns.reshape(P_SIZE, 2 * width)
    final = jnp.dot(az, columns, precision=HIGH, preferred_element_type=f32)
    fc, fs = final[:P_SIZE], final[P_SIZE:]
    re = (fc[:, :width] - fs[:, width:]) / P_SIZE
    im = (fc[:, width:] + fs[:, :width]) / P_SIZE
    return jnp.stack([re, im])


def solution(mesh):
    placed = (
        P(("scene", "scat")),
        P(None, ("scene", "scat")),
        P(("scene", "scat")),
        P(("scene", "scat")),
        P(("pulse", "scat"), None),
        P(("pulse", "scat"), None),
        P(),
    )
    return jax.shard_map(
        on_device,
        mesh=mesh,
        in_specs=placed,
        out_specs=P(None, "scene", ("pulse", "scat")),
        check_vma=False,
    )
```

```python
import functools

import jax
import jax.numpy as jnp
import numpy as np
from jax import lax
from jax.experimental import pallas as pl
from jax.experimental.pallas import tpu as pltpu
from jax.sharding import PartitionSpec as P

P_SIZE = 512
F_LEN = 4096
B = 1024
SHIFT = 16
STOLT = 128
BLOCKS = 32
SPACING = 2.0
NEAR = 700000.0
BIN_SIDE = 32
GROUP = 4
CHUNK = 1024
SLOTS = 192
WIDE = 128
AHEAD = 1024
SHARED = 1
STREAM = 512
HIGH = lax.Precision.HIGH
MESH = pl.DeviceIdType.MESH
IN_HBM = pl.BlockSpec(memory_space=pltpu.HBM)
IN_VMEM = pl.BlockSpec(memory_space=pltpu.VMEM)
f32 = jnp.float32
bf16 = jnp.bfloat16


def trig_coefs():
    x = np.cos(np.pi * (np.arange(400) + 0.5) / 400) * 0.5
    u = x * x
    s = np.polynomial.chebyshev.Chebyshev.fit(u, np.sin(np.pi * x) / x, 5).convert(
        kind=np.polynomial.Polynomial
    )
    c = np.polynomial.chebyshev.Chebyshev.fit(u, np.cos(np.pi * x), 5).convert(
        kind=np.polynomial.Polynomial
    )
    return [float(v) for v in s.coef], [float(v) for v in c.coef]


def horner(u, coefs):
    acc = jnp.full_like(u, coefs[-1])
    for c in coefs[-2::-1]:
        acc = acc * u + c
    return acc


def split(x):
    hi = x.astype(bf16)
    lo = (x - hi.astype(f32)).astype(bf16)
    return hi, lo


def np_split(x):
    x = np.asarray(x, np.float64)
    hi = np.asarray(x, jnp.bfloat16)
    lo = np.asarray(x - hi.astype(np.float64), jnp.bfloat16)
    return np.stack([hi, lo])


def dots(a, b, dims):
    d = functools.partial(
        lax.dot_general, dimension_numbers=(dims, ((), ())), preferred_element_type=f32
    )
    return d(a[0], b[0]) + (d(a[0], b[1]) + d(a[1], b[0]))


def in_hbm(arrays):
    return [pltpu.with_memory_space_constraint(a, pltpu.HBM) for a in arrays]


def joined(hi, lo, axis):
    return jnp.concatenate([hi, hi, lo], axis)


def triple(x, axis):
    hi, lo = split(x)
    return jnp.concatenate([hi, lo, hi], axis)


def product(a, b, dims=((1,), (0,))):
    return lax.dot_general(a, b, (dims, ((), ())), preferred_element_type=f32)


def bin_kernel(pulse_base, pos, amp, tgt, bnc, out, acc, *, pulses, sin_c, cos_c):
    step = pl.program_id(0)
    width = pos.shape[1]

    @pl.when(step == 0)
    def _():
        acc[...] = jnp.zeros_like(acc)

    base = pulse_base[0]
    ids = base + lax.broadcasted_iota(jnp.int32, (pulses, width), 0)
    along = (ids.astype(f32) - P_SIZE // 2) * SPACING
    target = tgt[...] + SHIFT * bnc[...]
    slant = NEAR + target.astype(f32)
    offset = along - pos[...]
    square = offset * offset
    excess = square / (jnp.sqrt(slant * slant + square) + slant)
    halves = excess * -128.0
    whole = jnp.round(halves)
    r = halves - whole
    u = r * r
    odd = whole - 2.0 * jnp.floor(whole * 0.5)
    sign = 1.0 - 2.0 * odd
    sin_p = sign * r * horner(u, sin_c)
    cos_p = sign * horner(u, cos_c)
    flip = 1.0 - 2.0 * bnc[...].astype(f32)
    are = flip * amp[0:1]
    aim = flip * amp[1:2]
    re = are * cos_p - aim * sin_p
    im = are * sin_p + aim * cos_p
    steer = jnp.concatenate([re, im], 0)
    hi, lo = split(steer)
    rhs = jnp.concatenate([hi, lo], 0)
    bins = lax.broadcasted_iota(jnp.int32, (B, width), 0)
    hot = jnp.where(bins == target, 1.0, 0.0).astype(bf16)
    acc[...] += lax.dot_general(
        hot, rhs, (((1,), (1,)), ((), ())), preferred_element_type=f32
    )

    @pl.when(step == pl.num_programs(0) - 1)
    def _():
        out[...] = acc[:, : 2 * pulses] + acc[:, 2 * pulses :]


def binning(positions, amplitude, cells, bounce, pulse_base, pulses):
    count = positions.shape[0]
    width = min(2048, count)
    sin_c, cos_c = trig_coefs()
    row = lambda n: pl.BlockSpec((n, width), lambda i: (0, i))
    return pl.pallas_call(
        functools.partial(bin_kernel, pulses=pulses, sin_c=sin_c, cos_c=cos_c),
        grid=(count // width,),
        in_specs=[pl.BlockSpec(memory_space=pltpu.SMEM), row(1), row(2), row(1), row(1)],
        out_specs=pl.BlockSpec((B, 2 * pulses), lambda i: (0, 0)),
        out_shape=jax.ShapeDtypeStruct((B, 2 * pulses), f32),
        scratch_shapes=[pltpu.VMEM((B, 4 * pulses), f32)],
        name="binning",
    )(
        pulse_base.reshape(1),
        positions.reshape(1, count),
        amplitude,
        cells.reshape(1, count),
        bounce.reshape(1, count),
    )


def range_trig_coefs(degree):
    x = np.cos(np.pi * (np.arange(400) + 0.5) / 400) * 0.5
    u = x * x
    fit = lambda y: np.polynomial.chebyshev.Chebyshev.fit(u, y, degree).convert(
        kind=np.polynomial.Polynomial
    )
    return [float(v) for v in fit(np.sin(np.pi * x) / x).coef], [
        float(v) for v in fit(np.cos(np.pi * x)).coef
    ]


def split3(x):
    hi = x.astype(bf16).astype(f32)
    rest = x - hi
    mid = rest.astype(bf16).astype(f32)
    return hi, mid, rest - mid


def echoes(data, base, bins, trig):
    where, re_amp, im_amp, rel = (data[j : j + 1] for j in range(4))
    re2, im2 = 2.0 * re_amp, 2.0 * im_amp
    inverse = 0.5 / (rel + (base.astype(f32) + NEAR))
    gain = inverse * -64.0
    bend = inverse * (1.0 / 64.0)
    width = data.shape[1]
    rows = lax.broadcasted_iota(jnp.int32, (bins, width), 0).astype(f32)
    hot = jnp.where(rows == rel, 1.0, 0.0).astype(bf16)
    hot = jnp.concatenate([hot, hot], 1)
    for q in range(P_SIZE // 128):
        parts = [[], []]
        for p in range(0, 128, 16):
            ids = lax.broadcasted_iota(jnp.int32, (16, width), 0)
            along = (ids + (q * 128 + p - P_SIZE // 2)).astype(f32) * SPACING
            offset = along - where
            t = offset * offset * gain
            y = t * bend
            t = t * (1.0 + y * (1.0 + 2.0 * y))
            r = t - jnp.round(t)
            u = r * r
            sn = r * horner(u, trig[0])
            cs = horner(u, trig[1])
            re = re_amp - sn * (re2 * sn + im2 * cs)
            im = im_amp + sn * (re2 * cs - im2 * sn)
            for c, v in enumerate((re, im)):
                parts[c].append(jnp.concatenate(split(v), 1))
        for c in range(2):
            lanes = slice(c * P_SIZE + q * 128, c * P_SIZE + (q + 1) * 128)
            yield lanes, product(hot, jnp.concatenate(parts[c], 0), ((1,), (1,)))


def range_bin_kernel(base_ref, *refs, span, trig):
    out, lead = refs[6:8]
    buf, load = refs[14:]
    cells8, bounce8, pos, amp, cells, bnc = refs[8:14]
    loads = [
        pltpu.make_async_copy(src, dst, load.at[i])
        for i, (src, dst) in enumerate(zip(refs[:6], refs[8:14]))
    ]
    for copy in loads:
        copy.start()
    for copy in loads:
        copy.wait()
    base = base_ref[0]
    rows = cells8.shape[0]
    chunks = rows // 8
    target = cells8[...] + SHIFT * bounce8[...] - base
    match = jnp.where((target >= 0) & (target < span), 1.0, 0.0)
    mb = match.astype(bf16)
    a = lax.broadcasted_iota(jnp.int32, (128, 128), 0)
    b = lax.broadcasted_iota(jnp.int32, (128, 128), 1)
    upto = jnp.where(a <= b, 1.0, 0.0).astype(bf16)
    count = jnp.dot(mb, upto, preferred_element_type=f32)
    total = jnp.dot(mb, jnp.ones((128, 128), bf16), preferred_element_type=f32)
    a = lax.broadcasted_iota(jnp.int32, (rows, rows), 0)
    b = lax.broadcasted_iota(jnp.int32, (rows, rows), 1)
    below = jnp.where((a // 8 == b // 8) & (b < a), 1.0, 0.0).astype(bf16)
    ahead = jnp.dot(below, total.astype(bf16), preferred_element_type=f32)
    rank = jnp.where(match > 0.0, count + ahead - 1.0, -1.0)
    counts = [
        jnp.sum(match[8 * c : 8 * c + 8]).astype(jnp.int32) for c in range(chunks)
    ]

    def values(c):
        lanes = slice(CHUNK * c, CHUNK * (c + 1))
        flip = 1.0 - 2.0 * bnc[:, lanes].astype(f32)
        rel = (cells[:, lanes] + SHIFT * bnc[:, lanes] - base).astype(f32)
        zero = jnp.zeros_like(rel)
        data = jnp.concatenate(
            [pos[:, lanes], amp[0:1, lanes] * flip, amp[1:2, lanes] * flip, rel] + [zero] * 4, 0
        )
        return jnp.concatenate(list(split3(data)) + [jnp.zeros_like(data)], 0).astype(bf16)

    def pick(c, first):
        slots = lax.broadcasted_iota(jnp.int32, (SLOTS, 128), 0).astype(f32) + first
        hot = jnp.concatenate(
            [jnp.where(rank[8 * c + j : 8 * c + j + 1] == slots, 1.0, 0.0) for j in range(8)], 1
        ).astype(bf16)
        return lax.dot_general(
            hot, values(c), (((1,), (1,)), ((), ())), preferred_element_type=f32
        )

    start = 0
    for c in range(chunks):
        buf[pl.ds(start, SLOTS), 0:32] = pick(c, 0.0)
        start = start + counts[c]
    most = functools.reduce(jnp.maximum, counts)

    @pl.when(most > SLOTS)
    def _():
        begin = 0
        for c in range(chunks):

            @pl.loop(0, (counts[c] + SLOTS - 1) // SLOTS)
            def _(i):
                first = (i * SLOTS).astype(f32)
                buf[pl.ds(begin + i * SLOTS, SLOTS), 0:32] = pick(c, first)

            begin = begin + counts[c]

    buf[pl.ds(start, AHEAD), :] = jnp.zeros((AHEAD, 128), f32)

    def data(first, width):
        cols = []
        for h in range(width // 128):
            t = buf[pl.ds(first + h * 128, 128), :].T
            cols.append(t[0:8] + t[8:16] + t[16:24])
        return jnp.concatenate(cols, 1)

    lead[...] = data(0, AHEAD)
    out[...] = jnp.zeros_like(out)

    @pl.loop(AHEAD // WIDE, (start + WIDE - 1) // WIDE)
    def _(i):
        for lanes, sums in echoes(data(i * WIDE, WIDE), base, span, trig):
            out[:, lanes] += sums


def range_binning(positions, amplitude, cells, bounce, base, span):
    count = positions.shape[0]
    rows = count // 128
    sources = (
        cells.reshape(rows, 128),
        bounce.reshape(rows, 128),
        positions.reshape(1, count),
        amplitude,
        cells.reshape(1, count),
        bounce.reshape(1, count),
    )
    return pl.pallas_call(
        functools.partial(range_bin_kernel, span=span, trig=range_trig_coefs(4)),
        in_specs=[pl.BlockSpec(memory_space=pltpu.SMEM)] + [IN_HBM] * len(sources),
        out_specs=(IN_VMEM, IN_VMEM),
        out_shape=(
            jax.ShapeDtypeStruct((span, 2 * P_SIZE), f32),
            jax.ShapeDtypeStruct((8, AHEAD), f32),
        ),
        scratch_shapes=[pltpu.VMEM(a.shape, a.dtype) for a in sources]
        + [
            pltpu.VMEM((count + SLOTS + AHEAD, 128), f32),
            pltpu.SemaphoreType.DMA((len(sources),)),
        ],
        compiler_params=pltpu.CompilerParams(vmem_limit_bytes=16 << 20),
        name="range_binning",
    )(base.reshape(1), *in_hbm(sources))


def complex_rows(c, s):
    return np.block([[c, s], [-s, c]])


def mid_factors(n_dev, order):
    side = np.arange(BIN_SIDE)
    t = np.arange(STOLT)
    eye = np.eye(GROUP)
    a = -2 * np.pi / STOLT * ((side[:, None] * t[None, :]) % STOLT)
    ta = complex_rows(np.cos(a), np.sin(a))[order]
    a = -2 * np.pi / F_LEN * (side[:, None] * t[None, :])
    wa = np.stack([np.tile(np.cos(a), (GROUP, 1)), np.tile(np.sin(a), (GROUP, 1))])
    a = -2 * np.pi / BIN_SIDE * ((side[:, None] * side[None, :]) % BIN_SIDE)
    c, s = np.kron(eye, np.cos(a)), np.kron(eye, np.sin(a))
    tb = complex_rows(c, s).T
    blk = np.arange(BLOCKS)
    a = 2 * np.pi / BLOCKS * ((blk[:, None] * blk[None, :]) % BLOCKS)
    c, s = np.kron(eye, np.cos(a)), np.kron(eye, np.sin(a))
    tc = complex_rows(c, s)
    a = 2 * np.pi / F_LEN * (t[:, None] * blk[None, :])
    wc = np.stack([np.tile(np.cos(a), (1, GROUP)), np.tile(np.sin(a), (1, GROUP))])
    a = 2 * np.pi / STOLT * ((t[:, None] * t[None, :]) % STOLT)
    td = complex_rows(np.cos(a), np.sin(a)).T / F_LEN
    td = td.reshape(2, n_dev, STOLT // n_dev, 2 * STOLT).transpose(1, 0, 2, 3)
    return ta, wa.astype(np.float32), tb, tc, wc.astype(np.float32), td


def mid_tables(n_dev, order):
    ta, wa, tb, tc, wc, td = mid_factors(n_dev, order)
    td = td.reshape(2 * STOLT, 2 * STOLT)
    return np_split(ta), wa, np_split(tb), np_split(tc), wc, np_split(td)


def core_tables(n_dev, order):
    ta, wa, tb, tc, wc, td = mid_factors(n_dev, order)
    td = td.reshape(n_dev, 2, -1, GROUP, 2 * STOLT).transpose(0, 2, 1, 3, 4)
    td = td.reshape(2 * STOLT, 2 * STOLT)
    forward, inverse = quarter_tables()
    return (
        np_split(forward),
        np_split(ta),
        wa,
        np_split(tb),
        np_split(tc),
        wc,
        np_split(td),
    ), np_split(inverse)


def mid_kernel(
    x, cos_p, sin_p, hot, kind, bank_hi, bank_lo, ta, wa, tb, tc, wc, td, out, xs, os, *, subs
):
    n = GROUP * BLOCKS
    step = pl.program_id(0)
    groups = x.shape[1]

    @pl.when(step == 0)
    def _():
        for g in range(groups):
            xs[g] = x[:, g, :]

    parts_hi, parts_lo = [], []
    for g in range(subs):
        lanes = slice(g * n, (g + 1) * n)
        y = dots(split(xs[step * subs + g]), (ta[0], ta[1]), ((0,), (0,)))
        yr, yi = y[:, :STOLT], y[:, STOLT:]
        y = jnp.concatenate([yr * wa[0] - yi * wa[1], yr * wa[1] + yi * wa[0]], 0)
        z = dots((tb[0], tb[1]), split(y), ((1,), (0,)))
        zr, zi = z[:n], z[n:]
        cp, sp = cos_p[lanes], sin_p[lanes]
        z = jnp.concatenate([zr * cp - zi * sp, zr * sp + zi * cp], 1)
        hi, lo = split(z)
        picked = jnp.dot(
            hot[g], jnp.concatenate([hi, lo], 1), preferred_element_type=f32
        ).astype(bf16)
        first, second = picked[:n], picked[n:]
        for c in range(2):
            for base, keep in ((0, parts_hi), (2 * STOLT, parts_lo)):
                cut = slice(base + c * STOLT, base + (c + 1) * STOLT)
                keep.append(jnp.concatenate([first[:, cut], second[:, cut]], 1))
    ghi = jnp.concatenate(parts_hi, 0)
    glo = jnp.concatenate(parts_lo, 0)
    kinds = kind[...].reshape(subs * 2 * n, 1)
    kinds = jnp.broadcast_to(kinds, (subs * 2 * n, STOLT))
    acc = jnp.zeros((subs * 2 * n, STOLT), f32)
    for k in range(0, bank_hi.shape[0], 2):
        khi = jnp.concatenate([bank_hi[k], bank_hi[k + 1]], 1)
        klo = jnp.concatenate([bank_lo[k], bank_lo[k + 1]], 1)
        r = dots((ghi, glo), (khi, klo), ((1,), (0,)))
        for half in range(2):
            acc = jnp.where(kinds == k + half, r[:, half * STOLT : (half + 1) * STOLT], acc)
    for g in range(subs):
        s = acc[g * 2 * n : (g + 1) * 2 * n]
        y = dots(split(s), (tc[0], tc[1]), ((0,), (0,)))
        yr, yi = y[:, :n], y[:, n:]
        y = jnp.concatenate([yr * wc[0] - yi * wc[1], yr * wc[1] + yi * wc[0]], 0)
        os[step * subs + g] = dots((td[0], td[1]), split(y), ((1,), (0,)))

    @pl.when(step == pl.num_programs(0) - 1)
    def _():
        for g in range(groups):
            out[:, g, :] = os[g]


def middle(x, cos_p, sin_p, hot, kind, bank_hi, bank_lo, tables):
    groups = x.shape[1]
    subs = min(4, groups)
    n = GROUP * BLOCKS
    whole = lambda a: pl.BlockSpec(a.shape, lambda i: (0,) * a.ndim)
    return pl.pallas_call(
        functools.partial(mid_kernel, subs=subs),
        grid=(groups // subs,),
        in_specs=[
            whole(x),
            pl.BlockSpec((subs * n, STOLT), lambda i: (i, 0)),
            pl.BlockSpec((subs * n, STOLT), lambda i: (i, 0)),
            pl.BlockSpec((subs, 2 * n, n), lambda i: (i, 0, 0)),
            pl.BlockSpec((subs, 2 * n, 1), lambda i: (i, 0, 0)),
            whole(bank_hi),
            whole(bank_lo),
        ]
        + [whole(t) for t in tables],
        out_specs=pl.BlockSpec((2 * STOLT, groups, n), lambda i: (0, 0, 0)),
        out_shape=jax.ShapeDtypeStruct((2 * STOLT, groups, n), f32),
        scratch_shapes=[
            pltpu.VMEM((groups, x.shape[0], n), f32),
            pltpu.VMEM((groups, 2 * STOLT, n), f32),
        ],
        name="middle",
    )(x, cos_p, sin_p, hot, kind, bank_hi, bank_lo, *tables)


def quarter_tables():
    q = P_SIZE // 4
    m = np.arange(q)
    fwd, inv = [], []
    for low in range(4):
        a = 2 * np.pi / P_SIZE * (((4 * m[:, None] + low) * m[None, :]) % P_SIZE)
        turn = a.reshape(-1, 2, q).transpose(1, 0, 2).reshape(q, q)
        fwd.append(np.concatenate([np.cos(turn), np.sin(turn)], 0))
        inv.append(np.concatenate([np.cos(a.T), np.sin(a.T)], 0) / P_SIZE)
    return np.stack(fwd), np.stack(inv)


def swap_blocks(arrays):
    count = len(arrays)
    lanes = arrays[0].shape[-1]
    size = lanes // count
    block = lax.broadcasted_iota(jnp.int32, arrays[0].shape, 1) // size
    outs = []
    for b in range(count):
        acc = None
        for a in range(count):
            shift = (a - b) % count * size
            moved = pltpu.roll(arrays[a], shift, 1) if shift else arrays[a]
            acc = moved if acc is None else jnp.where(block == a, moved, acc)
        outs.append(acc)
    return outs


def core_kernel(*refs, n_pulse, n_scat, subs, trig, trig_low):
    lead, partial = refs[:2]
    sources = refs[2:12]
    out = refs[12]
    local = refs[13:23]
    steps_in, kinds_in, bank, table, ta, wa, tb, tc, wc, td = local
    binned, peer, spec, x, hot, kind, banks, os, twin_os, *twin_in = refs[23:34]
    (
        load, own_store, pair_send, pair_recv, near_send, near_recv, far_send, far_recv,
        twin_send, twin_recv, half_send,
    ) = refs[34:]
    n_dev = n_pulse * n_scat
    pulse = lax.axis_index("pulse")
    scat = lax.axis_index("scat")
    me = pulse * n_scat + scat
    half = peer.shape[0]
    lanes = 2 * half
    size = P_SIZE // 4
    n = GROUP * BLOCKS
    groups = os.shape[1] + SHARED
    pieces = groups // subs
    reach = n_pulse // 2
    side = lax.div(pulse, reach)
    twin = lax.rem(pulse + reach, n_pulse) * n_scat + scat
    quads = lanes // BIN_SIDE
    unit = subs * quads
    per = os.shape[2]
    moves = [(a, b) for a in range(n_pulse) for b in range(n_scat) if (a, b) != (0, 0)]
    moves.sort(key=lambda m: (-min(m[0], n_pulse - m[0]), m))

    def other(a, b):
        return lax.rem(pulse + a, n_pulse), lax.rem(scat + b, n_scat)

    barrier = pltpu.get_barrier_semaphore()
    for a, b in moves:
        p, c = other(a, b)
        pl.semaphore_signal(
            barrier, inc=1, device_id={"pulse": p, "scat": c}, device_id_type=MESH
        )
    keep = pl.ds(pl.multiple_of(scat * half, half), half)
    give = pl.ds(pl.multiple_of((1 - scat) * half, half), half)
    loads = [
        pltpu.make_async_copy(src, dst, load.at[i])
        for i, (src, dst) in enumerate(zip(sources, local))
    ]
    for copy in loads:
        copy.start()
    for cut, sums in echoes(lead[...], pulse * 2 * half, 2 * half, trig_low):
        binned[:, cut] = partial[:, cut] + sums
    pl.semaphore_wait(barrier, n_dev - 1)

    pair = pltpu.make_async_remote_copy(
        src_ref=binned.at[give, :],
        dst_ref=peer,
        send_sem=pair_send,
        recv_sem=pair_recv,
        device_id={"pulse": pulse, "scat": 1 - scat},
        device_id_type=MESH,
    )
    pair.start()
    metas = []
    for i in range(2):
        loads[i].wait()
        copy = pltpu.make_async_remote_copy(
            src_ref=local[i],
            dst_ref=twin_in[i],
            send_sem=twin_send.at[i],
            recv_sem=twin_recv.at[i],
            device_id={"pulse": lax.rem(pulse + reach, n_pulse), "scat": scat},
            device_id_type=MESH,
        )
        copy.start()
        metas.append(copy)
    loads[3].wait()
    pair.wait()

    quarters = []
    for q in range(4):
        pair_of = []
        for c in range(2):
            cut = slice(c * P_SIZE + q * size, c * P_SIZE + (q + 1) * size)
            pair_of.append(binned[keep, cut] + peer[:, cut])
        quarters.append(pair_of)
    (r0, i0), (r1, i1), (r2, i2), (r3, i3) = quarters
    sr, si, dr, di = r0 + r2, i0 + i2, r0 - r2, i0 - i2
    tr, ti, er, ei = r1 + r3, i1 + i3, r1 - r3, i1 - i3
    mixed = (
        (sr + tr, si + ti),
        (dr + ei, di - er),
        (sr - tr, si - ti),
        (dr - ei, di + er),
    )
    low = lax.broadcasted_iota(jnp.int32, (size, lanes), 1) < half
    rows = []
    for k in range(4):
        g = product(
            joined(table[0, k], table[1, k], 1),
            triple(jnp.concatenate(mixed[k], 0), 1),
            ((1,), (1,)),
        )
        turned = pltpu.roll(g[size:], half, 1)
        rows.append(g[:size] + jnp.where(low, turned, -turned))
    for q, z in enumerate(swap_blocks(rows)):
        for h in range(subs):
            spec[pl.ds(q * subs + h, size // subs, stride=unit), :] = z[
                h * (size // subs) : (h + 1) * (size // subs)
            ]

    def piece(dev, i):
        return pl.ds(pl.multiple_of((dev * pieces + i) * unit, unit), unit)

    def source(p, c, i):
        if i < pieces:
            return piece(p * n_scat + c, i)
        return piece(lax.rem(p + reach, n_pulse) * n_scat + c, pieces - 1)

    own = pl.ds(pl.multiple_of(me * unit, unit), unit)
    for i in range(pieces + 1):
        for j, (a, b) in enumerate(moves):
            p, c = other(a, b)
            pltpu.make_async_remote_copy(
                src_ref=spec.at[source(p, c, i), :],
                dst_ref=x.at[i, own, :],
                send_sem=near_send.at[j],
                recv_sem=near_recv.at[i, me],
                device_id={"pulse": p, "scat": c},
                device_id_type=MESH,
            ).start()
    for i in range(pieces + 1):
        x[i, own, :] = spec[source(pulse, scat, i), :]

    for i in (2, 4, 5, 6, 7, 8, 9):
        loads[i].wait()
    for copy in metas:
        copy.wait()
    block = lax.broadcasted_iota(jnp.int32, (n, STOLT), 0)
    lane = lax.broadcasted_iota(jnp.int32, (n, STOLT), 1)
    spot = lane.astype(f32)
    above = (block // BLOCKS * BLOCKS).astype(f32)
    flat = []
    for i in range(2):
        both = [
            jnp.concatenate([ref[pl.ds(j, groups, stride=GROUP), :] for j in range(GROUP)], 1)
            for ref in (local[i], twin_in[i])
        ]
        flat.append(jnp.concatenate([both[0], both[1][groups - subs :]], 0))
    for g in range(groups + subs):
        first = jnp.broadcast_to(flat[0][g : g + 1].astype(f32), (n, n)).T + above
        hot[g, :n] = jnp.where(first == spot, 1.0, 0.0).astype(bf16)
        hot[g, n:] = jnp.where(first + 1.0 == spot, 1.0, 0.0).astype(bf16)
        kind[g] = jnp.broadcast_to(flat[1][g : g + 1], (8, n))
    for k in range(bank.shape[0]):
        turned = jnp.concatenate([bank[k, :STOLT].T, bank[k, STOLT:].T], 1)
        hi, lo = split(turned)
        banks[k * STOLT : (k + 1) * STOLT] = jnp.concatenate([hi, hi, lo], 1)

    cols = (lane + (block % BLOCKS) * STOLT).astype(f32)
    kr = 4.0 * np.pi / 3e8 * (9.6e9 + (cols - F_LEN // 2) * (1.5e8 / F_LEN))

    def phase(owner, g):
        row = owner * (groups * GROUP) + g * GROUP + block // BLOCKS
        centered = lax.rem(row + P_SIZE // 2, P_SIZE) - P_SIZE // 2
        along = 2.0 * np.pi / (P_SIZE * SPACING) * centered.astype(f32)
        squared = along * along
        depth = NEAR + B // 2
        theta = -depth * squared / (jnp.sqrt(kr * kr - squared) + kr)
        whole = jnp.round(theta * (0.5 / np.pi))
        for part in turn_parts():
            theta = theta - whole * part
        r = theta * (0.5 / np.pi)
        u = r * r
        sn = r * horner(u, trig[0])
        cs = horner(u, trig[1])
        return 1.0 - 2.0 * sn * sn, 2.0 * sn * cs

    def ranged(slot, owner, g, cut):
        i, h = lax.div(slot, subs), lax.rem(slot, subs)
        cp, sp = phase(owner, g)
        rows_in = x[i, pl.ds(h, n_dev * quads, stride=subs), :]
        y = product(triple(rows_in, 0), joined(ta[0], ta[1], 0), ((0,), (0,)))
        yr, yi = y[:, :STOLT], y[:, STOLT:]
        y = jnp.concatenate([yr * wa[0] - yi * wa[1], yr * wa[1] + yi * wa[0]], 0)
        z = product(joined(tb[0], tb[1], 1), triple(y, 0))
        zr, zi = z[:n], z[n:]
        z = jnp.concatenate([zr * cp - zi * sp, zr * sp + zi * cp], 1)
        picked = product(hot[slot], jnp.concatenate(split(z), 1)).astype(bf16)
        first, second = picked[:n], picked[n:]
        parts = []
        for base in (0, 2 * STOLT):
            cuts = [slice(base + c * STOLT, base + (c + 1) * STOLT) for c in range(2)]
            parts.append(
                jnp.concatenate(
                    [jnp.concatenate([first[:, v], second[:, v]], 1) for v in cuts], 0
                )
            )
        ghi, glo = parts
        windows = jnp.concatenate([ghi, glo, ghi], 1)
        kinds = jnp.concatenate([kind[slot, 0:1]] * 2, 1)
        acc = jnp.zeros((STOLT, 2 * n), f32)
        for first in range(0, banks.shape[0], STREAM):
            r = product(banks[first : first + STREAM], windows, ((1,), (1,)))
            for v in range(STREAM // STOLT):
                k = first // STOLT + v
                acc = jnp.where(kinds == k, r[v * STOLT : (v + 1) * STOLT], acc)
        y = product(triple(acc, 1), joined(tc[0], tc[1], 0))
        yr, yi = y[:, :n], y[:, n:]
        y = jnp.concatenate([yr * wc[0] - yi * wc[1], yr * wc[1] + yi * wc[0]], 0)
        z = product(joined(td[0, cut, :], td[1, cut, :], 1), triple(y, 0))
        return z.reshape(-1, per, n)

    def arrived(i):
        for a, b in moves:
            p, c = other(a, b)
            src = p * n_scat + c
            here = pl.ds(pl.multiple_of(src * unit, unit), unit)
            pltpu.make_async_copy(
                x.at[i, here, :], x.at[i, here, :], near_recv.at[i, src]
            ).wait()

    def step(g, carry):
        @pl.when(lax.rem(g, subs) == 0)
        def _():
            arrived(lax.div(g, subs))

        os[:, g] = ranged(g, me, g, slice(None))
        for j, (a, b) in enumerate(moves):
            p, c = other(a, b)
            pltpu.make_async_remote_copy(
                src_ref=os.at[p * n_scat + c, g],
                dst_ref=out.at[me, g],
                send_sem=far_send.at[j],
                recv_sem=far_recv.at[me],
                device_id={"pulse": p, "scat": c},
                device_id_type=MESH,
            ).start()
        return carry

    close = [(a, b) for a in range(reach) for b in range(n_scat) if (a, b) != (0, 0)]
    within = pulse - side * reach

    def beside(a, b):
        return lax.rem(within + a, reach), lax.rem(scat + b, n_scat)

    part = 2 * STOLT // 2
    served = pl.ds(pl.multiple_of(side * part, part), part)

    lax.fori_loop(0, groups - SHARED, step, 0)
    if SHARED == subs:
        arrived(pieces - 1)
    arrived(pieces)

    def half_step(t, carry):
        v, h = lax.div(t, SHARED), lax.rem(t, SHARED)
        owner = lax.rem(pulse + v * reach, n_pulse) * n_scat + scat
        g = groups - SHARED + h
        twin_os[v, :, h] = ranged(g + v * subs, owner, g, served)
        for j, (a, b) in enumerate(close):
            p, c = beside(a, b)
            pltpu.make_async_remote_copy(
                src_ref=twin_os.at[v, p * n_scat + c, h],
                dst_ref=out.at[owner, g],
                send_sem=half_send.at[j],
                recv_sem=far_recv.at[owner],
                device_id={"pulse": side * reach + p, "scat": c},
                device_id_type=MESH,
            ).start()
        return carry

    lax.fori_loop(0, 2 * SHARED, half_step, 0)
    first, last = pl.ds(0, groups - SHARED), pl.ds(groups - SHARED, SHARED)
    here = within * n_scat + scat
    stores = [
        pltpu.make_async_copy(src, dst, own_store.at[i])
        for i, (src, dst) in enumerate(
            (
                (os.at[me], out.at[me, first]),
                (twin_os.at[0, here], out.at[me, last]),
                (twin_os.at[1, here], out.at[twin, last]),
            )
        )
    ]
    for copy in stores:
        copy.start()
    for copy in stores:
        copy.wait()
    for j, (a, b) in enumerate(close):
        whole = os.at[0, pl.ds(0, 2 * SHARED)]
        pltpu.make_async_copy(whole, whole, half_send.at[j]).wait()
    for j, (a, b) in enumerate(moves):
        p, c = other(a, b)
        src = p * n_scat + c
        whole = spec.at[pl.ds(0, (pieces + 1) * unit), :]
        pltpu.make_async_copy(whole, whole, near_send.at[j]).wait()
        pltpu.make_async_copy(os.at[src], os.at[src], far_send.at[j]).wait()
        whole = out.at[src, first] if (a, b) == (reach, 0) else out.at[src]
        pltpu.make_async_copy(whole, whole, far_recv.at[src]).wait()


def turn_parts():
    parts, rest = [], 2.0 * np.pi
    for bits in (10, 22, 60):
        scale = 2.0**bits
        part = float(np.float32(np.round(rest * scale) / scale))
        parts.append(part)
        rest -= part
    return parts


def core(partial, lead, steps_in, kinds_in, bank, tables, n_pulse, n_scat):
    n_dev = n_pulse * n_scat
    groups = steps_in.shape[0] // GROUP
    subs = 2
    n = GROUP * BLOCKS
    span, width = partial.shape
    half = span // n_scat
    quads = 2 * half // BIN_SIDE
    kernels = bank.shape[0]
    per = 2 * STOLT // n_dev
    sources = (steps_in, kinds_in, bank, *tables)
    dma = pltpu.SemaphoreType.DMA
    return pl.pallas_call(
        functools.partial(
            core_kernel,
            n_pulse=n_pulse,
            n_scat=n_scat,
            subs=subs,
            trig=range_trig_coefs(5),
            trig_low=range_trig_coefs(4),
        ),
        in_specs=[IN_VMEM] * 2 + [IN_HBM] * len(sources),
        out_specs=pl.BlockSpec(memory_space=pl.ANY),
        out_shape=jax.ShapeDtypeStruct((n_dev, groups, per, n), f32),
        scratch_shapes=[pltpu.VMEM(a.shape, a.dtype) for a in sources]
        + [
            pltpu.VMEM((span, width), f32),
            pltpu.VMEM((half, width), f32),
            pltpu.VMEM((n_dev * groups * quads, n), f32),
            pltpu.VMEM((groups // subs + 1, n_dev * subs * quads, n), f32),
            pltpu.VMEM((groups + subs, 2 * n, n), bf16),
            pltpu.VMEM((groups + subs, 8, n), jnp.int32),
            pltpu.VMEM((kernels * STOLT, 6 * STOLT), bf16),
            pltpu.VMEM((n_dev, groups - SHARED, per, n), f32),
            pltpu.VMEM((2, n_dev // 2, SHARED, per, n), f32),
            pltpu.VMEM(steps_in.shape, steps_in.dtype),
            pltpu.VMEM(kinds_in.shape, kinds_in.dtype),
            dma((len(sources),)),
            dma((3,)),
            dma,
            dma,
            dma((n_dev,)),
            dma((groups // subs + 1, n_dev)),
            dma((n_dev,)),
            dma((n_dev,)),
            dma((2,)),
            dma((2,)),
            dma((n_dev // 2,)),
        ],
        compiler_params=pltpu.CompilerParams(
            collective_id=0, has_side_effects=True, vmem_limit_bytes=24 << 20
        ),
        name="core",
    )(lead, partial, *in_hbm(sources))


def image_kernel(x, table, out, done, sems):
    devs, kh, per, lanes = x.shape
    size = P_SIZE // 4
    copies = []
    for h in range(per // (2 * GROUP)):
        columns = [[] for _ in range(4)]
        for c in range(2):
            first = (2 * h + c) * GROUP
            tiles = [x[:, :, first + j, :].reshape(devs * kh, lanes) for j in range(4)]
            for k, z in enumerate(swap_blocks(tiles)):
                columns[k].append(z)
        v = []
        for k in range(4):
            g = product(
                joined(table[0, k], table[1, k], 1), triple(jnp.concatenate(columns[k], 1), 0)
            )
            cos_g, sin_g = g[:size], g[size:]
            v.append((cos_g[:, :lanes] - sin_g[:, lanes:], cos_g[:, lanes:] + sin_g[:, :lanes]))
        (r0, i0), (r1, i1), (r2, i2), (r3, i3) = v
        sr, si, dr, di = r0 + r2, i0 + i2, r0 - r2, i0 - i2
        tr, ti, er, ei = r1 + r3, i1 + i3, r1 - r3, i1 - i3
        mixed = (
            (sr + tr, si + ti),
            (dr - ei, di + er),
            (sr - tr, si - ti),
            (dr + ei, di - er),
        )
        for q in range(4):
            for c in range(2):
                done[h, c, q * size : (q + 1) * size, :] = mixed[q][c]
        copy = pltpu.make_async_copy(
            done.at[h], out.at[:, :, pl.ds(h * lanes, lanes)], sems.at[h]
        )
        copy.start()
        copies.append(copy)
    for copy in copies:
        copy.wait()


def reference_phase(row_ids, cols):
    centered = (row_ids + P_SIZE // 2) % P_SIZE - P_SIZE // 2
    along_k = 2.0 * jnp.pi / (P_SIZE * SPACING) * centered.astype(f32)
    kr = 4.0 * jnp.pi / 3e8 * (9.6e9 + (cols.astype(f32) - F_LEN // 2) * (1.5e8 / F_LEN))
    squared = along_k * along_k
    depth = NEAR + B // 2
    return (
        -depth
        * squared[:, None]
        / (jnp.sqrt(kr[None, :] * kr[None, :] - squared[:, None]) + kr[None, :])
    )


def on_device(positions, amplitude, range_cells, bounce, stolt_block, kernel_choice, kernel_bank):
    n_pulse = lax.axis_size("pulse")
    n_scat = lax.axis_size("scat")
    n_dev = n_pulse * n_scat
    pulse_here = lax.axis_index("pulse")
    scat_here = lax.axis_index("scat")
    pulses = P_SIZE // n_pulse
    rows = P_SIZE // n_dev
    width = F_LEN // n_dev
    groups = rows // GROUP
    n = GROUP * BLOCKS
    bins_scat = B // n_scat
    bins_here = bins_scat // n_pulse

    per = STOLT // n_dev
    span = B // n_pulse
    packed = (
        span == 128
        and n_scat == 2
        and per % 4 == 0
        and groups % 8 == 0
        and positions.shape[0] % CHUNK == 0
    )
    if packed:
        partial, lead = range_binning(
            positions, amplitude, range_cells, bounce, pulse_here * span, span
        )
        local = bins_here // BIN_SIDE
        i, s, c, l = np.meshgrid(
            np.arange(n_pulse), np.arange(n_scat), np.arange(2), np.arange(local), indexing="ij"
        )
        order = (c * BIN_SIDE + (i * n_scat + s) * local + l).reshape(-1)
        tables, backward = core_tables(n_dev, order)
        tables = tuple(jnp.asarray(t) for t in tables)
        columns = core(
            partial, lead, stolt_block, kernel_choice, kernel_bank, tables, n_pulse, n_scat
        )
        return pl.pallas_call(
            image_kernel,
            in_specs=[IN_VMEM, IN_VMEM],
            out_specs=pl.BlockSpec(memory_space=pl.ANY),
            out_shape=jax.ShapeDtypeStruct((2, P_SIZE, width), f32),
            scratch_shapes=[
                pltpu.VMEM((width // n, 2, P_SIZE, n), f32),
                pltpu.SemaphoreType.DMA((width // n,)),
            ],
            compiler_params=pltpu.CompilerParams(vmem_limit_bytes=16 << 20),
            name="image",
        )(columns, jnp.asarray(backward))

    ids = jnp.arange(GROUP, dtype=jnp.int32)[None, :, None] * BLOCKS
    first = stolt_block.reshape(groups, GROUP, BLOCKS) + ids
    pick = jnp.stack([first, first + 1], 1).reshape(groups, 2 * n, 1)
    hot = (pick == jnp.arange(n, dtype=jnp.int32)[None, None, :]).astype(bf16)
    kind = jnp.stack([kernel_choice.reshape(groups, n)] * 2, 1).reshape(groups, 2 * n, 1)
    bank_hi = lax.reduce_precision(kernel_bank, 8, 7)
    bank_lo = (kernel_bank - bank_hi).astype(bf16)
    bank_hi = bank_hi.astype(bf16)
    row_ids = (pulse_here * n_scat + scat_here) * rows + jnp.arange(rows, dtype=jnp.int32)
    theta = reference_phase(row_ids, jnp.arange(F_LEN, dtype=jnp.int32))
    theta = theta.reshape(rows * BLOCKS, STOLT)
    cos_p, sin_p = jnp.cos(theta), jnp.sin(theta)

    partial = binning(positions, amplitude, range_cells, bounce, pulse_here * pulses, pulses)
    partial = partial.reshape(n_scat, bins_scat, 2 * pulses)
    binned = lax.dynamic_index_in_dim(partial, scat_here, 0, keepdims=False)
    for shift in range(1, n_scat):
        other = lax.dynamic_index_in_dim(
            partial, (scat_here + shift) % n_scat, 0, keepdims=False
        )
        ring = [(i, (i + shift) % n_scat) for i in range(n_scat)]
        binned = binned + lax.ppermute(other, "scat", ring)
    turned = lax.all_to_all(
        binned.reshape(n_pulse, bins_here, 2 * pulses), "pulse", 0, 0, tiled=True
    )
    turned = turned.reshape(n_pulse, bins_here, 2, pulses).transpose(0, 3, 2, 1)
    turned = turned.reshape(P_SIZE, 2 * bins_here)
    k = np.arange(P_SIZE)
    angle = 2 * np.pi / P_SIZE * ((k[:, None] * k[None, :]) % P_SIZE)
    az = jnp.asarray(np.concatenate([np.cos(angle), np.sin(angle)], 0), f32)
    product = jnp.dot(az, turned, precision=HIGH, preferred_element_type=f32)
    pc, ps = product[:P_SIZE], product[P_SIZE:]
    spectrum = pc + jnp.concatenate([ps[:, bins_here:], -ps[:, :bins_here]], 1)
    az_rows = lax.all_to_all(
        spectrum.reshape(n_dev, rows, 2 * bins_here), ("pulse", "scat"), 0, 0, tiled=True
    )
    x = az_rows.reshape(n_pulse, n_scat, rows, 2, bins_here).transpose(3, 1, 0, 4, 2)
    x = x.reshape(2, BIN_SIDE, BIN_SIDE, rows).transpose(0, 1, 3, 2)
    x = x.reshape(2 * BIN_SIDE, groups, n)
    order = np.arange(2 * BIN_SIDE)

    tables = tuple(jnp.asarray(t) for t in mid_tables(n_dev, order))
    ranged = middle(x, cos_p, sin_p, hot, kind, bank_hi, bank_lo, tables)
    columns = lax.all_to_all(
        ranged.reshape(n_dev, 2 * per, rows * BLOCKS), ("pulse", "scat"), 0, 0, tiled=True
    )
    columns = columns.reshape(n_dev, 2, per, rows, BLOCKS).transpose(0, 3, 1, 2, 4)
    columns = columns.reshape(P_SIZE, 2 * width)
    final = jnp.dot(az, columns, precision=HIGH, preferred_element_type=f32)
    fc, fs = final[:P_SIZE], final[P_SIZE:]
    re = (fc[:, :width] - fs[:, width:]) / P_SIZE
    im = (fc[:, width:] + fs[:, :width]) / P_SIZE
    return jnp.stack([re, im])


def solution(mesh):
    placed = (
        P(("scene", "scat")),
        P(None, ("scene", "scat")),
        P(("scene", "scat")),
        P(("scene", "scat")),
        P(("pulse", "scat"), None),
        P(("pulse", "scat"), None),
        P(),
    )
    return jax.shard_map(
        on_device,
        mesh=mesh,
        in_specs=placed,
        out_specs=P(None, "scene", ("pulse", "scat")),
        check_vma=False,
    )
```

```python
import functools

import jax
import jax.numpy as jnp
import numpy as np
from jax import lax
from jax.experimental import pallas as pl
from jax.experimental.pallas import tpu as pltpu
from jax.sharding import PartitionSpec as P

P_SIZE = 512
F_LEN = 4096
B = 1024
SHIFT = 16
STOLT = 128
BLOCKS = 32
SPACING = 2.0
NEAR = 700000.0
BIN_SIDE = 32
GROUP = 4
CHUNK = 1024
SLOTS = 192
WIDE = 128
AHEAD = 1024
SHARED = 1
STREAM = 512
HIGH = lax.Precision.HIGH
MESH = pl.DeviceIdType.MESH
IN_HBM = pl.BlockSpec(memory_space=pltpu.HBM)
IN_VMEM = pl.BlockSpec(memory_space=pltpu.VMEM)
f32 = jnp.float32
bf16 = jnp.bfloat16


def trig_coefs():
    x = np.cos(np.pi * (np.arange(400) + 0.5) / 400) * 0.5
    u = x * x
    s = np.polynomial.chebyshev.Chebyshev.fit(u, np.sin(np.pi * x) / x, 5).convert(
        kind=np.polynomial.Polynomial
    )
    c = np.polynomial.chebyshev.Chebyshev.fit(u, np.cos(np.pi * x), 5).convert(
        kind=np.polynomial.Polynomial
    )
    return [float(v) for v in s.coef], [float(v) for v in c.coef]


def horner(u, coefs):
    acc = jnp.full_like(u, coefs[-1])
    for c in coefs[-2::-1]:
        acc = acc * u + c
    return acc


def split(x):
    hi = x.astype(bf16)
    lo = (x - hi.astype(f32)).astype(bf16)
    return hi, lo


def np_split(x):
    x = np.asarray(x, np.float64)
    hi = np.asarray(x, jnp.bfloat16)
    lo = np.asarray(x - hi.astype(np.float64), jnp.bfloat16)
    return np.stack([hi, lo])


def dots(a, b, dims):
    d = functools.partial(
        lax.dot_general, dimension_numbers=(dims, ((), ())), preferred_element_type=f32
    )
    return d(a[0], b[0]) + (d(a[0], b[1]) + d(a[1], b[0]))


def in_hbm(arrays):
    return [pltpu.with_memory_space_constraint(a, pltpu.HBM) for a in arrays]


def joined(hi, lo, axis):
    return jnp.concatenate([hi, hi, lo], axis)


def triple(x, axis):
    hi, lo = split(x)
    return jnp.concatenate([hi, lo, hi], axis)


def product(a, b, dims=((1,), (0,))):
    return lax.dot_general(a, b, (dims, ((), ())), preferred_element_type=f32)


def bin_kernel(pulse_base, pos, amp, tgt, bnc, out, acc, *, pulses, sin_c, cos_c):
    step = pl.program_id(0)
    width = pos.shape[1]

    @pl.when(step == 0)
    def _():
        acc[...] = jnp.zeros_like(acc)

    base = pulse_base[0]
    ids = base + lax.broadcasted_iota(jnp.int32, (pulses, width), 0)
    along = (ids.astype(f32) - P_SIZE // 2) * SPACING
    target = tgt[...] + SHIFT * bnc[...]
    slant = NEAR + target.astype(f32)
    offset = along - pos[...]
    square = offset * offset
    excess = square / (jnp.sqrt(slant * slant + square) + slant)
    halves = excess * -128.0
    whole = jnp.round(halves)
    r = halves - whole
    u = r * r
    odd = whole - 2.0 * jnp.floor(whole * 0.5)
    sign = 1.0 - 2.0 * odd
    sin_p = sign * r * horner(u, sin_c)
    cos_p = sign * horner(u, cos_c)
    flip = 1.0 - 2.0 * bnc[...].astype(f32)
    are = flip * amp[0:1]
    aim = flip * amp[1:2]
    re = are * cos_p - aim * sin_p
    im = are * sin_p + aim * cos_p
    steer = jnp.concatenate([re, im], 0)
    hi, lo = split(steer)
    rhs = jnp.concatenate([hi, lo], 0)
    bins = lax.broadcasted_iota(jnp.int32, (B, width), 0)
    hot = jnp.where(bins == target, 1.0, 0.0).astype(bf16)
    acc[...] += lax.dot_general(
        hot, rhs, (((1,), (1,)), ((), ())), preferred_element_type=f32
    )

    @pl.when(step == pl.num_programs(0) - 1)
    def _():
        out[...] = acc[:, : 2 * pulses] + acc[:, 2 * pulses :]


def binning(positions, amplitude, cells, bounce, pulse_base, pulses):
    count = positions.shape[0]
    width = min(2048, count)
    sin_c, cos_c = trig_coefs()
    row = lambda n: pl.BlockSpec((n, width), lambda i: (0, i))
    return pl.pallas_call(
        functools.partial(bin_kernel, pulses=pulses, sin_c=sin_c, cos_c=cos_c),
        grid=(count // width,),
        in_specs=[pl.BlockSpec(memory_space=pltpu.SMEM), row(1), row(2), row(1), row(1)],
        out_specs=pl.BlockSpec((B, 2 * pulses), lambda i: (0, 0)),
        out_shape=jax.ShapeDtypeStruct((B, 2 * pulses), f32),
        scratch_shapes=[pltpu.VMEM((B, 4 * pulses), f32)],
        name="binning",
    )(
        pulse_base.reshape(1),
        positions.reshape(1, count),
        amplitude,
        cells.reshape(1, count),
        bounce.reshape(1, count),
    )


def range_trig_coefs(degree):
    x = np.cos(np.pi * (np.arange(400) + 0.5) / 400) * 0.5
    u = x * x
    fit = lambda y: np.polynomial.chebyshev.Chebyshev.fit(u, y, degree).convert(
        kind=np.polynomial.Polynomial
    )
    return [float(v) for v in fit(np.sin(np.pi * x) / x).coef], [
        float(v) for v in fit(np.cos(np.pi * x)).coef
    ]


def split3(x):
    hi = x.astype(bf16).astype(f32)
    rest = x - hi
    mid = rest.astype(bf16).astype(f32)
    return hi, mid, rest - mid


def turn(r, trig):
    u = r * r
    sn = r * horner(u, trig[0])
    cs = horner(u, trig[1])
    twice = sn + sn
    return 1.0 - twice * sn, twice * cs


def times(a, b):
    return a[0] * b[0] - a[1] * b[1], a[0] * b[1] + a[1] * b[0]


def echoes(data, base, bins, trig):
    width = data.shape[1]
    chunk = min(width, CHUNK // 4)
    hots, tiles = [], [[[], []] for _ in range(P_SIZE // 128)]
    for left in range(0, width, chunk):
        where, re_amp, im_amp, rel = (data[j : j + 1, left : left + chunk] for j in range(4))
        re2, im2 = 2.0 * re_amp, 2.0 * im_amp
        inverse = 0.5 / (rel + (base.astype(f32) + NEAR))
        gain = inverse * -64.0
        gain2 = gain + gain
        bend = inverse * (1.0 / 64.0)
        rows = lax.broadcasted_iota(jnp.int32, (bins, chunk), 0).astype(f32)
        hot = jnp.where(rows == rel, 1.0, 0.0).astype(bf16)
        hots += [hot, hot]
        odd = lax.broadcasted_iota(jnp.int32, (8, chunk), 0).astype(f32) * 2.0 + 1.0
        even = turn(odd * odd * (SPACING * SPACING / 4.0) * gain, trig)
        for q in range(P_SIZE // 128):
            ids = lax.broadcasted_iota(jnp.int32, (16, chunk), 0)
            middle = (ids * 8 + (q * 128 - P_SIZE // 2)).astype(f32) + 3.5
            offset = middle * SPACING - where
            t = offset * offset * gain
            y = t * bend
            t = t * (1.0 + y * (1.0 + 2.0 * y))
            r = t - jnp.round(t)
            u = r * r
            sn = r * horner(u, trig[0])
            cs = horner(u, trig[1])
            at = (re_amp - sn * (re2 * sn + im2 * cs), im_amp + sn * (re2 * cs - im2 * sn))
            slope = offset * gain2 * (1.0 + y * (2.0 + 6.0 * y))
            power = turn(slope * (SPACING / 2.0), trig)
            square = (1.0 - 2.0 * power[1] * power[1], 2.0 * power[0] * power[1])
            made = [None] * 8
            for j in range(4):
                a = times(at, (even[0][j : j + 1], even[1][j : j + 1]))
                rr, ii = a[0] * power[0], a[1] * power[1]
                ri, ir = a[0] * power[1], a[1] * power[0]
                made[4 + j] = (rr - ii, ri + ir)
                made[3 - j] = (rr + ii, ir - ri)
                if j < 3:
                    power = times(power, square)
            for c in range(2):
                tiles[q][c].append(
                    jnp.concatenate([jnp.concatenate(split(v[c]), 1) for v in made], 0)
                )
    hot = jnp.concatenate(hots, 1)
    for q in range(P_SIZE // 128):
        for c in range(2):
            lanes = slice(c * P_SIZE + q * 128, c * P_SIZE + (q + 1) * 128)
            yield lanes, product(hot, jnp.concatenate(tiles[q][c], 1), ((1,), (1,)))


def range_bin_kernel(base_ref, *refs, span, trig):
    out, lead = refs[6:8]
    buf, load = refs[14:]
    cells8, bounce8, pos, amp, cells, bnc = refs[8:14]
    loads = [
        pltpu.make_async_copy(src, dst, load.at[i])
        for i, (src, dst) in enumerate(zip(refs[:6], refs[8:14]))
    ]
    for copy in loads:
        copy.start()
    for copy in loads:
        copy.wait()
    base = base_ref[0]
    rows = cells8.shape[0]
    chunks = rows // 8
    target = cells8[...] + SHIFT * bounce8[...] - base
    match = jnp.where((target >= 0) & (target < span), 1.0, 0.0)
    mb = match.astype(bf16)
    a = lax.broadcasted_iota(jnp.int32, (128, 128), 0)
    b = lax.broadcasted_iota(jnp.int32, (128, 128), 1)
    upto = jnp.where(a <= b, 1.0, 0.0).astype(bf16)
    count = jnp.dot(mb, upto, preferred_element_type=f32)
    total = jnp.dot(mb, jnp.ones((128, 128), bf16), preferred_element_type=f32)
    a = lax.broadcasted_iota(jnp.int32, (rows, rows), 0)
    b = lax.broadcasted_iota(jnp.int32, (rows, rows), 1)
    below = jnp.where((a // 8 == b // 8) & (b < a), 1.0, 0.0).astype(bf16)
    ahead = jnp.dot(below, total.astype(bf16), preferred_element_type=f32)
    rank = jnp.where(match > 0.0, count + ahead - 1.0, -1.0)
    counts = [
        jnp.sum(match[8 * c : 8 * c + 8]).astype(jnp.int32) for c in range(chunks)
    ]

    def values(c):
        lanes = slice(CHUNK * c, CHUNK * (c + 1))
        flip = 1.0 - 2.0 * bnc[:, lanes].astype(f32)
        rel = (cells[:, lanes] + SHIFT * bnc[:, lanes] - base).astype(f32)
        zero = jnp.zeros_like(rel)
        data = jnp.concatenate(
            [pos[:, lanes], amp[0:1, lanes] * flip, amp[1:2, lanes] * flip, rel] + [zero] * 4, 0
        )
        return jnp.concatenate(list(split3(data)) + [jnp.zeros_like(data)], 0).astype(bf16)

    def pick(c, first):
        slots = lax.broadcasted_iota(jnp.int32, (SLOTS, 128), 0).astype(f32) + first
        hot = jnp.concatenate(
            [jnp.where(rank[8 * c + j : 8 * c + j + 1] == slots, 1.0, 0.0) for j in range(8)], 1
        ).astype(bf16)
        return lax.dot_general(
            hot, values(c), (((1,), (1,)), ((), ())), preferred_element_type=f32
        )

    start = 0
    for c in range(chunks):
        buf[pl.ds(start, SLOTS), 0:32] = pick(c, 0.0)
        start = start + counts[c]
    most = functools.reduce(jnp.maximum, counts)

    @pl.when(most > SLOTS)
    def _():
        begin = 0
        for c in range(chunks):

            @pl.loop(0, (counts[c] + SLOTS - 1) // SLOTS)
            def _(i):
                first = (i * SLOTS).astype(f32)
                buf[pl.ds(begin + i * SLOTS, SLOTS), 0:32] = pick(c, first)

            begin = begin + counts[c]

    buf[pl.ds(start, AHEAD), :] = jnp.zeros((AHEAD, 128), f32)

    def data(first, width):
        cols = []
        for h in range(width // 128):
            t = buf[pl.ds(first + h * 128, 128), :].T
            cols.append(t[0:8] + t[8:16] + t[16:24])
        return jnp.concatenate(cols, 1)

    lead[...] = data(0, AHEAD)
    out[...] = jnp.zeros_like(out)

    @pl.loop(AHEAD // WIDE, (start + WIDE - 1) // WIDE)
    def _(i):
        for lanes, sums in echoes(data(i * WIDE, WIDE), base, span, trig):
            out[:, lanes] += sums


def range_binning(positions, amplitude, cells, bounce, base, span):
    count = positions.shape[0]
    rows = count // 128
    sources = (
        cells.reshape(rows, 128),
        bounce.reshape(rows, 128),
        positions.reshape(1, count),
        amplitude,
        cells.reshape(1, count),
        bounce.reshape(1, count),
    )
    return pl.pallas_call(
        functools.partial(range_bin_kernel, span=span, trig=range_trig_coefs(4)),
        in_specs=[pl.BlockSpec(memory_space=pltpu.SMEM)] + [IN_HBM] * len(sources),
        out_specs=(IN_VMEM, IN_VMEM),
        out_shape=(
            jax.ShapeDtypeStruct((span, 2 * P_SIZE), f32),
            jax.ShapeDtypeStruct((8, AHEAD), f32),
        ),
        scratch_shapes=[pltpu.VMEM(a.shape, a.dtype) for a in sources]
        + [
            pltpu.VMEM((count + SLOTS + AHEAD, 128), f32),
            pltpu.SemaphoreType.DMA((len(sources),)),
        ],
        compiler_params=pltpu.CompilerParams(vmem_limit_bytes=16 << 20),
        name="range_binning",
    )(base.reshape(1), *in_hbm(sources))


def complex_rows(c, s):
    return np.block([[c, s], [-s, c]])


def mid_factors(n_dev, order):
    side = np.arange(BIN_SIDE)
    t = np.arange(STOLT)
    eye = np.eye(GROUP)
    a = -2 * np.pi / STOLT * ((side[:, None] * t[None, :]) % STOLT)
    ta = complex_rows(np.cos(a), np.sin(a))[order]
    a = -2 * np.pi / F_LEN * (side[:, None] * t[None, :])
    wa = np.stack([np.tile(np.cos(a), (GROUP, 1)), np.tile(np.sin(a), (GROUP, 1))])
    a = -2 * np.pi / BIN_SIDE * ((side[:, None] * side[None, :]) % BIN_SIDE)
    c, s = np.kron(eye, np.cos(a)), np.kron(eye, np.sin(a))
    tb = complex_rows(c, s).T
    blk = np.arange(BLOCKS)
    a = 2 * np.pi / BLOCKS * ((blk[:, None] * blk[None, :]) % BLOCKS)
    c, s = np.kron(eye, np.cos(a)), np.kron(eye, np.sin(a))
    tc = complex_rows(c, s)
    a = 2 * np.pi / F_LEN * (t[:, None] * blk[None, :])
    wc = np.stack([np.tile(np.cos(a), (1, GROUP)), np.tile(np.sin(a), (1, GROUP))])
    a = 2 * np.pi / STOLT * ((t[:, None] * t[None, :]) % STOLT)
    td = complex_rows(np.cos(a), np.sin(a)).T / F_LEN
    td = td.reshape(2, n_dev, STOLT // n_dev, 2 * STOLT).transpose(1, 0, 2, 3)
    return ta, wa.astype(np.float32), tb, tc, wc.astype(np.float32), td


def mid_tables(n_dev, order):
    ta, wa, tb, tc, wc, td = mid_factors(n_dev, order)
    td = td.reshape(2 * STOLT, 2 * STOLT)
    return np_split(ta), wa, np_split(tb), np_split(tc), wc, np_split(td)


def core_tables(n_dev, order):
    ta, wa, tb, tc, wc, td = mid_factors(n_dev, order)
    td = td.reshape(n_dev, 2, -1, GROUP, 2 * STOLT).transpose(0, 2, 1, 3, 4)
    td = td.reshape(2 * STOLT, 2 * STOLT)
    forward, inverse = quarter_tables()
    return (
        np_split(forward),
        np_split(ta),
        wa,
        np_split(tb),
        np_split(tc),
        wc,
        np_split(td),
    ), np_split(inverse)


def mid_kernel(
    x, cos_p, sin_p, hot, kind, bank_hi, bank_lo, ta, wa, tb, tc, wc, td, out, xs, os, *, subs
):
    n = GROUP * BLOCKS
    step = pl.program_id(0)
    groups = x.shape[1]

    @pl.when(step == 0)
    def _():
        for g in range(groups):
            xs[g] = x[:, g, :]

    parts_hi, parts_lo = [], []
    for g in range(subs):
        lanes = slice(g * n, (g + 1) * n)
        y = dots(split(xs[step * subs + g]), (ta[0], ta[1]), ((0,), (0,)))
        yr, yi = y[:, :STOLT], y[:, STOLT:]
        y = jnp.concatenate([yr * wa[0] - yi * wa[1], yr * wa[1] + yi * wa[0]], 0)
        z = dots((tb[0], tb[1]), split(y), ((1,), (0,)))
        zr, zi = z[:n], z[n:]
        cp, sp = cos_p[lanes], sin_p[lanes]
        z = jnp.concatenate([zr * cp - zi * sp, zr * sp + zi * cp], 1)
        hi, lo = split(z)
        picked = jnp.dot(
            hot[g], jnp.concatenate([hi, lo], 1), preferred_element_type=f32
        ).astype(bf16)
        first, second = picked[:n], picked[n:]
        for c in range(2):
            for base, keep in ((0, parts_hi), (2 * STOLT, parts_lo)):
                cut = slice(base + c * STOLT, base + (c + 1) * STOLT)
                keep.append(jnp.concatenate([first[:, cut], second[:, cut]], 1))
    ghi = jnp.concatenate(parts_hi, 0)
    glo = jnp.concatenate(parts_lo, 0)
    kinds = kind[...].reshape(subs * 2 * n, 1)
    kinds = jnp.broadcast_to(kinds, (subs * 2 * n, STOLT))
    acc = jnp.zeros((subs * 2 * n, STOLT), f32)
    for k in range(0, bank_hi.shape[0], 2):
        khi = jnp.concatenate([bank_hi[k], bank_hi[k + 1]], 1)
        klo = jnp.concatenate([bank_lo[k], bank_lo[k + 1]], 1)
        r = dots((ghi, glo), (khi, klo), ((1,), (0,)))
        for half in range(2):
            acc = jnp.where(kinds == k + half, r[:, half * STOLT : (half + 1) * STOLT], acc)
    for g in range(subs):
        s = acc[g * 2 * n : (g + 1) * 2 * n]
        y = dots(split(s), (tc[0], tc[1]), ((0,), (0,)))
        yr, yi = y[:, :n], y[:, n:]
        y = jnp.concatenate([yr * wc[0] - yi * wc[1], yr * wc[1] + yi * wc[0]], 0)
        os[step * subs + g] = dots((td[0], td[1]), split(y), ((1,), (0,)))

    @pl.when(step == pl.num_programs(0) - 1)
    def _():
        for g in range(groups):
            out[:, g, :] = os[g]


def middle(x, cos_p, sin_p, hot, kind, bank_hi, bank_lo, tables):
    groups = x.shape[1]
    subs = min(4, groups)
    n = GROUP * BLOCKS
    whole = lambda a: pl.BlockSpec(a.shape, lambda i: (0,) * a.ndim)
    return pl.pallas_call(
        functools.partial(mid_kernel, subs=subs),
        grid=(groups // subs,),
        in_specs=[
            whole(x),
            pl.BlockSpec((subs * n, STOLT), lambda i: (i, 0)),
            pl.BlockSpec((subs * n, STOLT), lambda i: (i, 0)),
            pl.BlockSpec((subs, 2 * n, n), lambda i: (i, 0, 0)),
            pl.BlockSpec((subs, 2 * n, 1), lambda i: (i, 0, 0)),
            whole(bank_hi),
            whole(bank_lo),
        ]
        + [whole(t) for t in tables],
        out_specs=pl.BlockSpec((2 * STOLT, groups, n), lambda i: (0, 0, 0)),
        out_shape=jax.ShapeDtypeStruct((2 * STOLT, groups, n), f32),
        scratch_shapes=[
            pltpu.VMEM((groups, x.shape[0], n), f32),
            pltpu.VMEM((groups, 2 * STOLT, n), f32),
        ],
        name="middle",
    )(x, cos_p, sin_p, hot, kind, bank_hi, bank_lo, *tables)


def quarter_tables():
    q = P_SIZE // 4
    m = np.arange(q)
    fwd, inv = [], []
    for low in range(4):
        a = 2 * np.pi / P_SIZE * (((4 * m[:, None] + low) * m[None, :]) % P_SIZE)
        f = a.reshape(-1, 2, q).transpose(1, 0, 2).reshape(q, q // 8, 8)
        f = f.transpose(0, 2, 1).reshape(q, q)
        fwd.append(np.concatenate([np.cos(f), np.sin(f)], 0))
        inv.append(np.concatenate([np.cos(a.T), np.sin(a.T)], 0) / P_SIZE)
    return np.stack(fwd), np.stack(inv)


def swap_blocks(arrays):
    count = len(arrays)
    lanes = arrays[0].shape[-1]
    size = lanes // count
    block = lax.broadcasted_iota(jnp.int32, arrays[0].shape, 1) // size
    outs = []
    for b in range(count):
        acc = None
        for a in range(count):
            shift = (a - b) % count * size
            moved = pltpu.roll(arrays[a], shift, 1) if shift else arrays[a]
            acc = moved if acc is None else jnp.where(block == a, moved, acc)
        outs.append(acc)
    return outs


def core_kernel(*refs, n_pulse, n_scat, subs, trig, trig_low):
    lead, partial = refs[:2]
    sources = refs[2:12]
    out = refs[12]
    local = refs[13:23]
    steps_in, kinds_in, bank, table, ta, wa, tb, tc, wc, td = local
    binned, peer, spec, x, hot, kind, banks, os, twin_os, *twin_in = refs[23:34]
    (
        load, own_store, pair_send, pair_recv, near_send, near_recv, far_send, far_recv,
        twin_send, twin_recv, half_send,
    ) = refs[34:]
    n_dev = n_pulse * n_scat
    pulse = lax.axis_index("pulse")
    scat = lax.axis_index("scat")
    me = pulse * n_scat + scat
    half = peer.shape[0]
    lanes = 2 * half
    size = P_SIZE // 4
    n = GROUP * BLOCKS
    groups = os.shape[1] + SHARED
    pieces = groups // subs
    reach = n_pulse // 2
    side = lax.div(pulse, reach)
    twin = lax.rem(pulse + reach, n_pulse) * n_scat + scat
    quads = lanes // BIN_SIDE
    unit = subs * quads
    per = os.shape[2]
    moves = [(a, b) for a in range(n_pulse) for b in range(n_scat) if (a, b) != (0, 0)]
    moves.sort(key=lambda m: (-min(m[0], n_pulse - m[0]), m))

    def other(a, b):
        return lax.rem(pulse + a, n_pulse), lax.rem(scat + b, n_scat)

    barrier = pltpu.get_barrier_semaphore()
    for a, b in moves:
        p, c = other(a, b)
        pl.semaphore_signal(
            barrier, inc=1, device_id={"pulse": p, "scat": c}, device_id_type=MESH
        )
    keep = pl.ds(pl.multiple_of(scat * half, half), half)
    give = pl.ds(pl.multiple_of((1 - scat) * half, half), half)
    loads = [
        pltpu.make_async_copy(src, dst, load.at[i])
        for i, (src, dst) in enumerate(zip(sources, local))
    ]
    for copy in loads:
        copy.start()
    for cut, sums in echoes(lead[...], pulse * 2 * half, 2 * half, trig_low):
        binned[:, cut] = partial[:, cut] + sums
    pl.semaphore_wait(barrier, n_dev - 1)

    pair = pltpu.make_async_remote_copy(
        src_ref=binned.at[give, :],
        dst_ref=peer,
        send_sem=pair_send,
        recv_sem=pair_recv,
        device_id={"pulse": pulse, "scat": 1 - scat},
        device_id_type=MESH,
    )
    pair.start()
    metas = []
    for i in range(2):
        loads[i].wait()
        copy = pltpu.make_async_remote_copy(
            src_ref=local[i],
            dst_ref=twin_in[i],
            send_sem=twin_send.at[i],
            recv_sem=twin_recv.at[i],
            device_id={"pulse": lax.rem(pulse + reach, n_pulse), "scat": scat},
            device_id_type=MESH,
        )
        copy.start()
        metas.append(copy)
    loads[3].wait()
    pair.wait()

    quarters = []
    for q in range(4):
        pair_of = []
        for c in range(2):
            cut = slice(c * P_SIZE + q * size, c * P_SIZE + (q + 1) * size)
            pair_of.append(binned[keep, cut] + peer[:, cut])
        quarters.append(pair_of)
    (r0, i0), (r1, i1), (r2, i2), (r3, i3) = quarters
    sr, si, dr, di = r0 + r2, i0 + i2, r0 - r2, i0 - i2
    tr, ti, er, ei = r1 + r3, i1 + i3, r1 - r3, i1 - i3
    mixed = (
        (sr + tr, si + ti),
        (dr + ei, di - er),
        (sr - tr, si - ti),
        (dr - ei, di + er),
    )
    low = lax.broadcasted_iota(jnp.int32, (size, lanes), 1) < half
    rows = []
    for k in range(4):
        g = product(
            joined(table[0, k], table[1, k], 1),
            triple(jnp.concatenate(mixed[k], 0), 1),
            ((1,), (1,)),
        )
        turned = pltpu.roll(g[size:], half, 1)
        rows.append(g[:size] + jnp.where(low, turned, -turned))
    for q, z in enumerate(swap_blocks(rows)):
        for h in range(subs):
            spec[pl.ds(q * subs + h, size // subs, stride=unit), :] = z[
                h * (size // subs) : (h + 1) * (size // subs)
            ]

    def piece(dev, i):
        return pl.ds(pl.multiple_of((dev * pieces + i) * unit, unit), unit)

    def source(p, c, i):
        if i < pieces:
            return piece(p * n_scat + c, i)
        return piece(lax.rem(p + reach, n_pulse) * n_scat + c, pieces - 1)

    own = pl.ds(pl.multiple_of(me * unit, unit), unit)
    for i in range(pieces + 1):
        for j, (a, b) in enumerate(moves):
            p, c = other(a, b)
            pltpu.make_async_remote_copy(
                src_ref=spec.at[source(p, c, i), :],
                dst_ref=x.at[i, own, :],
                send_sem=near_send.at[j],
                recv_sem=near_recv.at[i, me],
                device_id={"pulse": p, "scat": c},
                device_id_type=MESH,
            ).start()
    for i in range(pieces + 1):
        x[i, own, :] = spec[source(pulse, scat, i), :]

    for i in (2, 4, 5, 6, 7, 8, 9):
        loads[i].wait()
    for copy in metas:
        copy.wait()
    block = lax.broadcasted_iota(jnp.int32, (n, STOLT), 0)
    lane = lax.broadcasted_iota(jnp.int32, (n, STOLT), 1)
    spot = lane.astype(f32)
    above = (block // BLOCKS * BLOCKS).astype(f32)
    flat = []
    for i in range(2):
        both = [
            jnp.concatenate([ref[pl.ds(j, groups, stride=GROUP), :] for j in range(GROUP)], 1)
            for ref in (local[i], twin_in[i])
        ]
        flat.append(jnp.concatenate([both[0], both[1][groups - subs :]], 0))
    for g in range(groups + subs):
        first = jnp.broadcast_to(flat[0][g : g + 1].astype(f32), (n, n)).T + above
        hot[g, :n] = jnp.where(first == spot, 1.0, 0.0).astype(bf16)
        hot[g, n:] = jnp.where(first + 1.0 == spot, 1.0, 0.0).astype(bf16)
        kind[g] = jnp.broadcast_to(flat[1][g : g + 1], (8, n))
    for k in range(bank.shape[0]):
        turned = jnp.concatenate([bank[k, :STOLT].T, bank[k, STOLT:].T], 1)
        hi, lo = split(turned)
        banks[k * STOLT : (k + 1) * STOLT] = jnp.concatenate([hi, hi, lo], 1)

    cols = (lane + (block % BLOCKS) * STOLT).astype(f32)
    kr = 4.0 * np.pi / 3e8 * (9.6e9 + (cols - F_LEN // 2) * (1.5e8 / F_LEN))

    def phase(owner, g):
        row = owner * (groups * GROUP) + g * GROUP + block // BLOCKS
        centered = lax.rem(row + P_SIZE // 2, P_SIZE) - P_SIZE // 2
        along = 2.0 * np.pi / (P_SIZE * SPACING) * centered.astype(f32)
        squared = along * along
        depth = NEAR + B // 2
        theta = -depth * squared / (jnp.sqrt(kr * kr - squared) + kr)
        whole = jnp.round(theta * (0.5 / np.pi))
        for part in turn_parts():
            theta = theta - whole * part
        r = theta * (0.5 / np.pi)
        u = r * r
        sn = r * horner(u, trig[0])
        cs = horner(u, trig[1])
        return 1.0 - 2.0 * sn * sn, 2.0 * sn * cs

    def ranged(slot, owner, g, cut):
        i, h = lax.div(slot, subs), lax.rem(slot, subs)
        cp, sp = phase(owner, g)
        rows_in = x[i, pl.ds(h, n_dev * quads, stride=subs), :]
        y = product(triple(rows_in, 0), joined(ta[0], ta[1], 0), ((0,), (0,)))
        yr, yi = y[:, :STOLT], y[:, STOLT:]
        y = jnp.concatenate([yr * wa[0] - yi * wa[1], yr * wa[1] + yi * wa[0]], 0)
        z = product(joined(tb[0], tb[1], 1), triple(y, 0))
        zr, zi = z[:n], z[n:]
        z = jnp.concatenate([zr * cp - zi * sp, zr * sp + zi * cp], 1)
        picked = product(hot[slot], jnp.concatenate(split(z), 1)).astype(bf16)
        first, second = picked[:n], picked[n:]
        parts = []
        for base in (0, 2 * STOLT):
            cuts = [slice(base + c * STOLT, base + (c + 1) * STOLT) for c in range(2)]
            parts.append(
                jnp.concatenate(
                    [jnp.concatenate([first[:, v], second[:, v]], 1) for v in cuts], 0
                )
            )
        ghi, glo = parts
        windows = jnp.concatenate([ghi, glo, ghi], 1)
        kinds = jnp.concatenate([kind[slot, 0:1]] * 2, 1)
        acc = jnp.zeros((STOLT, 2 * n), f32)
        for first in range(0, banks.shape[0], STREAM):
            r = product(banks[first : first + STREAM], windows, ((1,), (1,)))
            for v in range(STREAM // STOLT):
                k = first // STOLT + v
                acc = jnp.where(kinds == k, r[v * STOLT : (v + 1) * STOLT], acc)
        y = product(triple(acc, 1), joined(tc[0], tc[1], 0))
        yr, yi = y[:, :n], y[:, n:]
        y = jnp.concatenate([yr * wc[0] - yi * wc[1], yr * wc[1] + yi * wc[0]], 0)
        z = product(joined(td[0, cut, :], td[1, cut, :], 1), triple(y, 0))
        return z.reshape(-1, per, n)

    def arrived(i):
        for a, b in moves:
            p, c = other(a, b)
            src = p * n_scat + c
            here = pl.ds(pl.multiple_of(src * unit, unit), unit)
            pltpu.make_async_copy(
                x.at[i, here, :], x.at[i, here, :], near_recv.at[i, src]
            ).wait()

    def step(g, carry):
        @pl.when(lax.rem(g, subs) == 0)
        def _():
            arrived(lax.div(g, subs))

        os[:, g] = ranged(g, me, g, slice(None))
        for j, (a, b) in enumerate(moves):
            p, c = other(a, b)
            pltpu.make_async_remote_copy(
                src_ref=os.at[p * n_scat + c, g],
                dst_ref=out.at[me, g],
                send_sem=far_send.at[j],
                recv_sem=far_recv.at[me],
                device_id={"pulse": p, "scat": c},
                device_id_type=MESH,
            ).start()
        return carry

    close = [(a, b) for a in range(reach) for b in range(n_scat) if (a, b) != (0, 0)]
    within = pulse - side * reach

    def beside(a, b):
        return lax.rem(within + a, reach), lax.rem(scat + b, n_scat)

    part = 2 * STOLT // 2
    served = pl.ds(pl.multiple_of(side * part, part), part)

    lax.fori_loop(0, groups - SHARED, step, 0)
    if SHARED == subs:
        arrived(pieces - 1)
    arrived(pieces)

    def half_step(t, carry):
        v, h = lax.div(t, SHARED), lax.rem(t, SHARED)
        owner = lax.rem(pulse + v * reach, n_pulse) * n_scat + scat
        g = groups - SHARED + h
        twin_os[v, :, h] = ranged(g + v * subs, owner, g, served)
        for j, (a, b) in enumerate(close):
            p, c = beside(a, b)
            pltpu.make_async_remote_copy(
                src_ref=twin_os.at[v, p * n_scat + c, h],
                dst_ref=out.at[owner, g],
                send_sem=half_send.at[j],
                recv_sem=far_recv.at[owner],
                device_id={"pulse": side * reach + p, "scat": c},
                device_id_type=MESH,
            ).start()
        return carry

    lax.fori_loop(0, 2 * SHARED, half_step, 0)
    first, last = pl.ds(0, groups - SHARED), pl.ds(groups - SHARED, SHARED)
    here = within * n_scat + scat
    stores = [
        pltpu.make_async_copy(src, dst, own_store.at[i])
        for i, (src, dst) in enumerate(
            (
                (os.at[me], out.at[me, first]),
                (twin_os.at[0, here], out.at[me, last]),
                (twin_os.at[1, here], out.at[twin, last]),
            )
        )
    ]
    for copy in stores:
        copy.start()
    for copy in stores:
        copy.wait()
    for j, (a, b) in enumerate(close):
        whole = os.at[0, pl.ds(0, 2 * SHARED)]
        pltpu.make_async_copy(whole, whole, half_send.at[j]).wait()
    for j, (a, b) in enumerate(moves):
        p, c = other(a, b)
        src = p * n_scat + c
        whole = spec.at[pl.ds(0, (pieces + 1) * unit), :]
        pltpu.make_async_copy(whole, whole, near_send.at[j]).wait()
        pltpu.make_async_copy(os.at[src], os.at[src], far_send.at[j]).wait()
        whole = out.at[src, first] if (a, b) == (reach, 0) else out.at[src]
        pltpu.make_async_copy(whole, whole, far_recv.at[src]).wait()


def turn_parts():
    parts, rest = [], 2.0 * np.pi
    for bits in (10, 22, 60):
        scale = 2.0**bits
        part = float(np.float32(np.round(rest * scale) / scale))
        parts.append(part)
        rest -= part
    return parts


def core(partial, lead, steps_in, kinds_in, bank, tables, n_pulse, n_scat):
    n_dev = n_pulse * n_scat
    groups = steps_in.shape[0] // GROUP
    subs = 2
    n = GROUP * BLOCKS
    span, width = partial.shape
    half = span // n_scat
    quads = 2 * half // BIN_SIDE
    kernels = bank.shape[0]
    per = 2 * STOLT // n_dev
    sources = (steps_in, kinds_in, bank, *tables)
    dma = pltpu.SemaphoreType.DMA
    return pl.pallas_call(
        functools.partial(
            core_kernel,
            n_pulse=n_pulse,
            n_scat=n_scat,
            subs=subs,
            trig=range_trig_coefs(5),
            trig_low=range_trig_coefs(4),
        ),
        in_specs=[IN_VMEM] * 2 + [IN_HBM] * len(sources),
        out_specs=pl.BlockSpec(memory_space=pl.ANY),
        out_shape=jax.ShapeDtypeStruct((n_dev, groups, per, n), f32),
        scratch_shapes=[pltpu.VMEM(a.shape, a.dtype) for a in sources]
        + [
            pltpu.VMEM((span, width), f32),
            pltpu.VMEM((half, width), f32),
            pltpu.VMEM((n_dev * groups * quads, n), f32),
            pltpu.VMEM((groups // subs + 1, n_dev * subs * quads, n), f32),
            pltpu.VMEM((groups + subs, 2 * n, n), bf16),
            pltpu.VMEM((groups + subs, 8, n), jnp.int32),
            pltpu.VMEM((kernels * STOLT, 6 * STOLT), bf16),
            pltpu.VMEM((n_dev, groups - SHARED, per, n), f32),
            pltpu.VMEM((2, n_dev // 2, SHARED, per, n), f32),
            pltpu.VMEM(steps_in.shape, steps_in.dtype),
            pltpu.VMEM(kinds_in.shape, kinds_in.dtype),
            dma((len(sources),)),
            dma((3,)),
            dma,
            dma,
            dma((n_dev,)),
            dma((groups // subs + 1, n_dev)),
            dma((n_dev,)),
            dma((n_dev,)),
            dma((2,)),
            dma((2,)),
            dma((n_dev // 2,)),
        ],
        compiler_params=pltpu.CompilerParams(
            collective_id=0, has_side_effects=True, vmem_limit_bytes=24 << 20
        ),
        name="core",
    )(lead, partial, *in_hbm(sources))


def image_kernel(x, table, out, done, sems):
    devs, kh, per, lanes = x.shape
    size = P_SIZE // 4
    copies = []
    for h in range(per // (2 * GROUP)):
        columns = [[] for _ in range(4)]
        for c in range(2):
            first = (2 * h + c) * GROUP
            tiles = [x[:, :, first + j, :].reshape(devs * kh, lanes) for j in range(4)]
            for k, z in enumerate(swap_blocks(tiles)):
                columns[k].append(z)
        v = []
        for k in range(4):
            g = product(
                joined(table[0, k], table[1, k], 1), triple(jnp.concatenate(columns[k], 1), 0)
            )
            cos_g, sin_g = g[:size], g[size:]
            v.append((cos_g[:, :lanes] - sin_g[:, lanes:], cos_g[:, lanes:] + sin_g[:, :lanes]))
        (r0, i0), (r1, i1), (r2, i2), (r3, i3) = v
        sr, si, dr, di = r0 + r2, i0 + i2, r0 - r2, i0 - i2
        tr, ti, er, ei = r1 + r3, i1 + i3, r1 - r3, i1 - i3
        mixed = (
            (sr + tr, si + ti),
            (dr - ei, di + er),
            (sr - tr, si - ti),
            (dr + ei, di - er),
        )
        for q in range(4):
            for c in range(2):
                done[h, c, q * size : (q + 1) * size, :] = mixed[q][c]
        copy = pltpu.make_async_copy(
            done.at[h], out.at[:, :, pl.ds(h * lanes, lanes)], sems.at[h]
        )
        copy.start()
        copies.append(copy)
    for copy in copies:
        copy.wait()


def reference_phase(row_ids, cols):
    centered = (row_ids + P_SIZE // 2) % P_SIZE - P_SIZE // 2
    along_k = 2.0 * jnp.pi / (P_SIZE * SPACING) * centered.astype(f32)
    kr = 4.0 * jnp.pi / 3e8 * (9.6e9 + (cols.astype(f32) - F_LEN // 2) * (1.5e8 / F_LEN))
    squared = along_k * along_k
    depth = NEAR + B // 2
    return (
        -depth
        * squared[:, None]
        / (jnp.sqrt(kr[None, :] * kr[None, :] - squared[:, None]) + kr[None, :])
    )


def on_device(positions, amplitude, range_cells, bounce, stolt_block, kernel_choice, kernel_bank):
    n_pulse = lax.axis_size("pulse")
    n_scat = lax.axis_size("scat")
    n_dev = n_pulse * n_scat
    pulse_here = lax.axis_index("pulse")
    scat_here = lax.axis_index("scat")
    pulses = P_SIZE // n_pulse
    rows = P_SIZE // n_dev
    width = F_LEN // n_dev
    groups = rows // GROUP
    n = GROUP * BLOCKS
    bins_scat = B // n_scat
    bins_here = bins_scat // n_pulse

    per = STOLT // n_dev
    span = B // n_pulse
    packed = (
        span == 128
        and n_scat == 2
        and per % 4 == 0
        and groups % 8 == 0
        and positions.shape[0] % CHUNK == 0
    )
    if packed:
        partial, lead = range_binning(
            positions, amplitude, range_cells, bounce, pulse_here * span, span
        )
        local = bins_here // BIN_SIDE
        i, s, c, l = np.meshgrid(
            np.arange(n_pulse), np.arange(n_scat), np.arange(2), np.arange(local), indexing="ij"
        )
        order = (c * BIN_SIDE + (i * n_scat + s) * local + l).reshape(-1)
        tables, backward = core_tables(n_dev, order)
        tables = tuple(jnp.asarray(t) for t in tables)
        columns = core(
            partial, lead, stolt_block, kernel_choice, kernel_bank, tables, n_pulse, n_scat
        )
        return pl.pallas_call(
            image_kernel,
            in_specs=[IN_VMEM, IN_VMEM],
            out_specs=pl.BlockSpec(memory_space=pl.ANY),
            out_shape=jax.ShapeDtypeStruct((2, P_SIZE, width), f32),
            scratch_shapes=[
                pltpu.VMEM((width // n, 2, P_SIZE, n), f32),
                pltpu.SemaphoreType.DMA((width // n,)),
            ],
            compiler_params=pltpu.CompilerParams(vmem_limit_bytes=16 << 20),
            name="image",
        )(columns, jnp.asarray(backward))

    ids = jnp.arange(GROUP, dtype=jnp.int32)[None, :, None] * BLOCKS
    first = stolt_block.reshape(groups, GROUP, BLOCKS) + ids
    pick = jnp.stack([first, first + 1], 1).reshape(groups, 2 * n, 1)
    hot = (pick == jnp.arange(n, dtype=jnp.int32)[None, None, :]).astype(bf16)
    kind = jnp.stack([kernel_choice.reshape(groups, n)] * 2, 1).reshape(groups, 2 * n, 1)
    bank_hi = lax.reduce_precision(kernel_bank, 8, 7)
    bank_lo = (kernel_bank - bank_hi).astype(bf16)
    bank_hi = bank_hi.astype(bf16)
    row_ids = (pulse_here * n_scat + scat_here) * rows + jnp.arange(rows, dtype=jnp.int32)
    theta = reference_phase(row_ids, jnp.arange(F_LEN, dtype=jnp.int32))
    theta = theta.reshape(rows * BLOCKS, STOLT)
    cos_p, sin_p = jnp.cos(theta), jnp.sin(theta)

    partial = binning(positions, amplitude, range_cells, bounce, pulse_here * pulses, pulses)
    partial = partial.reshape(n_scat, bins_scat, 2 * pulses)
    binned = lax.dynamic_index_in_dim(partial, scat_here, 0, keepdims=False)
    for shift in range(1, n_scat):
        other = lax.dynamic_index_in_dim(
            partial, (scat_here + shift) % n_scat, 0, keepdims=False
        )
        ring = [(i, (i + shift) % n_scat) for i in range(n_scat)]
        binned = binned + lax.ppermute(other, "scat", ring)
    turned = lax.all_to_all(
        binned.reshape(n_pulse, bins_here, 2 * pulses), "pulse", 0, 0, tiled=True
    )
    turned = turned.reshape(n_pulse, bins_here, 2, pulses).transpose(0, 3, 2, 1)
    turned = turned.reshape(P_SIZE, 2 * bins_here)
    k = np.arange(P_SIZE)
    angle = 2 * np.pi / P_SIZE * ((k[:, None] * k[None, :]) % P_SIZE)
    az = jnp.asarray(np.concatenate([np.cos(angle), np.sin(angle)], 0), f32)
    product = jnp.dot(az, turned, precision=HIGH, preferred_element_type=f32)
    pc, ps = product[:P_SIZE], product[P_SIZE:]
    spectrum = pc + jnp.concatenate([ps[:, bins_here:], -ps[:, :bins_here]], 1)
    az_rows = lax.all_to_all(
        spectrum.reshape(n_dev, rows, 2 * bins_here), ("pulse", "scat"), 0, 0, tiled=True
    )
    x = az_rows.reshape(n_pulse, n_scat, rows, 2, bins_here).transpose(3, 1, 0, 4, 2)
    x = x.reshape(2, BIN_SIDE, BIN_SIDE, rows).transpose(0, 1, 3, 2)
    x = x.reshape(2 * BIN_SIDE, groups, n)
    order = np.arange(2 * BIN_SIDE)

    tables = tuple(jnp.asarray(t) for t in mid_tables(n_dev, order))
    ranged = middle(x, cos_p, sin_p, hot, kind, bank_hi, bank_lo, tables)
    columns = lax.all_to_all(
        ranged.reshape(n_dev, 2 * per, rows * BLOCKS), ("pulse", "scat"), 0, 0, tiled=True
    )
    columns = columns.reshape(n_dev, 2, per, rows, BLOCKS).transpose(0, 3, 1, 2, 4)
    columns = columns.reshape(P_SIZE, 2 * width)
    final = jnp.dot(az, columns, precision=HIGH, preferred_element_type=f32)
    fc, fs = final[:P_SIZE], final[P_SIZE:]
    re = (fc[:, :width] - fs[:, width:]) / P_SIZE
    im = (fc[:, width:] + fs[:, :width]) / P_SIZE
    return jnp.stack([re, im])


def solution(mesh):
    placed = (
        P(("scene", "scat")),
        P(None, ("scene", "scat")),
        P(("scene", "scat")),
        P(("scene", "scat")),
        P(("pulse", "scat"), None),
        P(("pulse", "scat"), None),
        P(),
    )
    return jax.shard_map(
        on_device,
        mesh=mesh,
        in_specs=placed,
        out_specs=P(None, "scene", ("pulse", "scat")),
        check_vma=False,
    )
```

```python
import functools

import jax
import jax.numpy as jnp
import numpy as np
from jax import lax
from jax.experimental import pallas as pl
from jax.experimental.pallas import tpu as pltpu
from jax.sharding import PartitionSpec as P

P_SIZE = 512
F_LEN = 4096
B = 1024
SHIFT = 16
STOLT = 128
BLOCKS = 32
SPACING = 2.0
NEAR = 700000.0
BIN_SIDE = 32
GROUP = 4
CHUNK = 512
SLOTS = 112
LANES = 256
WIDE = 128
AHEAD = 1024
SHARED = 1
STREAM = 512
HIGH = lax.Precision.HIGH
MESH = pl.DeviceIdType.MESH
IN_HBM = pl.BlockSpec(memory_space=pltpu.HBM)
IN_VMEM = pl.BlockSpec(memory_space=pltpu.VMEM)
f32 = jnp.float32
bf16 = jnp.bfloat16


def trig_coefs():
    x = np.cos(np.pi * (np.arange(400) + 0.5) / 400) * 0.5
    u = x * x
    s = np.polynomial.chebyshev.Chebyshev.fit(u, np.sin(np.pi * x) / x, 5).convert(
        kind=np.polynomial.Polynomial
    )
    c = np.polynomial.chebyshev.Chebyshev.fit(u, np.cos(np.pi * x), 5).convert(
        kind=np.polynomial.Polynomial
    )
    return [float(v) for v in s.coef], [float(v) for v in c.coef]


def horner(u, coefs):
    acc = jnp.full_like(u, coefs[-1])
    for c in coefs[-2::-1]:
        acc = acc * u + c
    return acc


def split(x):
    hi = x.astype(bf16)
    lo = (x - hi.astype(f32)).astype(bf16)
    return hi, lo


def np_split(x):
    x = np.asarray(x, np.float64)
    hi = np.asarray(x, jnp.bfloat16)
    lo = np.asarray(x - hi.astype(np.float64), jnp.bfloat16)
    return np.stack([hi, lo])


def dots(a, b, dims):
    d = functools.partial(
        lax.dot_general, dimension_numbers=(dims, ((), ())), preferred_element_type=f32
    )
    return d(a[0], b[0]) + (d(a[0], b[1]) + d(a[1], b[0]))


def in_hbm(arrays):
    return [pltpu.with_memory_space_constraint(a, pltpu.HBM) for a in arrays]


def joined(hi, lo, axis):
    return jnp.concatenate([hi, hi, lo], axis)


def triple(x, axis):
    hi, lo = split(x)
    return jnp.concatenate([hi, lo, hi], axis)


def product(a, b, dims=((1,), (0,))):
    return lax.dot_general(a, b, (dims, ((), ())), preferred_element_type=f32)


def bin_kernel(pulse_base, pos, amp, tgt, bnc, out, acc, *, pulses, sin_c, cos_c):
    step = pl.program_id(0)
    width = pos.shape[1]

    @pl.when(step == 0)
    def _():
        acc[...] = jnp.zeros_like(acc)

    base = pulse_base[0]
    ids = base + lax.broadcasted_iota(jnp.int32, (pulses, width), 0)
    along = (ids.astype(f32) - P_SIZE // 2) * SPACING
    target = tgt[...] + SHIFT * bnc[...]
    slant = NEAR + target.astype(f32)
    offset = along - pos[...]
    square = offset * offset
    excess = square / (jnp.sqrt(slant * slant + square) + slant)
    halves = excess * -128.0
    whole = jnp.round(halves)
    r = halves - whole
    u = r * r
    odd = whole - 2.0 * jnp.floor(whole * 0.5)
    sign = 1.0 - 2.0 * odd
    sin_p = sign * r * horner(u, sin_c)
    cos_p = sign * horner(u, cos_c)
    flip = 1.0 - 2.0 * bnc[...].astype(f32)
    are = flip * amp[0:1]
    aim = flip * amp[1:2]
    re = are * cos_p - aim * sin_p
    im = are * sin_p + aim * cos_p
    steer = jnp.concatenate([re, im], 0)
    hi, lo = split(steer)
    rhs = jnp.concatenate([hi, lo], 0)
    bins = lax.broadcasted_iota(jnp.int32, (B, width), 0)
    hot = jnp.where(bins == target, 1.0, 0.0).astype(bf16)
    acc[...] += lax.dot_general(
        hot, rhs, (((1,), (1,)), ((), ())), preferred_element_type=f32
    )

    @pl.when(step == pl.num_programs(0) - 1)
    def _():
        out[...] = acc[:, : 2 * pulses] + acc[:, 2 * pulses :]


def binning(positions, amplitude, cells, bounce, pulse_base, pulses):
    count = positions.shape[0]
    width = min(2048, count)
    sin_c, cos_c = trig_coefs()
    row = lambda n: pl.BlockSpec((n, width), lambda i: (0, i))
    return pl.pallas_call(
        functools.partial(bin_kernel, pulses=pulses, sin_c=sin_c, cos_c=cos_c),
        grid=(count // width,),
        in_specs=[pl.BlockSpec(memory_space=pltpu.SMEM), row(1), row(2), row(1), row(1)],
        out_specs=pl.BlockSpec((B, 2 * pulses), lambda i: (0, 0)),
        out_shape=jax.ShapeDtypeStruct((B, 2 * pulses), f32),
        scratch_shapes=[pltpu.VMEM((B, 4 * pulses), f32)],
        name="binning",
    )(
        pulse_base.reshape(1),
        positions.reshape(1, count),
        amplitude,
        cells.reshape(1, count),
        bounce.reshape(1, count),
    )


def range_trig_coefs(degree):
    x = np.cos(np.pi * (np.arange(400) + 0.5) / 400) * 0.5
    u = x * x
    fit = lambda y: np.polynomial.chebyshev.Chebyshev.fit(u, y, degree).convert(
        kind=np.polynomial.Polynomial
    )
    return [float(v) for v in fit(np.sin(np.pi * x) / x).coef], [
        float(v) for v in fit(np.cos(np.pi * x)).coef
    ]


def split3(x):
    hi = x.astype(bf16).astype(f32)
    rest = x - hi
    mid = rest.astype(bf16).astype(f32)
    return hi, mid, rest - mid


def turn(r, trig):
    u = r * r
    sn = r * horner(u, trig[0])
    cs = horner(u, trig[1])
    twice = sn + sn
    return 1.0 - twice * sn, twice * cs


def times(a, b):
    return a[0] * b[0] - a[1] * b[1], a[0] * b[1] + a[1] * b[0]


def echoes(data, base, bins, trig):
    width = data.shape[1]
    chunk = min(width, LANES)
    hots, tiles = [], [[[], []] for _ in range(P_SIZE // 128)]
    for left in range(0, width, chunk):
        where, re_amp, im_amp, rel = (data[j : j + 1, left : left + chunk] for j in range(4))
        re2, im2 = 2.0 * re_amp, 2.0 * im_amp
        inverse = 0.5 / (rel + (base.astype(f32) + NEAR))
        gain = inverse * -64.0
        gain2 = gain + gain
        bend = inverse * (1.0 / 64.0)
        rows = lax.broadcasted_iota(jnp.int32, (bins, chunk), 0).astype(f32)
        hot = jnp.where(rows == rel, 1.0, 0.0).astype(bf16)
        hots += [hot, hot]
        odd = lax.broadcasted_iota(jnp.int32, (8, chunk), 0).astype(f32) * 2.0 + 1.0
        even = turn(odd * odd * (SPACING * SPACING / 4.0) * gain, trig)
        for q in range(P_SIZE // 128):
            ids = lax.broadcasted_iota(jnp.int32, (16, chunk), 0)
            middle = (ids * 8 + (q * 128 - P_SIZE // 2)).astype(f32) + 3.5
            offset = middle * SPACING - where
            t = offset * offset * gain
            y = t * bend
            t = t * (1.0 + y * (1.0 + 2.0 * y))
            r = t - jnp.round(t)
            u = r * r
            sn = r * horner(u, trig[0])
            cs = horner(u, trig[1])
            at = (re_amp - sn * (re2 * sn + im2 * cs), im_amp + sn * (re2 * cs - im2 * sn))
            slope = offset * gain2 * (1.0 + y * (2.0 + 6.0 * y))
            power = turn(slope * (SPACING / 2.0), trig)
            square = (1.0 - 2.0 * power[1] * power[1], 2.0 * power[0] * power[1])
            made = [None] * 8
            for j in range(4):
                a = times(at, (even[0][j : j + 1], even[1][j : j + 1]))
                rr, ii = a[0] * power[0], a[1] * power[1]
                ri, ir = a[0] * power[1], a[1] * power[0]
                made[4 + j] = (rr - ii, ri + ir)
                made[3 - j] = (rr + ii, ir - ri)
                if j < 3:
                    power = times(power, square)
            for c in range(2):
                tiles[q][c].append(
                    jnp.concatenate([jnp.concatenate(split(v[c]), 1) for v in made], 0)
                )
    hot = jnp.concatenate(hots, 1)
    for q in range(P_SIZE // 128):
        for c in range(2):
            lanes = slice(c * P_SIZE + q * 128, c * P_SIZE + (q + 1) * 128)
            yield lanes, product(hot, jnp.concatenate(tiles[q][c], 1), ((1,), (1,)))


def range_bin_kernel(base_ref, *refs, span, trig):
    out, lead = refs[6:8]
    buf, load = refs[14:]
    cells8, bounce8, pos, amp, cells, bnc = refs[8:14]
    loads = [
        pltpu.make_async_copy(src, dst, load.at[i])
        for i, (src, dst) in enumerate(zip(refs[:6], refs[8:14]))
    ]
    for copy in loads:
        copy.start()
    for copy in loads:
        copy.wait()
    base = base_ref[0]
    rows = cells8.shape[0]
    deep = CHUNK // 128
    chunks = rows // deep
    target = cells8[...] + SHIFT * bounce8[...] - base
    match = jnp.where((target >= 0) & (target < span), 1.0, 0.0)
    mb = match.astype(bf16)
    a = lax.broadcasted_iota(jnp.int32, (128, 128), 0)
    b = lax.broadcasted_iota(jnp.int32, (128, 128), 1)
    upto = jnp.where(a <= b, 1.0, 0.0).astype(bf16)
    count = jnp.dot(mb, upto, preferred_element_type=f32)
    total = jnp.dot(mb, jnp.ones((128, 128), bf16), preferred_element_type=f32)
    a = lax.broadcasted_iota(jnp.int32, (rows, rows), 0)
    b = lax.broadcasted_iota(jnp.int32, (rows, rows), 1)
    below = jnp.where((a // deep == b // deep) & (b < a), 1.0, 0.0).astype(bf16)
    ahead = jnp.dot(below, total.astype(bf16), preferred_element_type=f32)
    rank = jnp.where(match > 0.0, count + ahead - 1.0, -1.0)
    counts = [
        jnp.sum(match[deep * c : deep * (c + 1)]).astype(jnp.int32) for c in range(chunks)
    ]

    def values(c):
        lanes = slice(CHUNK * c, CHUNK * (c + 1))
        flip = 1.0 - 2.0 * bnc[:, lanes].astype(f32)
        rel = (cells[:, lanes] + SHIFT * bnc[:, lanes] - base).astype(f32)
        zero = jnp.zeros_like(rel)
        data = jnp.concatenate(
            [pos[:, lanes], amp[0:1, lanes] * flip, amp[1:2, lanes] * flip, rel] + [zero] * 4, 0
        )
        return jnp.concatenate(list(split3(data)) + [jnp.zeros_like(data)], 0).astype(bf16)

    def pick(c, first):
        slots = lax.broadcasted_iota(jnp.int32, (SLOTS, 128), 0).astype(f32) + first
        hot = jnp.concatenate(
            [
                jnp.where(rank[deep * c + j : deep * c + j + 1] == slots, 1.0, 0.0)
                for j in range(deep)
            ],
            1,
        ).astype(bf16)
        return lax.dot_general(
            hot, values(c), (((1,), (1,)), ((), ())), preferred_element_type=f32
        )

    start = 0
    for c in range(chunks):
        buf[pl.ds(start, SLOTS), 0:32] = pick(c, 0.0)
        start = start + counts[c]
    most = functools.reduce(jnp.maximum, counts)

    @pl.when(most > SLOTS)
    def _():
        begin = 0
        for c in range(chunks):

            @pl.loop(0, (counts[c] + SLOTS - 1) // SLOTS)
            def _(i):
                first = (i * SLOTS).astype(f32)
                buf[pl.ds(begin + i * SLOTS, SLOTS), 0:32] = pick(c, first)

            begin = begin + counts[c]

    buf[pl.ds(start, AHEAD), :] = jnp.zeros((AHEAD, 128), f32)

    def data(first, width):
        cols = []
        for h in range(width // 128):
            t = buf[pl.ds(first + h * 128, 128), :].T
            cols.append(t[0:8] + t[8:16] + t[16:24])
        return jnp.concatenate(cols, 1)

    lead[...] = data(0, AHEAD)
    out[...] = jnp.zeros_like(out)

    @pl.loop(AHEAD // WIDE, (start + WIDE - 1) // WIDE)
    def _(i):
        for lanes, sums in echoes(data(i * WIDE, WIDE), base, span, trig):
            out[:, lanes] += sums


def range_binning(positions, amplitude, cells, bounce, base, span):
    count = positions.shape[0]
    rows = count // 128
    sources = (
        cells.reshape(rows, 128),
        bounce.reshape(rows, 128),
        positions.reshape(1, count),
        amplitude,
        cells.reshape(1, count),
        bounce.reshape(1, count),
    )
    return pl.pallas_call(
        functools.partial(range_bin_kernel, span=span, trig=range_trig_coefs(4)),
        in_specs=[pl.BlockSpec(memory_space=pltpu.SMEM)] + [IN_HBM] * len(sources),
        out_specs=(IN_VMEM, IN_VMEM),
        out_shape=(
            jax.ShapeDtypeStruct((span, 2 * P_SIZE), f32),
            jax.ShapeDtypeStruct((8, AHEAD), f32),
        ),
        scratch_shapes=[pltpu.VMEM(a.shape, a.dtype) for a in sources]
        + [
            pltpu.VMEM((count + SLOTS + AHEAD, 128), f32),
            pltpu.SemaphoreType.DMA((len(sources),)),
        ],
        compiler_params=pltpu.CompilerParams(vmem_limit_bytes=16 << 20),
        name="range_binning",
    )(base.reshape(1), *in_hbm(sources))


def complex_rows(c, s):
    return np.block([[c, s], [-s, c]])


def mid_factors(n_dev, order):
    side = np.arange(BIN_SIDE)
    t = np.arange(STOLT)
    eye = np.eye(GROUP)
    a = -2 * np.pi / STOLT * ((side[:, None] * t[None, :]) % STOLT)
    ta = complex_rows(np.cos(a), np.sin(a))[order]
    a = -2 * np.pi / F_LEN * (side[:, None] * t[None, :])
    wa = np.stack([np.tile(np.cos(a), (GROUP, 1)), np.tile(np.sin(a), (GROUP, 1))])
    a = -2 * np.pi / BIN_SIDE * ((side[:, None] * side[None, :]) % BIN_SIDE)
    c, s = np.kron(eye, np.cos(a)), np.kron(eye, np.sin(a))
    tb = complex_rows(c, s).T
    blk = np.arange(BLOCKS)
    a = 2 * np.pi / BLOCKS * ((blk[:, None] * blk[None, :]) % BLOCKS)
    c, s = np.kron(eye, np.cos(a)), np.kron(eye, np.sin(a))
    tc = complex_rows(c, s)
    a = 2 * np.pi / F_LEN * (t[:, None] * blk[None, :])
    wc = np.stack([np.tile(np.cos(a), (1, GROUP)), np.tile(np.sin(a), (1, GROUP))])
    a = 2 * np.pi / STOLT * ((t[:, None] * t[None, :]) % STOLT)
    td = complex_rows(np.cos(a), np.sin(a)).T / F_LEN
    td = td.reshape(2, n_dev, STOLT // n_dev, 2 * STOLT).transpose(1, 0, 2, 3)
    return ta, wa.astype(np.float32), tb, tc, wc.astype(np.float32), td


def mid_tables(n_dev, order):
    ta, wa, tb, tc, wc, td = mid_factors(n_dev, order)
    td = td.reshape(2 * STOLT, 2 * STOLT)
    return np_split(ta), wa, np_split(tb), np_split(tc), wc, np_split(td)


def core_tables(n_dev, order):
    ta, wa, tb, tc, wc, td = mid_factors(n_dev, order)
    td = td.reshape(n_dev, 2, -1, GROUP, 2 * STOLT).transpose(0, 2, 1, 3, 4)
    td = td.reshape(2 * STOLT, 2 * STOLT)
    forward, inverse = quarter_tables()
    return (
        np_split(forward),
        np_split(ta),
        wa,
        np_split(tb),
        np_split(tc),
        wc,
        np_split(td),
    ), np_split(inverse)


def mid_kernel(
    x, cos_p, sin_p, hot, kind, bank_hi, bank_lo, ta, wa, tb, tc, wc, td, out, xs, os, *, subs
):
    n = GROUP * BLOCKS
    step = pl.program_id(0)
    groups = x.shape[1]

    @pl.when(step == 0)
    def _():
        for g in range(groups):
            xs[g] = x[:, g, :]

    parts_hi, parts_lo = [], []
    for g in range(subs):
        lanes = slice(g * n, (g + 1) * n)
        y = dots(split(xs[step * subs + g]), (ta[0], ta[1]), ((0,), (0,)))
        yr, yi = y[:, :STOLT], y[:, STOLT:]
        y = jnp.concatenate([yr * wa[0] - yi * wa[1], yr * wa[1] + yi * wa[0]], 0)
        z = dots((tb[0], tb[1]), split(y), ((1,), (0,)))
        zr, zi = z[:n], z[n:]
        cp, sp = cos_p[lanes], sin_p[lanes]
        z = jnp.concatenate([zr * cp - zi * sp, zr * sp + zi * cp], 1)
        hi, lo = split(z)
        picked = jnp.dot(
            hot[g], jnp.concatenate([hi, lo], 1), preferred_element_type=f32
        ).astype(bf16)
        first, second = picked[:n], picked[n:]
        for c in range(2):
            for base, keep in ((0, parts_hi), (2 * STOLT, parts_lo)):
                cut = slice(base + c * STOLT, base + (c + 1) * STOLT)
                keep.append(jnp.concatenate([first[:, cut], second[:, cut]], 1))
    ghi = jnp.concatenate(parts_hi, 0)
    glo = jnp.concatenate(parts_lo, 0)
    kinds = kind[...].reshape(subs * 2 * n, 1)
    kinds = jnp.broadcast_to(kinds, (subs * 2 * n, STOLT))
    acc = jnp.zeros((subs * 2 * n, STOLT), f32)
    for k in range(0, bank_hi.shape[0], 2):
        khi = jnp.concatenate([bank_hi[k], bank_hi[k + 1]], 1)
        klo = jnp.concatenate([bank_lo[k], bank_lo[k + 1]], 1)
        r = dots((ghi, glo), (khi, klo), ((1,), (0,)))
        for half in range(2):
            acc = jnp.where(kinds == k + half, r[:, half * STOLT : (half + 1) * STOLT], acc)
    for g in range(subs):
        s = acc[g * 2 * n : (g + 1) * 2 * n]
        y = dots(split(s), (tc[0], tc[1]), ((0,), (0,)))
        yr, yi = y[:, :n], y[:, n:]
        y = jnp.concatenate([yr * wc[0] - yi * wc[1], yr * wc[1] + yi * wc[0]], 0)
        os[step * subs + g] = dots((td[0], td[1]), split(y), ((1,), (0,)))

    @pl.when(step == pl.num_programs(0) - 1)
    def _():
        for g in range(groups):
            out[:, g, :] = os[g]


def middle(x, cos_p, sin_p, hot, kind, bank_hi, bank_lo, tables):
    groups = x.shape[1]
    subs = min(4, groups)
    n = GROUP * BLOCKS
    whole = lambda a: pl.BlockSpec(a.shape, lambda i: (0,) * a.ndim)
    return pl.pallas_call(
        functools.partial(mid_kernel, subs=subs),
        grid=(groups // subs,),
        in_specs=[
            whole(x),
            pl.BlockSpec((subs * n, STOLT), lambda i: (i, 0)),
            pl.BlockSpec((subs * n, STOLT), lambda i: (i, 0)),
            pl.BlockSpec((subs, 2 * n, n), lambda i: (i, 0, 0)),
            pl.BlockSpec((subs, 2 * n, 1), lambda i: (i, 0, 0)),
            whole(bank_hi),
            whole(bank_lo),
        ]
        + [whole(t) for t in tables],
        out_specs=pl.BlockSpec((2 * STOLT, groups, n), lambda i: (0, 0, 0)),
        out_shape=jax.ShapeDtypeStruct((2 * STOLT, groups, n), f32),
        scratch_shapes=[
            pltpu.VMEM((groups, x.shape[0], n), f32),
            pltpu.VMEM((groups, 2 * STOLT, n), f32),
        ],
        name="middle",
    )(x, cos_p, sin_p, hot, kind, bank_hi, bank_lo, *tables)


def quarter_tables():
    q = P_SIZE // 4
    m = np.arange(q)
    fwd, inv = [], []
    for low in range(4):
        a = 2 * np.pi / P_SIZE * (((4 * m[:, None] + low) * m[None, :]) % P_SIZE)
        f = a.reshape(-1, 2, q).transpose(1, 0, 2).reshape(q, q // 8, 8)
        f = f.transpose(0, 2, 1).reshape(q, q)
        fwd.append(np.concatenate([np.cos(f), np.sin(f)], 0))
        inv.append(np.concatenate([np.cos(a.T), np.sin(a.T)], 0) / P_SIZE)
    return np.stack(fwd), np.stack(inv)


def swap_blocks(arrays):
    count = len(arrays)
    lanes = arrays[0].shape[-1]
    size = lanes // count
    block = lax.broadcasted_iota(jnp.int32, arrays[0].shape, 1) // size
    outs = []
    for b in range(count):
        acc = None
        for a in range(count):
            shift = (a - b) % count * size
            moved = pltpu.roll(arrays[a], shift, 1) if shift else arrays[a]
            acc = moved if acc is None else jnp.where(block == a, moved, acc)
        outs.append(acc)
    return outs


def core_kernel(*refs, n_pulse, n_scat, subs, trig, trig_low):
    lead, partial = refs[:2]
    sources = refs[2:12]
    out = refs[12]
    local = refs[13:23]
    steps_in, kinds_in, bank, table, ta, wa, tb, tc, wc, td = local
    binned, peer, spec, x, hot, kind, banks, os, twin_os, *twin_in = refs[23:34]
    (
        load, own_store, pair_send, pair_recv, near_send, near_recv, far_send, far_recv,
        twin_send, twin_recv, half_send,
    ) = refs[34:]
    n_dev = n_pulse * n_scat
    pulse = lax.axis_index("pulse")
    scat = lax.axis_index("scat")
    me = pulse * n_scat + scat
    half = peer.shape[0]
    lanes = 2 * half
    size = P_SIZE // 4
    n = GROUP * BLOCKS
    groups = os.shape[1] + SHARED
    pieces = groups // subs
    reach = n_pulse // 2
    side = lax.div(pulse, reach)
    twin = lax.rem(pulse + reach, n_pulse) * n_scat + scat
    quads = lanes // BIN_SIDE
    unit = subs * quads
    per = os.shape[2]
    moves = [(a, b) for a in range(n_pulse) for b in range(n_scat) if (a, b) != (0, 0)]
    moves.sort(key=lambda m: (-min(m[0], n_pulse - m[0]), m))

    def other(a, b):
        return lax.rem(pulse + a, n_pulse), lax.rem(scat + b, n_scat)

    barrier = pltpu.get_barrier_semaphore()
    for a, b in moves:
        p, c = other(a, b)
        pl.semaphore_signal(
            barrier, inc=1, device_id={"pulse": p, "scat": c}, device_id_type=MESH
        )
    keep = pl.ds(pl.multiple_of(scat * half, half), half)
    give = pl.ds(pl.multiple_of((1 - scat) * half, half), half)
    loads = [
        pltpu.make_async_copy(src, dst, load.at[i])
        for i, (src, dst) in enumerate(zip(sources, local))
    ]
    for copy in loads:
        copy.start()
    for cut, sums in echoes(lead[...], pulse * 2 * half, 2 * half, trig_low):
        binned[:, cut] = partial[:, cut] + sums
    pl.semaphore_wait(barrier, n_dev - 1)

    pair = pltpu.make_async_remote_copy(
        src_ref=binned.at[give, :],
        dst_ref=peer,
        send_sem=pair_send,
        recv_sem=pair_recv,
        device_id={"pulse": pulse, "scat": 1 - scat},
        device_id_type=MESH,
    )
    pair.start()
    metas = []
    for i in range(2):
        loads[i].wait()
        copy = pltpu.make_async_remote_copy(
            src_ref=local[i],
            dst_ref=twin_in[i],
            send_sem=twin_send.at[i],
            recv_sem=twin_recv.at[i],
            device_id={"pulse": lax.rem(pulse + reach, n_pulse), "scat": scat},
            device_id_type=MESH,
        )
        copy.start()
        metas.append(copy)
    loads[3].wait()
    pair.wait()

    quarters = []
    for q in range(4):
        pair_of = []
        for c in range(2):
            cut = slice(c * P_SIZE + q * size, c * P_SIZE + (q + 1) * size)
            pair_of.append(binned[keep, cut] + peer[:, cut])
        quarters.append(pair_of)
    (r0, i0), (r1, i1), (r2, i2), (r3, i3) = quarters
    sr, si, dr, di = r0 + r2, i0 + i2, r0 - r2, i0 - i2
    tr, ti, er, ei = r1 + r3, i1 + i3, r1 - r3, i1 - i3
    mixed = (
        (sr + tr, si + ti),
        (dr + ei, di - er),
        (sr - tr, si - ti),
        (dr - ei, di + er),
    )
    low = lax.broadcasted_iota(jnp.int32, (size, lanes), 1) < half
    rows = []
    for k in range(4):
        g = product(
            joined(table[0, k], table[1, k], 1),
            triple(jnp.concatenate(mixed[k], 0), 1),
            ((1,), (1,)),
        )
        turned = pltpu.roll(g[size:], half, 1)
        rows.append(g[:size] + jnp.where(low, turned, -turned))
    for q, z in enumerate(swap_blocks(rows)):
        for h in range(subs):
            spec[pl.ds(q * subs + h, size // subs, stride=unit), :] = z[
                h * (size // subs) : (h + 1) * (size // subs)
            ]

    def piece(dev, i):
        return pl.ds(pl.multiple_of((dev * pieces + i) * unit, unit), unit)

    def source(p, c, i):
        if i < pieces:
            return piece(p * n_scat + c, i)
        return piece(lax.rem(p + reach, n_pulse) * n_scat + c, pieces - 1)

    own = pl.ds(pl.multiple_of(me * unit, unit), unit)
    for i in range(pieces + 1):
        for j, (a, b) in enumerate(moves):
            p, c = other(a, b)
            pltpu.make_async_remote_copy(
                src_ref=spec.at[source(p, c, i), :],
                dst_ref=x.at[i, own, :],
                send_sem=near_send.at[j],
                recv_sem=near_recv.at[i, me],
                device_id={"pulse": p, "scat": c},
                device_id_type=MESH,
            ).start()
    for i in range(pieces + 1):
        x[i, own, :] = spec[source(pulse, scat, i), :]

    for i in (2, 4, 5, 6, 7, 8, 9):
        loads[i].wait()
    for copy in metas:
        copy.wait()
    block = lax.broadcasted_iota(jnp.int32, (n, STOLT), 0)
    lane = lax.broadcasted_iota(jnp.int32, (n, STOLT), 1)
    spot = lane.astype(f32)
    above = (block // BLOCKS * BLOCKS).astype(f32)
    flat = []
    for i in range(2):
        both = [
            jnp.concatenate([ref[pl.ds(j, groups, stride=GROUP), :] for j in range(GROUP)], 1)
            for ref in (local[i], twin_in[i])
        ]
        flat.append(jnp.concatenate([both[0], both[1][groups - subs :]], 0))
    for g in range(groups + subs):
        first = jnp.broadcast_to(flat[0][g : g + 1].astype(f32), (n, n)).T + above
        hot[g, :n] = jnp.where(first == spot, 1.0, 0.0).astype(bf16)
        hot[g, n:] = jnp.where(first + 1.0 == spot, 1.0, 0.0).astype(bf16)
        kind[g] = jnp.broadcast_to(flat[1][g : g + 1], (8, n))
    for k in range(bank.shape[0]):
        turned = jnp.concatenate([bank[k, :STOLT].T, bank[k, STOLT:].T], 1)
        hi, lo = split(turned)
        banks[k * STOLT : (k + 1) * STOLT] = jnp.concatenate([hi, hi, lo], 1)

    cols = (lane + (block % BLOCKS) * STOLT).astype(f32)
    kr = 4.0 * np.pi / 3e8 * (9.6e9 + (cols - F_LEN // 2) * (1.5e8 / F_LEN))

    def phase(owner, g):
        row = owner * (groups * GROUP) + g * GROUP + block // BLOCKS
        centered = lax.rem(row + P_SIZE // 2, P_SIZE) - P_SIZE // 2
        along = 2.0 * np.pi / (P_SIZE * SPACING) * centered.astype(f32)
        squared = along * along
        depth = NEAR + B // 2
        theta = -depth * squared / (jnp.sqrt(kr * kr - squared) + kr)
        whole = jnp.round(theta * (0.5 / np.pi))
        for part in turn_parts():
            theta = theta - whole * part
        r = theta * (0.5 / np.pi)
        u = r * r
        sn = r * horner(u, trig[0])
        cs = horner(u, trig[1])
        return 1.0 - 2.0 * sn * sn, 2.0 * sn * cs

    def ranged(slot, owner, g, cut):
        i, h = lax.div(slot, subs), lax.rem(slot, subs)
        cp, sp = phase(owner, g)
        rows_in = x[i, pl.ds(h, n_dev * quads, stride=subs), :]
        y = product(triple(rows_in, 0), joined(ta[0], ta[1], 0), ((0,), (0,)))
        yr, yi = y[:, :STOLT], y[:, STOLT:]
        y = jnp.concatenate([yr * wa[0] - yi * wa[1], yr * wa[1] + yi * wa[0]], 0)
        z = product(joined(tb[0], tb[1], 1), triple(y, 0))
        zr, zi = z[:n], z[n:]
        z = jnp.concatenate([zr * cp - zi * sp, zr * sp + zi * cp], 1)
        picked = product(hot[slot], jnp.concatenate(split(z), 1)).astype(bf16)
        first, second = picked[:n], picked[n:]
        parts = []
        for base in (0, 2 * STOLT):
            cuts = [slice(base + c * STOLT, base + (c + 1) * STOLT) for c in range(2)]
            parts.append(
                jnp.concatenate(
                    [jnp.concatenate([first[:, v], second[:, v]], 1) for v in cuts], 0
                )
            )
        ghi, glo = parts
        windows = jnp.concatenate([ghi, glo, ghi], 1)
        kinds = jnp.concatenate([kind[slot, 0:1]] * 2, 1)
        acc = jnp.zeros((STOLT, 2 * n), f32)
        for first in range(0, banks.shape[0], STREAM):
            r = product(banks[first : first + STREAM], windows, ((1,), (1,)))
            for v in range(STREAM // STOLT):
                k = first // STOLT + v
                acc = jnp.where(kinds == k, r[v * STOLT : (v + 1) * STOLT], acc)
        y = product(triple(acc, 1), joined(tc[0], tc[1], 0))
        yr, yi = y[:, :n], y[:, n:]
        y = jnp.concatenate([yr * wc[0] - yi * wc[1], yr * wc[1] + yi * wc[0]], 0)
        z = product(joined(td[0, cut, :], td[1, cut, :], 1), triple(y, 0))
        return z.reshape(-1, per, n)

    def arrived(i):
        for a, b in moves:
            p, c = other(a, b)
            src = p * n_scat + c
            here = pl.ds(pl.multiple_of(src * unit, unit), unit)
            pltpu.make_async_copy(
                x.at[i, here, :], x.at[i, here, :], near_recv.at[i, src]
            ).wait()

    def step(g, carry):
        @pl.when(lax.rem(g, subs) == 0)
        def _():
            arrived(lax.div(g, subs))

        os[:, g] = ranged(g, me, g, slice(None))
        for j, (a, b) in enumerate(moves):
            p, c = other(a, b)
            pltpu.make_async_remote_copy(
                src_ref=os.at[p * n_scat + c, g],
                dst_ref=out.at[me, g],
                send_sem=far_send.at[j],
                recv_sem=far_recv.at[me],
                device_id={"pulse": p, "scat": c},
                device_id_type=MESH,
            ).start()
        return carry

    close = [(a, b) for a in range(reach) for b in range(n_scat) if (a, b) != (0, 0)]
    within = pulse - side * reach

    def beside(a, b):
        return lax.rem(within + a, reach), lax.rem(scat + b, n_scat)

    part = 2 * STOLT // 2
    served = pl.ds(pl.multiple_of(side * part, part), part)

    lax.fori_loop(0, groups - SHARED, step, 0)
    if SHARED == subs:
        arrived(pieces - 1)
    arrived(pieces)

    def half_step(t, carry):
        v, h = lax.div(t, SHARED), lax.rem(t, SHARED)
        owner = lax.rem(pulse + v * reach, n_pulse) * n_scat + scat
        g = groups - SHARED + h
        twin_os[v, :, h] = ranged(g + v * subs, owner, g, served)
        for j, (a, b) in enumerate(close):
            p, c = beside(a, b)
            pltpu.make_async_remote_copy(
                src_ref=twin_os.at[v, p * n_scat + c, h],
                dst_ref=out.at[owner, g],
                send_sem=half_send.at[j],
                recv_sem=far_recv.at[owner],
                device_id={"pulse": side * reach + p, "scat": c},
                device_id_type=MESH,
            ).start()
        return carry

    lax.fori_loop(0, 2 * SHARED, half_step, 0)
    first, last = pl.ds(0, groups - SHARED), pl.ds(groups - SHARED, SHARED)
    here = within * n_scat + scat
    stores = [
        pltpu.make_async_copy(src, dst, own_store.at[i])
        for i, (src, dst) in enumerate(
            (
                (os.at[me], out.at[me, first]),
                (twin_os.at[0, here], out.at[me, last]),
                (twin_os.at[1, here], out.at[twin, last]),
            )
        )
    ]
    for copy in stores:
        copy.start()
    for copy in stores:
        copy.wait()
    for j, (a, b) in enumerate(close):
        whole = os.at[0, pl.ds(0, 2 * SHARED)]
        pltpu.make_async_copy(whole, whole, half_send.at[j]).wait()
    for j, (a, b) in enumerate(moves):
        p, c = other(a, b)
        src = p * n_scat + c
        whole = spec.at[pl.ds(0, (pieces + 1) * unit), :]
        pltpu.make_async_copy(whole, whole, near_send.at[j]).wait()
        pltpu.make_async_copy(os.at[src], os.at[src], far_send.at[j]).wait()
        whole = out.at[src, first] if (a, b) == (reach, 0) else out.at[src]
        pltpu.make_async_copy(whole, whole, far_recv.at[src]).wait()


def turn_parts():
    parts, rest = [], 2.0 * np.pi
    for bits in (10, 22, 60):
        scale = 2.0**bits
        part = float(np.float32(np.round(rest * scale) / scale))
        parts.append(part)
        rest -= part
    return parts


def core(partial, lead, steps_in, kinds_in, bank, tables, n_pulse, n_scat):
    n_dev = n_pulse * n_scat
    groups = steps_in.shape[0] // GROUP
    subs = 2
    n = GROUP * BLOCKS
    span, width = partial.shape
    half = span // n_scat
    quads = 2 * half // BIN_SIDE
    kernels = bank.shape[0]
    per = 2 * STOLT // n_dev
    sources = (steps_in, kinds_in, bank, *tables)
    dma = pltpu.SemaphoreType.DMA
    return pl.pallas_call(
        functools.partial(
            core_kernel,
            n_pulse=n_pulse,
            n_scat=n_scat,
            subs=subs,
            trig=range_trig_coefs(5),
            trig_low=range_trig_coefs(4),
        ),
        in_specs=[IN_VMEM] * 2 + [IN_HBM] * len(sources),
        out_specs=pl.BlockSpec(memory_space=pl.ANY),
        out_shape=jax.ShapeDtypeStruct((n_dev, groups, per, n), f32),
        scratch_shapes=[pltpu.VMEM(a.shape, a.dtype) for a in sources]
        + [
            pltpu.VMEM((span, width), f32),
            pltpu.VMEM((half, width), f32),
            pltpu.VMEM((n_dev * groups * quads, n), f32),
            pltpu.VMEM((groups // subs + 1, n_dev * subs * quads, n), f32),
            pltpu.VMEM((groups + subs, 2 * n, n), bf16),
            pltpu.VMEM((groups + subs, 8, n), jnp.int32),
            pltpu.VMEM((kernels * STOLT, 6 * STOLT), bf16),
            pltpu.VMEM((n_dev, groups - SHARED, per, n), f32),
            pltpu.VMEM((2, n_dev // 2, SHARED, per, n), f32),
            pltpu.VMEM(steps_in.shape, steps_in.dtype),
            pltpu.VMEM(kinds_in.shape, kinds_in.dtype),
            dma((len(sources),)),
            dma((3,)),
            dma,
            dma,
            dma((n_dev,)),
            dma((groups // subs + 1, n_dev)),
            dma((n_dev,)),
            dma((n_dev,)),
            dma((2,)),
            dma((2,)),
            dma((n_dev // 2,)),
        ],
        compiler_params=pltpu.CompilerParams(
            collective_id=0, has_side_effects=True, vmem_limit_bytes=24 << 20
        ),
        name="core",
    )(lead, partial, *in_hbm(sources))


def image_kernel(x, table, out, done, sems):
    lanes = x.shape[1]
    per = x.shape[0] * GROUP // P_SIZE
    size = P_SIZE // 4
    copies = []
    for h in range(per // (2 * GROUP)):
        columns = [[] for _ in range(4)]
        for c in range(2):
            first = (2 * h + c) * GROUP
            tiles = [x[pl.ds(first + j, size, stride=per), :] for j in range(4)]
            for k, z in enumerate(swap_blocks(tiles)):
                columns[k].append(z)
        v = []
        for k in range(4):
            g = product(
                joined(table[0, k], table[1, k], 1), triple(jnp.concatenate(columns[k], 1), 0)
            )
            cos_g, sin_g = g[:size], g[size:]
            v.append((cos_g[:, :lanes] - sin_g[:, lanes:], cos_g[:, lanes:] + sin_g[:, :lanes]))
        (r0, i0), (r1, i1), (r2, i2), (r3, i3) = v
        sr, si, dr, di = r0 + r2, i0 + i2, r0 - r2, i0 - i2
        tr, ti, er, ei = r1 + r3, i1 + i3, r1 - r3, i1 - i3
        mixed = (
            (sr + tr, si + ti),
            (dr - ei, di + er),
            (sr - tr, si - ti),
            (dr + ei, di - er),
        )
        for q in range(4):
            for c in range(2):
                done[h, c, q * size : (q + 1) * size, :] = mixed[q][c]
        copy = pltpu.make_async_copy(
            done.at[h], out.at[:, :, pl.ds(h * lanes, lanes)], sems.at[h]
        )
        copy.start()
        copies.append(copy)
    for copy in copies:
        copy.wait()


def reference_phase(row_ids, cols):
    centered = (row_ids + P_SIZE // 2) % P_SIZE - P_SIZE // 2
    along_k = 2.0 * jnp.pi / (P_SIZE * SPACING) * centered.astype(f32)
    kr = 4.0 * jnp.pi / 3e8 * (9.6e9 + (cols.astype(f32) - F_LEN // 2) * (1.5e8 / F_LEN))
    squared = along_k * along_k
    depth = NEAR + B // 2
    return (
        -depth
        * squared[:, None]
        / (jnp.sqrt(kr[None, :] * kr[None, :] - squared[:, None]) + kr[None, :])
    )


def on_device(positions, amplitude, range_cells, bounce, stolt_block, kernel_choice, kernel_bank):
    n_pulse = lax.axis_size("pulse")
    n_scat = lax.axis_size("scat")
    n_dev = n_pulse * n_scat
    pulse_here = lax.axis_index("pulse")
    scat_here = lax.axis_index("scat")
    pulses = P_SIZE // n_pulse
    rows = P_SIZE // n_dev
    width = F_LEN // n_dev
    groups = rows // GROUP
    n = GROUP * BLOCKS
    bins_scat = B // n_scat
    bins_here = bins_scat // n_pulse

    per = STOLT // n_dev
    span = B // n_pulse
    packed = (
        span == 128
        and n_scat == 2
        and per % 4 == 0
        and groups % 8 == 0
        and positions.shape[0] % CHUNK == 0
    )
    if packed:
        partial, lead = range_binning(
            positions, amplitude, range_cells, bounce, pulse_here * span, span
        )
        local = bins_here // BIN_SIDE
        i, s, c, l = np.meshgrid(
            np.arange(n_pulse), np.arange(n_scat), np.arange(2), np.arange(local), indexing="ij"
        )
        order = (c * BIN_SIDE + (i * n_scat + s) * local + l).reshape(-1)
        tables, backward = core_tables(n_dev, order)
        tables = tuple(jnp.asarray(t) for t in tables)
        columns = core(
            partial, lead, stolt_block, kernel_choice, kernel_bank, tables, n_pulse, n_scat
        )
        return pl.pallas_call(
            image_kernel,
            in_specs=[IN_VMEM, IN_VMEM],
            out_specs=pl.BlockSpec(memory_space=pl.ANY),
            out_shape=jax.ShapeDtypeStruct((2, P_SIZE, width), f32),
            scratch_shapes=[
                pltpu.VMEM((width // n, 2, P_SIZE, n), f32),
                pltpu.SemaphoreType.DMA((width // n,)),
            ],
            compiler_params=pltpu.CompilerParams(vmem_limit_bytes=16 << 20),
            name="image",
        )(columns.reshape(-1, n), jnp.asarray(backward))

    ids = jnp.arange(GROUP, dtype=jnp.int32)[None, :, None] * BLOCKS
    first = stolt_block.reshape(groups, GROUP, BLOCKS) + ids
    pick = jnp.stack([first, first + 1], 1).reshape(groups, 2 * n, 1)
    hot = (pick == jnp.arange(n, dtype=jnp.int32)[None, None, :]).astype(bf16)
    kind = jnp.stack([kernel_choice.reshape(groups, n)] * 2, 1).reshape(groups, 2 * n, 1)
    bank_hi = lax.reduce_precision(kernel_bank, 8, 7)
    bank_lo = (kernel_bank - bank_hi).astype(bf16)
    bank_hi = bank_hi.astype(bf16)
    row_ids = (pulse_here * n_scat + scat_here) * rows + jnp.arange(rows, dtype=jnp.int32)
    theta = reference_phase(row_ids, jnp.arange(F_LEN, dtype=jnp.int32))
    theta = theta.reshape(rows * BLOCKS, STOLT)
    cos_p, sin_p = jnp.cos(theta), jnp.sin(theta)

    partial = binning(positions, amplitude, range_cells, bounce, pulse_here * pulses, pulses)
    partial = partial.reshape(n_scat, bins_scat, 2 * pulses)
    binned = lax.dynamic_index_in_dim(partial, scat_here, 0, keepdims=False)
    for shift in range(1, n_scat):
        other = lax.dynamic_index_in_dim(
            partial, (scat_here + shift) % n_scat, 0, keepdims=False
        )
        ring = [(i, (i + shift) % n_scat) for i in range(n_scat)]
        binned = binned + lax.ppermute(other, "scat", ring)
    turned = lax.all_to_all(
        binned.reshape(n_pulse, bins_here, 2 * pulses), "pulse", 0, 0, tiled=True
    )
    turned = turned.reshape(n_pulse, bins_here, 2, pulses).transpose(0, 3, 2, 1)
    turned = turned.reshape(P_SIZE, 2 * bins_here)
    k = np.arange(P_SIZE)
    angle = 2 * np.pi / P_SIZE * ((k[:, None] * k[None, :]) % P_SIZE)
    az = jnp.asarray(np.concatenate([np.cos(angle), np.sin(angle)], 0), f32)
    product = jnp.dot(az, turned, precision=HIGH, preferred_element_type=f32)
    pc, ps = product[:P_SIZE], product[P_SIZE:]
    spectrum = pc + jnp.concatenate([ps[:, bins_here:], -ps[:, :bins_here]], 1)
    az_rows = lax.all_to_all(
        spectrum.reshape(n_dev, rows, 2 * bins_here), ("pulse", "scat"), 0, 0, tiled=True
    )
    x = az_rows.reshape(n_pulse, n_scat, rows, 2, bins_here).transpose(3, 1, 0, 4, 2)
    x = x.reshape(2, BIN_SIDE, BIN_SIDE, rows).transpose(0, 1, 3, 2)
    x = x.reshape(2 * BIN_SIDE, groups, n)
    order = np.arange(2 * BIN_SIDE)

    tables = tuple(jnp.asarray(t) for t in mid_tables(n_dev, order))
    ranged = middle(x, cos_p, sin_p, hot, kind, bank_hi, bank_lo, tables)
    columns = lax.all_to_all(
        ranged.reshape(n_dev, 2 * per, rows * BLOCKS), ("pulse", "scat"), 0, 0, tiled=True
    )
    columns = columns.reshape(n_dev, 2, per, rows, BLOCKS).transpose(0, 3, 1, 2, 4)
    columns = columns.reshape(P_SIZE, 2 * width)
    final = jnp.dot(az, columns, precision=HIGH, preferred_element_type=f32)
    fc, fs = final[:P_SIZE], final[P_SIZE:]
    re = (fc[:, :width] - fs[:, width:]) / P_SIZE
    im = (fc[:, width:] + fs[:, :width]) / P_SIZE
    return jnp.stack([re, im])


def solution(mesh):
    placed = (
        P(("scene", "scat")),
        P(None, ("scene", "scat")),
        P(("scene", "scat")),
        P(("scene", "scat")),
        P(("pulse", "scat"), None),
        P(("pulse", "scat"), None),
        P(),
    )
    return jax.shard_map(
        on_device,
        mesh=mesh,
        in_specs=placed,
        out_specs=P(None, "scene", ("pulse", "scat")),
        check_vma=False,
    )
```

```python
import functools

import jax
import jax.numpy as jnp
import numpy as np
from jax import lax
from jax.experimental import pallas as pl
from jax.experimental.pallas import tpu as pltpu
from jax.sharding import PartitionSpec as P

P_SIZE = 512
F_LEN = 4096
B = 1024
SHIFT = 16
STOLT = 128
BLOCKS = 32
SPACING = 2.0
NEAR = 700000.0
BIN_SIDE = 32
GROUP = 4
CHUNK = 512
SLOTS = 112
LANES = 128
WIDE = 128
AHEAD = 1152
SHARED = 1
STREAM = 512
HIGH = lax.Precision.HIGH
MESH = pl.DeviceIdType.MESH
IN_HBM = pl.BlockSpec(memory_space=pltpu.HBM)
IN_VMEM = pl.BlockSpec(memory_space=pltpu.VMEM)
f32 = jnp.float32
bf16 = jnp.bfloat16


def trig_coefs():
    x = np.cos(np.pi * (np.arange(400) + 0.5) / 400) * 0.5
    u = x * x
    s = np.polynomial.chebyshev.Chebyshev.fit(u, np.sin(np.pi * x) / x, 5).convert(
        kind=np.polynomial.Polynomial
    )
    c = np.polynomial.chebyshev.Chebyshev.fit(u, np.cos(np.pi * x), 5).convert(
        kind=np.polynomial.Polynomial
    )
    return [float(v) for v in s.coef], [float(v) for v in c.coef]


def horner(u, coefs):
    acc = jnp.full_like(u, coefs[-1])
    for c in coefs[-2::-1]:
        acc = acc * u + c
    return acc


def split(x):
    hi = x.astype(bf16)
    lo = (x - hi.astype(f32)).astype(bf16)
    return hi, lo


def np_split(x):
    x = np.asarray(x, np.float64)
    hi = np.asarray(x, jnp.bfloat16)
    lo = np.asarray(x - hi.astype(np.float64), jnp.bfloat16)
    return np.stack([hi, lo])


def dots(a, b, dims):
    d = functools.partial(
        lax.dot_general, dimension_numbers=(dims, ((), ())), preferred_element_type=f32
    )
    return d(a[0], b[0]) + (d(a[0], b[1]) + d(a[1], b[0]))


def in_hbm(arrays):
    return [pltpu.with_memory_space_constraint(a, pltpu.HBM) for a in arrays]


def joined(hi, lo, axis):
    return jnp.concatenate([hi, hi, lo], axis)


def triple(x, axis):
    hi, lo = split(x)
    return jnp.concatenate([hi, lo, hi], axis)


def product(a, b, dims=((1,), (0,))):
    return lax.dot_general(a, b, (dims, ((), ())), preferred_element_type=f32)


def bin_kernel(pulse_base, pos, amp, tgt, bnc, out, acc, *, pulses, sin_c, cos_c):
    step = pl.program_id(0)
    width = pos.shape[1]

    @pl.when(step == 0)
    def _():
        acc[...] = jnp.zeros_like(acc)

    base = pulse_base[0]
    ids = base + lax.broadcasted_iota(jnp.int32, (pulses, width), 0)
    along = (ids.astype(f32) - P_SIZE // 2) * SPACING
    target = tgt[...] + SHIFT * bnc[...]
    slant = NEAR + target.astype(f32)
    offset = along - pos[...]
    square = offset * offset
    excess = square / (jnp.sqrt(slant * slant + square) + slant)
    halves = excess * -128.0
    whole = jnp.round(halves)
    r = halves - whole
    u = r * r
    odd = whole - 2.0 * jnp.floor(whole * 0.5)
    sign = 1.0 - 2.0 * odd
    sin_p = sign * r * horner(u, sin_c)
    cos_p = sign * horner(u, cos_c)
    flip = 1.0 - 2.0 * bnc[...].astype(f32)
    are = flip * amp[0:1]
    aim = flip * amp[1:2]
    re = are * cos_p - aim * sin_p
    im = are * sin_p + aim * cos_p
    steer = jnp.concatenate([re, im], 0)
    hi, lo = split(steer)
    rhs = jnp.concatenate([hi, lo], 0)
    bins = lax.broadcasted_iota(jnp.int32, (B, width), 0)
    hot = jnp.where(bins == target, 1.0, 0.0).astype(bf16)
    acc[...] += lax.dot_general(
        hot, rhs, (((1,), (1,)), ((), ())), preferred_element_type=f32
    )

    @pl.when(step == pl.num_programs(0) - 1)
    def _():
        out[...] = acc[:, : 2 * pulses] + acc[:, 2 * pulses :]


def binning(positions, amplitude, cells, bounce, pulse_base, pulses):
    count = positions.shape[0]
    width = min(2048, count)
    sin_c, cos_c = trig_coefs()
    row = lambda n: pl.BlockSpec((n, width), lambda i: (0, i))
    return pl.pallas_call(
        functools.partial(bin_kernel, pulses=pulses, sin_c=sin_c, cos_c=cos_c),
        grid=(count // width,),
        in_specs=[pl.BlockSpec(memory_space=pltpu.SMEM), row(1), row(2), row(1), row(1)],
        out_specs=pl.BlockSpec((B, 2 * pulses), lambda i: (0, 0)),
        out_shape=jax.ShapeDtypeStruct((B, 2 * pulses), f32),
        scratch_shapes=[pltpu.VMEM((B, 4 * pulses), f32)],
        name="binning",
    )(
        pulse_base.reshape(1),
        positions.reshape(1, count),
        amplitude,
        cells.reshape(1, count),
        bounce.reshape(1, count),
    )


def range_trig_coefs(degree):
    x = np.cos(np.pi * (np.arange(400) + 0.5) / 400) * 0.5
    u = x * x
    fit = lambda y: np.polynomial.chebyshev.Chebyshev.fit(u, y, degree).convert(
        kind=np.polynomial.Polynomial
    )
    return [float(v) for v in fit(np.sin(np.pi * x) / x).coef], [
        float(v) for v in fit(np.cos(np.pi * x)).coef
    ]


def split3(x):
    hi = x.astype(bf16).astype(f32)
    rest = x - hi
    mid = rest.astype(bf16).astype(f32)
    return hi, mid, rest - mid


def turn(r, trig):
    u = r * r
    sn = r * horner(u, trig[0])
    cs = horner(u, trig[1])
    twice = sn + sn
    return 1.0 - twice * sn, twice * cs


def times(a, b):
    return a[0] * b[0] - a[1] * b[1], a[0] * b[1] + a[1] * b[0]


def echoes(data, base, bins, trig):
    width = data.shape[1]
    chunk = min(width, LANES)
    hots, tiles = [], [[[], []] for _ in range(P_SIZE // 128)]
    for left in range(0, width, chunk):
        where, re_amp, im_amp, rel = (data[j : j + 1, left : left + chunk] for j in range(4))
        re2, im2 = 2.0 * re_amp, 2.0 * im_amp
        inverse = 0.5 / (rel + (base.astype(f32) + NEAR))
        gain = inverse * -64.0
        gain2 = gain + gain
        bend = inverse * (1.0 / 64.0)
        rows = lax.broadcasted_iota(jnp.int32, (bins, chunk), 0).astype(f32)
        hot = jnp.where(rows == rel, 1.0, 0.0).astype(bf16)
        hots += [hot, hot]
        odd = lax.broadcasted_iota(jnp.int32, (8, chunk), 0).astype(f32) * 2.0 + 1.0
        even = turn(odd * odd * (SPACING * SPACING / 4.0) * gain, trig)
        for q in range(P_SIZE // 128):
            ids = lax.broadcasted_iota(jnp.int32, (16, chunk), 0)
            middle = (ids * 8 + (q * 128 - P_SIZE // 2)).astype(f32) + 3.5
            offset = middle * SPACING - where
            t = offset * offset * gain
            y = t * bend
            t = t * (1.0 + y * (1.0 + 2.0 * y))
            r = t - jnp.round(t)
            u = r * r
            sn = r * horner(u, trig[0])
            cs = horner(u, trig[1])
            at = (re_amp - sn * (re2 * sn + im2 * cs), im_amp + sn * (re2 * cs - im2 * sn))
            slope = offset * gain2 * (1.0 + y * (2.0 + 6.0 * y))
            power = turn(slope * (SPACING / 2.0), trig)
            square = (1.0 - 2.0 * power[1] * power[1], 2.0 * power[0] * power[1])
            made = [None] * 8
            for j in range(4):
                a = times(at, (even[0][j : j + 1], even[1][j : j + 1]))
                rr, ii = a[0] * power[0], a[1] * power[1]
                ri, ir = a[0] * power[1], a[1] * power[0]
                made[4 + j] = (rr - ii, ri + ir)
                made[3 - j] = (rr + ii, ir - ri)
                if j < 3:
                    power = times(power, square)
            for c in range(2):
                tiles[q][c].append(
                    jnp.concatenate([jnp.concatenate(split(v[c]), 1) for v in made], 0)
                )
    hot = jnp.concatenate(hots, 1)
    for q in range(P_SIZE // 128):
        for c in range(2):
            lanes = slice(c * P_SIZE + q * 128, c * P_SIZE + (q + 1) * 128)
            yield lanes, product(hot, jnp.concatenate(tiles[q][c], 1), ((1,), (1,)))


def range_bin_kernel(base_ref, *refs, span, trig):
    out, lead = refs[6:8]
    buf, load = refs[14:]
    cells8, bounce8, pos, amp, cells, bnc = refs[8:14]
    loads = [
        pltpu.make_async_copy(src, dst, load.at[i])
        for i, (src, dst) in enumerate(zip(refs[:6], refs[8:14]))
    ]
    for copy in loads:
        copy.start()
    for copy in loads:
        copy.wait()
    base = base_ref[0]
    rows = cells8.shape[0]
    deep = CHUNK // 128
    chunks = rows // deep
    target = cells8[...] + SHIFT * bounce8[...] - base
    match = jnp.where((target >= 0) & (target < span), 1.0, 0.0)
    mb = match.astype(bf16)
    a = lax.broadcasted_iota(jnp.int32, (128, 128), 0)
    b = lax.broadcasted_iota(jnp.int32, (128, 128), 1)
    upto = jnp.where(a <= b, 1.0, 0.0).astype(bf16)
    count = jnp.dot(mb, upto, preferred_element_type=f32)
    total = jnp.dot(mb, jnp.ones((128, 128), bf16), preferred_element_type=f32)
    a = lax.broadcasted_iota(jnp.int32, (rows, rows), 0)
    b = lax.broadcasted_iota(jnp.int32, (rows, rows), 1)
    below = jnp.where((a // deep == b // deep) & (b < a), 1.0, 0.0).astype(bf16)
    ahead = jnp.dot(below, total.astype(bf16), preferred_element_type=f32)
    rank = jnp.where(match > 0.0, count + ahead - 1.0, -1.0)
    counts = [
        jnp.sum(match[deep * c : deep * (c + 1)]).astype(jnp.int32) for c in range(chunks)
    ]

    def values(c):
        lanes = slice(CHUNK * c, CHUNK * (c + 1))
        flip = 1.0 - 2.0 * bnc[:, lanes].astype(f32)
        rel = (cells[:, lanes] + SHIFT * bnc[:, lanes] - base).astype(f32)
        zero = jnp.zeros_like(rel)
        data = jnp.concatenate(
            [pos[:, lanes], amp[0:1, lanes] * flip, amp[1:2, lanes] * flip, rel] + [zero] * 4, 0
        )
        return jnp.concatenate(list(split3(data)) + [jnp.zeros_like(data)], 0).astype(bf16)

    def pick(c, first):
        slots = lax.broadcasted_iota(jnp.int32, (SLOTS, 128), 0).astype(f32) + first
        hot = jnp.concatenate(
            [
                jnp.where(rank[deep * c + j : deep * c + j + 1] == slots, 1.0, 0.0)
                for j in range(deep)
            ],
            1,
        ).astype(bf16)
        return lax.dot_general(
            hot, values(c), (((1,), (1,)), ((), ())), preferred_element_type=f32
        )

    start = 0
    for c in range(chunks):
        buf[pl.ds(start, SLOTS), 0:32] = pick(c, 0.0)
        start = start + counts[c]
    most = functools.reduce(jnp.maximum, counts)

    @pl.when(most > SLOTS)
    def _():
        begin = 0
        for c in range(chunks):

            @pl.loop(0, (counts[c] + SLOTS - 1) // SLOTS)
            def _(i):
                first = (i * SLOTS).astype(f32)
                buf[pl.ds(begin + i * SLOTS, SLOTS), 0:32] = pick(c, first)

            begin = begin + counts[c]

    buf[pl.ds(start, AHEAD), :] = jnp.zeros((AHEAD, 128), f32)

    def data(first, width):
        cols = []
        for h in range(width // 128):
            t = buf[pl.ds(first + h * 128, 128), :].T
            cols.append(t[0:8] + t[8:16] + t[16:24])
        return jnp.concatenate(cols, 1)

    lead[...] = data(0, AHEAD)
    out[...] = jnp.zeros_like(out)

    @pl.loop(AHEAD // WIDE, (start + WIDE - 1) // WIDE)
    def _(i):
        for lanes, sums in echoes(data(i * WIDE, WIDE), base, span, trig):
            out[:, lanes] += sums


def range_binning(positions, amplitude, cells, bounce, base, span):
    count = positions.shape[0]
    rows = count // 128
    sources = (
        cells.reshape(rows, 128),
        bounce.reshape(rows, 128),
        positions.reshape(1, count),
        amplitude,
        cells.reshape(1, count),
        bounce.reshape(1, count),
    )
    return pl.pallas_call(
        functools.partial(range_bin_kernel, span=span, trig=range_trig_coefs(4)),
        in_specs=[pl.BlockSpec(memory_space=pltpu.SMEM)] + [IN_HBM] * len(sources),
        out_specs=(IN_VMEM, IN_VMEM),
        out_shape=(
            jax.ShapeDtypeStruct((span, 2 * P_SIZE), f32),
            jax.ShapeDtypeStruct((8, AHEAD), f32),
        ),
        scratch_shapes=[pltpu.VMEM(a.shape, a.dtype) for a in sources]
        + [
            pltpu.VMEM((count + SLOTS + AHEAD, 128), f32),
            pltpu.SemaphoreType.DMA((len(sources),)),
        ],
        compiler_params=pltpu.CompilerParams(vmem_limit_bytes=16 << 20),
        name="range_binning",
    )(base.reshape(1), *in_hbm(sources))


def complex_rows(c, s):
    return np.block([[c, s], [-s, c]])


def mid_factors(n_dev, order):
    side = np.arange(BIN_SIDE)
    t = np.arange(STOLT)
    eye = np.eye(GROUP)
    a = -2 * np.pi / STOLT * ((side[:, None] * t[None, :]) % STOLT)
    ta = complex_rows(np.cos(a), np.sin(a))[order]
    a = -2 * np.pi / F_LEN * (side[:, None] * t[None, :])
    wa = np.stack([np.tile(np.cos(a), (GROUP, 1)), np.tile(np.sin(a), (GROUP, 1))])
    a = -2 * np.pi / BIN_SIDE * ((side[:, None] * side[None, :]) % BIN_SIDE)
    c, s = np.kron(eye, np.cos(a)), np.kron(eye, np.sin(a))
    tb = complex_rows(c, s).T
    blk = np.arange(BLOCKS)
    a = 2 * np.pi / BLOCKS * ((blk[:, None] * blk[None, :]) % BLOCKS)
    c, s = np.kron(eye, np.cos(a)), np.kron(eye, np.sin(a))
    tc = complex_rows(c, s)
    a = 2 * np.pi / F_LEN * (t[:, None] * blk[None, :])
    wc = np.stack([np.tile(np.cos(a), (1, GROUP)), np.tile(np.sin(a), (1, GROUP))])
    a = 2 * np.pi / STOLT * ((t[:, None] * t[None, :]) % STOLT)
    td = complex_rows(np.cos(a), np.sin(a)).T / F_LEN
    td = td.reshape(2, n_dev, STOLT // n_dev, 2 * STOLT).transpose(1, 0, 2, 3)
    return ta, wa.astype(np.float32), tb, tc, wc.astype(np.float32), td


def mid_tables(n_dev, order):
    ta, wa, tb, tc, wc, td = mid_factors(n_dev, order)
    td = td.reshape(2 * STOLT, 2 * STOLT)
    return np_split(ta), wa, np_split(tb), np_split(tc), wc, np_split(td)


def core_tables(n_dev, order):
    ta, wa, tb, tc, wc, td = mid_factors(n_dev, order)
    td = td.reshape(n_dev, 2, -1, GROUP, 2 * STOLT).transpose(0, 2, 1, 3, 4)
    td = td.reshape(2 * STOLT, 2 * STOLT)
    forward, inverse = quarter_tables()
    return (
        np_split(forward),
        np_split(ta),
        wa,
        np_split(tb),
        np_split(tc),
        wc,
        np_split(td),
    ), np_split(inverse)


def mid_kernel(
    x, cos_p, sin_p, hot, kind, bank_hi, bank_lo, ta, wa, tb, tc, wc, td, out, xs, os, *, subs
):
    n = GROUP * BLOCKS
    step = pl.program_id(0)
    groups = x.shape[1]

    @pl.when(step == 0)
    def _():
        for g in range(groups):
            xs[g] = x[:, g, :]

    parts_hi, parts_lo = [], []
    for g in range(subs):
        lanes = slice(g * n, (g + 1) * n)
        y = dots(split(xs[step * subs + g]), (ta[0], ta[1]), ((0,), (0,)))
        yr, yi = y[:, :STOLT], y[:, STOLT:]
        y = jnp.concatenate([yr * wa[0] - yi * wa[1], yr * wa[1] + yi * wa[0]], 0)
        z = dots((tb[0], tb[1]), split(y), ((1,), (0,)))
        zr, zi = z[:n], z[n:]
        cp, sp = cos_p[lanes], sin_p[lanes]
        z = jnp.concatenate([zr * cp - zi * sp, zr * sp + zi * cp], 1)
        hi, lo = split(z)
        picked = jnp.dot(
            hot[g], jnp.concatenate([hi, lo], 1), preferred_element_type=f32
        ).astype(bf16)
        first, second = picked[:n], picked[n:]
        for c in range(2):
            for base, keep in ((0, parts_hi), (2 * STOLT, parts_lo)):
                cut = slice(base + c * STOLT, base + (c + 1) * STOLT)
                keep.append(jnp.concatenate([first[:, cut], second[:, cut]], 1))
    ghi = jnp.concatenate(parts_hi, 0)
    glo = jnp.concatenate(parts_lo, 0)
    kinds = kind[...].reshape(subs * 2 * n, 1)
    kinds = jnp.broadcast_to(kinds, (subs * 2 * n, STOLT))
    acc = jnp.zeros((subs * 2 * n, STOLT), f32)
    for k in range(0, bank_hi.shape[0], 2):
        khi = jnp.concatenate([bank_hi[k], bank_hi[k + 1]], 1)
        klo = jnp.concatenate([bank_lo[k], bank_lo[k + 1]], 1)
        r = dots((ghi, glo), (khi, klo), ((1,), (0,)))
        for half in range(2):
            acc = jnp.where(kinds == k + half, r[:, half * STOLT : (half + 1) * STOLT], acc)
    for g in range(subs):
        s = acc[g * 2 * n : (g + 1) * 2 * n]
        y = dots(split(s), (tc[0], tc[1]), ((0,), (0,)))
        yr, yi = y[:, :n], y[:, n:]
        y = jnp.concatenate([yr * wc[0] - yi * wc[1], yr * wc[1] + yi * wc[0]], 0)
        os[step * subs + g] = dots((td[0], td[1]), split(y), ((1,), (0,)))

    @pl.when(step == pl.num_programs(0) - 1)
    def _():
        for g in range(groups):
            out[:, g, :] = os[g]


def middle(x, cos_p, sin_p, hot, kind, bank_hi, bank_lo, tables):
    groups = x.shape[1]
    subs = min(4, groups)
    n = GROUP * BLOCKS
    whole = lambda a: pl.BlockSpec(a.shape, lambda i: (0,) * a.ndim)
    return pl.pallas_call(
        functools.partial(mid_kernel, subs=subs),
        grid=(groups // subs,),
        in_specs=[
            whole(x),
            pl.BlockSpec((subs * n, STOLT), lambda i: (i, 0)),
            pl.BlockSpec((subs * n, STOLT), lambda i: (i, 0)),
            pl.BlockSpec((subs, 2 * n, n), lambda i: (i, 0, 0)),
            pl.BlockSpec((subs, 2 * n, 1), lambda i: (i, 0, 0)),
            whole(bank_hi),
            whole(bank_lo),
        ]
        + [whole(t) for t in tables],
        out_specs=pl.BlockSpec((2 * STOLT, groups, n), lambda i: (0, 0, 0)),
        out_shape=jax.ShapeDtypeStruct((2 * STOLT, groups, n), f32),
        scratch_shapes=[
            pltpu.VMEM((groups, x.shape[0], n), f32),
            pltpu.VMEM((groups, 2 * STOLT, n), f32),
        ],
        name="middle",
    )(x, cos_p, sin_p, hot, kind, bank_hi, bank_lo, *tables)


def quarter_tables():
    q = P_SIZE // 4
    m = np.arange(q)
    fwd, inv = [], []
    for low in range(4):
        a = 2 * np.pi / P_SIZE * (((4 * m[:, None] + low) * m[None, :]) % P_SIZE)
        f = a.reshape(-1, 2, q).transpose(1, 0, 2).reshape(q, q // 8, 8)
        f = f.transpose(0, 2, 1).reshape(q, q)
        fwd.append(np.concatenate([np.cos(f), np.sin(f)], 0))
        inv.append(np.concatenate([np.cos(a.T), np.sin(a.T)], 0) / P_SIZE)
    return np.stack(fwd), np.stack(inv)


def swap_blocks(arrays):
    count = len(arrays)
    lanes = arrays[0].shape[-1]
    size = lanes // count
    block = lax.broadcasted_iota(jnp.int32, arrays[0].shape, 1) // size
    outs = []
    for b in range(count):
        acc = None
        for a in range(count):
            shift = (a - b) % count * size
            moved = pltpu.roll(arrays[a], shift, 1) if shift else arrays[a]
            acc = moved if acc is None else jnp.where(block == a, moved, acc)
        outs.append(acc)
    return outs


def core_kernel(*refs, n_pulse, n_scat, subs, trig, trig_low):
    lead, partial = refs[:2]
    sources = refs[2:12]
    out = refs[12]
    local = refs[13:23]
    steps_in, kinds_in, bank, table, ta, wa, tb, tc, wc, td = local
    binned, peer, spec, x, hot, kind, banks, os, twin_os, *twin_in = refs[23:34]
    lone, twin_x = refs[34:36]
    (
        load, own_store, pair_send, pair_recv, near_send, near_recv, far_send, far_recv,
        twin_send, twin_recv, half_send, lone_send,
    ) = refs[36:]
    n_dev = n_pulse * n_scat
    pulse = lax.axis_index("pulse")
    scat = lax.axis_index("scat")
    me = pulse * n_scat + scat
    half = peer.shape[0]
    lanes = 2 * half
    size = P_SIZE // 4
    n = GROUP * BLOCKS
    groups = os.shape[1] + SHARED
    pieces = groups // subs
    reach = n_pulse // 2
    side = lax.div(pulse, reach)
    twin = lax.rem(pulse + reach, n_pulse) * n_scat + scat
    quads = lanes // BIN_SIDE
    unit = subs * quads
    per = os.shape[2]
    moves = [(a, b) for a in range(n_pulse) for b in range(n_scat) if (a, b) != (0, 0)]
    moves.sort(key=lambda m: (-min(m[0], n_pulse - m[0]), m))

    def other(a, b):
        return lax.rem(pulse + a, n_pulse), lax.rem(scat + b, n_scat)

    barrier = pltpu.get_barrier_semaphore()
    for a, b in moves:
        p, c = other(a, b)
        pl.semaphore_signal(
            barrier, inc=1, device_id={"pulse": p, "scat": c}, device_id_type=MESH
        )
    keep = pl.ds(pl.multiple_of(scat * half, half), half)
    give = pl.ds(pl.multiple_of((1 - scat) * half, half), half)
    loads = [
        pltpu.make_async_copy(src, dst, load.at[i])
        for i, (src, dst) in enumerate(zip(sources, local))
    ]
    for copy in loads:
        copy.start()
    for cut, sums in echoes(lead[...], pulse * 2 * half, 2 * half, trig_low):
        binned[:, cut] = partial[:, cut] + sums
    pl.semaphore_wait(barrier, n_dev - 1)

    pair = pltpu.make_async_remote_copy(
        src_ref=binned.at[give, :],
        dst_ref=peer,
        send_sem=pair_send,
        recv_sem=pair_recv,
        device_id={"pulse": pulse, "scat": 1 - scat},
        device_id_type=MESH,
    )
    pair.start()
    metas = []
    for i in range(2):
        loads[i].wait()
        copy = pltpu.make_async_remote_copy(
            src_ref=local[i],
            dst_ref=twin_in[i],
            send_sem=twin_send.at[i],
            recv_sem=twin_recv.at[i],
            device_id={"pulse": lax.rem(pulse + reach, n_pulse), "scat": scat},
            device_id_type=MESH,
        )
        copy.start()
        metas.append(copy)
    loads[3].wait()
    pair.wait()

    quarters = []
    for q in range(4):
        pair_of = []
        for c in range(2):
            cut = slice(c * P_SIZE + q * size, c * P_SIZE + (q + 1) * size)
            pair_of.append(binned[keep, cut] + peer[:, cut])
        quarters.append(pair_of)
    (r0, i0), (r1, i1), (r2, i2), (r3, i3) = quarters
    sr, si, dr, di = r0 + r2, i0 + i2, r0 - r2, i0 - i2
    tr, ti, er, ei = r1 + r3, i1 + i3, r1 - r3, i1 - i3
    mixed = (
        (sr + tr, si + ti),
        (dr + ei, di - er),
        (sr - tr, si - ti),
        (dr - ei, di + er),
    )
    low = lax.broadcasted_iota(jnp.int32, (size, lanes), 1) < half
    rows = []
    for k in range(4):
        g = product(
            joined(table[0, k], table[1, k], 1),
            triple(jnp.concatenate(mixed[k], 0), 1),
            ((1,), (1,)),
        )
        turned = pltpu.roll(g[size:], half, 1)
        rows.append(g[:size] + jnp.where(low, turned, -turned))
    for q, z in enumerate(swap_blocks(rows)):
        for h in range(subs):
            spec[pl.ds(q * subs + h, size // subs, stride=unit), :] = z[
                h * (size // subs) : (h + 1) * (size // subs)
            ]

    def piece(dev, i):
        return pl.ds(pl.multiple_of((dev * pieces + i) * unit, unit), unit)

    for q in range(quads):
        row = (pieces - 1) * unit + q * subs + subs - 1
        lone[:, q, :] = spec[pl.ds(row, n_dev, stride=pieces * unit), :]

    def twin_of(p, c):
        return lax.rem(p + reach, n_pulse) * n_scat + c

    own = pl.ds(pl.multiple_of(me * unit, unit), unit)
    for i in range(pieces + 1):
        for j, (a, b) in enumerate(moves):
            p, c = other(a, b)
            if i < pieces:
                src, dst = spec.at[piece(p * n_scat + c, i), :], x.at[i, own, :]
            else:
                src, dst = lone.at[twin_of(p, c)], twin_x.at[me]
            pltpu.make_async_remote_copy(
                src_ref=src,
                dst_ref=dst,
                send_sem=(near_send if i < pieces else lone_send).at[j],
                recv_sem=near_recv.at[i, me],
                device_id={"pulse": p, "scat": c},
                device_id_type=MESH,
            ).start()
    for i in range(pieces):
        x[i, own, :] = spec[piece(me, i), :]
    twin_x[me] = lone[twin_of(pulse, scat)]

    for i in (2, 4, 5, 6, 7, 8, 9):
        loads[i].wait()
    for copy in metas:
        copy.wait()
    block = lax.broadcasted_iota(jnp.int32, (n, STOLT), 0)
    lane = lax.broadcasted_iota(jnp.int32, (n, STOLT), 1)
    spot = lane.astype(f32)
    above = (block // BLOCKS * BLOCKS).astype(f32)
    flat = []
    for i in range(2):
        both = [
            jnp.concatenate([ref[pl.ds(j, groups, stride=GROUP), :] for j in range(GROUP)], 1)
            for ref in (local[i], twin_in[i])
        ]
        flat.append(jnp.concatenate([both[0], both[1][groups - subs :]], 0))
    for g in range(groups + subs):
        first = jnp.broadcast_to(flat[0][g : g + 1].astype(f32), (n, n)).T + above
        hot[g, :n] = jnp.where(first == spot, 1.0, 0.0).astype(bf16)
        hot[g, n:] = jnp.where(first + 1.0 == spot, 1.0, 0.0).astype(bf16)
        kind[g] = jnp.broadcast_to(flat[1][g : g + 1], (8, n))
    for k in range(bank.shape[0]):
        turned = jnp.concatenate([bank[k, :STOLT].T, bank[k, STOLT:].T], 1)
        hi, lo = split(turned)
        banks[k * STOLT : (k + 1) * STOLT] = jnp.concatenate([hi, hi, lo], 1)

    cols = (lane + (block % BLOCKS) * STOLT).astype(f32)
    kr = 4.0 * np.pi / 3e8 * (9.6e9 + (cols - F_LEN // 2) * (1.5e8 / F_LEN))

    def phase(owner, g):
        row = owner * (groups * GROUP) + g * GROUP + block // BLOCKS
        centered = lax.rem(row + P_SIZE // 2, P_SIZE) - P_SIZE // 2
        along = 2.0 * np.pi / (P_SIZE * SPACING) * centered.astype(f32)
        squared = along * along
        depth = NEAR + B // 2
        theta = -depth * squared / (jnp.sqrt(kr * kr - squared) + kr)
        whole = jnp.round(theta * (0.5 / np.pi))
        for part in turn_parts():
            theta = theta - whole * part
        r = theta * (0.5 / np.pi)
        u = r * r
        sn = r * horner(u, trig[0])
        cs = horner(u, trig[1])
        return 1.0 - 2.0 * sn * sn, 2.0 * sn * cs

    def ranged(slot, owner, g, cut):
        i, h = lax.div(slot, subs), lax.rem(slot, subs)
        cp, sp = phase(owner, g)
        rows_in = x[i, pl.ds(h, n_dev * quads, stride=subs), :]
        y = product(triple(rows_in, 0), joined(ta[0], ta[1], 0), ((0,), (0,)))
        yr, yi = y[:, :STOLT], y[:, STOLT:]
        y = jnp.concatenate([yr * wa[0] - yi * wa[1], yr * wa[1] + yi * wa[0]], 0)
        z = product(joined(tb[0], tb[1], 1), triple(y, 0))
        zr, zi = z[:n], z[n:]
        z = jnp.concatenate([zr * cp - zi * sp, zr * sp + zi * cp], 1)
        picked = product(hot[slot], jnp.concatenate(split(z), 1)).astype(bf16)
        first, second = picked[:n], picked[n:]
        parts = []
        for base in (0, 2 * STOLT):
            cuts = [slice(base + c * STOLT, base + (c + 1) * STOLT) for c in range(2)]
            parts.append(
                jnp.concatenate(
                    [jnp.concatenate([first[:, v], second[:, v]], 1) for v in cuts], 0
                )
            )
        ghi, glo = parts
        windows = jnp.concatenate([ghi, glo, ghi], 1)
        kinds = jnp.concatenate([kind[slot, 0:1]] * 2, 1)
        acc = jnp.zeros((STOLT, 2 * n), f32)
        for first in range(0, banks.shape[0], STREAM):
            r = product(banks[first : first + STREAM], windows, ((1,), (1,)))
            for v in range(STREAM // STOLT):
                k = first // STOLT + v
                acc = jnp.where(kinds == k, r[v * STOLT : (v + 1) * STOLT], acc)
        y = product(triple(acc, 1), joined(tc[0], tc[1], 0))
        yr, yi = y[:, :n], y[:, n:]
        y = jnp.concatenate([yr * wc[0] - yi * wc[1], yr * wc[1] + yi * wc[0]], 0)
        z = product(joined(td[0, cut, :], td[1, cut, :], 1), triple(y, 0))
        return z.reshape(-1, per, n)

    def arrived(i):
        for a, b in moves:
            p, c = other(a, b)
            src = p * n_scat + c
            here = pl.ds(pl.multiple_of(src * unit, unit), unit)
            pltpu.make_async_copy(
                x.at[i, here, :], x.at[i, here, :], near_recv.at[i, src]
            ).wait()

    def step(g, carry):
        @pl.when(lax.rem(g, subs) == 0)
        def _():
            arrived(lax.div(g, subs))

        os[:, g] = ranged(g, me, g, slice(None))
        for j, (a, b) in enumerate(moves):
            p, c = other(a, b)
            pltpu.make_async_remote_copy(
                src_ref=os.at[p * n_scat + c, g],
                dst_ref=out.at[me, g],
                send_sem=far_send.at[j],
                recv_sem=far_recv.at[me],
                device_id={"pulse": p, "scat": c},
                device_id_type=MESH,
            ).start()
        return carry

    close = [(a, b) for a in range(reach) for b in range(n_scat) if (a, b) != (0, 0)]
    within = pulse - side * reach

    def beside(a, b):
        return lax.rem(within + a, reach), lax.rem(scat + b, n_scat)

    part = 2 * STOLT // 2
    served = pl.ds(pl.multiple_of(side * part, part), part)

    lax.fori_loop(0, groups - SHARED, step, 0)
    for a, b in moves:
        p, c = other(a, b)
        src = p * n_scat + c
        pltpu.make_async_copy(
            twin_x.at[src], twin_x.at[src], near_recv.at[pieces, src]
        ).wait()
    x[pieces, pl.ds(subs - 1, n_dev * quads, stride=subs), :] = twin_x[...].reshape(-1, n)

    def half_step(t, carry):
        v, h = lax.div(t, SHARED), lax.rem(t, SHARED)
        owner = lax.rem(pulse + v * reach, n_pulse) * n_scat + scat
        g = groups - SHARED + h
        twin_os[v, :, h] = ranged(g + v * subs, owner, g, served)
        for j, (a, b) in enumerate(close):
            p, c = beside(a, b)
            pltpu.make_async_remote_copy(
                src_ref=twin_os.at[v, p * n_scat + c, h],
                dst_ref=out.at[owner, g],
                send_sem=half_send.at[j],
                recv_sem=far_recv.at[owner],
                device_id={"pulse": side * reach + p, "scat": c},
                device_id_type=MESH,
            ).start()
        return carry

    lax.fori_loop(0, 2 * SHARED, half_step, 0)
    first, last = pl.ds(0, groups - SHARED), pl.ds(groups - SHARED, SHARED)
    here = within * n_scat + scat
    stores = [
        pltpu.make_async_copy(src, dst, own_store.at[i])
        for i, (src, dst) in enumerate(
            (
                (os.at[me], out.at[me, first]),
                (twin_os.at[0, here], out.at[me, last]),
                (twin_os.at[1, here], out.at[twin, last]),
            )
        )
    ]
    for copy in stores:
        copy.start()
    for copy in stores:
        copy.wait()
    for j, (a, b) in enumerate(close):
        whole = os.at[0, pl.ds(0, 2 * SHARED)]
        pltpu.make_async_copy(whole, whole, half_send.at[j]).wait()
    for j, (a, b) in enumerate(moves):
        p, c = other(a, b)
        src = p * n_scat + c
        whole = spec.at[pl.ds(0, pieces * unit), :]
        pltpu.make_async_copy(whole, whole, near_send.at[j]).wait()
        pltpu.make_async_copy(lone.at[0], lone.at[0], lone_send.at[j]).wait()
        pltpu.make_async_copy(os.at[src], os.at[src], far_send.at[j]).wait()
        whole = out.at[src, first] if (a, b) == (reach, 0) else out.at[src]
        pltpu.make_async_copy(whole, whole, far_recv.at[src]).wait()


def turn_parts():
    parts, rest = [], 2.0 * np.pi
    for bits in (10, 22, 60):
        scale = 2.0**bits
        part = float(np.float32(np.round(rest * scale) / scale))
        parts.append(part)
        rest -= part
    return parts


def core(partial, lead, steps_in, kinds_in, bank, tables, n_pulse, n_scat):
    n_dev = n_pulse * n_scat
    groups = steps_in.shape[0] // GROUP
    subs = 2
    n = GROUP * BLOCKS
    span, width = partial.shape
    half = span // n_scat
    quads = 2 * half // BIN_SIDE
    kernels = bank.shape[0]
    per = 2 * STOLT // n_dev
    sources = (steps_in, kinds_in, bank, *tables)
    dma = pltpu.SemaphoreType.DMA
    return pl.pallas_call(
        functools.partial(
            core_kernel,
            n_pulse=n_pulse,
            n_scat=n_scat,
            subs=subs,
            trig=range_trig_coefs(5),
            trig_low=range_trig_coefs(4),
        ),
        in_specs=[IN_VMEM] * 2 + [IN_HBM] * len(sources),
        out_specs=pl.BlockSpec(memory_space=pl.ANY),
        out_shape=jax.ShapeDtypeStruct((n_dev, groups, per, n), f32),
        scratch_shapes=[pltpu.VMEM(a.shape, a.dtype) for a in sources]
        + [
            pltpu.VMEM((span, width), f32),
            pltpu.VMEM((half, width), f32),
            pltpu.VMEM((n_dev * groups * quads, n), f32),
            pltpu.VMEM((groups // subs + 1, n_dev * subs * quads, n), f32),
            pltpu.VMEM((groups + subs, 2 * n, n), bf16),
            pltpu.VMEM((groups + subs, 8, n), jnp.int32),
            pltpu.VMEM((kernels * STOLT, 6 * STOLT), bf16),
            pltpu.VMEM((n_dev, groups - SHARED, per, n), f32),
            pltpu.VMEM((2, n_dev // 2, SHARED, per, n), f32),
            pltpu.VMEM(steps_in.shape, steps_in.dtype),
            pltpu.VMEM(kinds_in.shape, kinds_in.dtype),
            pltpu.VMEM((n_dev, quads, n), f32),
            pltpu.VMEM((n_dev, quads, n), f32),
            dma((len(sources),)),
            dma((3,)),
            dma,
            dma,
            dma((n_dev,)),
            dma((groups // subs + 1, n_dev)),
            dma((n_dev,)),
            dma((n_dev,)),
            dma((2,)),
            dma((2,)),
            dma((n_dev // 2,)),
            dma((n_dev,)),
        ],
        compiler_params=pltpu.CompilerParams(
            collective_id=0, has_side_effects=True, vmem_limit_bytes=24 << 20
        ),
        name="core",
    )(lead, partial, *in_hbm(sources))


def image_kernel(x, table, out, done, sems):
    lanes = x.shape[1]
    per = x.shape[0] * GROUP // P_SIZE
    size = P_SIZE // 4
    copies = []
    for h in range(per // (2 * GROUP)):
        columns = [[] for _ in range(4)]
        for c in range(2):
            first = (2 * h + c) * GROUP
            tiles = [x[pl.ds(first + j, size, stride=per), :] for j in range(4)]
            for k, z in enumerate(swap_blocks(tiles)):
                columns[k].append(z)
        v = []
        for k in range(4):
            g = product(
                joined(table[0, k], table[1, k], 1), triple(jnp.concatenate(columns[k], 1), 0)
            )
            cos_g, sin_g = g[:size], g[size:]
            v.append((cos_g[:, :lanes] - sin_g[:, lanes:], cos_g[:, lanes:] + sin_g[:, :lanes]))
        (r0, i0), (r1, i1), (r2, i2), (r3, i3) = v
        sr, si, dr, di = r0 + r2, i0 + i2, r0 - r2, i0 - i2
        tr, ti, er, ei = r1 + r3, i1 + i3, r1 - r3, i1 - i3
        mixed = (
            (sr + tr, si + ti),
            (dr - ei, di + er),
            (sr - tr, si - ti),
            (dr + ei, di - er),
        )
        for q in range(4):
            for c in range(2):
                done[h, c, q * size : (q + 1) * size, :] = mixed[q][c]
        copy = pltpu.make_async_copy(
            done.at[h], out.at[:, :, pl.ds(h * lanes, lanes)], sems.at[h]
        )
        copy.start()
        copies.append(copy)
    for copy in copies:
        copy.wait()


def reference_phase(row_ids, cols):
    centered = (row_ids + P_SIZE // 2) % P_SIZE - P_SIZE // 2
    along_k = 2.0 * jnp.pi / (P_SIZE * SPACING) * centered.astype(f32)
    kr = 4.0 * jnp.pi / 3e8 * (9.6e9 + (cols.astype(f32) - F_LEN // 2) * (1.5e8 / F_LEN))
    squared = along_k * along_k
    depth = NEAR + B // 2
    return (
        -depth
        * squared[:, None]
        / (jnp.sqrt(kr[None, :] * kr[None, :] - squared[:, None]) + kr[None, :])
    )


def on_device(positions, amplitude, range_cells, bounce, stolt_block, kernel_choice, kernel_bank):
    n_pulse = lax.axis_size("pulse")
    n_scat = lax.axis_size("scat")
    n_dev = n_pulse * n_scat
    pulse_here = lax.axis_index("pulse")
    scat_here = lax.axis_index("scat")
    pulses = P_SIZE // n_pulse
    rows = P_SIZE // n_dev
    width = F_LEN // n_dev
    groups = rows // GROUP
    n = GROUP * BLOCKS
    bins_scat = B // n_scat
    bins_here = bins_scat // n_pulse

    per = STOLT // n_dev
    span = B // n_pulse
    packed = (
        span == 128
        and n_scat == 2
        and per % 4 == 0
        and groups % 8 == 0
        and positions.shape[0] % CHUNK == 0
    )
    if packed:
        partial, lead = range_binning(
            positions, amplitude, range_cells, bounce, pulse_here * span, span
        )
        local = bins_here // BIN_SIDE
        i, s, c, l = np.meshgrid(
            np.arange(n_pulse), np.arange(n_scat), np.arange(2), np.arange(local), indexing="ij"
        )
        order = (c * BIN_SIDE + (i * n_scat + s) * local + l).reshape(-1)
        tables, backward = core_tables(n_dev, order)
        tables = tuple(jnp.asarray(t) for t in tables)
        columns = core(
            partial, lead, stolt_block, kernel_choice, kernel_bank, tables, n_pulse, n_scat
        )
        return pl.pallas_call(
            image_kernel,
            in_specs=[IN_VMEM, IN_VMEM],
            out_specs=pl.BlockSpec(memory_space=pl.ANY),
            out_shape=jax.ShapeDtypeStruct((2, P_SIZE, width), f32),
            scratch_shapes=[
                pltpu.VMEM((width // n, 2, P_SIZE, n), f32),
                pltpu.SemaphoreType.DMA((width // n,)),
            ],
            compiler_params=pltpu.CompilerParams(vmem_limit_bytes=16 << 20),
            name="image",
        )(columns.reshape(-1, n), jnp.asarray(backward))

    ids = jnp.arange(GROUP, dtype=jnp.int32)[None, :, None] * BLOCKS
    first = stolt_block.reshape(groups, GROUP, BLOCKS) + ids
    pick = jnp.stack([first, first + 1], 1).reshape(groups, 2 * n, 1)
    hot = (pick == jnp.arange(n, dtype=jnp.int32)[None, None, :]).astype(bf16)
    kind = jnp.stack([kernel_choice.reshape(groups, n)] * 2, 1).reshape(groups, 2 * n, 1)
    bank_hi = lax.reduce_precision(kernel_bank, 8, 7)
    bank_lo = (kernel_bank - bank_hi).astype(bf16)
    bank_hi = bank_hi.astype(bf16)
    row_ids = (pulse_here * n_scat + scat_here) * rows + jnp.arange(rows, dtype=jnp.int32)
    theta = reference_phase(row_ids, jnp.arange(F_LEN, dtype=jnp.int32))
    theta = theta.reshape(rows * BLOCKS, STOLT)
    cos_p, sin_p = jnp.cos(theta), jnp.sin(theta)

    partial = binning(positions, amplitude, range_cells, bounce, pulse_here * pulses, pulses)
    partial = partial.reshape(n_scat, bins_scat, 2 * pulses)
    binned = lax.dynamic_index_in_dim(partial, scat_here, 0, keepdims=False)
    for shift in range(1, n_scat):
        other = lax.dynamic_index_in_dim(
            partial, (scat_here + shift) % n_scat, 0, keepdims=False
        )
        ring = [(i, (i + shift) % n_scat) for i in range(n_scat)]
        binned = binned + lax.ppermute(other, "scat", ring)
    turned = lax.all_to_all(
        binned.reshape(n_pulse, bins_here, 2 * pulses), "pulse", 0, 0, tiled=True
    )
    turned = turned.reshape(n_pulse, bins_here, 2, pulses).transpose(0, 3, 2, 1)
    turned = turned.reshape(P_SIZE, 2 * bins_here)
    k = np.arange(P_SIZE)
    angle = 2 * np.pi / P_SIZE * ((k[:, None] * k[None, :]) % P_SIZE)
    az = jnp.asarray(np.concatenate([np.cos(angle), np.sin(angle)], 0), f32)
    product = jnp.dot(az, turned, precision=HIGH, preferred_element_type=f32)
    pc, ps = product[:P_SIZE], product[P_SIZE:]
    spectrum = pc + jnp.concatenate([ps[:, bins_here:], -ps[:, :bins_here]], 1)
    az_rows = lax.all_to_all(
        spectrum.reshape(n_dev, rows, 2 * bins_here), ("pulse", "scat"), 0, 0, tiled=True
    )
    x = az_rows.reshape(n_pulse, n_scat, rows, 2, bins_here).transpose(3, 1, 0, 4, 2)
    x = x.reshape(2, BIN_SIDE, BIN_SIDE, rows).transpose(0, 1, 3, 2)
    x = x.reshape(2 * BIN_SIDE, groups, n)
    order = np.arange(2 * BIN_SIDE)

    tables = tuple(jnp.asarray(t) for t in mid_tables(n_dev, order))
    ranged = middle(x, cos_p, sin_p, hot, kind, bank_hi, bank_lo, tables)
    columns = lax.all_to_all(
        ranged.reshape(n_dev, 2 * per, rows * BLOCKS), ("pulse", "scat"), 0, 0, tiled=True
    )
    columns = columns.reshape(n_dev, 2, per, rows, BLOCKS).transpose(0, 3, 1, 2, 4)
    columns = columns.reshape(P_SIZE, 2 * width)
    final = jnp.dot(az, columns, precision=HIGH, preferred_element_type=f32)
    fc, fs = final[:P_SIZE], final[P_SIZE:]
    re = (fc[:, :width] - fs[:, width:]) / P_SIZE
    im = (fc[:, width:] + fs[:, :width]) / P_SIZE
    return jnp.stack([re, im])


def solution(mesh):
    placed = (
        P(("scene", "scat")),
        P(None, ("scene", "scat")),
        P(("scene", "scat")),
        P(("scene", "scat")),
        P(("pulse", "scat"), None),
        P(("pulse", "scat"), None),
        P(),
    )
    return jax.shard_map(
        on_device,
        mesh=mesh,
        in_specs=placed,
        out_specs=P(None, "scene", ("pulse", "scat")),
        check_vma=False,
    )
```

```python
import functools

import jax
import jax.numpy as jnp
import numpy as np
from jax import lax
from jax.experimental import pallas as pl
from jax.experimental.pallas import tpu as pltpu
from jax.sharding import PartitionSpec as P

P_SIZE = 512
F_LEN = 4096
B = 1024
SHIFT = 16
STOLT = 128
BLOCKS = 32
SPACING = 2.0
NEAR = 700000.0
BIN_SIDE = 32
GROUP = 4
CHUNK = 512
SLOTS = 112
LANES = 128
WIDE = 128
AHEAD = 1152
SHARED = 1
STREAM = 512
HIGH = lax.Precision.HIGH
MESH = pl.DeviceIdType.MESH
IN_HBM = pl.BlockSpec(memory_space=pltpu.HBM)
IN_VMEM = pl.BlockSpec(memory_space=pltpu.VMEM)
f32 = jnp.float32
bf16 = jnp.bfloat16


def trig_coefs():
    x = np.cos(np.pi * (np.arange(400) + 0.5) / 400) * 0.5
    u = x * x
    s = np.polynomial.chebyshev.Chebyshev.fit(u, np.sin(np.pi * x) / x, 5).convert(
        kind=np.polynomial.Polynomial
    )
    c = np.polynomial.chebyshev.Chebyshev.fit(u, np.cos(np.pi * x), 5).convert(
        kind=np.polynomial.Polynomial
    )
    return [float(v) for v in s.coef], [float(v) for v in c.coef]


def horner(u, coefs):
    acc = jnp.full_like(u, coefs[-1])
    for c in coefs[-2::-1]:
        acc = acc * u + c
    return acc


def split(x):
    hi = x.astype(bf16)
    lo = (x - hi.astype(f32)).astype(bf16)
    return hi, lo


def np_split(x):
    x = np.asarray(x, np.float64)
    hi = np.asarray(x, jnp.bfloat16)
    lo = np.asarray(x - hi.astype(np.float64), jnp.bfloat16)
    return np.stack([hi, lo])


def dots(a, b, dims):
    d = functools.partial(
        lax.dot_general, dimension_numbers=(dims, ((), ())), preferred_element_type=f32
    )
    return d(a[0], b[0]) + (d(a[0], b[1]) + d(a[1], b[0]))


def in_hbm(arrays):
    return [pltpu.with_memory_space_constraint(a, pltpu.HBM) for a in arrays]


def joined(hi, lo, axis):
    return jnp.concatenate([hi, hi, lo], axis)


def triple(x, axis):
    hi, lo = split(x)
    return jnp.concatenate([hi, lo, hi], axis)


def product(a, b, dims=((1,), (0,))):
    return lax.dot_general(a, b, (dims, ((), ())), preferred_element_type=f32)


def bin_kernel(pulse_base, pos, amp, tgt, bnc, out, acc, *, pulses, sin_c, cos_c):
    step = pl.program_id(0)
    width = pos.shape[1]

    @pl.when(step == 0)
    def _():
        acc[...] = jnp.zeros_like(acc)

    base = pulse_base[0]
    ids = base + lax.broadcasted_iota(jnp.int32, (pulses, width), 0)
    along = (ids.astype(f32) - P_SIZE // 2) * SPACING
    target = tgt[...] + SHIFT * bnc[...]
    slant = NEAR + target.astype(f32)
    offset = along - pos[...]
    square = offset * offset
    excess = square / (jnp.sqrt(slant * slant + square) + slant)
    halves = excess * -128.0
    whole = jnp.round(halves)
    r = halves - whole
    u = r * r
    odd = whole - 2.0 * jnp.floor(whole * 0.5)
    sign = 1.0 - 2.0 * odd
    sin_p = sign * r * horner(u, sin_c)
    cos_p = sign * horner(u, cos_c)
    flip = 1.0 - 2.0 * bnc[...].astype(f32)
    are = flip * amp[0:1]
    aim = flip * amp[1:2]
    re = are * cos_p - aim * sin_p
    im = are * sin_p + aim * cos_p
    steer = jnp.concatenate([re, im], 0)
    hi, lo = split(steer)
    rhs = jnp.concatenate([hi, lo], 0)
    bins = lax.broadcasted_iota(jnp.int32, (B, width), 0)
    hot = jnp.where(bins == target, 1.0, 0.0).astype(bf16)
    acc[...] += lax.dot_general(
        hot, rhs, (((1,), (1,)), ((), ())), preferred_element_type=f32
    )

    @pl.when(step == pl.num_programs(0) - 1)
    def _():
        out[...] = acc[:, : 2 * pulses] + acc[:, 2 * pulses :]


def binning(positions, amplitude, cells, bounce, pulse_base, pulses):
    count = positions.shape[0]
    width = min(2048, count)
    sin_c, cos_c = trig_coefs()
    row = lambda n: pl.BlockSpec((n, width), lambda i: (0, i))
    return pl.pallas_call(
        functools.partial(bin_kernel, pulses=pulses, sin_c=sin_c, cos_c=cos_c),
        grid=(count // width,),
        in_specs=[pl.BlockSpec(memory_space=pltpu.SMEM), row(1), row(2), row(1), row(1)],
        out_specs=pl.BlockSpec((B, 2 * pulses), lambda i: (0, 0)),
        out_shape=jax.ShapeDtypeStruct((B, 2 * pulses), f32),
        scratch_shapes=[pltpu.VMEM((B, 4 * pulses), f32)],
        name="binning",
    )(
        pulse_base.reshape(1),
        positions.reshape(1, count),
        amplitude,
        cells.reshape(1, count),
        bounce.reshape(1, count),
    )


def range_trig_coefs(degree):
    x = np.cos(np.pi * (np.arange(400) + 0.5) / 400) * 0.5
    u = x * x
    fit = lambda y: np.polynomial.chebyshev.Chebyshev.fit(u, y, degree).convert(
        kind=np.polynomial.Polynomial
    )
    return [float(v) for v in fit(np.sin(np.pi * x) / x).coef], [
        float(v) for v in fit(np.cos(np.pi * x)).coef
    ]


def split3(x):
    hi = x.astype(bf16).astype(f32)
    rest = x - hi
    mid = rest.astype(bf16).astype(f32)
    return hi, mid, rest - mid


def turn(r, trig):
    u = r * r
    sn = r * horner(u, trig[0])
    cs = horner(u, trig[1])
    twice = sn + sn
    return 1.0 - twice * sn, twice * cs


def times(a, b):
    return a[0] * b[0] - a[1] * b[1], a[0] * b[1] + a[1] * b[0]


def echoes(data, base, bins, trig):
    width = data.shape[1]
    chunk = min(width, LANES)
    hots, tiles = [], [[[], []] for _ in range(P_SIZE // 128)]
    for left in range(0, width, chunk):
        where, re_amp, im_amp, rel = (data[j : j + 1, left : left + chunk] for j in range(4))
        re2, im2 = 2.0 * re_amp, 2.0 * im_amp
        inverse = 0.5 / (rel + (base.astype(f32) + NEAR))
        gain = inverse * -64.0
        gain2 = gain + gain
        bend = inverse * (1.0 / 64.0)
        rows = lax.broadcasted_iota(jnp.int32, (bins, chunk), 0).astype(f32)
        hot = jnp.where(rows == rel, 1.0, 0.0).astype(bf16)
        hots += [hot, hot]
        odd = lax.broadcasted_iota(jnp.int32, (8, chunk), 0).astype(f32) * 2.0 + 1.0
        even = turn(odd * odd * (SPACING * SPACING / 4.0) * gain, trig)
        for q in range(P_SIZE // 128):
            ids = lax.broadcasted_iota(jnp.int32, (16, chunk), 0)
            middle = (ids * 8 + (q * 128 - P_SIZE // 2)).astype(f32) + 3.5
            offset = middle * SPACING - where
            t = offset * offset * gain
            y = t * bend
            t = t * (1.0 + y * (1.0 + 2.0 * y))
            r = t - jnp.round(t)
            u = r * r
            sn = r * horner(u, trig[0])
            cs = horner(u, trig[1])
            at = (re_amp - sn * (re2 * sn + im2 * cs), im_amp + sn * (re2 * cs - im2 * sn))
            slope = offset * gain2 * (1.0 + y * (2.0 + 6.0 * y))
            power = turn(slope * (SPACING / 2.0), trig)
            square = (1.0 - 2.0 * power[1] * power[1], 2.0 * power[0] * power[1])
            made = [None] * 8
            for j in range(4):
                a = times(at, (even[0][j : j + 1], even[1][j : j + 1]))
                rr, ii = a[0] * power[0], a[1] * power[1]
                ri, ir = a[0] * power[1], a[1] * power[0]
                made[4 + j] = (rr - ii, ri + ir)
                made[3 - j] = (rr + ii, ir - ri)
                if j < 3:
                    power = times(power, square)
            for c in range(2):
                tiles[q][c].append(
                    jnp.concatenate([jnp.concatenate(split(v[c]), 1) for v in made], 0)
                )
    hot = jnp.concatenate(hots, 1)
    for q in range(P_SIZE // 128):
        for c in range(2):
            lanes = slice(c * P_SIZE + q * 128, c * P_SIZE + (q + 1) * 128)
            yield lanes, product(hot, jnp.concatenate(tiles[q][c], 1), ((1,), (1,)))


def range_bin_kernel(base_ref, *refs, span, trig):
    out, lead = refs[6:8]
    buf, load = refs[14:]
    cells8, bounce8, pos, amp, cells, bnc = refs[8:14]
    loads = [
        pltpu.make_async_copy(src, dst, load.at[i])
        for i, (src, dst) in enumerate(zip(refs[:6], refs[8:14]))
    ]
    for copy in loads:
        copy.start()
    for copy in loads:
        copy.wait()
    base = base_ref[0]
    rows = cells8.shape[0]
    deep = CHUNK // 128
    chunks = rows // deep
    target = cells8[...] + SHIFT * bounce8[...] - base
    match = jnp.where((target >= 0) & (target < span), 1.0, 0.0)
    mb = match.astype(bf16)
    a = lax.broadcasted_iota(jnp.int32, (128, 128), 0)
    b = lax.broadcasted_iota(jnp.int32, (128, 128), 1)
    upto = jnp.where(a <= b, 1.0, 0.0).astype(bf16)
    count = jnp.dot(mb, upto, preferred_element_type=f32)
    total = jnp.dot(mb, jnp.ones((128, 128), bf16), preferred_element_type=f32)
    a = lax.broadcasted_iota(jnp.int32, (rows, rows), 0)
    b = lax.broadcasted_iota(jnp.int32, (rows, rows), 1)
    below = jnp.where((a // deep == b // deep) & (b < a), 1.0, 0.0).astype(bf16)
    ahead = jnp.dot(below, total.astype(bf16), preferred_element_type=f32)
    rank = jnp.where(match > 0.0, count + ahead - 1.0, -1.0)
    counts = [
        jnp.sum(match[deep * c : deep * (c + 1)]).astype(jnp.int32) for c in range(chunks)
    ]

    def values(c):
        lanes = slice(CHUNK * c, CHUNK * (c + 1))
        flip = 1.0 - 2.0 * bnc[:, lanes].astype(f32)
        rel = (cells[:, lanes] + SHIFT * bnc[:, lanes] - base).astype(f32)
        zero = jnp.zeros_like(rel)
        data = jnp.concatenate(
            [pos[:, lanes], amp[0:1, lanes] * flip, amp[1:2, lanes] * flip, rel] + [zero] * 4, 0
        )
        return jnp.concatenate(list(split3(data)) + [jnp.zeros_like(data)], 0).astype(bf16)

    def pick(c, first):
        slots = lax.broadcasted_iota(jnp.int32, (SLOTS, 128), 0).astype(f32) + first
        hot = jnp.concatenate(
            [
                jnp.where(rank[deep * c + j : deep * c + j + 1] == slots, 1.0, 0.0)
                for j in range(deep)
            ],
            1,
        ).astype(bf16)
        return lax.dot_general(
            hot, values(c), (((1,), (1,)), ((), ())), preferred_element_type=f32
        )

    start = 0
    for c in range(chunks):
        buf[pl.ds(start, SLOTS), 0:32] = pick(c, 0.0)
        start = start + counts[c]
    most = functools.reduce(jnp.maximum, counts)

    @pl.when(most > SLOTS)
    def _():
        begin = 0
        for c in range(chunks):

            @pl.loop(0, (counts[c] + SLOTS - 1) // SLOTS)
            def _(i):
                first = (i * SLOTS).astype(f32)
                buf[pl.ds(begin + i * SLOTS, SLOTS), 0:32] = pick(c, first)

            begin = begin + counts[c]

    buf[pl.ds(start, AHEAD), :] = jnp.zeros((AHEAD, 128), f32)

    def data(first, width):
        cols = []
        for h in range(width // 128):
            t = buf[pl.ds(first + h * 128, 128), :].T
            cols.append(t[0:8] + t[8:16] + t[16:24])
        return jnp.concatenate(cols, 1)

    lead[...] = data(0, AHEAD)
    out[...] = jnp.zeros_like(out)

    @pl.loop(AHEAD // WIDE, (start + WIDE - 1) // WIDE)
    def _(i):
        for lanes, sums in echoes(data(i * WIDE, WIDE), base, span, trig):
            out[:, lanes] += sums


def range_binning(positions, amplitude, cells, bounce, base, span):
    count = positions.shape[0]
    rows = count // 128
    sources = (
        cells.reshape(rows, 128),
        bounce.reshape(rows, 128),
        positions.reshape(1, count),
        amplitude,
        cells.reshape(1, count),
        bounce.reshape(1, count),
    )
    return pl.pallas_call(
        functools.partial(range_bin_kernel, span=span, trig=range_trig_coefs(4)),
        in_specs=[pl.BlockSpec(memory_space=pltpu.SMEM)] + [IN_HBM] * len(sources),
        out_specs=(IN_VMEM, IN_VMEM),
        out_shape=(
            jax.ShapeDtypeStruct((span, 2 * P_SIZE), f32),
            jax.ShapeDtypeStruct((8, AHEAD), f32),
        ),
        scratch_shapes=[pltpu.VMEM(a.shape, a.dtype) for a in sources]
        + [
            pltpu.VMEM((count + SLOTS + AHEAD, 128), f32),
            pltpu.SemaphoreType.DMA((len(sources),)),
        ],
        compiler_params=pltpu.CompilerParams(vmem_limit_bytes=16 << 20),
        name="range_binning",
    )(base.reshape(1), *in_hbm(sources))


def complex_rows(c, s):
    return np.block([[c, s], [-s, c]])


def mid_factors(n_dev, order):
    side = np.arange(BIN_SIDE)
    t = np.arange(STOLT)
    eye = np.eye(GROUP)
    a = -2 * np.pi / STOLT * ((side[:, None] * t[None, :]) % STOLT)
    ta = complex_rows(np.cos(a), np.sin(a))[order]
    a = -2 * np.pi / F_LEN * (side[:, None] * t[None, :])
    wa = np.stack([np.tile(np.cos(a), (GROUP, 1)), np.tile(np.sin(a), (GROUP, 1))])
    a = -2 * np.pi / BIN_SIDE * ((side[:, None] * side[None, :]) % BIN_SIDE)
    c, s = np.kron(eye, np.cos(a)), np.kron(eye, np.sin(a))
    tb = complex_rows(c, s).T
    blk = np.arange(BLOCKS)
    a = 2 * np.pi / BLOCKS * ((blk[:, None] * blk[None, :]) % BLOCKS)
    c, s = np.kron(eye, np.cos(a)), np.kron(eye, np.sin(a))
    tc = complex_rows(c, s)
    a = 2 * np.pi / F_LEN * (t[:, None] * blk[None, :])
    wc = np.stack([np.tile(np.cos(a), (1, GROUP)), np.tile(np.sin(a), (1, GROUP))])
    a = 2 * np.pi / STOLT * ((t[:, None] * t[None, :]) % STOLT)
    td = complex_rows(np.cos(a), np.sin(a)).T / F_LEN
    td = td.reshape(2, n_dev, STOLT // n_dev, 2 * STOLT).transpose(1, 0, 2, 3)
    return ta, wa.astype(np.float32), tb, tc, wc.astype(np.float32), td


def mid_tables(n_dev, order):
    ta, wa, tb, tc, wc, td = mid_factors(n_dev, order)
    td = td.reshape(2 * STOLT, 2 * STOLT)
    return np_split(ta), wa, np_split(tb), np_split(tc), wc, np_split(td)


def core_tables(n_dev, order):
    ta, wa, tb, tc, wc, td = mid_factors(n_dev, order)
    td = td.reshape(n_dev, 2, -1, GROUP, 2 * STOLT).transpose(0, 2, 1, 3, 4)
    td = td.reshape(2 * STOLT, 2 * STOLT)
    forward, inverse = quarter_tables()
    return (
        np_split(forward),
        np_split(ta),
        wa,
        np_split(tb),
        np_split(tc),
        wc,
        np_split(td),
    ), np_split(inverse)


def mid_kernel(
    x, cos_p, sin_p, hot, kind, bank_hi, bank_lo, ta, wa, tb, tc, wc, td, out, xs, os, *, subs
):
    n = GROUP * BLOCKS
    step = pl.program_id(0)
    groups = x.shape[1]

    @pl.when(step == 0)
    def _():
        for g in range(groups):
            xs[g] = x[:, g, :]

    parts_hi, parts_lo = [], []
    for g in range(subs):
        lanes = slice(g * n, (g + 1) * n)
        y = dots(split(xs[step * subs + g]), (ta[0], ta[1]), ((0,), (0,)))
        yr, yi = y[:, :STOLT], y[:, STOLT:]
        y = jnp.concatenate([yr * wa[0] - yi * wa[1], yr * wa[1] + yi * wa[0]], 0)
        z = dots((tb[0], tb[1]), split(y), ((1,), (0,)))
        zr, zi = z[:n], z[n:]
        cp, sp = cos_p[lanes], sin_p[lanes]
        z = jnp.concatenate([zr * cp - zi * sp, zr * sp + zi * cp], 1)
        hi, lo = split(z)
        picked = jnp.dot(
            hot[g], jnp.concatenate([hi, lo], 1), preferred_element_type=f32
        ).astype(bf16)
        first, second = picked[:n], picked[n:]
        for c in range(2):
            for base, keep in ((0, parts_hi), (2 * STOLT, parts_lo)):
                cut = slice(base + c * STOLT, base + (c + 1) * STOLT)
                keep.append(jnp.concatenate([first[:, cut], second[:, cut]], 1))
    ghi = jnp.concatenate(parts_hi, 0)
    glo = jnp.concatenate(parts_lo, 0)
    kinds = kind[...].reshape(subs * 2 * n, 1)
    kinds = jnp.broadcast_to(kinds, (subs * 2 * n, STOLT))
    acc = jnp.zeros((subs * 2 * n, STOLT), f32)
    for k in range(0, bank_hi.shape[0], 2):
        khi = jnp.concatenate([bank_hi[k], bank_hi[k + 1]], 1)
        klo = jnp.concatenate([bank_lo[k], bank_lo[k + 1]], 1)
        r = dots((ghi, glo), (khi, klo), ((1,), (0,)))
        for half in range(2):
            acc = jnp.where(kinds == k + half, r[:, half * STOLT : (half + 1) * STOLT], acc)
    for g in range(subs):
        s = acc[g * 2 * n : (g + 1) * 2 * n]
        y = dots(split(s), (tc[0], tc[1]), ((0,), (0,)))
        yr, yi = y[:, :n], y[:, n:]
        y = jnp.concatenate([yr * wc[0] - yi * wc[1], yr * wc[1] + yi * wc[0]], 0)
        os[step * subs + g] = dots((td[0], td[1]), split(y), ((1,), (0,)))

    @pl.when(step == pl.num_programs(0) - 1)
    def _():
        for g in range(groups):
            out[:, g, :] = os[g]


def middle(x, cos_p, sin_p, hot, kind, bank_hi, bank_lo, tables):
    groups = x.shape[1]
    subs = min(4, groups)
    n = GROUP * BLOCKS
    whole = lambda a: pl.BlockSpec(a.shape, lambda i: (0,) * a.ndim)
    return pl.pallas_call(
        functools.partial(mid_kernel, subs=subs),
        grid=(groups // subs,),
        in_specs=[
            whole(x),
            pl.BlockSpec((subs * n, STOLT), lambda i: (i, 0)),
            pl.BlockSpec((subs * n, STOLT), lambda i: (i, 0)),
            pl.BlockSpec((subs, 2 * n, n), lambda i: (i, 0, 0)),
            pl.BlockSpec((subs, 2 * n, 1), lambda i: (i, 0, 0)),
            whole(bank_hi),
            whole(bank_lo),
        ]
        + [whole(t) for t in tables],
        out_specs=pl.BlockSpec((2 * STOLT, groups, n), lambda i: (0, 0, 0)),
        out_shape=jax.ShapeDtypeStruct((2 * STOLT, groups, n), f32),
        scratch_shapes=[
            pltpu.VMEM((groups, x.shape[0], n), f32),
            pltpu.VMEM((groups, 2 * STOLT, n), f32),
        ],
        name="middle",
    )(x, cos_p, sin_p, hot, kind, bank_hi, bank_lo, *tables)


def quarter_tables():
    q = P_SIZE // 4
    m = np.arange(q)
    fwd, inv = [], []
    for low in range(4):
        a = 2 * np.pi / P_SIZE * (((4 * m[:, None] + low) * m[None, :]) % P_SIZE)
        f = a.reshape(-1, 2, q).transpose(1, 0, 2).reshape(q, q // 8, 8)
        f = f.transpose(0, 2, 1).reshape(q, q)
        fwd.append(np.concatenate([np.cos(f), np.sin(f)], 0))
        inv.append(np.concatenate([np.cos(a.T), np.sin(a.T)], 0) / P_SIZE)
    return np.stack(fwd), np.stack(inv)


def swap_blocks(arrays):
    arrays = list(arrays)
    count = len(arrays)
    lanes = arrays[0].shape[-1]
    block = lax.broadcasted_iota(jnp.int32, arrays[0].shape, 1) // (lanes // count)
    step = count // 2
    while step:
        shift = step * (lanes // count)
        low = block // step % 2 == 0
        for i in range(count):
            if i // step % 2 == 0:
                a, b = arrays[i], arrays[i + step]
                arrays[i] = jnp.where(low, a, pltpu.roll(b, shift, 1))
                arrays[i + step] = jnp.where(low, pltpu.roll(a, lanes - shift, 1), b)
        step //= 2
    return arrays


def core_kernel(*refs, n_pulse, n_scat, subs, trig, trig_low):
    lead, partial = refs[:2]
    sources = refs[2:12]
    out = refs[12]
    local = refs[13:23]
    steps_in, kinds_in, bank, table, ta, wa, tb, tc, wc, td = local
    binned, peer, spec, x, hot, kind, banks, os, twin_os, *twin_in = refs[23:34]
    lone, twin_x = refs[34:36]
    (
        load, own_store, pair_send, pair_recv, near_send, near_recv, far_send, far_recv,
        twin_send, twin_recv, half_send, lone_send,
    ) = refs[36:]
    n_dev = n_pulse * n_scat
    pulse = lax.axis_index("pulse")
    scat = lax.axis_index("scat")
    me = pulse * n_scat + scat
    half = peer.shape[0]
    lanes = 2 * half
    size = P_SIZE // 4
    n = GROUP * BLOCKS
    groups = os.shape[1] + SHARED
    pieces = groups // subs
    reach = n_pulse // 2
    side = lax.div(pulse, reach)
    twin = lax.rem(pulse + reach, n_pulse) * n_scat + scat
    quads = lanes // BIN_SIDE
    unit = subs * quads
    per = os.shape[2]
    moves = [(a, b) for a in range(n_pulse) for b in range(n_scat) if (a, b) != (0, 0)]
    moves.sort(key=lambda m: (-min(m[0], n_pulse - m[0]), m))

    def other(a, b):
        return lax.rem(pulse + a, n_pulse), lax.rem(scat + b, n_scat)

    barrier = pltpu.get_barrier_semaphore()
    for a, b in moves:
        p, c = other(a, b)
        pl.semaphore_signal(
            barrier, inc=1, device_id={"pulse": p, "scat": c}, device_id_type=MESH
        )
    keep = pl.ds(pl.multiple_of(scat * half, half), half)
    give = pl.ds(pl.multiple_of((1 - scat) * half, half), half)
    loads = [
        pltpu.make_async_copy(src, dst, load.at[i])
        for i, (src, dst) in enumerate(zip(sources, local))
    ]
    for copy in loads:
        copy.start()
    for cut, sums in echoes(lead[...], pulse * 2 * half, 2 * half, trig_low):
        binned[:, cut] = partial[:, cut] + sums
    pl.semaphore_wait(barrier, n_dev - 1)

    pair = pltpu.make_async_remote_copy(
        src_ref=binned.at[give, :],
        dst_ref=peer,
        send_sem=pair_send,
        recv_sem=pair_recv,
        device_id={"pulse": pulse, "scat": 1 - scat},
        device_id_type=MESH,
    )
    pair.start()
    metas = []
    for i in range(2):
        loads[i].wait()
        copy = pltpu.make_async_remote_copy(
            src_ref=local[i],
            dst_ref=twin_in[i],
            send_sem=twin_send.at[i],
            recv_sem=twin_recv.at[i],
            device_id={"pulse": lax.rem(pulse + reach, n_pulse), "scat": scat},
            device_id_type=MESH,
        )
        copy.start()
        metas.append(copy)
    loads[3].wait()
    pair.wait()

    quarters = []
    for q in range(4):
        pair_of = []
        for c in range(2):
            cut = slice(c * P_SIZE + q * size, c * P_SIZE + (q + 1) * size)
            pair_of.append(binned[keep, cut] + peer[:, cut])
        quarters.append(pair_of)
    (r0, i0), (r1, i1), (r2, i2), (r3, i3) = quarters
    sr, si, dr, di = r0 + r2, i0 + i2, r0 - r2, i0 - i2
    tr, ti, er, ei = r1 + r3, i1 + i3, r1 - r3, i1 - i3
    mixed = (
        (sr + tr, si + ti),
        (dr + ei, di - er),
        (sr - tr, si - ti),
        (dr - ei, di + er),
    )
    low = lax.broadcasted_iota(jnp.int32, (size, lanes), 1) < half
    rows = []
    for k in range(4):
        g = product(
            joined(table[0, k], table[1, k], 1),
            triple(jnp.concatenate(mixed[k], 0), 1),
            ((1,), (1,)),
        )
        turned = pltpu.roll(g[size:], half, 1)
        rows.append(g[:size] + jnp.where(low, turned, -turned))
    for q, z in enumerate(swap_blocks(rows)):
        for h in range(subs):
            spec[pl.ds(q * subs + h, size // subs, stride=unit), :] = z[
                h * (size // subs) : (h + 1) * (size // subs)
            ]

    def piece(dev, i):
        return pl.ds(pl.multiple_of((dev * pieces + i) * unit, unit), unit)

    for q in range(quads):
        row = (pieces - 1) * unit + q * subs + subs - 1
        lone[:, q, :] = spec[pl.ds(row, n_dev, stride=pieces * unit), :]

    def twin_of(p, c):
        return lax.rem(p + reach, n_pulse) * n_scat + c

    own = pl.ds(pl.multiple_of(me * unit, unit), unit)
    for i in range(pieces + 1):
        for j, (a, b) in enumerate(moves):
            p, c = other(a, b)
            if i < pieces:
                src, dst = spec.at[piece(p * n_scat + c, i), :], x.at[i, own, :]
            else:
                src, dst = lone.at[twin_of(p, c)], twin_x.at[me]
            pltpu.make_async_remote_copy(
                src_ref=src,
                dst_ref=dst,
                send_sem=(near_send if i < pieces else lone_send).at[j],
                recv_sem=near_recv.at[i, me],
                device_id={"pulse": p, "scat": c},
                device_id_type=MESH,
            ).start()
    for i in range(pieces):
        x[i, own, :] = spec[piece(me, i), :]
    twin_x[me] = lone[twin_of(pulse, scat)]

    for i in (2, 4, 5, 6, 7, 8, 9):
        loads[i].wait()
    for copy in metas:
        copy.wait()
    block = lax.broadcasted_iota(jnp.int32, (n, STOLT), 0)
    lane = lax.broadcasted_iota(jnp.int32, (n, STOLT), 1)
    spot = lane.astype(f32)
    above = (block // BLOCKS * BLOCKS).astype(f32)
    flat = []
    for i in range(2):
        both = [
            jnp.concatenate([ref[pl.ds(j, groups, stride=GROUP), :] for j in range(GROUP)], 1)
            for ref in (local[i], twin_in[i])
        ]
        flat.append(jnp.concatenate([both[0], both[1][groups - subs :]], 0))
    for g in range(groups + subs):
        first = jnp.broadcast_to(flat[0][g : g + 1].astype(f32), (n, n)).T + above
        hot[g, :n] = jnp.where(first == spot, 1.0, 0.0).astype(bf16)
        hot[g, n:] = jnp.where(first + 1.0 == spot, 1.0, 0.0).astype(bf16)
        kind[g] = jnp.broadcast_to(flat[1][g : g + 1], (8, n))
    for k in range(bank.shape[0]):
        turned = jnp.concatenate([bank[k, :STOLT].T, bank[k, STOLT:].T], 1)
        hi, lo = split(turned)
        banks[k * STOLT : (k + 1) * STOLT] = jnp.concatenate([hi, hi, lo], 1)

    cols = (lane + (block % BLOCKS) * STOLT).astype(f32)
    kr = 4.0 * np.pi / 3e8 * (9.6e9 + (cols - F_LEN // 2) * (1.5e8 / F_LEN))

    def phase(owner, g):
        row = owner * (groups * GROUP) + g * GROUP + block // BLOCKS
        centered = lax.rem(row + P_SIZE // 2, P_SIZE) - P_SIZE // 2
        along = 2.0 * np.pi / (P_SIZE * SPACING) * centered.astype(f32)
        squared = along * along
        depth = NEAR + B // 2
        theta = -depth * squared / (jnp.sqrt(kr * kr - squared) + kr)
        whole = jnp.round(theta * (0.5 / np.pi))
        for part in turn_parts():
            theta = theta - whole * part
        r = theta * (0.5 / np.pi)
        u = r * r
        sn = r * horner(u, trig[0])
        cs = horner(u, trig[1])
        return 1.0 - 2.0 * sn * sn, 2.0 * sn * cs

    def ranged(slot, owner, g, cut):
        i, h = lax.div(slot, subs), lax.rem(slot, subs)
        cp, sp = phase(owner, g)
        rows_in = x[i, pl.ds(h, n_dev * quads, stride=subs), :]
        y = product(triple(rows_in, 0), joined(ta[0], ta[1], 0), ((0,), (0,)))
        yr, yi = y[:, :STOLT], y[:, STOLT:]
        y = jnp.concatenate([yr * wa[0] - yi * wa[1], yr * wa[1] + yi * wa[0]], 0)
        z = product(joined(tb[0], tb[1], 1), triple(y, 0))
        zr, zi = z[:n], z[n:]
        z = jnp.concatenate([zr * cp - zi * sp, zr * sp + zi * cp], 1)
        picked = product(hot[slot], jnp.concatenate(split(z), 1)).astype(bf16)
        first, second = picked[:n], picked[n:]
        parts = []
        for base in (0, 2 * STOLT):
            cuts = [slice(base + c * STOLT, base + (c + 1) * STOLT) for c in range(2)]
            parts.append(
                jnp.concatenate(
                    [jnp.concatenate([first[:, v], second[:, v]], 1) for v in cuts], 0
                )
            )
        ghi, glo = parts
        windows = jnp.concatenate([ghi, glo, ghi], 1)
        kinds = jnp.concatenate([kind[slot, 0:1]] * 2, 1)
        acc = jnp.zeros((STOLT, 2 * n), f32)
        for first in range(0, banks.shape[0], STREAM):
            r = product(banks[first : first + STREAM], windows, ((1,), (1,)))
            for v in range(STREAM // STOLT):
                k = first // STOLT + v
                acc = jnp.where(kinds == k, r[v * STOLT : (v + 1) * STOLT], acc)
        y = product(triple(acc, 1), joined(tc[0], tc[1], 0))
        yr, yi = y[:, :n], y[:, n:]
        y = jnp.concatenate([yr * wc[0] - yi * wc[1], yr * wc[1] + yi * wc[0]], 0)
        z = product(joined(td[0, cut, :], td[1, cut, :], 1), triple(y, 0))
        return z.reshape(-1, per, n)

    def arrived(i):
        for a, b in moves:
            p, c = other(a, b)
            src = p * n_scat + c
            here = pl.ds(pl.multiple_of(src * unit, unit), unit)
            pltpu.make_async_copy(
                x.at[i, here, :], x.at[i, here, :], near_recv.at[i, src]
            ).wait()

    def step(g, carry):
        @pl.when(lax.rem(g, subs) == 0)
        def _():
            arrived(lax.div(g, subs))

        os[:, g] = ranged(g, me, g, slice(None))
        for j, (a, b) in enumerate(moves):
            p, c = other(a, b)
            pltpu.make_async_remote_copy(
                src_ref=os.at[p * n_scat + c, g],
                dst_ref=out.at[me, g],
                send_sem=far_send.at[j],
                recv_sem=far_recv.at[me],
                device_id={"pulse": p, "scat": c},
                device_id_type=MESH,
            ).start()
        return carry

    close = [(a, b) for a in range(reach) for b in range(n_scat) if (a, b) != (0, 0)]
    within = pulse - side * reach

    def beside(a, b):
        return lax.rem(within + a, reach), lax.rem(scat + b, n_scat)

    part = 2 * STOLT // 2
    served = pl.ds(pl.multiple_of(side * part, part), part)

    lax.fori_loop(0, groups - SHARED, step, 0)
    for a, b in moves:
        p, c = other(a, b)
        src = p * n_scat + c
        pltpu.make_async_copy(
            twin_x.at[src], twin_x.at[src], near_recv.at[pieces, src]
        ).wait()
    x[pieces, pl.ds(subs - 1, n_dev * quads, stride=subs), :] = twin_x[...].reshape(-1, n)

    def half_step(t, carry):
        v, h = lax.div(t, SHARED), lax.rem(t, SHARED)
        owner = lax.rem(pulse + v * reach, n_pulse) * n_scat + scat
        g = groups - SHARED + h
        twin_os[v, :, h] = ranged(g + v * subs, owner, g, served)
        for j, (a, b) in enumerate(close):
            p, c = beside(a, b)
            pltpu.make_async_remote_copy(
                src_ref=twin_os.at[v, p * n_scat + c, h],
                dst_ref=out.at[owner, g],
                send_sem=half_send.at[j],
                recv_sem=far_recv.at[owner],
                device_id={"pulse": side * reach + p, "scat": c},
                device_id_type=MESH,
            ).start()
        return carry

    lax.fori_loop(0, 2 * SHARED, half_step, 0)
    first, last = pl.ds(0, groups - SHARED), pl.ds(groups - SHARED, SHARED)
    here = within * n_scat + scat
    stores = [
        pltpu.make_async_copy(src, dst, own_store.at[i])
        for i, (src, dst) in enumerate(
            (
                (os.at[me], out.at[me, first]),
                (twin_os.at[0, here], out.at[me, last]),
                (twin_os.at[1, here], out.at[twin, last]),
            )
        )
    ]
    for copy in stores:
        copy.start()
    for copy in stores:
        copy.wait()
    for j, (a, b) in enumerate(close):
        whole = os.at[0, pl.ds(0, 2 * SHARED)]
        pltpu.make_async_copy(whole, whole, half_send.at[j]).wait()
    for j, (a, b) in enumerate(moves):
        p, c = other(a, b)
        src = p * n_scat + c
        whole = spec.at[pl.ds(0, pieces * unit), :]
        pltpu.make_async_copy(whole, whole, near_send.at[j]).wait()
        pltpu.make_async_copy(lone.at[0], lone.at[0], lone_send.at[j]).wait()
        pltpu.make_async_copy(os.at[src], os.at[src], far_send.at[j]).wait()
        whole = out.at[src, first] if (a, b) == (reach, 0) else out.at[src]
        pltpu.make_async_copy(whole, whole, far_recv.at[src]).wait()


def turn_parts():
    parts, rest = [], 2.0 * np.pi
    for bits in (10, 22, 60):
        scale = 2.0**bits
        part = float(np.float32(np.round(rest * scale) / scale))
        parts.append(part)
        rest -= part
    return parts


def core(partial, lead, steps_in, kinds_in, bank, tables, n_pulse, n_scat):
    n_dev = n_pulse * n_scat
    groups = steps_in.shape[0] // GROUP
    subs = 2
    n = GROUP * BLOCKS
    span, width = partial.shape
    half = span // n_scat
    quads = 2 * half // BIN_SIDE
    kernels = bank.shape[0]
    per = 2 * STOLT // n_dev
    sources = (steps_in, kinds_in, bank, *tables)
    dma = pltpu.SemaphoreType.DMA
    return pl.pallas_call(
        functools.partial(
            core_kernel,
            n_pulse=n_pulse,
            n_scat=n_scat,
            subs=subs,
            trig=range_trig_coefs(5),
            trig_low=range_trig_coefs(4),
        ),
        in_specs=[IN_VMEM] * 2 + [IN_HBM] * len(sources),
        out_specs=pl.BlockSpec(memory_space=pl.ANY),
        out_shape=jax.ShapeDtypeStruct((n_dev, groups, per, n), f32),
        scratch_shapes=[pltpu.VMEM(a.shape, a.dtype) for a in sources]
        + [
            pltpu.VMEM((span, width), f32),
            pltpu.VMEM((half, width), f32),
            pltpu.VMEM((n_dev * groups * quads, n), f32),
            pltpu.VMEM((groups // subs + 1, n_dev * subs * quads, n), f32),
            pltpu.VMEM((groups + subs, 2 * n, n), bf16),
            pltpu.VMEM((groups + subs, 8, n), jnp.int32),
            pltpu.VMEM((kernels * STOLT, 6 * STOLT), bf16),
            pltpu.VMEM((n_dev, groups - SHARED, per, n), f32),
            pltpu.VMEM((2, n_dev // 2, SHARED, per, n), f32),
            pltpu.VMEM(steps_in.shape, steps_in.dtype),
            pltpu.VMEM(kinds_in.shape, kinds_in.dtype),
            pltpu.VMEM((n_dev, quads, n), f32),
            pltpu.VMEM((n_dev, quads, n), f32),
            dma((len(sources),)),
            dma((3,)),
            dma,
            dma,
            dma((n_dev,)),
            dma((groups // subs + 1, n_dev)),
            dma((n_dev,)),
            dma((n_dev,)),
            dma((2,)),
            dma((2,)),
            dma((n_dev // 2,)),
            dma((n_dev,)),
        ],
        compiler_params=pltpu.CompilerParams(
            collective_id=0, has_side_effects=True, vmem_limit_bytes=24 << 20
        ),
        name="core",
    )(lead, partial, *in_hbm(sources))


def image_kernel(x, table, out, done, sems):
    lanes = x.shape[1]
    per = x.shape[0] * GROUP // P_SIZE
    size = P_SIZE // 4
    copies = []
    for h in range(per // (2 * GROUP)):
        columns = [[] for _ in range(4)]
        for c in range(2):
            first = (2 * h + c) * GROUP
            tiles = [x[pl.ds(first + j, size, stride=per), :] for j in range(4)]
            for k, z in enumerate(swap_blocks(tiles)):
                columns[k].append(z)
        v = []
        for k in range(4):
            g = product(
                joined(table[0, k], table[1, k], 1), triple(jnp.concatenate(columns[k], 1), 0)
            )
            cos_g, sin_g = g[:size], g[size:]
            v.append((cos_g[:, :lanes] - sin_g[:, lanes:], cos_g[:, lanes:] + sin_g[:, :lanes]))
        (r0, i0), (r1, i1), (r2, i2), (r3, i3) = v
        sr, si, dr, di = r0 + r2, i0 + i2, r0 - r2, i0 - i2
        tr, ti, er, ei = r1 + r3, i1 + i3, r1 - r3, i1 - i3
        mixed = (
            (sr + tr, si + ti),
            (dr - ei, di + er),
            (sr - tr, si - ti),
            (dr + ei, di - er),
        )
        for q in range(4):
            for c in range(2):
                done[h, c, q * size : (q + 1) * size, :] = mixed[q][c]
        copy = pltpu.make_async_copy(
            done.at[h], out.at[:, :, pl.ds(h * lanes, lanes)], sems.at[h]
        )
        copy.start()
        copies.append(copy)
    for copy in copies:
        copy.wait()


def reference_phase(row_ids, cols):
    centered = (row_ids + P_SIZE // 2) % P_SIZE - P_SIZE // 2
    along_k = 2.0 * jnp.pi / (P_SIZE * SPACING) * centered.astype(f32)
    kr = 4.0 * jnp.pi / 3e8 * (9.6e9 + (cols.astype(f32) - F_LEN // 2) * (1.5e8 / F_LEN))
    squared = along_k * along_k
    depth = NEAR + B // 2
    return (
        -depth
        * squared[:, None]
        / (jnp.sqrt(kr[None, :] * kr[None, :] - squared[:, None]) + kr[None, :])
    )


def on_device(positions, amplitude, range_cells, bounce, stolt_block, kernel_choice, kernel_bank):
    n_pulse = lax.axis_size("pulse")
    n_scat = lax.axis_size("scat")
    n_dev = n_pulse * n_scat
    pulse_here = lax.axis_index("pulse")
    scat_here = lax.axis_index("scat")
    pulses = P_SIZE // n_pulse
    rows = P_SIZE // n_dev
    width = F_LEN // n_dev
    groups = rows // GROUP
    n = GROUP * BLOCKS
    bins_scat = B // n_scat
    bins_here = bins_scat // n_pulse

    per = STOLT // n_dev
    span = B // n_pulse
    packed = (
        span == 128
        and n_scat == 2
        and per % 4 == 0
        and groups % 8 == 0
        and positions.shape[0] % CHUNK == 0
    )
    if packed:
        partial, lead = range_binning(
            positions, amplitude, range_cells, bounce, pulse_here * span, span
        )
        local = bins_here // BIN_SIDE
        i, s, c, l = np.meshgrid(
            np.arange(n_pulse), np.arange(n_scat), np.arange(2), np.arange(local), indexing="ij"
        )
        order = (c * BIN_SIDE + (i * n_scat + s) * local + l).reshape(-1)
        tables, backward = core_tables(n_dev, order)
        tables = tuple(jnp.asarray(t) for t in tables)
        columns = core(
            partial, lead, stolt_block, kernel_choice, kernel_bank, tables, n_pulse, n_scat
        )
        return pl.pallas_call(
            image_kernel,
            in_specs=[IN_VMEM, IN_VMEM],
            out_specs=pl.BlockSpec(memory_space=pl.ANY),
            out_shape=jax.ShapeDtypeStruct((2, P_SIZE, width), f32),
            scratch_shapes=[
                pltpu.VMEM((width // n, 2, P_SIZE, n), f32),
                pltpu.SemaphoreType.DMA((width // n,)),
            ],
            compiler_params=pltpu.CompilerParams(vmem_limit_bytes=16 << 20),
            name="image",
        )(columns.reshape(-1, n), jnp.asarray(backward))

    ids = jnp.arange(GROUP, dtype=jnp.int32)[None, :, None] * BLOCKS
    first = stolt_block.reshape(groups, GROUP, BLOCKS) + ids
    pick = jnp.stack([first, first + 1], 1).reshape(groups, 2 * n, 1)
    hot = (pick == jnp.arange(n, dtype=jnp.int32)[None, None, :]).astype(bf16)
    kind = jnp.stack([kernel_choice.reshape(groups, n)] * 2, 1).reshape(groups, 2 * n, 1)
    bank_hi = lax.reduce_precision(kernel_bank, 8, 7)
    bank_lo = (kernel_bank - bank_hi).astype(bf16)
    bank_hi = bank_hi.astype(bf16)
    row_ids = (pulse_here * n_scat + scat_here) * rows + jnp.arange(rows, dtype=jnp.int32)
    theta = reference_phase(row_ids, jnp.arange(F_LEN, dtype=jnp.int32))
    theta = theta.reshape(rows * BLOCKS, STOLT)
    cos_p, sin_p = jnp.cos(theta), jnp.sin(theta)

    partial = binning(positions, amplitude, range_cells, bounce, pulse_here * pulses, pulses)
    partial = partial.reshape(n_scat, bins_scat, 2 * pulses)
    binned = lax.dynamic_index_in_dim(partial, scat_here, 0, keepdims=False)
    for shift in range(1, n_scat):
        other = lax.dynamic_index_in_dim(
            partial, (scat_here + shift) % n_scat, 0, keepdims=False
        )
        ring = [(i, (i + shift) % n_scat) for i in range(n_scat)]
        binned = binned + lax.ppermute(other, "scat", ring)
    turned = lax.all_to_all(
        binned.reshape(n_pulse, bins_here, 2 * pulses), "pulse", 0, 0, tiled=True
    )
    turned = turned.reshape(n_pulse, bins_here, 2, pulses).transpose(0, 3, 2, 1)
    turned = turned.reshape(P_SIZE, 2 * bins_here)
    k = np.arange(P_SIZE)
    angle = 2 * np.pi / P_SIZE * ((k[:, None] * k[None, :]) % P_SIZE)
    az = jnp.asarray(np.concatenate([np.cos(angle), np.sin(angle)], 0), f32)
    product = jnp.dot(az, turned, precision=HIGH, preferred_element_type=f32)
    pc, ps = product[:P_SIZE], product[P_SIZE:]
    spectrum = pc + jnp.concatenate([ps[:, bins_here:], -ps[:, :bins_here]], 1)
    az_rows = lax.all_to_all(
        spectrum.reshape(n_dev, rows, 2 * bins_here), ("pulse", "scat"), 0, 0, tiled=True
    )
    x = az_rows.reshape(n_pulse, n_scat, rows, 2, bins_here).transpose(3, 1, 0, 4, 2)
    x = x.reshape(2, BIN_SIDE, BIN_SIDE, rows).transpose(0, 1, 3, 2)
    x = x.reshape(2 * BIN_SIDE, groups, n)
    order = np.arange(2 * BIN_SIDE)

    tables = tuple(jnp.asarray(t) for t in mid_tables(n_dev, order))
    ranged = middle(x, cos_p, sin_p, hot, kind, bank_hi, bank_lo, tables)
    columns = lax.all_to_all(
        ranged.reshape(n_dev, 2 * per, rows * BLOCKS), ("pulse", "scat"), 0, 0, tiled=True
    )
    columns = columns.reshape(n_dev, 2, per, rows, BLOCKS).transpose(0, 3, 1, 2, 4)
    columns = columns.reshape(P_SIZE, 2 * width)
    final = jnp.dot(az, columns, precision=HIGH, preferred_element_type=f32)
    fc, fs = final[:P_SIZE], final[P_SIZE:]
    re = (fc[:, :width] - fs[:, width:]) / P_SIZE
    im = (fc[:, width:] + fs[:, :width]) / P_SIZE
    return jnp.stack([re, im])


def solution(mesh):
    placed = (
        P(("scene", "scat")),
        P(None, ("scene", "scat")),
        P(("scene", "scat")),
        P(("scene", "scat")),
        P(("pulse", "scat"), None),
        P(("pulse", "scat"), None),
        P(),
    )
    return jax.shard_map(
        on_device,
        mesh=mesh,
        in_specs=placed,
        out_specs=P(None, "scene", ("pulse", "scat")),
        check_vma=False,
    )
```
